32 devices in a mesh: dp: 8 (over z, y), tensor: 4 (over x, core).
Axes of the slice: x: 2, y: 2, z: 4, core: 2. Of those that a mesh axis runs over, the one named last changes fastest.
Arguments:
- tokens: bfloat16 [8192, 2048], P(('dp', 'tensor')), may hold values from -6 to 6
- lengths: int32 [8], P('dp'), may hold values from 256 to 1024, as said below
- attn_gain: bfloat16 [2048], replicated, may hold values from 0.25 to 1.75
- w_query: bfloat16 [2048, 2048], P('dp', 'tensor'), may hold values from -0.125 to 0.125
- w_key: bfloat16 [2048, 512], P('dp', 'tensor'), may hold values from -0.125 to 0.125
- w_value: bfloat16 [2048, 512], P('dp', 'tensor'), may hold values from -0.125 to 0.125
- w_output: bfloat16 [2048, 2048], P('tensor', 'dp'), may hold values from -1 to 1
- mlp_gain: bfloat16 [2048], replicated, may hold values from 0.25 to 1.75
- w_gate: bfloat16 [2048, 8192], P('dp', 'tensor'), may hold values from -0.125 to 0.125
- w_up: bfloat16 [2048, 8192], P('dp', 'tensor'), may hold values from -0.125 to 0.125
- w_down: bfloat16 [8192, 2048], P('tensor', 'dp'), may hold values from -0.125 to 0.125
- cotangent: bfloat16 [8192, 2048], P(('dp', 'tensor')), may hold values from -6 to 6
Outputs:
- layer_out: bfloat16 [8192, 2048], P(('dp', 'tensor'))
- grad_tokens: float32 [8192, 2048], P(('dp', 'tensor'))
- grad_query: float32 [2048, 2048], P('dp', 'tensor')
- grad_key: float32 [2048, 512], P('dp', 'tensor')
- grad_value: float32 [2048, 512], P('dp', 'tensor')
- grad_output: float32 [2048, 2048], P('tensor', 'dp')
- grad_gate: float32 [2048, 8192], P('dp', 'tensor')
- grad_up: float32 [2048, 8192], P('dp', 'tensor')
- grad_down: float32 [8192, 2048], P('tensor', 'dp')
- grad_attn_gain: float32 [2048], P(('dp', 'tensor'))
- grad_mlp_gain: float32 [2048], P(('dp', 'tensor'))
The draws below stay inside these ranges and needn't reach their ends.
Inputs may be any that keep to these rules, and one draw needn't show every extreme that they name: `lengths`: each of the 8 sequences has a valid length from 256 to 1024; at least one has length exactly 1024.
All inputs are finite; a program needn't handle non-finite values.
Results may differ from the reference program's by a relative error of at most 0.015.
Values may be sent and summed in bfloat16 or wider, within the bound.
A program may use at most 192 MiB of HBM per device.

```python
import jax
import jax.numpy as jnp
from jax import lax

D = 2048
H = 32
KV = 8
HD = 64
FF = 8192
LEN = 1024
MIN_LEN = 256
SEQS = 8
TOKENS = 8192


def draw_lengths(key, part):
    key_lens = jax.random.fold_in(key, 11)
    key_long = jax.random.fold_in(key, 23)
    drawn_lens = jax.random.randint(key_lens, (SEQS,), MIN_LEN, LEN + 1, dtype=jnp.int32)
    longest = jax.random.randint(key_long, (), 0, SEQS, dtype=jnp.int32)
    return jnp.where(jnp.arange(SEQS, dtype=jnp.int32) == longest, LEN, drawn_lens).astype(jnp.int32)


def spiked(drawn, rng, source, target, blocks, factor):
    def block_of(dim):
        return (jnp.arange(drawn.shape[dim]) // (drawn.shape[dim] // blocks)).reshape((-1,) + (1,) * (drawn.ndim - 1 - dim))

    near = jax.random.permutation(rng, blocks)[block_of(target)]
    other_side = (block_of(target) + blocks // 2) % blocks
    return jnp.where((block_of(source) == near) | (block_of(source) == other_side), factor * drawn, drawn)


def block_levels(own_key, dims, cuts, low, top_value):
    level = 1.0
    for position, parts in cuts:
        steps = jax.random.uniform(jax.random.fold_in(jax.random.fold_in(own_key, 6), position), (parts,), jnp.float32, low / len(cuts), top_value / len(cuts))
        level = level * jnp.repeat(jnp.exp(steps), dims[position] // parts).reshape((-1,) + (1,) * (len(dims) - 1 - position))
    return level


def gaussian(key, extent, width, limit, split=(), held_as=jnp.bfloat16):
    entries = jax.random.normal(key, extent, jnp.float32) * width
    if len(split) > 0:
        entries = block_levels(key, extent, split, -0.22, 0.18) * entries
    return jnp.clip(entries, min=-limit, max=limit).astype(held_as)


def gaussian_with(own_key, extent, width, reach, cuts, heavy, held_as=jnp.bfloat16):
    values = width * jax.random.normal(own_key, extent, jnp.float32)
    if cuts:
        values = values * block_levels(own_key, extent, cuts, -0.22, 0.18)
    return jnp.clip(spiked(values, jax.random.fold_in(own_key, 3), *heavy), -reach, reach).astype(held_as)


def setup_inputs(seed: int = 0) -> dict:
    key_of = jax.random.split(jax.random.key(seed), 13)
    return {
        "tokens": gaussian(key_of[0], (TOKENS, D), 1.0, 6.0, ((0, 32),)),
        "lengths": draw_lengths(jax.random.fold_in(key_of[12], 71), 0),
        "attn_gain": jnp.clip(1.0 + 0.15 * jax.random.normal(key_of[2], (D,), jnp.float32), 0.25, 1.75).astype(jnp.bfloat16),
        "w_query": gaussian(key_of[3], (D, H * HD), D ** -0.5, 0.125, ((0, 8), (1, 4))),
        "w_key": gaussian(key_of[4], (D, KV * HD), D ** -0.5, 0.125, ((0, 8), (1, 4))),
        "w_value": gaussian(key_of[5], (D, KV * HD), D ** -0.5, 0.125, ((0, 8), (1, 4))),
        "w_output": gaussian(key_of[6], (H * HD, D), (H * HD // 64) ** -0.5, 1.0, ((0, 4), (1, 8))),
        "mlp_gain": jnp.clip(1.0 + 0.15 * jax.random.normal(key_of[7], (D,), jnp.float32), 0.25, 1.75).astype(jnp.bfloat16),
        "w_gate": gaussian(key_of[8], (D, FF), D ** -0.5, 0.125, ((0, 8), (1, 4))),
        "w_up": gaussian(key_of[9], (D, FF), D ** -0.5, 0.125, ((0, 8), (1, 4))),
        "w_down": gaussian(key_of[10], (FF, D), (FF // 4) ** -0.5, 0.125, ((0, 4), (1, 8))),
        "cotangent": gaussian_with(key_of[11], (TOKENS, D), 1.0, 6.0, ((0, 32),), (0, 1, 32, 2.75)),
    }


@jax.custom_vjp
def low(v):
    return lax.optimization_barrier(v.astype(jnp.bfloat16)).astype(jnp.float32)

@jax.custom_vjp
def low_back(v):
    return v

def low_keep(v):
    return (low(v), None)

def low_pass(kept, grad):
    return (grad,)

def back_keep(v):
    return (v, None)

def back_low(kept, grad):
    return (low(grad),)
low.defvjp(low_keep, low_pass)
low_back.defvjp(back_keep, back_low)
epsilon = 1e-05
theta = 500000.0

def matmul(left, right):
    return jnp.dot(left, right, precision=lax.Precision.HIGHEST)

def rms_scale(vector, gain):
    return vector * lax.rsqrt(lax.optimization_barrier(jnp.mean(vector * vector, axis=-1, keepdims=True)) + epsilon) * gain

def rotate_half(vector):
    half_size = vector.shape[-1] // 2
    return jnp.concatenate([-vector[..., half_size:], vector[..., :half_size]], axis=-1)

def rope_frequencies():
    half_size = HD // 2
    base_freq = theta ** (-(jnp.arange(half_size, dtype=jnp.float32) * 2.0) / HD)
    wavelength = 2.0 * jnp.pi / base_freq
    smooth = (8192.0 / wavelength - 1.0) / 3.0
    middle = (1.0 - smooth) * base_freq / 32.0 + smooth * base_freq
    return jnp.where(wavelength < 2048.0, base_freq, jnp.where(wavelength > 8192.0, base_freq / 32.0, middle))

def rope_tables():
    frequency = rope_frequencies()
    angles = jnp.arange(LEN, dtype=jnp.float32)[:, None] * frequency[None, :]
    angles = jnp.concatenate([angles, angles], axis=1)
    return (jnp.cos(angles), jnp.sin(angles))

def rope_apply(vector, cosine_table, sine_table):
    return vector * cosine_table[:, None, :] + rotate_half(vector) * sine_table[:, None, :]

def block_forward(sequence_in, length, params):
    w_query, w_key, w_value, w_output, w_gate, w_up, w_down, attn_gain, mlp_gain = params
    cosine_table, sine_table = rope_tables()
    normed_attn = low(rms_scale(sequence_in, attn_gain))
    query_pre = low_back(matmul(normed_attn, w_query))
    key_pre = low_back(matmul(normed_attn, w_key))
    value_pre = low_back(matmul(normed_attn, w_value))
    queries = low(rope_apply(query_pre.reshape(LEN, H, HD), cosine_table, sine_table))
    queries = queries.reshape(LEN, KV, H // KV, HD)
    key_vecs = low(rope_apply(key_pre.reshape(LEN, KV, HD), cosine_table, sine_table))
    values = low(value_pre).reshape(LEN, KV, HD)
    scores = jnp.einsum('qkrd,jkd->krqj', queries, key_vecs, precision=lax.Precision.HIGHEST)
    scores = low_back(scores * HD ** (-0.5))
    positions = jnp.arange(LEN)
    allowed = (positions[None, :] <= positions[:, None]) & (positions[None, :] < length)
    scores = jnp.where(allowed, scores, -1e+30)
    row_max = lax.optimization_barrier(jnp.max(scores, axis=-1, keepdims=True))
    exp_scores = jnp.exp(scores - row_max)
    soft_weights = exp_scores / lax.optimization_barrier(jnp.sum(exp_scores, axis=-1, keepdims=True))
    head_out = jnp.einsum('krqj,jkd->qkrd', low(soft_weights), values, precision=lax.Precision.HIGHEST)
    head_out = low(low_back(head_out.reshape(LEN, H * HD)))
    attn_branch = low_back(matmul(head_out, w_output))
    hidden = sequence_in + attn_branch
    normed_mlp = low(rms_scale(hidden, mlp_gain))
    gate_proj = low_back(matmul(normed_mlp, w_gate))
    up_proj = low_back(matmul(normed_mlp, w_up))
    activated = low(gate_proj * jax.nn.sigmoid(gate_proj) * up_proj)
    mlp_branch = low_back(matmul(activated, w_down))
    return hidden + mlp_branch

def reference(tokens, lengths, attn_gain, w_query, w_key, w_value, w_output, mlp_gain, w_gate, w_up, w_down, cotangent):
    params = tuple((item.astype(jnp.float32) for item in (w_query, w_key, w_value, w_output, w_gate, w_up, w_down, attn_gain, mlp_gain)))
    inputs = tokens.astype(jnp.float32).reshape(SEQS, LEN, D)
    positions = jnp.arange(LEN)
    row_mask = (positions[None, :] < lengths[:, None]).astype(jnp.float32)
    cot_masked = cotangent.astype(jnp.float32).reshape(SEQS, LEN, D) * row_mask[:, :, None]

    def one_sequence(carry, item):
        sequence_in, length, cot_seq = item
        result, pull = jax.vjp(lambda seq_val, par_val: block_forward(seq_val, length, par_val), sequence_in, params)
        grad_in, grad_params = pull(cot_seq)
        carry = jax.tree.map(lambda acc_val, new_val: acc_val + new_val, carry, grad_params)
        return (carry, (result, grad_in))
    zeros_init = jax.tree.map(lambda item: jnp.zeros_like(item), params)
    totals, (results, grad_inputs) = lax.scan(one_sequence, zeros_init, (inputs, lengths, cot_masked))
    layer_out = results.reshape(TOKENS, D).astype(jnp.bfloat16)
    grad_tokens = grad_inputs.reshape(TOKENS, D)
    return (layer_out, grad_tokens, totals[0], totals[1], totals[2], totals[3], totals[4], totals[5], totals[6], totals[7], totals[8])
```

```python
import functools

import jax
import jax.numpy as jnp
from jax import lax
from jax.experimental import pallas as pl
from jax.experimental.pallas import tpu as pltpu
from jax.sharding import PartitionSpec as P

HD = 64
LEN = 1024
QB = 256

epsilon = 1e-05
theta = 500000.0
MESH_ID = pl.DeviceIdType.MESH
BF16 = jnp.bfloat16
F32 = jnp.float32


def rope_frequencies():
    half_size = HD // 2
    base_freq = theta ** (-(jnp.arange(half_size, dtype=jnp.float32) * 2.0) / HD)
    wavelength = 2.0 * jnp.pi / base_freq
    smooth = (8192.0 / wavelength - 1.0) / 3.0
    middle = (1.0 - smooth) * base_freq / 32.0 + smooth * base_freq
    return jnp.where(
        wavelength < 2048.0, base_freq, jnp.where(wavelength > 8192.0, base_freq / 32.0, middle)
    )


def rope_tables():
    angles = jnp.arange(LEN, dtype=jnp.float32)[:, None] * rope_frequencies()[None, :]
    cosine, sine = jnp.cos(angles), jnp.sin(angles)
    return (
        jnp.concatenate([cosine] * 4, axis=1),
        jnp.concatenate([-sine, sine, -sine, sine], axis=1),
    )


def lane_index(shape):
    return lax.broadcasted_iota(jnp.int32, shape, 1)


def swap_halves(value):
    low = lane_index(value.shape) % HD < HD // 2
    return jnp.where(low, pltpu.roll(value, 128 - HD // 2, 1), pltpu.roll(value, HD // 2, 1))


def nt_dot(left, right):
    return lax.dot_general(left, right, (((1,), (1,)), ((), ())), preferred_element_type=F32)


def tn_dot(left, right):
    return lax.dot_general(left, right, (((0,), (0,)), ((), ())), preferred_element_type=F32)


def project_kernel(x_ref, wq_ref, wk_ref, wv_ref, cos_ref, sin_ref, q_ref, k_ref, v_ref):
    rows = x_ref[...]
    cosine, sine = cos_ref[...], sin_ref[...]

    def rope(value):
        return (value * cosine + swap_halves(value) * sine).astype(BF16)

    for block in range(q_ref.shape[1] // 256):
        cols = slice(block * 256, (block + 1) * 256)
        value = jnp.dot(rows, wq_ref[:, cols], preferred_element_type=F32)
        for half in range(2):
            start = block * 256 + half * 128
            q_ref[:, start : start + 128] = rope(value[:, half * 128 : half * 128 + 128])
    k_ref[...] = rope(jnp.dot(rows, wk_ref[...], preferred_element_type=F32))
    v_ref[...] = jnp.dot(rows, wv_ref[...], preferred_element_type=F32).astype(BF16)


def project(rows, w_query, w_key, w_value, cosine, sine):
    total, width = rows.shape
    block = 256

    def whole(array):
        return pl.BlockSpec(array.shape, lambda i: (0, 0))

    def by_rows(cols):
        return pl.BlockSpec((block, cols), lambda i: (i, 0))

    shapes = [w_query.shape[1], w_key.shape[1], w_value.shape[1]]
    return pl.pallas_call(
        project_kernel,
        grid=(total // block,),
        out_shape=[jax.ShapeDtypeStruct((total, s), BF16) for s in shapes],
        in_specs=[by_rows(width), whole(w_query), whole(w_key), whole(w_value)]
        + [by_rows(128)] * 2,
        out_specs=[by_rows(s) for s in shapes],
        compiler_params=pltpu.CompilerParams(vmem_limit_bytes=32 << 20),
        cost_estimate=pl.CostEstimate(
            flops=2 * total * width * sum(shapes), bytes_accessed=8 << 20, transcendentals=0
        ),
        name="project",
    )(rows, w_query, w_key, w_value, cosine, sine)


def pick_head(pair, which, kv):
    moved = jnp.where(kv == which, pair, pltpu.roll(pair, HD, 1))
    return jnp.where(lane_index(pair.shape) // HD == kv, moved, jnp.zeros_like(moved))


def join_heads(first, second, kv):
    first = jnp.where(kv == 0, first, pltpu.roll(first, HD, 1))
    second = jnp.where(kv == 1, second, pltpu.roll(second, HD, 1))
    return jnp.where(lane_index(first.shape) < HD, first, second)


def attend_kernel(length_ref, q_ref, k_ref, v_ref, o_ref):
    kv = pl.program_id(0) // 2
    length = length_ref[0]
    for block in range(LEN // QB):
        rows = slice(block * QB, (block + 1) * QB)
        keys = (block + 1) * QB
        pair = (q_ref[rows, :].astype(F32) * HD**-0.5).astype(F32)
        query_pos = block * QB + lax.broadcasted_iota(jnp.int32, (QB, keys), 0)
        key_pos = lax.broadcasted_iota(jnp.int32, (QB, keys), 1)
        allowed = (key_pos <= query_pos) & (key_pos < length)
        outs = []
        for which in range(2):
            query = pick_head(pair, which, kv).astype(BF16)
            scores = jnp.where(allowed, nt_dot(query, k_ref[:keys, :]), -1e30)
            exps = jnp.exp(scores - jnp.max(scores, axis=1, keepdims=True))
            probs = (exps / jnp.sum(exps, axis=1, keepdims=True)).astype(BF16)
            outs.append(jnp.dot(probs, v_ref[:keys, :], preferred_element_type=F32))
        o_ref[rows, :] = join_heads(outs[0], outs[1], kv).astype(BF16)


def attend(queries, keys, values, lengths):
    pairs = queries.shape[1] // 128
    whole = pl.BlockSpec((LEN, 128), lambda i: (0, 0))
    paired = pl.BlockSpec((LEN, 128), lambda i: (0, i))
    return pl.pallas_call(
        attend_kernel,
        grid=(pairs,),
        out_shape=jax.ShapeDtypeStruct(queries.shape, BF16),
        in_specs=[pl.BlockSpec(memory_space=pltpu.SMEM), paired, whole, whole],
        out_specs=paired,
        compiler_params=pltpu.CompilerParams(vmem_limit_bytes=48 << 20),
        cost_estimate=pl.CostEstimate(
            flops=12 << 30, bytes_accessed=4 << 20, transcendentals=8 << 20
        ),
        name="attend",
    )(lengths, queries, keys, values)


def attend_back_kernel(
    length_ref, q_ref, k_ref, v_ref, g_ref, cos_ref, sin_ref, gq_ref, gk_ref, gv_ref, acc_k, acc_v
):
    pair_index = pl.program_id(0)
    kv = pair_index // 2
    length = length_ref[0]

    @pl.when(pair_index == 0)
    def _():
        acc_k[...] = jnp.zeros_like(acc_k)
        acc_v[...] = jnp.zeros_like(acc_v)

    def rope_back(grads, rows):
        return grads * cos_ref[rows, :] + swap_halves(grads) * (-sin_ref[rows, :])

    for block in range(LEN // QB):
        rows = slice(block * QB, (block + 1) * QB)
        keys = (block + 1) * QB
        pair = q_ref[rows, :].astype(F32) * HD**-0.5
        grad_pair = g_ref[rows, :].astype(F32)
        key_pos = lax.broadcasted_iota(jnp.int32, (keys, QB), 0)
        query_pos = block * QB + lax.broadcasted_iota(jnp.int32, (keys, QB), 1)
        allowed = (key_pos <= query_pos) & (key_pos < length)
        key_vecs = k_ref[:keys, :]
        grad_queries = []
        for which in range(2):
            query = pick_head(pair, which, kv).astype(BF16)
            grad = pick_head(grad_pair, which, kv).astype(BF16)
            scores = jnp.where(allowed, nt_dot(key_vecs, query), -1e30)
            exps = jnp.exp(scores - jnp.max(scores, axis=0, keepdims=True))
            probs = exps / jnp.sum(exps, axis=0, keepdims=True)
            grad_probs = nt_dot(v_ref[:keys, :], grad)
            inner = jnp.sum(probs * grad_probs, axis=0, keepdims=True)
            grad_scores = (probs * (grad_probs - inner)).astype(BF16)
            acc_v[:keys, :] += jnp.dot(probs.astype(BF16), grad, preferred_element_type=F32)
            acc_k[:keys, :] += jnp.dot(grad_scores, query, preferred_element_type=F32)
            grad_queries.append(tn_dot(grad_scores, key_vecs) * HD**-0.5)
        joined = join_heads(grad_queries[0], grad_queries[1], kv)
        gq_ref[rows, :] = rope_back(joined, rows).astype(BF16)

    @pl.when(pair_index == pl.num_programs(0) - 1)
    def _():
        gk_ref[...] = rope_back(acc_k[...], slice(None)).astype(BF16)
        gv_ref[...] = acc_v[...].astype(BF16)


def attend_back(queries, keys, values, grad_heads, lengths, cosine, sine):
    pairs = queries.shape[1] // 128
    whole = pl.BlockSpec((LEN, 128), lambda i: (0, 0))
    paired = pl.BlockSpec((LEN, 128), lambda i: (0, i))
    narrow = jax.ShapeDtypeStruct((LEN, 128), BF16)
    return pl.pallas_call(
        attend_back_kernel,
        grid=(pairs,),
        out_shape=[jax.ShapeDtypeStruct(queries.shape, BF16), narrow, narrow],
        in_specs=[pl.BlockSpec(memory_space=pltpu.SMEM), paired, whole, whole, paired]
        + [whole] * 2,
        out_specs=[paired, whole, whole],
        scratch_shapes=[pltpu.VMEM((LEN, 128), F32)] * 2,
        compiler_params=pltpu.CompilerParams(vmem_limit_bytes=48 << 20),
        cost_estimate=pl.CostEstimate(
            flops=24 << 30, bytes_accessed=8 << 20, transcendentals=8 << 20
        ),
        name="attend_back",
    )(lengths, queries, keys, values, grad_heads, cosine, sine)


def ring_place(index, count):
    odd = index % 2
    return (1 - odd) * (index // 2) + odd * (count - 1 - index // 2)


def ring_member(place, count):
    high = place // (count // 2)
    return (1 - high) * (2 * place) + high * (2 * (count - 1 - place) + 1)


def ring_setup(count):
    place = ring_place(lax.axis_index("dp"), count)
    ahead = ring_member((place + 1) % count, count)
    behind = ring_member((place + count - 1) % count, count)
    barrier = pltpu.get_barrier_semaphore()
    for other in (ahead, behind):
        pl.semaphore_signal(barrier, inc=1, device_id={"dp": other}, device_id_type=MESH_ID)
    pl.semaphore_wait(barrier, 2)
    return place, (ahead, behind)


def member_at(place, side, steps, count):
    if side == 0:
        return ring_member((place + count - steps) % count, count)
    return ring_member((place + steps) % count, count)


def piece(ref, shape, axis, member, side, part, parts):
    rows, cols = shape
    sub = rows // (2 * parts)
    start = (side * parts + part) * sub
    if axis is None:
        return ref.at[pl.ds(start, sub), :]
    if axis == 0:
        return ref.at[pl.ds(pl.multiple_of(member * rows + start, sub), sub), :]
    return ref.at[pl.ds(start, sub), pl.ds(pl.multiple_of(member * cols, cols), cols)]


def gather_kernel(count, items, *refs):
    num = len(items)
    shards, outs = refs[:num], refs[num : 2 * num]
    stage = refs[2 * num : 3 * num]
    send_sems, recv_sems, local_sem = refs[3 * num :]
    place, neighbours = ring_setup(count)
    me = lax.axis_index("dp")
    slots = [(k, part) for k in range(num) for part in range(items[k][2])]

    def copy(step, side, slot):
        item, part = slots[slot]
        shape, axis, parts = items[item]
        origin = member_at(place, side, step, count)
        target = piece(outs[item], shape, axis, origin, side, part, parts)
        return target, pltpu.make_async_remote_copy(
            src_ref=target,
            dst_ref=target,
            send_sem=send_sems.at[side, step, slot],
            recv_sem=recv_sems.at[side, step, slot],
            device_id={"dp": neighbours[side]},
            device_id_type=MESH_ID,
        )

    for slot, (item, part) in enumerate(slots):
        shape, axis, parts = items[item]
        for side in range(2):
            pltpu.make_async_remote_copy(
                src_ref=piece(shards[item], shape, None, 0, side, part, parts),
                dst_ref=piece(outs[item], shape, axis, me, side, part, parts),
                send_sem=send_sems.at[side, 0, slot],
                recv_sem=recv_sems.at[side, 0, slot],
                device_id={"dp": neighbours[side]},
                device_id_type=MESH_ID,
            ).start()
    loads = [
        pltpu.make_async_copy(shards[k], stage[k], local_sem.at[k]) for k in range(num)
    ]
    for load in loads:
        load.start()
    stores = []
    for k in range(num):
        loads[k].wait()
        shape, axis, parts = items[k]
        rows, cols = shape
        if axis == 0:
            own = outs[k].at[pl.ds(pl.multiple_of(me * rows, rows), rows), :]
        else:
            own = outs[k].at[:, pl.ds(pl.multiple_of(me * cols, cols), cols)]
        stores.append(pltpu.make_async_copy(stage[k], own, local_sem.at[k]))
        stores[-1].start()

    def hop(step, carry):
        for slot in range(len(slots)):
            for side in range(2):
                copy(step - 1, side, slot)[1].wait_recv()
                copy(step, side, slot)[1].start()
        return carry

    lax.fori_loop(1, count - 1, hop, 0)
    for slot in range(len(slots)):
        for side in range(2):
            copy(count - 2, side, slot)[1].wait_recv()
    for store in stores:
        store.wait()

    def drain(step, carry):
        for slot in range(len(slots)):
            for side in range(2):
                copy(step, side, slot)[1].wait_send()
        return carry

    lax.fori_loop(0, count - 1, drain, 0)


def ring_gather(shards, axes, parts, count, collective_id):
    turned = [a == 1 and s.shape[1] % 128 != 0 for s, a in zip(shards, axes)]
    if any(turned):
        shards = [s.T if t else s for s, t in zip(shards, turned)]
        axes = [0 if t else a for a, t in zip(axes, turned)]
        outs = ring_gather(shards, axes, parts, count, collective_id)
        return [o.T if t else o for o, t in zip(outs, turned)]
    items = tuple((s.shape, a, q) for s, a, q in zip(shards, axes, parts))
    slots = sum(parts)
    outs = [
        jax.ShapeDtypeStruct(
            (s.shape[0] * count, s.shape[1]) if a == 0 else (s.shape[0], s.shape[1] * count),
            s.dtype,
        )
        for s, a in zip(shards, axes)
    ]
    num = len(shards)
    nbytes = sum(s.size * 2 * (count - 1) for s in shards)
    return pl.pallas_call(
        functools.partial(gather_kernel, count, items),
        out_shape=outs,
        in_specs=[pl.BlockSpec(memory_space=pl.ANY)] * num,
        out_specs=[pl.BlockSpec(memory_space=pl.ANY)] * num,
        scratch_shapes=[pltpu.VMEM(s.shape, s.dtype) for s in shards]
        + [
            pltpu.SemaphoreType.DMA((2, count - 1, slots)),
            pltpu.SemaphoreType.DMA((2, count - 1, slots)),
            pltpu.SemaphoreType.DMA((num,)),
        ],
        compiler_params=pltpu.CompilerParams(collective_id=collective_id, has_side_effects=True),
        cost_estimate=pl.CostEstimate(flops=0, bytes_accessed=20 * nbytes, transcendentals=0),
        name=f"ring_gather_{collective_id}",
    )(*shards)


def scatter_kernel(count, items, *refs):
    num = len(items)
    partials, outs = refs[:num], refs[num : 2 * num]
    own = refs[2 * num : 3 * num]
    held = refs[3 * num : 4 * num]
    total = refs[4 * num : 5 * num]
    send_sems, recv_sems, load_sems, store_sems = refs[5 * num :]
    slots = [(k, part) for k in range(num) for part in range(items[k][2])]

    def load(step, side, slot, place):
        item, part = slots[slot]
        shape, axis, parts = items[item]
        member = member_at(place, side, step + 1, count)
        return pltpu.make_async_copy(
            piece(partials[item], shape, axis, member, side, part, parts),
            own[item].at[side, step, part],
            load_sems.at[side, step, slot],
        )

    start_place = ring_place(lax.axis_index("dp"), count)

    def load_all(step, carry):
        for slot in range(len(slots)):
            for side in range(2):
                load(step, side, slot, start_place).start()
        return carry

    lax.fori_loop(0, count, load_all, 0)
    place, neighbours = ring_setup(count)

    def send(step, side, slot, source):
        item, part = slots[slot]
        return pltpu.make_async_remote_copy(
            src_ref=source,
            dst_ref=held[item].at[side, step, part],
            send_sem=send_sems.at[side, step, slot],
            recv_sem=recv_sems.at[side, step, slot],
            device_id={"dp": neighbours[side]},
            device_id_type=MESH_ID,
        )

    for slot, (item, part) in enumerate(slots):
        for side in range(2):
            load(0, side, slot, place).wait()
            send(0, side, slot, own[item].at[side, 0, part]).start()

    def hop(step, carry):
        for slot, (item, part) in enumerate(slots):
            for side in range(2):
                load(step, side, slot, place).wait()
                arrived = held[item].at[side, step - 1, part]
                send(step - 1, side, slot, arrived).wait_recv()
                arrived[...] = (
                    arrived[...].astype(jnp.float32)
                    + own[item][side, step, part].astype(jnp.float32)
                ).astype(jnp.bfloat16)
                send(step, side, slot, arrived).start()
        return carry

    lax.fori_loop(1, count - 1, hop, 0)
    last = count - 1
    stores = []
    for slot, (item, part) in enumerate(slots):
        shape, axis, parts = items[item]
        for side in range(2):
            load(last, side, slot, place).wait()
            arrived = held[item].at[side, last - 1, part]
            send(last - 1, side, slot, arrived).wait_recv()
            total[item][side, part] = arrived[...].astype(jnp.float32) + own[item][
                side, last, part
            ].astype(jnp.float32)
            stores.append(
                pltpu.make_async_copy(
                    total[item].at[side, part],
                    piece(outs[item], shape, None, 0, side, part, parts),
                    store_sems.at[side, slot],
                )
            )
            stores[-1].start()
    for store in stores:
        store.wait()

    def drain(step, carry):
        for slot, (item, part) in enumerate(slots):
            for side in range(2):
                send(step, side, slot, held[item].at[side, 0, part]).wait_send()
        return carry

    lax.fori_loop(0, count - 1, drain, 0)


def ring_scatter(partials, axes, parts, count, collective_id):
    turned = [a == 1 and p.shape[1] // count % 128 != 0 for p, a in zip(partials, axes)]
    if any(turned):
        partials = [p.T if t else p for p, t in zip(partials, turned)]
        axes = [0 if t else a for a, t in zip(axes, turned)]
        outs = ring_scatter(partials, axes, parts, count, collective_id)
        return [o.T if t else o for o, t in zip(outs, turned)]
    shapes = [
        (p.shape[0] // count, p.shape[1]) if a == 0 else (p.shape[0], p.shape[1] // count)
        for p, a in zip(partials, axes)
    ]
    items = tuple((s, a, q) for s, a, q in zip(shapes, axes, parts))
    slots = sum(parts)
    num = len(partials)

    def buffers(depth, dtype):
        return [
            pltpu.VMEM((2,) + depth + (q, s[0] // (2 * q), s[1]), dtype)
            for s, q in zip(shapes, parts)
        ]

    nbytes = sum(p.size * 2 for p in partials)
    return pl.pallas_call(
        functools.partial(scatter_kernel, count, items),
        out_shape=[jax.ShapeDtypeStruct(s, jnp.float32) for s in shapes],
        in_specs=[pl.BlockSpec(memory_space=pl.ANY)] * num,
        out_specs=[pl.BlockSpec(memory_space=pl.ANY)] * num,
        scratch_shapes=buffers((count,), jnp.bfloat16)
        + buffers((count - 1,), jnp.bfloat16)
        + buffers((), jnp.float32)
        + [
            pltpu.SemaphoreType.DMA((2, count - 1, slots)),
            pltpu.SemaphoreType.DMA((2, count - 1, slots)),
            pltpu.SemaphoreType.DMA((2, count, slots)),
            pltpu.SemaphoreType.DMA((2, slots)),
        ],
        compiler_params=pltpu.CompilerParams(
            collective_id=collective_id, has_side_effects=True, vmem_limit_bytes=48 << 20
        ),
        cost_estimate=pl.CostEstimate(flops=0, bytes_accessed=20 * nbytes, transcendentals=0),
        name=f"ring_scatter_{collective_id}",
    )(*partials)


def after(value, *deps):
    return lax.optimization_barrier((value,) + deps)[0]


def gather_rows(value):
    return lax.all_gather(value, "tensor", axis=0, tiled=True)


def scatter_rows(value):
    return lax.psum_scatter(value.astype(BF16), "tensor", scatter_dimension=0, tiled=True).astype(
        F32
    )


def share_kernel(count, group, parts_ref, out_ref, first, sums, second, sems):
    row, col = lax.axis_index("dp"), lax.axis_index("tensor")
    barrier = pltpu.get_barrier_semaphore()

    def in_group(shift):
        return {"tensor": (col + shift) % group}

    def in_column(shift):
        return {"dp": (row + shift) % count}

    def greet(device):
        pl.semaphore_signal(barrier, inc=1, device_id=device, device_id_type=MESH_ID)

    for shift in range(1, group):
        greet(in_group(shift))
    for shift in range(1, count):
        greet(in_column(shift))
    pl.semaphore_wait(barrier, group + count - 2)

    def exchange(shift, slot, source, target, device):
        return pltpu.make_async_remote_copy(
            src_ref=source,
            dst_ref=target,
            send_sem=sems.at[0, slot],
            recv_sem=sems.at[1, slot],
            device_id=device,
            device_id_type=MESH_ID,
        )

    moves = [
        exchange(s, s - 1, parts_ref.at[(col + s) % group], first.at[s - 1], in_group(s))
        for s in range(1, group)
    ]
    for move in moves:
        move.start()
    total = parts_ref[col]
    for shift, move in enumerate(moves):
        move.wait()
        total = total + first[shift]
    sums[...] = total
    moves = [
        exchange(
            s, group + s - 2, sums.at[(row + s) % count], second.at[s - 1], in_column(s)
        )
        for s in range(1, count)
    ]
    for move in moves:
        move.start()
    total = sums[row]
    for shift, move in enumerate(moves):
        move.wait()
        total = total + second[shift]
    out_ref[...] = total


def sum_shares(first, second, count, group, collective_id):
    share = first.shape[0] // (count * group)
    pair = jnp.stack([first, second]).reshape(2, count, group, share)
    parts = jnp.transpose(pair, (2, 1, 0, 3)).reshape(group, count, 1, 2 * share)
    width = (2 * share + 127) // 128 * 128
    parts = jnp.pad(parts, ((0, 0), (0, 0), (0, 7), (0, width - 2 * share)))
    tile = (8, width)
    out = pl.pallas_call(
        functools.partial(share_kernel, count, group),
        out_shape=jax.ShapeDtypeStruct(tile, F32),
        in_specs=[pl.BlockSpec(memory_space=pltpu.VMEM)],
        out_specs=pl.BlockSpec(memory_space=pltpu.VMEM),
        scratch_shapes=[
            pltpu.VMEM((group - 1, count) + tile, F32),
            pltpu.VMEM((count,) + tile, F32),
            pltpu.VMEM((count - 1,) + tile, F32),
            pltpu.SemaphoreType.DMA((2, group + count - 2)),
        ],
        compiler_params=pltpu.CompilerParams(collective_id=collective_id, has_side_effects=True),
        name="sum_shares",
    )(parts)
    return out[0, :share], out[0, share : 2 * share]


def dot(left, right):
    return jnp.dot(left, right, preferred_element_type=F32)


def body(
    count,
    group,
    tokens,
    lengths,
    attn_gain,
    w_query,
    w_key,
    w_value,
    w_output,
    mlp_gain,
    w_gate,
    w_up,
    w_down,
    cotangent,
):
    local_rows = tokens.shape[0]
    token_full = tokens.astype(F32)
    gain_attn = attn_gain.astype(F32)
    gain_mlp = mlp_gain.astype(F32)
    row_pos = lax.axis_index("tensor") * local_rows + jnp.arange(local_rows)
    valid_rows = (row_pos < lengths[0]).astype(F32)
    cot_masked = cotangent.astype(F32) * valid_rows[:, None]
    cosine, sine = rope_tables()

    inv_first = lax.rsqrt(jnp.mean(token_full * token_full, axis=1, keepdims=True) + epsilon)
    normed_attn = (token_full * inv_first * gain_attn).astype(BF16)
    rows_attn = gather_rows(normed_attn)
    query_all, key_all, value_all, output_all = ring_gather(
        [after(w_query, normed_attn), w_key, w_value, w_output],
        (0, 0, 0, 1), (1, 1, 1, 1), count, 0,
    )
    grad_branch = gather_rows(after(cot_masked.astype(BF16), rows_attn))
    queries, keys, values = project(rows_attn, query_all, key_all, value_all, cosine, sine)
    head_out = attend(queries, keys, values, lengths)
    attn_part = dot(head_out, output_all).astype(BF16)
    attn_branch = scatter_rows(attn_part)
    (gate_all,) = ring_gather([after(w_gate, attn_part)], (0,), (2,), count, 1)
    hidden = token_full + attn_branch
    inv_second = lax.rsqrt(jnp.mean(hidden * hidden, axis=1, keepdims=True) + epsilon)
    normed_mlp = (hidden * inv_second * gain_mlp).astype(BF16)
    normed_mlp = after(normed_mlp, gate_all)
    rows_mlp = gather_rows(normed_mlp)
    (up_all,) = ring_gather([after(w_up, normed_mlp)], (0,), (2,), count, 2)
    gate_proj = dot(rows_mlp, after(gate_all, up_all))
    up_proj = dot(rows_mlp, up_all)
    gate_sig = jax.nn.sigmoid(gate_proj)
    activated = (gate_proj * gate_sig * up_proj).astype(BF16)
    (down_all,) = ring_gather([after(w_down, up_all)], (1,), (2,), count, 3)
    mlp_part = dot(activated, down_all).astype(BF16)
    mlp_branch = scatter_rows(mlp_part)
    layer_out = (hidden + mlp_branch).astype(BF16)

    grad_act = nt_dot(grad_branch, after(down_all, mlp_part))
    grad_gate_pre = (grad_act * up_proj * gate_sig * (1.0 + gate_proj * (1.0 - gate_sig))).astype(
        BF16
    )
    grad_up_pre = (grad_act * gate_proj * gate_sig).astype(BF16)
    norm_part = (nt_dot(grad_gate_pre, gate_all) + nt_dot(grad_up_pre, up_all)).astype(BF16)
    down_part = tn_dot(activated, after(grad_branch, norm_part)).astype(BF16)
    grad_norm_two = scatter_rows(after(norm_part, mlp_branch))
    (grad_down,) = ring_scatter([down_part], (1,), (2,), count, 4)
    scaled_two = grad_norm_two * gain_mlp
    gain_two_part = jnp.sum(grad_norm_two * hidden * inv_second, axis=0)
    grad_hidden = (
        cot_masked
        + inv_second * scaled_two
        - hidden * inv_second**3 * jnp.mean(scaled_two * hidden, axis=1, keepdims=True)
    )
    grad_hidden = after(grad_hidden, grad_down)
    grad_attn = gather_rows(grad_hidden.astype(BF16))
    gate_part = tn_dot(rows_mlp, after(grad_gate_pre, grad_hidden)).astype(BF16)
    up_part = tn_dot(rows_mlp, after(grad_up_pre, gate_part)).astype(BF16)
    grad_heads = nt_dot(after(grad_attn, up_part), output_all).astype(BF16)
    grad_qpre, grad_kpre, grad_vpre = attend_back(
        queries, keys, values, grad_heads, lengths, cosine, sine
    )
    token_part = (
        nt_dot(grad_qpre, query_all) + nt_dot(grad_kpre, key_all) + nt_dot(grad_vpre, value_all)
    ).astype(BF16)
    grad_norm_one = scatter_rows(token_part)
    (grad_gate,) = ring_scatter([after(gate_part, token_part)], (0,), (2,), count, 5)
    output_part = tn_dot(head_out, grad_attn).astype(BF16)
    query_part = tn_dot(rows_attn, grad_qpre).astype(BF16)
    key_part = tn_dot(rows_attn, grad_kpre).astype(BF16)
    value_part = tn_dot(rows_attn, grad_vpre).astype(BF16)
    (grad_up,) = ring_scatter([after(up_part, grad_gate)], (0,), (2,), count, 6)
    scaled_one = grad_norm_one * gain_attn
    gain_one_part = jnp.sum(grad_norm_one * token_full * inv_first, axis=0)
    grad_tokens = (
        grad_hidden
        + inv_first * scaled_one
        - token_full * inv_first**3 * jnp.mean(scaled_one * token_full, axis=1, keepdims=True)
    )
    grad_attn_gain, grad_mlp_gain = sum_shares(gain_one_part, gain_two_part, count, group, 8)
    grad_query, grad_key, grad_value, grad_output = ring_scatter(
        [after(query_part, grad_up, grad_attn_gain), key_part, value_part, output_part],
        (0, 0, 0, 1), (1, 1, 1, 1), count, 7,
    )
    return (
        layer_out,
        grad_tokens,
        grad_query,
        grad_key,
        grad_value,
        grad_output,
        grad_gate,
        grad_up,
        grad_down,
        grad_attn_gain,
        grad_mlp_gain,
    )


def solution(mesh):
    rows = P(("dp", "tensor"), None)
    tall = P("dp", "tensor")
    wide = P("tensor", "dp")
    share = P(("dp", "tensor"))
    in_specs = (rows, P("dp"), P(), tall, tall, tall, wide, P(), tall, tall, wide, rows)
    out_specs = (rows, rows, tall, tall, tall, wide, tall, tall, wide, share, share)
    return jax.shard_map(
        functools.partial(body, mesh.shape["dp"], mesh.shape["tensor"]),
        mesh=mesh,
        in_specs=in_specs,
        out_specs=out_specs,
        check_vma=False,
    )
```

```python
import functools

import jax
import jax.numpy as jnp
from jax import lax
from jax.experimental import pallas as pl
from jax.experimental.pallas import tpu as pltpu
from jax.sharding import PartitionSpec as P

HD = 64
LEN = 1024
QB = 256

epsilon = 1e-05
theta = 500000.0
MESH_ID = pl.DeviceIdType.MESH
BF16 = jnp.bfloat16
F32 = jnp.float32


def rope_frequencies():
    half_size = HD // 2
    base_freq = theta ** (-(jnp.arange(half_size, dtype=jnp.float32) * 2.0) / HD)
    wavelength = 2.0 * jnp.pi / base_freq
    smooth = (8192.0 / wavelength - 1.0) / 3.0
    middle = (1.0 - smooth) * base_freq / 32.0 + smooth * base_freq
    return jnp.where(
        wavelength < 2048.0, base_freq, jnp.where(wavelength > 8192.0, base_freq / 32.0, middle)
    )


def rope_tables():
    angles = jnp.arange(LEN, dtype=jnp.float32)[:, None] * rope_frequencies()[None, :]
    cosine, sine = jnp.cos(angles), jnp.sin(angles)
    return (
        jnp.concatenate([cosine] * 4, axis=1),
        jnp.concatenate([-sine, sine, -sine, sine], axis=1),
    )


def lane_index(shape):
    return lax.broadcasted_iota(jnp.int32, shape, 1)


def swap_halves(value):
    low = lane_index(value.shape) % HD < HD // 2
    return jnp.where(low, pltpu.roll(value, 128 - HD // 2, 1), pltpu.roll(value, HD // 2, 1))


def nt_dot(left, right):
    return lax.dot_general(left, right, (((1,), (1,)), ((), ())), preferred_element_type=F32)


def tn_dot(left, right):
    return lax.dot_general(left, right, (((0,), (0,)), ((), ())), preferred_element_type=F32)


def project_kernel(x_ref, wq_ref, wk_ref, wv_ref, cos_ref, sin_ref, q_ref, k_ref, v_ref):
    rows = x_ref[...]
    cosine, sine = cos_ref[...], sin_ref[...]

    def rope(value):
        return (value * cosine + swap_halves(value) * sine).astype(BF16)

    for block in range(q_ref.shape[1] // 256):
        cols = slice(block * 256, (block + 1) * 256)
        value = jnp.dot(rows, wq_ref[:, cols], preferred_element_type=F32)
        for half in range(2):
            start = block * 256 + half * 128
            q_ref[:, start : start + 128] = rope(value[:, half * 128 : half * 128 + 128])
    k_ref[...] = rope(jnp.dot(rows, wk_ref[...], preferred_element_type=F32))
    v_ref[...] = jnp.dot(rows, wv_ref[...], preferred_element_type=F32).astype(BF16)


def project(rows, w_query, w_key, w_value, cosine, sine):
    total, width = rows.shape
    block = 256

    def whole(array):
        return pl.BlockSpec(array.shape, lambda i: (0, 0))

    def by_rows(cols):
        return pl.BlockSpec((block, cols), lambda i: (i, 0))

    shapes = [w_query.shape[1], w_key.shape[1], w_value.shape[1]]
    return pl.pallas_call(
        project_kernel,
        grid=(total // block,),
        out_shape=[jax.ShapeDtypeStruct((total, s), BF16) for s in shapes],
        in_specs=[by_rows(width), whole(w_query), whole(w_key), whole(w_value)]
        + [by_rows(128)] * 2,
        out_specs=[by_rows(s) for s in shapes],
        compiler_params=pltpu.CompilerParams(vmem_limit_bytes=32 << 20),
        cost_estimate=pl.CostEstimate(
            flops=2 * total * width * sum(shapes), bytes_accessed=8 << 20, transcendentals=0
        ),
        name="project",
    )(rows, w_query, w_key, w_value, cosine, sine)


def pick_head(pair, which, kv):
    moved = jnp.where(kv == which, pair, pltpu.roll(pair, HD, 1))
    return jnp.where(lane_index(pair.shape) // HD == kv, moved, jnp.zeros_like(moved))


def join_heads(first, second, kv):
    first = jnp.where(kv == 0, first, pltpu.roll(first, HD, 1))
    second = jnp.where(kv == 1, second, pltpu.roll(second, HD, 1))
    return jnp.where(lane_index(first.shape) < HD, first, second)


def attend_kernel(length_ref, q_ref, k_ref, v_ref, o_ref):
    kv = pl.program_id(0) // 2
    length = length_ref[0]
    for block in range(LEN // QB):
        rows = slice(block * QB, (block + 1) * QB)
        keys = (block + 1) * QB
        pair = (q_ref[rows, :].astype(F32) * HD**-0.5).astype(F32)
        query_pos = block * QB + lax.broadcasted_iota(jnp.int32, (QB, keys), 0)
        key_pos = lax.broadcasted_iota(jnp.int32, (QB, keys), 1)
        allowed = (key_pos <= query_pos) & (key_pos < length)
        outs = []
        for which in range(2):
            query = pick_head(pair, which, kv).astype(BF16)
            scores = jnp.where(allowed, nt_dot(query, k_ref[:keys, :]), -1e30)
            exps = jnp.exp(scores - jnp.max(scores, axis=1, keepdims=True))
            probs = (exps / jnp.sum(exps, axis=1, keepdims=True)).astype(BF16)
            outs.append(jnp.dot(probs, v_ref[:keys, :], preferred_element_type=F32))
        o_ref[rows, :] = join_heads(outs[0], outs[1], kv).astype(BF16)


def attend(queries, keys, values, lengths):
    pairs = queries.shape[1] // 128
    whole = pl.BlockSpec((LEN, 128), lambda i: (0, 0))
    paired = pl.BlockSpec((LEN, 128), lambda i: (0, i))
    return pl.pallas_call(
        attend_kernel,
        grid=(pairs,),
        out_shape=jax.ShapeDtypeStruct(queries.shape, BF16),
        in_specs=[pl.BlockSpec(memory_space=pltpu.SMEM), paired, whole, whole],
        out_specs=paired,
        compiler_params=pltpu.CompilerParams(vmem_limit_bytes=48 << 20),
        cost_estimate=pl.CostEstimate(
            flops=12 << 30, bytes_accessed=4 << 20, transcendentals=8 << 20
        ),
        name="attend",
    )(lengths, queries, keys, values)


def attend_back_kernel(
    length_ref, q_ref, k_ref, v_ref, g_ref, cos_ref, sin_ref, gq_ref, gk_ref, gv_ref, acc_k, acc_v
):
    pair_index = pl.program_id(0)
    kv = pair_index // 2
    length = length_ref[0]

    @pl.when(pair_index == 0)
    def _():
        acc_k[...] = jnp.zeros_like(acc_k)
        acc_v[...] = jnp.zeros_like(acc_v)

    def rope_back(grads, rows):
        return grads * cos_ref[rows, :] + swap_halves(grads) * (-sin_ref[rows, :])

    for block in range(LEN // QB):
        rows = slice(block * QB, (block + 1) * QB)
        keys = (block + 1) * QB
        pair = q_ref[rows, :].astype(F32) * HD**-0.5
        grad_pair = g_ref[rows, :].astype(F32)
        key_pos = lax.broadcasted_iota(jnp.int32, (keys, QB), 0)
        query_pos = block * QB + lax.broadcasted_iota(jnp.int32, (keys, QB), 1)
        allowed = (key_pos <= query_pos) & (key_pos < length)
        key_vecs = k_ref[:keys, :]
        grad_queries = []
        for which in range(2):
            query = pick_head(pair, which, kv).astype(BF16)
            grad = pick_head(grad_pair, which, kv).astype(BF16)
            scores = jnp.where(allowed, nt_dot(key_vecs, query), -1e30)
            exps = jnp.exp(scores - jnp.max(scores, axis=0, keepdims=True))
            probs = exps / jnp.sum(exps, axis=0, keepdims=True)
            grad_probs = nt_dot(v_ref[:keys, :], grad)
            inner = jnp.sum(probs * grad_probs, axis=0, keepdims=True)
            grad_scores = (probs * (grad_probs - inner)).astype(BF16)
            acc_v[:keys, :] += jnp.dot(probs.astype(BF16), grad, preferred_element_type=F32)
            acc_k[:keys, :] += jnp.dot(grad_scores, query, preferred_element_type=F32)
            grad_queries.append(tn_dot(grad_scores, key_vecs) * HD**-0.5)
        joined = join_heads(grad_queries[0], grad_queries[1], kv)
        gq_ref[rows, :] = rope_back(joined, rows).astype(BF16)

    @pl.when(pair_index == pl.num_programs(0) - 1)
    def _():
        gk_ref[...] = rope_back(acc_k[...], slice(None)).astype(BF16)
        gv_ref[...] = acc_v[...].astype(BF16)


def attend_back(queries, keys, values, grad_heads, lengths, cosine, sine):
    pairs = queries.shape[1] // 128
    whole = pl.BlockSpec((LEN, 128), lambda i: (0, 0))
    paired = pl.BlockSpec((LEN, 128), lambda i: (0, i))
    narrow = jax.ShapeDtypeStruct((LEN, 128), BF16)
    return pl.pallas_call(
        attend_back_kernel,
        grid=(pairs,),
        out_shape=[jax.ShapeDtypeStruct(queries.shape, BF16), narrow, narrow],
        in_specs=[pl.BlockSpec(memory_space=pltpu.SMEM), paired, whole, whole, paired]
        + [whole] * 2,
        out_specs=[paired, whole, whole],
        scratch_shapes=[pltpu.VMEM((LEN, 128), F32)] * 2,
        compiler_params=pltpu.CompilerParams(vmem_limit_bytes=48 << 20),
        cost_estimate=pl.CostEstimate(
            flops=24 << 30, bytes_accessed=8 << 20, transcendentals=8 << 20
        ),
        name="attend_back",
    )(lengths, queries, keys, values, grad_heads, cosine, sine)


def ring_place(index, count):
    odd = index % 2
    return (1 - odd) * (index // 2) + odd * (count - 1 - index // 2)


def ring_member(place, count):
    high = place // (count // 2)
    return (1 - high) * (2 * place) + high * (2 * (count - 1 - place) + 1)


def ring_setup(count):
    place = ring_place(lax.axis_index("dp"), count)
    ahead = ring_member((place + 1) % count, count)
    behind = ring_member((place + count - 1) % count, count)
    barrier = pltpu.get_barrier_semaphore()
    for other in (ahead, behind):
        pl.semaphore_signal(barrier, inc=1, device_id={"dp": other}, device_id_type=MESH_ID)
    pl.semaphore_wait(barrier, 2)
    return place, (ahead, behind)


def member_at(place, side, steps, count):
    if side == 0:
        return ring_member((place + count - steps) % count, count)
    return ring_member((place + steps) % count, count)


def piece(ref, shape, axis, member, side, part, parts):
    rows, cols = shape
    sub = rows // (2 * parts)
    start = (side * parts + part) * sub
    if axis is None:
        return ref.at[pl.ds(start, sub), :]
    if axis == 0:
        return ref.at[pl.ds(pl.multiple_of(member * rows + start, sub), sub), :]
    return ref.at[pl.ds(start, sub), pl.ds(pl.multiple_of(member * cols, cols), cols)]


def gather_kernel(count, items, *refs):
    num = len(items)
    shards, outs = refs[:num], refs[num : 2 * num]
    stage = refs[2 * num : 3 * num]
    send_sems, recv_sems, local_sem = refs[3 * num :]
    place, neighbours = ring_setup(count)
    me = lax.axis_index("dp")
    slots = [(k, part) for k in range(num) for part in range(items[k][2])]

    def copy(step, side, slot):
        item, part = slots[slot]
        shape, axis, parts = items[item]
        origin = member_at(place, side, step, count)
        target = piece(outs[item], shape, axis, origin, side, part, parts)
        return target, pltpu.make_async_remote_copy(
            src_ref=target,
            dst_ref=target,
            send_sem=send_sems.at[side, step, slot],
            recv_sem=recv_sems.at[side, step, slot],
            device_id={"dp": neighbours[side]},
            device_id_type=MESH_ID,
        )

    for slot, (item, part) in enumerate(slots):
        shape, axis, parts = items[item]
        for side in range(2):
            pltpu.make_async_remote_copy(
                src_ref=piece(shards[item], shape, None, 0, side, part, parts),
                dst_ref=piece(outs[item], shape, axis, me, side, part, parts),
                send_sem=send_sems.at[side, 0, slot],
                recv_sem=recv_sems.at[side, 0, slot],
                device_id={"dp": neighbours[side]},
                device_id_type=MESH_ID,
            ).start()
    loads = [
        pltpu.make_async_copy(shards[k], stage[k], local_sem.at[k]) for k in range(num)
    ]
    for load in loads:
        load.start()
    stores = []
    for k in range(num):
        loads[k].wait()
        shape, axis, parts = items[k]
        rows, cols = shape
        if axis == 0:
            own = outs[k].at[pl.ds(pl.multiple_of(me * rows, rows), rows), :]
        else:
            own = outs[k].at[:, pl.ds(pl.multiple_of(me * cols, cols), cols)]
        stores.append(pltpu.make_async_copy(stage[k], own, local_sem.at[k]))
        stores[-1].start()

    def hop(step, carry):
        for slot in range(len(slots)):
            for side in range(2):
                copy(step - 1, side, slot)[1].wait_recv()
                copy(step, side, slot)[1].start()
        return carry

    lax.fori_loop(1, count - 1, hop, 0)
    for slot in range(len(slots)):
        for side in range(2):
            copy(count - 2, side, slot)[1].wait_recv()
    for store in stores:
        store.wait()

    def drain(step, carry):
        for slot in range(len(slots)):
            for side in range(2):
                copy(step, side, slot)[1].wait_send()
        return carry

    lax.fori_loop(0, count - 1, drain, 0)


def ring_gather(shards, axes, parts, count, collective_id):
    turned = [a == 1 and s.shape[1] % 128 != 0 for s, a in zip(shards, axes)]
    if any(turned):
        shards = [s.T if t else s for s, t in zip(shards, turned)]
        axes = [0 if t else a for a, t in zip(axes, turned)]
        outs = ring_gather(shards, axes, parts, count, collective_id)
        return [o.T if t else o for o, t in zip(outs, turned)]
    items = tuple((s.shape, a, q) for s, a, q in zip(shards, axes, parts))
    slots = sum(parts)
    outs = [
        jax.ShapeDtypeStruct(
            (s.shape[0] * count, s.shape[1]) if a == 0 else (s.shape[0], s.shape[1] * count),
            s.dtype,
        )
        for s, a in zip(shards, axes)
    ]
    num = len(shards)
    nbytes = sum(s.size * 2 * (count - 1) for s in shards)
    return pl.pallas_call(
        functools.partial(gather_kernel, count, items),
        out_shape=outs,
        in_specs=[pl.BlockSpec(memory_space=pl.ANY)] * num,
        out_specs=[pl.BlockSpec(memory_space=pl.ANY)] * num,
        scratch_shapes=[pltpu.VMEM(s.shape, s.dtype) for s in shards]
        + [
            pltpu.SemaphoreType.DMA((2, count - 1, slots)),
            pltpu.SemaphoreType.DMA((2, count - 1, slots)),
            pltpu.SemaphoreType.DMA((num,)),
        ],
        compiler_params=pltpu.CompilerParams(collective_id=collective_id, has_side_effects=True),
        cost_estimate=pl.CostEstimate(flops=0, bytes_accessed=20 * nbytes, transcendentals=0),
        name=f"ring_gather_{collective_id}",
    )(*shards)


def scatter_kernel(count, items, *refs):
    num = len(items)
    partials, outs = refs[:num], refs[num : 2 * num]
    own = refs[2 * num : 3 * num]
    held = refs[3 * num : 4 * num]
    total = refs[4 * num : 5 * num]
    send_sems, recv_sems, load_sems, store_sems = refs[5 * num :]
    slots = [(k, part) for k in range(num) for part in range(items[k][2])]

    def load(step, side, slot, place):
        item, part = slots[slot]
        shape, axis, parts = items[item]
        member = member_at(place, side, step + 1, count)
        return pltpu.make_async_copy(
            piece(partials[item], shape, axis, member, side, part, parts),
            own[item].at[side, step, part],
            load_sems.at[side, step, slot],
        )

    start_place = ring_place(lax.axis_index("dp"), count)

    def load_all(step, carry):
        for slot in range(len(slots)):
            for side in range(2):
                load(step, side, slot, start_place).start()
        return carry

    lax.fori_loop(0, count, load_all, 0)
    place, neighbours = ring_setup(count)

    def send(step, side, slot, source):
        item, part = slots[slot]
        return pltpu.make_async_remote_copy(
            src_ref=source,
            dst_ref=held[item].at[side, step, part],
            send_sem=send_sems.at[side, step, slot],
            recv_sem=recv_sems.at[side, step, slot],
            device_id={"dp": neighbours[side]},
            device_id_type=MESH_ID,
        )

    for slot, (item, part) in enumerate(slots):
        for side in range(2):
            load(0, side, slot, place).wait()
            send(0, side, slot, own[item].at[side, 0, part]).start()

    def hop(step, carry):
        for slot, (item, part) in enumerate(slots):
            for side in range(2):
                load(step, side, slot, place).wait()
                arrived = held[item].at[side, step - 1, part]
                send(step - 1, side, slot, arrived).wait_recv()
                arrived[...] = (
                    arrived[...].astype(jnp.float32)
                    + own[item][side, step, part].astype(jnp.float32)
                ).astype(jnp.bfloat16)
                send(step, side, slot, arrived).start()
        return carry

    lax.fori_loop(1, count - 1, hop, 0)
    last = count - 1
    stores = []
    for slot, (item, part) in enumerate(slots):
        shape, axis, parts = items[item]
        for side in range(2):
            load(last, side, slot, place).wait()
            arrived = held[item].at[side, last - 1, part]
            send(last - 1, side, slot, arrived).wait_recv()
            total[item][side, part] = arrived[...].astype(jnp.float32) + own[item][
                side, last, part
            ].astype(jnp.float32)
            stores.append(
                pltpu.make_async_copy(
                    total[item].at[side, part],
                    piece(outs[item], shape, None, 0, side, part, parts),
                    store_sems.at[side, slot],
                )
            )
            stores[-1].start()
    for store in stores:
        store.wait()

    def drain(step, carry):
        for slot, (item, part) in enumerate(slots):
            for side in range(2):
                send(step, side, slot, held[item].at[side, 0, part]).wait_send()
        return carry

    lax.fori_loop(0, count - 1, drain, 0)


def ring_scatter(partials, axes, parts, count, collective_id):
    turned = [a == 1 and p.shape[1] // count % 128 != 0 for p, a in zip(partials, axes)]
    if any(turned):
        partials = [p.T if t else p for p, t in zip(partials, turned)]
        axes = [0 if t else a for a, t in zip(axes, turned)]
        outs = ring_scatter(partials, axes, parts, count, collective_id)
        return [o.T if t else o for o, t in zip(outs, turned)]
    shapes = [
        (p.shape[0] // count, p.shape[1]) if a == 0 else (p.shape[0], p.shape[1] // count)
        for p, a in zip(partials, axes)
    ]
    items = tuple((s, a, q) for s, a, q in zip(shapes, axes, parts))
    slots = sum(parts)
    num = len(partials)

    def buffers(depth, dtype):
        return [
            pltpu.VMEM((2,) + depth + (q, s[0] // (2 * q), s[1]), dtype)
            for s, q in zip(shapes, parts)
        ]

    nbytes = sum(p.size * 2 for p in partials)
    return pl.pallas_call(
        functools.partial(scatter_kernel, count, items),
        out_shape=[jax.ShapeDtypeStruct(s, jnp.float32) for s in shapes],
        in_specs=[pl.BlockSpec(memory_space=pl.ANY)] * num,
        out_specs=[pl.BlockSpec(memory_space=pl.ANY)] * num,
        scratch_shapes=buffers((count,), jnp.bfloat16)
        + buffers((count - 1,), jnp.bfloat16)
        + buffers((), jnp.float32)
        + [
            pltpu.SemaphoreType.DMA((2, count - 1, slots)),
            pltpu.SemaphoreType.DMA((2, count - 1, slots)),
            pltpu.SemaphoreType.DMA((2, count, slots)),
            pltpu.SemaphoreType.DMA((2, slots)),
        ],
        compiler_params=pltpu.CompilerParams(
            collective_id=collective_id, has_side_effects=True, vmem_limit_bytes=48 << 20
        ),
        cost_estimate=pl.CostEstimate(flops=0, bytes_accessed=20 * nbytes, transcendentals=0),
        name=f"ring_scatter_{collective_id}",
    )(*partials)


def scatter_dot_kernel(count, items, parts, extra, *refs):
    num = len(items)
    base = 6 * num + 5
    beside = None
    if extra is not None:
        builder, takes, gives = extra
        given, refs = refs[2 * num : 2 * num + takes], refs[: 2 * num] + refs[2 * num + takes :]
        made, refs = refs[3 * num : 3 * num + gives], refs[: 3 * num] + refs[3 * num + gives :]
        spare, refs = refs[3 * num + base :], refs[: 3 * num + base]
    lefts, rights, outs = refs[:num], refs[num : 2 * num], refs[2 * num : 3 * num]
    refs = refs[3 * num :]
    left_bufs, right_bufs = refs[:num], refs[num : 2 * num]
    firsts, owns, helds, totals = (refs[(2 + i) * num : (3 + i) * num] for i in range(4))
    send_sems, recv_sems, left_sems, right_sems, store_sems = refs[6 * num :]
    entry_place = ring_place(lax.axis_index("dp"), count)

    def load_right(item):
        return pltpu.make_async_copy(rights[item], right_bufs[item], right_sems.at[item])

    def load_left(step, side, item, place):
        block, _ = items[item]
        member = member_at(place, side, step + 1, count)
        slot = step % 2
        return pltpu.make_async_copy(
            lefts[item].at[:, pl.ds(pl.multiple_of(member * block, block), block)],
            left_bufs[item].at[side, slot],
            left_sems.at[side, slot, item],
        )

    for item in range(num):
        load_right(item).start()
        for side in range(2):
            load_left(0, side, item, entry_place).start()
    if extra is not None:
        beside = builder(count, given, made, spare, right_bufs)
        beside.begin()
    place, neighbours = ring_setup(count)
    pairs = [(item, side) for item in range(num) for side in range(2)]

    def own_sum(step, side, item):
        _, half = items[item]
        return tn_dot(
            left_bufs[item][side, step % 2], right_bufs[item][:, side * half : (side + 1) * half]
        )

    def send(step, side, item, part, source):
        return pltpu.make_async_remote_copy(
            src_ref=source.at[part],
            dst_ref=helds[item].at[side, step, part],
            send_sem=send_sems.at[side, step, item * parts + part],
            recv_sem=recv_sems.at[side, step, item * parts + part],
            device_id={"dp": neighbours[side]},
            device_id_type=MESH_ID,
        )

    def prefetch(step):
        for item, side in pairs:
            load_left(step, side, item, place).start()

    prefetch(1)
    for item in range(num):
        load_right(item).wait()
    for item, side in pairs:
        load_left(0, side, item, place).wait()
        firsts[item][side] = own_sum(0, side, item).astype(BF16).reshape(firsts[item].shape[1:])
        for part in range(parts):
            send(0, side, item, part, firsts[item].at[side]).start()
    if beside:
        beside.compute(0)

    def hop(step, carry):
        prefetch(step + 1)
        for item, side in pairs:
            load_left(step, side, item, place).wait()
            owns[item][side] = own_sum(step, side, item).reshape(owns[item].shape[1:])
        if beside:
            beside.compute(step)
        for part in range(parts):
            for item, side in pairs:
                arrived = helds[item].at[side, step - 1]
                send(step - 1, side, item, part, arrived).wait_recv()
                arrived[part] = (
                    arrived[part].astype(F32) + owns[item][side, part]
                ).astype(BF16)
                send(step, side, item, part, arrived).start()
        return carry

    lax.fori_loop(1, count - 1, hop, 0)
    last = count - 1
    for item, side in pairs:
        load_left(last, side, item, place).wait()
        owns[item][side] = own_sum(last, side, item).reshape(owns[item].shape[1:])
    if beside:
        beside.compute(last)
    stores = []
    for part in range(parts):
        for item, side in pairs:
            block, half = items[item]
            arrived = helds[item].at[side, last - 1]
            send(last - 1, side, item, part, arrived).wait_recv()
            totals[item][side, part] = arrived[part].astype(F32) + owns[item][side, part]
            stores.append(
                pltpu.make_async_copy(
                    totals[item].at[side, part],
                    outs[item].at[
                        pl.ds(part * (block // parts), block // parts),
                        pl.ds(side * half, half),
                    ],
                    store_sems.at[side, item * parts + part],
                )
            )
            stores[-1].start()
    for store in stores:
        store.wait()
    if beside:
        beside.finish()

    def drain(step, carry):
        for part in range(parts):
            for item, side in pairs:
                send(step, side, item, part, helds[item].at[side, 0]).wait_send()
        return carry

    lax.fori_loop(0, count - 1, drain, 0)


def ring_scatter_dots(jobs, parts, count, collective_id, extra=None):
    builder, given, made, spare = extra or (None, [], [], [])
    lefts, rights = [j[0] for j in jobs], [j[1] for j in jobs]
    rows = lefts[0].shape[0]
    items = tuple((l.shape[1] // count, r.shape[1] // 2) for l, r in jobs)
    num = len(jobs)

    def buffers(depth, dtype):
        return [pltpu.VMEM(depth + (parts, b // parts, h), dtype) for b, h in items]

    slots = num * parts
    flops = sum(2 * rows * l.shape[1] * r.shape[1] for l, r in jobs)
    nbytes = sum(2 * l.shape[1] * r.shape[1] for l, r in jobs)
    return pl.pallas_call(
        functools.partial(
            scatter_dot_kernel,
            count,
            items,
            parts,
            (builder, len(given), len(made)) if extra else None,
        ),
        out_shape=[jax.ShapeDtypeStruct((b, 2 * h), F32) for b, h in items] + made,
        in_specs=[pl.BlockSpec(memory_space=pl.ANY)] * (2 * num + len(given)),
        out_specs=[pl.BlockSpec(memory_space=pl.ANY)] * (num + len(made)),
        scratch_shapes=[pltpu.VMEM((2, 2, rows, b), BF16) for b, _ in items]
        + [pltpu.VMEM(r.shape, BF16) for r in rights]
        + buffers((2,), BF16)
        + buffers((2,), F32)
        + buffers((2, count - 1), BF16)
        + buffers((2,), F32)
        + [
            pltpu.SemaphoreType.DMA((2, count - 1, slots)),
            pltpu.SemaphoreType.DMA((2, count - 1, slots)),
            pltpu.SemaphoreType.DMA((2, 2, num)),
            pltpu.SemaphoreType.DMA((num,)),
            pltpu.SemaphoreType.DMA((2, slots)),
        ]
        + spare,
        compiler_params=pltpu.CompilerParams(
            collective_id=collective_id, has_side_effects=True, vmem_limit_bytes=60 << 20
        ),
        cost_estimate=pl.CostEstimate(
            flops=flops, bytes_accessed=20 * nbytes, transcendentals=0
        ),
        name=f"ring_scatter_{collective_id}",
    )(*lefts, *rights, *given)


class NormWork:
    def __init__(self, count, given, made, spare, rights):
        self.grads, self.weights, self.down = given[:2], given[2:4], given[4]
        self.outs = made
        self.grad_bufs, self.row_bufs, self.down_bufs, self.stage = spare[0], *spare[1:4]
        self.grad_sems, self.row_sems, self.down_sems, self.out_sems = spare[4:]
        self.act = rights[0]
        self.count = count
        self.block = self.row_bufs.shape[2]

    def load_grad(self, which):
        return pltpu.make_async_copy(
            self.grads[which], self.grad_bufs.at[which], self.grad_sems.at[which]
        )

    def spot(self, step):
        return pl.ds(pl.multiple_of(step * self.block, self.block), self.block)

    def loads(self, step):
        slot = step % 2
        rows = [
            pltpu.make_async_copy(
                self.weights[which].at[self.spot(step), :],
                self.row_bufs.at[which, slot],
                self.row_sems.at[which, slot],
            )
            for which in range(2)
        ]
        down = pltpu.make_async_copy(
            self.down.at[:, self.spot(step)], self.down_bufs.at[slot], self.down_sems.at[slot]
        )
        return rows + [down]

    def store(self, which, step):
        slot = step % 2
        return pltpu.make_async_copy(
            self.stage.at[which, slot],
            self.outs[which].at[:, self.spot(step)],
            self.out_sems.at[which, slot],
        )

    def begin(self):
        for which in range(2):
            self.load_grad(which).start()
        for copy in self.loads(0):
            copy.start()

    def compute(self, step):
        last = self.count - 1
        if isinstance(step, int):
            if step < last:
                for copy in self.loads(step + 1):
                    copy.start()
            if step == 0:
                for which in range(2):
                    self.load_grad(which).wait()
            if step >= 2:
                for which in range(2):
                    self.store(which, step - 2).wait()
        else:
            for copy in self.loads(step + 1):
                copy.start()

            @pl.when(step >= 2)
            def _():
                for which in range(2):
                    self.store(which, step - 2).wait()

        for copy in self.loads(step):
            copy.wait()
        slot = step % 2
        for top in range(0, self.act.shape[0], 256):
            band = pl.ds(top, 256)
            norm = nt_dot(self.grad_bufs[0, band, :], self.row_bufs[0, slot])
            norm += nt_dot(self.grad_bufs[1, band, :], self.row_bufs[1, slot])
            self.stage[0, slot, band, :] = norm.astype(BF16)
            value = jnp.dot(
                self.act[band, :], self.down_bufs[slot], preferred_element_type=F32
            )
            self.stage[1, slot, band, :] = value.astype(BF16)
        for which in range(2):
            self.store(which, step).start()

    def finish(self):
        for step in range(max(self.count - 2, 0), self.count):
            for which in range(2):
                self.store(which, step).wait()


def down_ring(grad_branch, activated, grad_gate, grad_up, gate_all, up_all, down_all, count, cid):
    rows, hidden = activated.shape
    width = gate_all.shape[0]
    block = width // count
    wide = jax.ShapeDtypeStruct((rows, width), BF16)
    spare = [
        pltpu.VMEM((2, rows, hidden), BF16),
        pltpu.VMEM((2, 2, block, hidden), BF16),
        pltpu.VMEM((2, hidden, block), BF16),
        pltpu.VMEM((2, 2, rows, block), BF16),
        pltpu.SemaphoreType.DMA((2,)),
        pltpu.SemaphoreType.DMA((2, 2)),
        pltpu.SemaphoreType.DMA((2,)),
        pltpu.SemaphoreType.DMA((2, 2)),
    ]
    given = [grad_gate, grad_up, gate_all, up_all, down_all]
    return ring_scatter_dots(
        [(grad_branch, activated)], 2, count, cid, (NormWork, given, [wide, wide], spare)
    )


def mlp_kernel(count, *refs):
    x_hbm, wg_hbm, wu_hbm, shard, gb_hbm = refs[:5]
    act_hbm, gg_hbm, gu_hbm, down_all = refs[5:9]
    x_buf, gb_buf, w_bufs, gate_slope, up_slope, acc, half_bufs, stage, own_stage = refs[9:18]
    send_sems, recv_sems, w_sems, in_sems, half_sems, out_sems, local_sem = refs[18:]
    rows, width = x_buf.shape
    hidden = acc.shape[1]
    block = width // count
    cols = w_bufs.shape[-1]
    steps = hidden // cols
    half = hidden // 2
    parts = send_sems.shape[2]
    me = lax.axis_index("dp")

    def load_weights(step, which):
        source = (wg_hbm, wu_hbm)[which]
        return pltpu.make_async_copy(
            source.at[:, pl.ds(pl.multiple_of(step * cols, cols), cols)],
            w_bufs.at[which, step % 2],
            w_sems.at[which, step % 2],
        )

    load_x = pltpu.make_async_copy(x_hbm, x_buf, in_sems.at[0])
    load_gb = pltpu.make_async_copy(gb_hbm, gb_buf, in_sems.at[1])
    load_own = pltpu.make_async_copy(shard, own_stage, local_sem)
    load_x.start()
    for which in range(2):
        load_weights(0, which).start()
    load_own.start()
    load_gb.start()
    place, neighbours = ring_setup(count)

    def target(ref, member, side, part):
        return piece(ref, (hidden, block), 1, member, side, part, parts)

    def hop(step, side, part):
        ref = target(down_all, member_at(place, side, step, count), side, part)
        return pltpu.make_async_remote_copy(
            src_ref=ref,
            dst_ref=ref,
            send_sem=send_sems.at[side, step, part],
            recv_sem=recv_sems.at[side, step, part],
            device_id={"dp": neighbours[side]},
            device_id_type=MESH_ID,
        )

    for part in range(parts):
        for side in range(2):
            pltpu.make_async_remote_copy(
                src_ref=piece(shard, (hidden, block), None, 0, side, part, parts),
                dst_ref=target(down_all, me, side, part),
                send_sem=send_sems.at[side, 0, part],
                recv_sem=recv_sems.at[side, 0, part],
                device_id={"dp": neighbours[side]},
                device_id_type=MESH_ID,
            ).start()

    def pump(step):
        for part in range(parts):
            for side in range(2):
                hop(step - 1, side, part).wait_recv()
                hop(step, side, part).start()

    load_own.wait()
    store_own = pltpu.make_async_copy(
        own_stage, down_all.at[:, pl.ds(pl.multiple_of(me * block, block), block)], local_sem
    )
    store_own.start()
    load_x.wait()

    def store(ref, which, step):
        return pltpu.make_async_copy(
            stage.at[which, step % 2],
            ref.at[:, pl.ds(pl.multiple_of(step * cols, cols), cols)],
            out_sems.at[which, step % 2],
        )

    def forward(step, carry):
        @pl.when(step + 1 < steps)
        def _():
            for which in range(2):
                load_weights(step + 1, which).start()

        @pl.when(step >= 2)
        def _():
            store(act_hbm, 0, step - 2).wait()

        for which in range(2):
            load_weights(step, which).wait()
        here = pl.ds(pl.multiple_of(step * cols, cols), cols)
        for top in range(0, rows, 256):
            band = pl.ds(top, 256)
            lines = x_buf[band, :]
            gate = jnp.dot(lines, w_bufs[0, step % 2], preferred_element_type=F32)
            up = jnp.dot(lines, w_bufs[1, step % 2], preferred_element_type=F32)
            sig = jax.nn.sigmoid(gate)
            silu = gate * sig
            stage[0, step % 2, band, :] = (silu * up).astype(BF16)
            gate_slope[band, here] = up * sig * (1.0 + gate * (1.0 - sig))
            up_slope[band, here] = silu
        store(act_hbm, 0, step).start()

        turn = step // 2

        @pl.when((step % 2 == 0) & (turn >= 1) & (turn <= count - 2))
        def _():
            pump(turn)

        return carry

    lax.fori_loop(0, steps, forward, 0)
    for step in range(max(steps - 2, 0), steps):
        store(act_hbm, 0, step).wait()
    pumped = min((steps - 1) // 2, count - 2)
    load_gb.wait()

    def load_half(step, side):
        member = member_at(place, side, step, count)
        return pltpu.make_async_copy(
            down_all.at[
                pl.ds(side * half, half), pl.ds(pl.multiple_of(member * block, block), block)
            ],
            half_bufs.at[side],
            half_sems.at[side],
        )

    def backward(step, carry):
        @pl.when((step > pumped) & (step <= count - 2))
        def _():
            pump(step)

        @pl.when(step == count - 1)
        def _():
            for part in range(parts):
                for side in range(2):
                    hop(count - 2, side, part).wait_recv()

        for side in range(2):
            load_half(step, side).start()
        for side in range(2):
            member = member_at(place, side, step, count)
            load_half(step, side).wait()
            for top in range(0, rows, 256):
                band = pl.ds(top, 256)
                lines = gb_buf[band, pl.ds(pl.multiple_of(member * block, block), block)]
                value = nt_dot(lines, half_bufs[side])
                spot = (band, pl.ds(side * half, half))

                @pl.when(step == 0)
                def _():
                    acc[spot] = value

                @pl.when(step > 0)
                def _():
                    acc[spot] += value

        return carry

    store_own.wait()
    lax.fori_loop(0, count, backward, 0)

    def slopes(step, carry):
        @pl.when(step >= 2)
        def _():
            store(gg_hbm, 1, step - 2).wait()
            store(gu_hbm, 2, step - 2).wait()

        here = pl.ds(pl.multiple_of(step * cols, cols), cols)
        for top in range(0, rows, 256):
            band = pl.ds(top, 256)
            value = acc[band, here]
            stage[1, step % 2, band, :] = (value * gate_slope[band, here]).astype(BF16)
            stage[2, step % 2, band, :] = (value * up_slope[band, here]).astype(BF16)
        store(gg_hbm, 1, step).start()
        store(gu_hbm, 2, step).start()
        return carry

    lax.fori_loop(0, steps, slopes, 0)
    for step in range(max(steps - 2, 0), steps):
        store(gg_hbm, 1, step).wait()
        store(gu_hbm, 2, step).wait()

    def drain(step, carry):
        for part in range(parts):
            for side in range(2):
                hop(step, side, part).wait_send()
        return carry

    lax.fori_loop(0, count - 1, drain, 0)


def mlp_ring(rows_mlp, gate_all, up_all, w_down, grad_branch, count, collective_id):
    rows, width = rows_mlp.shape
    hidden, block = w_down.shape
    cols, parts = 256, 2
    wide = jax.ShapeDtypeStruct((rows, hidden), BF16)
    return pl.pallas_call(
        functools.partial(mlp_kernel, count),
        out_shape=[wide] * 3 + [jax.ShapeDtypeStruct((hidden, width), BF16)],
        in_specs=[pl.BlockSpec(memory_space=pl.ANY)] * 5,
        out_specs=[pl.BlockSpec(memory_space=pl.ANY)] * 4,
        scratch_shapes=[
            pltpu.VMEM((rows, width), BF16),
            pltpu.VMEM((rows, width), BF16),
            pltpu.VMEM((2, 2, width, cols), BF16),
            pltpu.VMEM((rows, hidden), F32),
            pltpu.VMEM((rows, hidden), F32),
            pltpu.VMEM((rows, hidden), F32),
            pltpu.VMEM((2, hidden // 2, block), BF16),
            pltpu.VMEM((3, 2, rows, cols), BF16),
            pltpu.VMEM((hidden, block), BF16),
            pltpu.SemaphoreType.DMA((2, count - 1, parts)),
            pltpu.SemaphoreType.DMA((2, count - 1, parts)),
            pltpu.SemaphoreType.DMA((2, 2)),
            pltpu.SemaphoreType.DMA((2,)),
            pltpu.SemaphoreType.DMA((2,)),
            pltpu.SemaphoreType.DMA((3, 2)),
            pltpu.SemaphoreType.DMA,
        ],
        compiler_params=pltpu.CompilerParams(
            collective_id=collective_id, has_side_effects=True, vmem_limit_bytes=60 << 20
        ),
        cost_estimate=pl.CostEstimate(
            flops=6 * rows * width * hidden,
            bytes_accessed=40 * hidden * width,
            transcendentals=rows * hidden,
        ),
        name="mlp_ring",
    )(rows_mlp, gate_all, up_all, w_down, grad_branch)


def ring_weight_grads(jobs, parts, count, collective_id):
    if all(left.shape[1] // count % 128 == 0 for left, _ in jobs):
        return ring_scatter_dots(jobs, parts, count, collective_id)
    partials = [tn_dot(left, right).astype(BF16) for left, right in jobs]
    num = len(jobs)
    return ring_scatter(partials, [0] * num, [parts] * num, count, collective_id)


def after(value, *deps):
    return lax.optimization_barrier((value,) + deps)[0]


def gather_rows(value):
    return lax.all_gather(value, "tensor", axis=0, tiled=True)


def scatter_rows(value):
    return lax.psum_scatter(value.astype(BF16), "tensor", scatter_dimension=0, tiled=True).astype(
        F32
    )


def share_kernel(count, group, parts_ref, out_ref, first, sums, second, sems):
    row, col = lax.axis_index("dp"), lax.axis_index("tensor")
    barrier = pltpu.get_barrier_semaphore()

    def in_group(shift):
        return {"tensor": (col + shift) % group}

    def in_column(shift):
        return {"dp": (row + shift) % count}

    def greet(device):
        pl.semaphore_signal(barrier, inc=1, device_id=device, device_id_type=MESH_ID)

    for shift in range(1, group):
        greet(in_group(shift))
    for shift in range(1, count):
        greet(in_column(shift))
    pl.semaphore_wait(barrier, group + count - 2)

    def exchange(shift, slot, source, target, device):
        return pltpu.make_async_remote_copy(
            src_ref=source,
            dst_ref=target,
            send_sem=sems.at[0, slot],
            recv_sem=sems.at[1, slot],
            device_id=device,
            device_id_type=MESH_ID,
        )

    moves = [
        exchange(s, s - 1, parts_ref.at[(col + s) % group], first.at[s - 1], in_group(s))
        for s in range(1, group)
    ]
    for move in moves:
        move.start()
    total = parts_ref[col]
    for shift, move in enumerate(moves):
        move.wait()
        total = total + first[shift]
    sums[...] = total
    moves = [
        exchange(
            s, group + s - 2, sums.at[(row + s) % count], second.at[s - 1], in_column(s)
        )
        for s in range(1, count)
    ]
    for move in moves:
        move.start()
    total = sums[row]
    for shift, move in enumerate(moves):
        move.wait()
        total = total + second[shift]
    out_ref[...] = total


def sum_shares(first, second, count, group, collective_id):
    share = first.shape[0] // (count * group)
    pair = jnp.stack([first, second]).reshape(2, count, group, share)
    parts = jnp.transpose(pair, (2, 1, 0, 3)).reshape(group, count, 1, 2 * share)
    width = (2 * share + 127) // 128 * 128
    parts = jnp.pad(parts, ((0, 0), (0, 0), (0, 7), (0, width - 2 * share)))
    tile = (8, width)
    out = pl.pallas_call(
        functools.partial(share_kernel, count, group),
        out_shape=jax.ShapeDtypeStruct(tile, F32),
        in_specs=[pl.BlockSpec(memory_space=pltpu.VMEM)],
        out_specs=pl.BlockSpec(memory_space=pltpu.VMEM),
        scratch_shapes=[
            pltpu.VMEM((group - 1, count) + tile, F32),
            pltpu.VMEM((count,) + tile, F32),
            pltpu.VMEM((count - 1,) + tile, F32),
            pltpu.SemaphoreType.DMA((2, group + count - 2)),
        ],
        compiler_params=pltpu.CompilerParams(collective_id=collective_id, has_side_effects=True),
        name="sum_shares",
    )(parts)
    return out[0, :share], out[0, share : 2 * share]


def dot(left, right):
    return jnp.dot(left, right, preferred_element_type=F32)


def body(
    count,
    group,
    tokens,
    lengths,
    attn_gain,
    w_query,
    w_key,
    w_value,
    w_output,
    mlp_gain,
    w_gate,
    w_up,
    w_down,
    cotangent,
):
    local_rows = tokens.shape[0]
    token_full = tokens.astype(F32)
    gain_attn = attn_gain.astype(F32)
    gain_mlp = mlp_gain.astype(F32)
    row_pos = lax.axis_index("tensor") * local_rows + jnp.arange(local_rows)
    valid_rows = (row_pos < lengths[0]).astype(F32)
    cot_masked = cotangent.astype(F32) * valid_rows[:, None]
    cosine, sine = rope_tables()

    inv_first = lax.rsqrt(jnp.mean(token_full * token_full, axis=1, keepdims=True) + epsilon)
    normed_attn = (token_full * inv_first * gain_attn).astype(BF16)
    rows_attn = gather_rows(normed_attn)
    query_all, key_all, value_all, output_all = ring_gather(
        [after(w_query, normed_attn), w_key, w_value, w_output],
        (0, 0, 0, 1), (1, 1, 1, 1), count, 0,
    )
    grad_branch = gather_rows(after(cot_masked.astype(BF16), rows_attn))
    queries, keys, values = project(rows_attn, query_all, key_all, value_all, cosine, sine)
    head_out = attend(queries, keys, values, lengths)
    attn_part = dot(head_out, output_all).astype(BF16)
    attn_branch = scatter_rows(attn_part)
    (gate_all,) = ring_gather([after(w_gate, attn_part)], (0,), (2,), count, 1)
    hidden = token_full + attn_branch
    inv_second = lax.rsqrt(jnp.mean(hidden * hidden, axis=1, keepdims=True) + epsilon)
    normed_mlp = (hidden * inv_second * gain_mlp).astype(BF16)
    normed_mlp = after(normed_mlp, gate_all)
    rows_mlp = gather_rows(normed_mlp)
    (up_all,) = ring_gather([after(w_up, normed_mlp)], (0,), (2,), count, 2)
    if w_down.shape[1] % 128 == 0:
        activated, grad_gate_pre, grad_up_pre, down_all = mlp_ring(
            rows_mlp, gate_all, after(up_all, rows_mlp), w_down, grad_branch, count, 3
        )
        grad_down, norm_part, mlp_part = down_ring(
            grad_branch, activated, grad_gate_pre, grad_up_pre, gate_all, up_all, down_all,
            count, 4,
        )
    else:
        gate_proj = dot(rows_mlp, gate_all)
        up_proj = dot(rows_mlp, up_all)
        gate_sig = jax.nn.sigmoid(gate_proj)
        activated = (gate_proj * gate_sig * up_proj).astype(BF16)
        (down_all,) = ring_gather([after(w_down, up_all)], (1,), (2,), count, 3)
        mlp_part = dot(activated, down_all).astype(BF16)
        grad_act = nt_dot(grad_branch, down_all)
        grad_gate_pre = (
            grad_act * up_proj * gate_sig * (1.0 + gate_proj * (1.0 - gate_sig))
        ).astype(BF16)
        grad_up_pre = (grad_act * gate_proj * gate_sig).astype(BF16)
        norm_part = (nt_dot(grad_gate_pre, gate_all) + nt_dot(grad_up_pre, up_all)).astype(BF16)
        (grad_down,) = ring_weight_grads([(grad_branch, activated)], 2, count, 4)
    grad_norm_two = scatter_rows(norm_part)
    (grad_gate,) = ring_weight_grads(
        [(after(rows_mlp, norm_part), grad_gate_pre)], 2, count, 5
    )
    mlp_branch = scatter_rows(after(mlp_part, grad_norm_two, grad_gate))
    layer_out = (hidden + mlp_branch).astype(BF16)
    scaled_two = grad_norm_two * gain_mlp
    gain_two_part = jnp.sum(grad_norm_two * hidden * inv_second, axis=0)
    grad_hidden = (
        cot_masked
        + inv_second * scaled_two
        - hidden * inv_second**3 * jnp.mean(scaled_two * hidden, axis=1, keepdims=True)
    )
    grad_hidden = after(grad_hidden, grad_gate)
    grad_attn = gather_rows(grad_hidden.astype(BF16))
    (grad_up,) = ring_weight_grads(
        [(after(rows_mlp, grad_hidden), grad_up_pre)], 2, count, 6
    )
    grad_heads = nt_dot(after(grad_attn, grad_up), output_all).astype(BF16)
    grad_qpre, grad_kpre, grad_vpre = attend_back(
        queries, keys, values, grad_heads, lengths, cosine, sine
    )
    token_part = (
        nt_dot(grad_qpre, query_all) + nt_dot(grad_kpre, key_all) + nt_dot(grad_vpre, value_all)
    ).astype(BF16)
    grad_norm_one = scatter_rows(token_part)
    grad_qkv = jnp.concatenate([grad_qpre, grad_kpre, grad_vpre], axis=1)
    scaled_one = grad_norm_one * gain_attn
    gain_one_part = jnp.sum(grad_norm_one * token_full * inv_first, axis=0)
    grad_tokens = (
        grad_hidden
        + inv_first * scaled_one
        - token_full * inv_first**3 * jnp.mean(scaled_one * token_full, axis=1, keepdims=True)
    )
    attn_grads, grad_output = ring_weight_grads(
        [(after(rows_attn, token_part), grad_qkv), (grad_attn, head_out)], 1, count, 7
    )
    grad_attn_gain, grad_mlp_gain = sum_shares(
        after(gain_one_part, attn_grads), gain_two_part, count, group, 8
    )
    query_cols, key_cols = grad_qpre.shape[1], grad_kpre.shape[1]
    grad_query = attn_grads[:, :query_cols]
    grad_key = attn_grads[:, query_cols : query_cols + key_cols]
    grad_value = attn_grads[:, query_cols + key_cols :]
    grad_output, grad_down = grad_output.T, grad_down.T
    return (
        layer_out,
        grad_tokens,
        grad_query,
        grad_key,
        grad_value,
        grad_output,
        grad_gate,
        grad_up,
        grad_down,
        grad_attn_gain,
        grad_mlp_gain,
    )


def solution(mesh):
    rows = P(("dp", "tensor"), None)
    tall = P("dp", "tensor")
    wide = P("tensor", "dp")
    share = P(("dp", "tensor"))
    in_specs = (rows, P("dp"), P(), tall, tall, tall, wide, P(), tall, tall, wide, rows)
    out_specs = (rows, rows, tall, tall, tall, wide, tall, tall, wide, share, share)
    return jax.shard_map(
        functools.partial(body, mesh.shape["dp"], mesh.shape["tensor"]),
        mesh=mesh,
        in_specs=in_specs,
        out_specs=out_specs,
        check_vma=False,
    )
```

```python
import functools

import jax
import jax.numpy as jnp
from jax import lax
from jax.experimental import pallas as pl
from jax.experimental.pallas import tpu as pltpu
from jax.sharding import PartitionSpec as P

HD = 64
LEN = 1024
QB = 256

epsilon = 1e-05
theta = 500000.0
MESH_ID = pl.DeviceIdType.MESH
BF16 = jnp.bfloat16
ANY = pl.BlockSpec(memory_space=pl.ANY)
F32 = jnp.float32


def rope_frequencies():
    half_size = HD // 2
    base_freq = theta ** (-(jnp.arange(half_size, dtype=jnp.float32) * 2.0) / HD)
    wavelength = 2.0 * jnp.pi / base_freq
    smooth = (8192.0 / wavelength - 1.0) / 3.0
    middle = (1.0 - smooth) * base_freq / 32.0 + smooth * base_freq
    return jnp.where(
        wavelength < 2048.0, base_freq, jnp.where(wavelength > 8192.0, base_freq / 32.0, middle)
    )


def rope_tables():
    angles = jnp.arange(LEN, dtype=jnp.float32)[:, None] * rope_frequencies()[None, :]
    cosine, sine = jnp.cos(angles), jnp.sin(angles)
    return (
        jnp.concatenate([cosine] * 4, axis=1),
        jnp.concatenate([-sine, sine, -sine, sine], axis=1),
    )


def lane_index(shape):
    return lax.broadcasted_iota(jnp.int32, shape, 1)


def swap_halves(value):
    low = lane_index(value.shape) % HD < HD // 2
    return jnp.where(low, pltpu.roll(value, 128 - HD // 2, 1), pltpu.roll(value, HD // 2, 1))


def nt_dot(left, right):
    return lax.dot_general(left, right, (((1,), (1,)), ((), ())), preferred_element_type=F32)


def tn_dot(left, right):
    return lax.dot_general(left, right, (((0,), (0,)), ((), ())), preferred_element_type=F32)


def rope(value, cosine, sine):
    return (value * cosine + swap_halves(value) * sine).astype(BF16)


def rope_back(grads, cosine, sine):
    return (grads * cosine - swap_halves(grads) * sine).astype(BF16)


def project_rows(rows, wq_ref, wk_ref, wv_ref, cosine, sine, q_ref, k_ref, v_ref):
    for block in range(q_ref.shape[1] // 256):
        cols = slice(block * 256, (block + 1) * 256)
        value = jnp.dot(rows, wq_ref[:, cols], preferred_element_type=F32)
        for half in range(2):
            start = block * 256 + half * 128
            q_ref[:, start : start + 128] = rope(
                value[:, half * 128 : half * 128 + 128], cosine, sine
            )
    k_ref[...] = rope(jnp.dot(rows, wk_ref[...], preferred_element_type=F32), cosine, sine)
    v_ref[...] = jnp.dot(rows, wv_ref[...], preferred_element_type=F32).astype(BF16)


def project_kernel(x_ref, wq_ref, wk_ref, wv_ref, cos_ref, sin_ref, q_ref, k_ref, v_ref):
    project_rows(
        x_ref[...], wq_ref, wk_ref, wv_ref, cos_ref[...], sin_ref[...], q_ref, k_ref, v_ref
    )


def project(rows, w_query, w_key, w_value, cosine, sine):
    total, width = rows.shape
    block = 256

    def whole(array):
        return pl.BlockSpec(array.shape, lambda i: (0, 0))

    def by_rows(cols):
        return pl.BlockSpec((block, cols), lambda i: (i, 0))

    shapes = [w_query.shape[1], w_key.shape[1], w_value.shape[1]]
    return pl.pallas_call(
        project_kernel,
        grid=(total // block,),
        out_shape=[jax.ShapeDtypeStruct((total, s), BF16) for s in shapes],
        in_specs=[by_rows(width), whole(w_query), whole(w_key), whole(w_value)]
        + [by_rows(128)] * 2,
        out_specs=[by_rows(s) for s in shapes],
        compiler_params=pltpu.CompilerParams(vmem_limit_bytes=32 << 20),
        cost_estimate=pl.CostEstimate(
            flops=2 * total * width * sum(shapes), bytes_accessed=8 << 20, transcendentals=0
        ),
        name="project",
    )(rows, w_query, w_key, w_value, cosine, sine)


def pick_head(pair, which, kv):
    moved = jnp.where(kv == which, pair, pltpu.roll(pair, HD, 1))
    return jnp.where(lane_index(pair.shape) // HD == kv, moved, jnp.zeros_like(moved))


def join_heads(first, second, kv):
    first = jnp.where(kv == 0, first, pltpu.roll(first, HD, 1))
    second = jnp.where(kv == 1, second, pltpu.roll(second, HD, 1))
    return jnp.where(lane_index(first.shape) < HD, first, second)


def attend_pair(length, kv, q_ref, k_ref, v_ref, o_ref):
    for block in range(LEN // QB):
        rows = slice(block * QB, (block + 1) * QB)
        keys = (block + 1) * QB
        pair = q_ref[rows, :].astype(F32) * HD**-0.5
        query_pos = block * QB + lax.broadcasted_iota(jnp.int32, (QB, keys), 0)
        key_pos = lax.broadcasted_iota(jnp.int32, (QB, keys), 1)
        allowed = (key_pos <= query_pos) & (key_pos < length)
        outs = []
        for which in range(2):
            query = pick_head(pair, which, kv).astype(BF16)
            scores = jnp.where(allowed, nt_dot(query, k_ref[:keys, :]), -1e30)
            exps = jnp.exp(scores - jnp.max(scores, axis=1, keepdims=True))
            probs = (exps / jnp.sum(exps, axis=1, keepdims=True)).astype(BF16)
            outs.append(jnp.dot(probs, v_ref[:keys, :], preferred_element_type=F32))
        o_ref[rows, :] = join_heads(outs[0], outs[1], kv).astype(BF16)


def attend_kernel(length_ref, q_ref, k_ref, v_ref, o_ref):
    attend_pair(length_ref[0], pl.program_id(0) // 2, q_ref, k_ref, v_ref, o_ref)


def attend(queries, keys, values, lengths):
    pairs = queries.shape[1] // 128
    whole = pl.BlockSpec((LEN, 128), lambda i: (0, 0))
    paired = pl.BlockSpec((LEN, 128), lambda i: (0, i))
    return pl.pallas_call(
        attend_kernel,
        grid=(pairs,),
        out_shape=jax.ShapeDtypeStruct(queries.shape, BF16),
        in_specs=[pl.BlockSpec(memory_space=pltpu.SMEM), paired, whole, whole],
        out_specs=paired,
        compiler_params=pltpu.CompilerParams(vmem_limit_bytes=48 << 20),
        cost_estimate=pl.CostEstimate(
            flops=12 << 30, bytes_accessed=4 << 20, transcendentals=8 << 20
        ),
        name="attend",
    )(lengths, queries, keys, values)


def attend_back_pair(
    length, kv, q_ref, k_ref, v_ref, g_ref, cos_ref, sin_ref, gq_ref, acc_k, acc_v
):
    for block in range(LEN // QB):
        rows = slice(block * QB, (block + 1) * QB)
        keys = (block + 1) * QB
        pair = q_ref[rows, :].astype(F32) * HD**-0.5
        grad_pair = g_ref[rows, :].astype(F32)
        key_pos = lax.broadcasted_iota(jnp.int32, (keys, QB), 0)
        query_pos = block * QB + lax.broadcasted_iota(jnp.int32, (keys, QB), 1)
        allowed = (key_pos <= query_pos) & (key_pos < length)
        key_vecs = k_ref[:keys, :]
        grad_queries = []
        for which in range(2):
            query = pick_head(pair, which, kv).astype(BF16)
            grad = pick_head(grad_pair, which, kv).astype(BF16)
            scores = jnp.where(allowed, nt_dot(key_vecs, query), -1e30)
            exps = jnp.exp(scores - jnp.max(scores, axis=0, keepdims=True))
            probs = exps / jnp.sum(exps, axis=0, keepdims=True)
            grad_probs = nt_dot(v_ref[:keys, :], grad)
            inner = jnp.sum(probs * grad_probs, axis=0, keepdims=True)
            grad_scores = (probs * (grad_probs - inner)).astype(BF16)
            acc_v[:keys, :] += jnp.dot(probs.astype(BF16), grad, preferred_element_type=F32)
            acc_k[:keys, :] += jnp.dot(grad_scores, query, preferred_element_type=F32)
            grad_queries.append(tn_dot(grad_scores, key_vecs) * HD**-0.5)
        joined = join_heads(grad_queries[0], grad_queries[1], kv)
        gq_ref[rows, :] = rope_back(joined, cos_ref[rows, :], sin_ref[rows, :])


def attend_back_kernel(
    length_ref, q_ref, k_ref, v_ref, g_ref, cos_ref, sin_ref, gq_ref, gk_ref, gv_ref, acc_k, acc_v
):
    pair_index = pl.program_id(0)

    @pl.when(pair_index == 0)
    def _():
        acc_k[...] = jnp.zeros_like(acc_k)
        acc_v[...] = jnp.zeros_like(acc_v)

    attend_back_pair(
        length_ref[0], pair_index // 2, q_ref, k_ref, v_ref, g_ref, cos_ref, sin_ref, gq_ref,
        acc_k, acc_v,
    )

    @pl.when(pair_index == pl.num_programs(0) - 1)
    def _():
        gk_ref[...] = rope_back(acc_k[...], cos_ref[...], sin_ref[...])
        gv_ref[...] = acc_v[...].astype(BF16)


def attend_back(queries, keys, values, grad_heads, lengths, cosine, sine):
    pairs = queries.shape[1] // 128
    whole = pl.BlockSpec((LEN, 128), lambda i: (0, 0))
    paired = pl.BlockSpec((LEN, 128), lambda i: (0, i))
    narrow = jax.ShapeDtypeStruct((LEN, 128), BF16)
    return pl.pallas_call(
        attend_back_kernel,
        grid=(pairs,),
        out_shape=[jax.ShapeDtypeStruct(queries.shape, BF16), narrow, narrow],
        in_specs=[pl.BlockSpec(memory_space=pltpu.SMEM), paired, whole, whole, paired]
        + [whole] * 2,
        out_specs=[paired, whole, whole],
        scratch_shapes=[pltpu.VMEM((LEN, 128), F32)] * 2,
        compiler_params=pltpu.CompilerParams(vmem_limit_bytes=48 << 20),
        cost_estimate=pl.CostEstimate(
            flops=24 << 30, bytes_accessed=8 << 20, transcendentals=8 << 20
        ),
        name="attend_back",
    )(lengths, queries, keys, values, grad_heads, cosine, sine)


def ring_place(index, count):
    odd = index % 2
    return (1 - odd) * (index // 2) + odd * (count - 1 - index // 2)


def ring_member(place, count):
    high = place // (count // 2)
    return (1 - high) * (2 * place) + high * (2 * (count - 1 - place) + 1)


def ring_setup(count):
    place = ring_place(lax.axis_index("dp"), count)
    ahead = ring_member((place + 1) % count, count)
    behind = ring_member((place + count - 1) % count, count)
    barrier = pltpu.get_barrier_semaphore()
    for other in (ahead, behind):
        pl.semaphore_signal(barrier, inc=1, device_id={"dp": other}, device_id_type=MESH_ID)
    pl.semaphore_wait(barrier, 2)
    return place, (ahead, behind)


def member_at(place, side, steps, count):
    if side == 0:
        return ring_member((place + count - steps) % count, count)
    return ring_member((place + steps) % count, count)


def piece(ref, shape, axis, member, side, part, parts):
    rows, cols = shape
    sub = rows // (2 * parts)
    start = (side * parts + part) * sub
    if axis is None:
        return ref.at[pl.ds(start, sub), :]
    if axis == 0:
        return ref.at[pl.ds(pl.multiple_of(member * rows + start, sub), sub), :]
    return ref.at[pl.ds(start, sub), pl.ds(pl.multiple_of(member * cols, cols), cols)]


def gather_kernel(count, items, *refs):
    num = len(items)
    shards, outs = refs[:num], refs[num : 2 * num]
    stage = refs[2 * num : 3 * num]
    send_sems, recv_sems, local_sem = refs[3 * num :]
    place, neighbours = ring_setup(count)
    me = lax.axis_index("dp")
    slots = [(k, part) for k in range(num) for part in range(items[k][2])]

    def copy(step, side, slot):
        item, part = slots[slot]
        shape, axis, parts = items[item]
        origin = member_at(place, side, step, count)
        target = piece(outs[item], shape, axis, origin, side, part, parts)
        return target, pltpu.make_async_remote_copy(
            src_ref=target,
            dst_ref=target,
            send_sem=send_sems.at[side, step, slot],
            recv_sem=recv_sems.at[side, step, slot],
            device_id={"dp": neighbours[side]},
            device_id_type=MESH_ID,
        )

    for slot, (item, part) in enumerate(slots):
        shape, axis, parts = items[item]
        for side in range(2):
            pltpu.make_async_remote_copy(
                src_ref=piece(shards[item], shape, None, 0, side, part, parts),
                dst_ref=piece(outs[item], shape, axis, me, side, part, parts),
                send_sem=send_sems.at[side, 0, slot],
                recv_sem=recv_sems.at[side, 0, slot],
                device_id={"dp": neighbours[side]},
                device_id_type=MESH_ID,
            ).start()
    loads = [
        pltpu.make_async_copy(shards[k], stage[k], local_sem.at[k]) for k in range(num)
    ]
    for load in loads:
        load.start()
    stores = []
    for k in range(num):
        loads[k].wait()
        shape, axis, parts = items[k]
        rows, cols = shape
        if axis == 0:
            own = outs[k].at[pl.ds(pl.multiple_of(me * rows, rows), rows), :]
        else:
            own = outs[k].at[:, pl.ds(pl.multiple_of(me * cols, cols), cols)]
        stores.append(pltpu.make_async_copy(stage[k], own, local_sem.at[k]))
        stores[-1].start()

    def hop(step, carry):
        for slot in range(len(slots)):
            for side in range(2):
                copy(step - 1, side, slot)[1].wait_recv()
                copy(step, side, slot)[1].start()
        return carry

    lax.fori_loop(1, count - 1, hop, 0)
    for slot in range(len(slots)):
        for side in range(2):
            copy(count - 2, side, slot)[1].wait_recv()
    for store in stores:
        store.wait()

    def drain(step, carry):
        for slot in range(len(slots)):
            for side in range(2):
                copy(step, side, slot)[1].wait_send()
        return carry

    lax.fori_loop(0, count - 1, drain, 0)


def ring_gather(shards, axes, parts, count, collective_id):
    turned = [a == 1 and s.shape[1] % 128 != 0 for s, a in zip(shards, axes)]
    if any(turned):
        shards = [s.T if t else s for s, t in zip(shards, turned)]
        axes = [0 if t else a for a, t in zip(axes, turned)]
        outs = ring_gather(shards, axes, parts, count, collective_id)
        return [o.T if t else o for o, t in zip(outs, turned)]
    items = tuple((s.shape, a, q) for s, a, q in zip(shards, axes, parts))
    slots = sum(parts)
    outs = [
        jax.ShapeDtypeStruct(
            (s.shape[0] * count, s.shape[1]) if a == 0 else (s.shape[0], s.shape[1] * count),
            s.dtype,
        )
        for s, a in zip(shards, axes)
    ]
    num = len(shards)
    nbytes = sum(s.size * 2 * (count - 1) for s in shards)
    return pl.pallas_call(
        functools.partial(gather_kernel, count, items),
        out_shape=outs,
        in_specs=[pl.BlockSpec(memory_space=pl.ANY)] * num,
        out_specs=[pl.BlockSpec(memory_space=pl.ANY)] * num,
        scratch_shapes=[pltpu.VMEM(s.shape, s.dtype) for s in shards]
        + [
            pltpu.SemaphoreType.DMA((2, count - 1, slots)),
            pltpu.SemaphoreType.DMA((2, count - 1, slots)),
            pltpu.SemaphoreType.DMA((num,)),
        ],
        compiler_params=pltpu.CompilerParams(collective_id=collective_id, has_side_effects=True),
        cost_estimate=pl.CostEstimate(flops=0, bytes_accessed=20 * nbytes, transcendentals=0),
        name=f"ring_gather_{collective_id}",
    )(*shards)


def scatter_kernel(count, items, *refs):
    num = len(items)
    partials, outs = refs[:num], refs[num : 2 * num]
    own = refs[2 * num : 3 * num]
    held = refs[3 * num : 4 * num]
    total = refs[4 * num : 5 * num]
    send_sems, recv_sems, load_sems, store_sems = refs[5 * num :]
    slots = [(k, part) for k in range(num) for part in range(items[k][2])]

    def load(step, side, slot, place):
        item, part = slots[slot]
        shape, axis, parts = items[item]
        member = member_at(place, side, step + 1, count)
        return pltpu.make_async_copy(
            piece(partials[item], shape, axis, member, side, part, parts),
            own[item].at[side, step, part],
            load_sems.at[side, step, slot],
        )

    start_place = ring_place(lax.axis_index("dp"), count)

    def load_all(step, carry):
        for slot in range(len(slots)):
            for side in range(2):
                load(step, side, slot, start_place).start()
        return carry

    lax.fori_loop(0, count, load_all, 0)
    place, neighbours = ring_setup(count)

    def send(step, side, slot, source):
        item, part = slots[slot]
        return pltpu.make_async_remote_copy(
            src_ref=source,
            dst_ref=held[item].at[side, step, part],
            send_sem=send_sems.at[side, step, slot],
            recv_sem=recv_sems.at[side, step, slot],
            device_id={"dp": neighbours[side]},
            device_id_type=MESH_ID,
        )

    for slot, (item, part) in enumerate(slots):
        for side in range(2):
            load(0, side, slot, place).wait()
            send(0, side, slot, own[item].at[side, 0, part]).start()

    def hop(step, carry):
        for slot, (item, part) in enumerate(slots):
            for side in range(2):
                load(step, side, slot, place).wait()
                arrived = held[item].at[side, step - 1, part]
                send(step - 1, side, slot, arrived).wait_recv()
                arrived[...] = (
                    arrived[...].astype(jnp.float32)
                    + own[item][side, step, part].astype(jnp.float32)
                ).astype(jnp.bfloat16)
                send(step, side, slot, arrived).start()
        return carry

    lax.fori_loop(1, count - 1, hop, 0)
    last = count - 1
    stores = []
    for slot, (item, part) in enumerate(slots):
        shape, axis, parts = items[item]
        for side in range(2):
            load(last, side, slot, place).wait()
            arrived = held[item].at[side, last - 1, part]
            send(last - 1, side, slot, arrived).wait_recv()
            total[item][side, part] = arrived[...].astype(jnp.float32) + own[item][
                side, last, part
            ].astype(jnp.float32)
            stores.append(
                pltpu.make_async_copy(
                    total[item].at[side, part],
                    piece(outs[item], shape, None, 0, side, part, parts),
                    store_sems.at[side, slot],
                )
            )
            stores[-1].start()
    for store in stores:
        store.wait()

    def drain(step, carry):
        for slot, (item, part) in enumerate(slots):
            for side in range(2):
                send(step, side, slot, held[item].at[side, 0, part]).wait_send()
        return carry

    lax.fori_loop(0, count - 1, drain, 0)


def ring_scatter(partials, axes, parts, count, collective_id):
    turned = [a == 1 and p.shape[1] // count % 128 != 0 for p, a in zip(partials, axes)]
    if any(turned):
        partials = [p.T if t else p for p, t in zip(partials, turned)]
        axes = [0 if t else a for a, t in zip(axes, turned)]
        outs = ring_scatter(partials, axes, parts, count, collective_id)
        return [o.T if t else o for o, t in zip(outs, turned)]
    shapes = [
        (p.shape[0] // count, p.shape[1]) if a == 0 else (p.shape[0], p.shape[1] // count)
        for p, a in zip(partials, axes)
    ]
    items = tuple((s, a, q) for s, a, q in zip(shapes, axes, parts))
    slots = sum(parts)
    num = len(partials)

    def buffers(depth, dtype):
        return [
            pltpu.VMEM((2,) + depth + (q, s[0] // (2 * q), s[1]), dtype)
            for s, q in zip(shapes, parts)
        ]

    nbytes = sum(p.size * 2 for p in partials)
    return pl.pallas_call(
        functools.partial(scatter_kernel, count, items),
        out_shape=[jax.ShapeDtypeStruct(s, jnp.float32) for s in shapes],
        in_specs=[pl.BlockSpec(memory_space=pl.ANY)] * num,
        out_specs=[pl.BlockSpec(memory_space=pl.ANY)] * num,
        scratch_shapes=buffers((count,), jnp.bfloat16)
        + buffers((count - 1,), jnp.bfloat16)
        + buffers((), jnp.float32)
        + [
            pltpu.SemaphoreType.DMA((2, count - 1, slots)),
            pltpu.SemaphoreType.DMA((2, count - 1, slots)),
            pltpu.SemaphoreType.DMA((2, count, slots)),
            pltpu.SemaphoreType.DMA((2, slots)),
        ],
        compiler_params=pltpu.CompilerParams(
            collective_id=collective_id, has_side_effects=True, vmem_limit_bytes=48 << 20
        ),
        cost_estimate=pl.CostEstimate(flops=0, bytes_accessed=20 * nbytes, transcendentals=0),
        name=f"ring_scatter_{collective_id}",
    )(*partials)


def scatter_dot_kernel(count, items, parts, extra, *refs):
    num = len(items)
    base = 6 * num + 5
    beside = None
    if extra is not None:
        builder, takes, gives = extra
        given, refs = refs[2 * num : 2 * num + takes], refs[: 2 * num] + refs[2 * num + takes :]
        made, refs = refs[3 * num : 3 * num + gives], refs[: 3 * num] + refs[3 * num + gives :]
        spare, refs = refs[3 * num + base :], refs[: 3 * num + base]
    lefts, rights, outs = refs[:num], refs[num : 2 * num], refs[2 * num : 3 * num]
    refs = refs[3 * num :]
    left_bufs, right_bufs = refs[:num], refs[num : 2 * num]
    firsts, owns, helds, totals = (refs[(2 + i) * num : (3 + i) * num] for i in range(4))
    send_sems, recv_sems, left_sems, right_sems, store_sems = refs[6 * num :]
    entry_place = ring_place(lax.axis_index("dp"), count)

    def load_right(item):
        return pltpu.make_async_copy(rights[item], right_bufs[item], right_sems.at[item])

    def load_left(step, side, item, place):
        block, _ = items[item]
        member = member_at(place, side, step + 1, count)
        slot = step % 2
        return pltpu.make_async_copy(
            lefts[item].at[:, pl.ds(pl.multiple_of(member * block, block), block)],
            left_bufs[item].at[side, slot],
            left_sems.at[side, slot, item],
        )

    for item in range(num):
        load_right(item).start()
        for side in range(2):
            load_left(0, side, item, entry_place).start()
    if extra is not None:
        beside = builder(count, given, made, spare, right_bufs)
        beside.begin()
    place, neighbours = ring_setup(count)
    pairs = [(item, side) for item in range(num) for side in range(2)]

    def own_sum(step, side, item):
        _, half = items[item]
        return tn_dot(
            left_bufs[item][side, step % 2], right_bufs[item][:, side * half : (side + 1) * half]
        )

    def send(step, side, item, part, source):
        return pltpu.make_async_remote_copy(
            src_ref=source.at[part],
            dst_ref=helds[item].at[side, step, part],
            send_sem=send_sems.at[side, step, item * parts + part],
            recv_sem=recv_sems.at[side, step, item * parts + part],
            device_id={"dp": neighbours[side]},
            device_id_type=MESH_ID,
        )

    def prefetch(step):
        for item, side in pairs:
            load_left(step, side, item, place).start()

    prefetch(1)
    for item in range(num):
        load_right(item).wait()
    for item, side in pairs:
        load_left(0, side, item, place).wait()
        firsts[item][side] = own_sum(0, side, item).astype(BF16).reshape(firsts[item].shape[1:])
        for part in range(parts):
            send(0, side, item, part, firsts[item].at[side]).start()
    if beside:
        beside.compute(0)

    def hop(step, carry):
        prefetch(step + 1)
        for item, side in pairs:
            load_left(step, side, item, place).wait()
            owns[item][side] = own_sum(step, side, item).reshape(owns[item].shape[1:])
        if beside:
            beside.compute(step)
        for part in range(parts):
            for item, side in pairs:
                arrived = helds[item].at[side, step - 1]
                send(step - 1, side, item, part, arrived).wait_recv()
                arrived[part] = (
                    arrived[part].astype(F32) + owns[item][side, part]
                ).astype(BF16)
                send(step, side, item, part, arrived).start()
        return carry

    lax.fori_loop(1, count - 1, hop, 0)
    last = count - 1
    for item, side in pairs:
        load_left(last, side, item, place).wait()
        owns[item][side] = own_sum(last, side, item).reshape(owns[item].shape[1:])
    if beside:
        beside.compute(last)
    stores = []
    for part in range(parts):
        for item, side in pairs:
            block, half = items[item]
            arrived = helds[item].at[side, last - 1]
            send(last - 1, side, item, part, arrived).wait_recv()
            totals[item][side, part] = arrived[part].astype(F32) + owns[item][side, part]
            stores.append(
                pltpu.make_async_copy(
                    totals[item].at[side, part],
                    outs[item].at[
                        pl.ds(part * (block // parts), block // parts),
                        pl.ds(side * half, half),
                    ],
                    store_sems.at[side, item * parts + part],
                )
            )
            stores[-1].start()
    for store in stores:
        store.wait()
    if beside:
        beside.finish()

    def drain(step, carry):
        for part in range(parts):
            for item, side in pairs:
                send(step, side, item, part, helds[item].at[side, 0]).wait_send()
        return carry

    lax.fori_loop(0, count - 1, drain, 0)


def ring_scatter_dots(jobs, parts, count, collective_id, extra=None):
    builder, given, given_specs, made, spare = extra or (None, [], [], [], [])
    lefts, rights = [j[0] for j in jobs], [j[1] for j in jobs]
    rows = lefts[0].shape[0]
    items = tuple((l.shape[1] // count, r.shape[1] // 2) for l, r in jobs)
    num = len(jobs)

    def buffers(depth, dtype):
        return [pltpu.VMEM(depth + (parts, b // parts, h), dtype) for b, h in items]

    slots = num * parts
    flops = sum(2 * rows * l.shape[1] * r.shape[1] for l, r in jobs)
    nbytes = sum(2 * l.shape[1] * r.shape[1] for l, r in jobs)
    return pl.pallas_call(
        functools.partial(
            scatter_dot_kernel,
            count,
            items,
            parts,
            (builder, len(given), len(made)) if extra else None,
        ),
        out_shape=[jax.ShapeDtypeStruct((b, 2 * h), F32) for b, h in items] + made,
        in_specs=[pl.BlockSpec(memory_space=pl.ANY)] * (2 * num) + given_specs,
        out_specs=[pl.BlockSpec(memory_space=pl.ANY)] * (num + len(made)),
        scratch_shapes=[pltpu.VMEM((2, 2, rows, b), BF16) for b, _ in items]
        + [pltpu.VMEM(r.shape, BF16) for r in rights]
        + buffers((2,), BF16)
        + buffers((2,), F32)
        + buffers((2, count - 1), BF16)
        + buffers((2,), F32)
        + [
            pltpu.SemaphoreType.DMA((2, count - 1, slots)),
            pltpu.SemaphoreType.DMA((2, count - 1, slots)),
            pltpu.SemaphoreType.DMA((2, 2, num)),
            pltpu.SemaphoreType.DMA((num,)),
            pltpu.SemaphoreType.DMA((2, slots)),
        ]
        + spare,
        compiler_params=pltpu.CompilerParams(
            collective_id=collective_id, has_side_effects=True, vmem_limit_bytes=60 << 20
        ),
        cost_estimate=pl.CostEstimate(
            flops=flops, bytes_accessed=20 * nbytes, transcendentals=0
        ),
        name=f"ring_scatter_{collective_id}",
    )(*lefts, *rights, *given)


class NormWork:
    def __init__(self, count, given, made, spare, rights):
        self.grads, self.gates = given[:2], tuple(given[2:4])
        self.up, self.down = given[4:]
        self.outs = made
        self.grad_bufs, self.row_bufs, self.down_bufs, self.stage = spare[0], *spare[1:4]
        self.grad_sems, self.row_sems, self.down_sems, self.out_sems = spare[4:]
        self.act = rights[0]
        self.count = count
        self.block = self.row_bufs.shape[2]

    def load_grad(self, which):
        return pltpu.make_async_copy(
            self.grads[which], self.grad_bufs.at[which], self.grad_sems.at[which]
        )

    def spot(self, step):
        return pl.ds(pl.multiple_of(step * self.block, self.block), self.block)

    def loads(self, step):
        slot = step % 2
        edge = self.gates[0].shape[1]
        gate = self.row_bufs.at[0, slot]
        targets = [gate.at[:, :edge], gate.at[:, edge:], self.row_bufs.at[1, slot]]
        rows = [
            pltpu.make_async_copy(
                source.at[self.spot(step), :], target, self.row_sems.at[which, slot]
            )
            for which, (source, target) in enumerate(zip(self.gates + (self.up,), targets))
        ]
        down = pltpu.make_async_copy(
            self.down.at[:, self.spot(step)], self.down_bufs.at[slot], self.down_sems.at[slot]
        )
        return rows + [down]

    def store(self, which, step):
        slot = step % 2
        return pltpu.make_async_copy(
            self.stage.at[which, slot],
            self.outs[which].at[:, self.spot(step)],
            self.out_sems.at[which, slot],
        )

    def begin(self):
        for which in range(2):
            self.load_grad(which).start()
        for copy in self.loads(0):
            copy.start()

    def compute(self, step):
        last = self.count - 1
        if isinstance(step, int):
            if step < last:
                for copy in self.loads(step + 1):
                    copy.start()
            if step == 0:
                for which in range(2):
                    self.load_grad(which).wait()
            if step >= 2:
                for which in range(2):
                    self.store(which, step - 2).wait()
        else:
            for copy in self.loads(step + 1):
                copy.start()

            @pl.when(step >= 2)
            def _():
                for which in range(2):
                    self.store(which, step - 2).wait()

        for copy in self.loads(step):
            copy.wait()
        slot = step % 2
        for top in range(0, self.act.shape[0], 256):
            band = pl.ds(top, 256)
            norm = nt_dot(self.grad_bufs[0, band, :], self.row_bufs[0, slot])
            norm += nt_dot(self.grad_bufs[1, band, :], self.row_bufs[1, slot])
            self.stage[0, slot, band, :] = norm.astype(BF16)
            value = jnp.dot(
                self.act[band, :], self.down_bufs[slot], preferred_element_type=F32
            )
            self.stage[1, slot, band, :] = value.astype(BF16)
        for which in range(2):
            self.store(which, step).start()

    def finish(self):
        for step in range(max(self.count - 2, 0), self.count):
            for which in range(2):
                self.store(which, step).wait()


def down_ring(grad_branch, activated, grad_gate, grad_up, gates, up_all, down_all, count, cid):
    rows, hidden = activated.shape
    width = up_all.shape[0]
    block = width // count
    wide = jax.ShapeDtypeStruct((rows, width), BF16)
    spare = [
        pltpu.VMEM((2, rows, hidden), BF16),
        pltpu.VMEM((2, 2, block, hidden), BF16),
        pltpu.VMEM((2, hidden, block), BF16),
        pltpu.VMEM((2, 2, rows, block), BF16),
        pltpu.SemaphoreType.DMA((2,)),
        pltpu.SemaphoreType.DMA((3, 2)),
        pltpu.SemaphoreType.DMA((2,)),
        pltpu.SemaphoreType.DMA((2, 2)),
    ]
    given = [grad_gate, grad_up, *gates, up_all, down_all]
    return ring_scatter_dots(
        [(grad_branch, activated)], 2, count, cid, (NormWork, given, [ANY] * 6, [wide, wide], spare)
    )


def mlp_kernel(count, *refs):
    x_hbm, wg_hbm, wg_rest, wu_hbm, shard, gb_hbm = refs[:6]
    act_hbm, gg_hbm, gu_hbm, down_all = refs[6:10]
    x_buf, gb_buf, w_bufs, gate_slope, up_slope, acc, half_bufs, stage, own_stage = refs[10:19]
    send_sems, recv_sems, w_sems, in_sems, half_sems, out_sems, local_sem = refs[19:]
    rows, width = x_buf.shape
    hidden = acc.shape[1]
    block = width // count
    cols = w_bufs.shape[-1]
    steps = hidden // cols
    half = hidden // 2
    parts = send_sems.shape[2]
    me = lax.axis_index("dp")

    gate_steps = wg_hbm.shape[1] // cols

    def load_weights(step, which, source=None):
        start = step - gate_steps if source is wg_rest else step
        source = (wg_hbm, wu_hbm)[which] if source is None else source
        return pltpu.make_async_copy(
            source.at[:, pl.ds(pl.multiple_of(start * cols, cols), cols)],
            w_bufs.at[which, step % 2],
            w_sems.at[which, step % 2],
        )

    def fetch(step):
        load_weights(step, 1).start()

        @pl.when(step < gate_steps)
        def _():
            load_weights(step, 0).start()

        @pl.when(step >= gate_steps)
        def _():
            load_weights(step, 0, wg_rest).start()

    load_x = pltpu.make_async_copy(x_hbm, x_buf, in_sems.at[0])
    load_gb = pltpu.make_async_copy(gb_hbm, gb_buf, in_sems.at[1])
    load_own = pltpu.make_async_copy(shard, own_stage, local_sem)
    load_x.start()
    for which in range(2):
        load_weights(0, which).start()
    load_own.start()
    load_gb.start()
    place, neighbours = ring_setup(count)

    def target(ref, member, side, part):
        return piece(ref, (hidden, block), 1, member, side, part, parts)

    def hop(step, side, part):
        ref = target(down_all, member_at(place, side, step, count), side, part)
        return pltpu.make_async_remote_copy(
            src_ref=ref,
            dst_ref=ref,
            send_sem=send_sems.at[side, step, part],
            recv_sem=recv_sems.at[side, step, part],
            device_id={"dp": neighbours[side]},
            device_id_type=MESH_ID,
        )

    for part in range(parts):
        for side in range(2):
            pltpu.make_async_remote_copy(
                src_ref=piece(shard, (hidden, block), None, 0, side, part, parts),
                dst_ref=target(down_all, me, side, part),
                send_sem=send_sems.at[side, 0, part],
                recv_sem=recv_sems.at[side, 0, part],
                device_id={"dp": neighbours[side]},
                device_id_type=MESH_ID,
            ).start()

    def pump(step):
        for part in range(parts):
            for side in range(2):
                hop(step - 1, side, part).wait_recv()
                hop(step, side, part).start()

    load_own.wait()
    store_own = pltpu.make_async_copy(
        own_stage, down_all.at[:, pl.ds(pl.multiple_of(me * block, block), block)], local_sem
    )
    store_own.start()
    load_x.wait()

    def store(ref, which, step):
        return pltpu.make_async_copy(
            stage.at[which, step % 2],
            ref.at[:, pl.ds(pl.multiple_of(step * cols, cols), cols)],
            out_sems.at[which, step % 2],
        )

    def forward(step, carry):
        @pl.when(step + 1 < steps)
        def _():
            fetch(step + 1)

        @pl.when(step >= 2)
        def _():
            store(act_hbm, 0, step - 2).wait()

        load_weights(step, 1).wait()

        @pl.when(step < gate_steps)
        def _():
            load_weights(step, 0).wait()

        @pl.when(step >= gate_steps)
        def _():
            load_weights(step, 0, wg_rest).wait()

        here = pl.ds(pl.multiple_of(step * cols, cols), cols)
        for top in range(0, rows, 256):
            band = pl.ds(top, 256)
            lines = x_buf[band, :]
            gate = jnp.dot(lines, w_bufs[0, step % 2], preferred_element_type=F32)
            up = jnp.dot(lines, w_bufs[1, step % 2], preferred_element_type=F32)
            sig = jax.nn.sigmoid(gate)
            silu = gate * sig
            stage[0, step % 2, band, :] = (silu * up).astype(BF16)
            gate_slope[band, here] = up * sig * (1.0 + gate * (1.0 - sig))
            up_slope[band, here] = silu
        store(act_hbm, 0, step).start()

        turn = (step + 1) // 2

        @pl.when((step % 2 == 1) & (turn <= count - 2))
        def _():
            pump(turn)

        return carry

    lax.fori_loop(0, steps, forward, 0)
    for step in range(max(steps - 2, 0), steps):
        store(act_hbm, 0, step).wait()
    pumped = min(steps // 2, count - 2)
    load_gb.wait()

    def load_half(step, side):
        member = member_at(place, side, step, count)
        return pltpu.make_async_copy(
            down_all.at[
                pl.ds(side * half, half), pl.ds(pl.multiple_of(member * block, block), block)
            ],
            half_bufs.at[side],
            half_sems.at[side],
        )

    def backward(step, carry):
        @pl.when((step > pumped) & (step <= count - 2))
        def _():
            pump(step)

        @pl.when(step == count - 1)
        def _():
            for part in range(parts):
                for side in range(2):
                    hop(count - 2, side, part).wait_recv()

        for side in range(2):
            load_half(step, side).start()
        for side in range(2):
            member = member_at(place, side, step, count)
            load_half(step, side).wait()
            for top in range(0, rows, 256):
                band = pl.ds(top, 256)
                lines = gb_buf[band, pl.ds(pl.multiple_of(member * block, block), block)]
                value = nt_dot(lines, half_bufs[side])
                spot = (band, pl.ds(side * half, half))

                @pl.when(step == 0)
                def _():
                    acc[spot] = value

                @pl.when(step > 0)
                def _():
                    acc[spot] += value

        return carry

    store_own.wait()
    lax.fori_loop(0, count, backward, 0)

    def slopes(step, carry):
        @pl.when(step >= 2)
        def _():
            store(gg_hbm, 1, step - 2).wait()
            store(gu_hbm, 2, step - 2).wait()

        here = pl.ds(pl.multiple_of(step * cols, cols), cols)
        for top in range(0, rows, 256):
            band = pl.ds(top, 256)
            value = acc[band, here]
            stage[1, step % 2, band, :] = (value * gate_slope[band, here]).astype(BF16)
            stage[2, step % 2, band, :] = (value * up_slope[band, here]).astype(BF16)
        store(gg_hbm, 1, step).start()
        store(gu_hbm, 2, step).start()
        return carry

    lax.fori_loop(0, steps, slopes, 0)
    for step in range(max(steps - 2, 0), steps):
        store(gg_hbm, 1, step).wait()
        store(gu_hbm, 2, step).wait()

    def drain(step, carry):
        for part in range(parts):
            for side in range(2):
                hop(step, side, part).wait_send()
        return carry

    lax.fori_loop(0, count - 1, drain, 0)


def mlp_ring(rows_mlp, gates, up_all, w_down, grad_branch, count, collective_id):
    rows, width = rows_mlp.shape
    hidden, block = w_down.shape
    cols, parts = 256, 2
    wide = jax.ShapeDtypeStruct((rows, hidden), BF16)
    return pl.pallas_call(
        functools.partial(mlp_kernel, count),
        out_shape=[wide] * 3 + [jax.ShapeDtypeStruct((hidden, width), BF16)],
        in_specs=[ANY] * 6,
        out_specs=[pl.BlockSpec(memory_space=pl.ANY)] * 4,
        scratch_shapes=[
            pltpu.VMEM((rows, width), BF16),
            pltpu.VMEM((rows, width), BF16),
            pltpu.VMEM((2, 2, width, cols), BF16),
            pltpu.VMEM((rows, hidden), F32),
            pltpu.VMEM((rows, hidden), F32),
            pltpu.VMEM((rows, hidden), F32),
            pltpu.VMEM((2, hidden // 2, block), BF16),
            pltpu.VMEM((3, 2, rows, cols), BF16),
            pltpu.VMEM((hidden, block), BF16),
            pltpu.SemaphoreType.DMA((2, count - 1, parts)),
            pltpu.SemaphoreType.DMA((2, count - 1, parts)),
            pltpu.SemaphoreType.DMA((2, 2)),
            pltpu.SemaphoreType.DMA((2,)),
            pltpu.SemaphoreType.DMA((2,)),
            pltpu.SemaphoreType.DMA((3, 2)),
            pltpu.SemaphoreType.DMA,
        ],
        compiler_params=pltpu.CompilerParams(
            collective_id=collective_id, has_side_effects=True, vmem_limit_bytes=60 << 20
        ),
        cost_estimate=pl.CostEstimate(
            flops=6 * rows * width * hidden,
            bytes_accessed=40 * hidden * width,
            transcendentals=rows * hidden,
        ),
        name="mlp_ring",
    )(rows_mlp, *gates, up_all, w_down, grad_branch)


class HeadWork:
    def __init__(self, count, given, made, spare, rights):
        self.length, self.sources = given[0], given[1:]
        self.grads_out, self.token_out = made
        num = len(self.sources)
        self.bufs = spare[:num]
        self.heads, self.grads, self.acc_k, self.acc_v, self.stage = spare[num : num + 5]
        self.in_sems, self.out_sems = spare[num + 5 :]

    def load(self, which):
        return pltpu.make_async_copy(
            self.sources[which], self.bufs[which], self.in_sems.at[which]
        )

    def begin(self):
        for which in range(len(self.sources)):
            self.load(which).start()

    def store(self, band):
        rows = self.stage.shape[1]
        return pltpu.make_async_copy(
            self.stage.at[band % 2],
            self.token_out.at[pl.ds(band * rows, rows), :],
            self.out_sems.at[band % 2],
        )

    def store_grads(self):
        return pltpu.make_async_copy(self.grads, self.grads_out, self.out_sems.at[2])

    def tokens(self, bands):
        w_query, w_key, w_value = self.bufs[7:]
        rows = self.stage.shape[1]
        inner = w_query.shape[1]
        for band in bands:
            if band >= 2:
                self.store(band - 2).wait()
            lines = slice(band * rows, (band + 1) * rows)
            for left in range(0, w_query.shape[0], 512):
                cols = slice(left, left + 512)
                value = nt_dot(self.grads[lines, :inner], w_query[cols, :])
                value += nt_dot(self.grads[lines, inner : inner + 128], w_key[cols, :])
                value += nt_dot(self.grads[lines, inner + 128 :], w_value[cols, :])
                self.stage[band % 2, :, cols] = value.astype(BF16)
            self.store(band).start()

    def compute(self, step):
        grad_attn, w_output, queries, keys, values, cosine, sine = self.bufs[:7]
        inner = queries.shape[1]
        pairs = inner // 128
        if isinstance(step, int):
            if step == 0:
                for which in range(len(self.sources)):
                    self.load(which).wait()
                for top in range(0, LEN, 256):
                    rows = slice(top, top + 256)
                    self.heads[rows, :] = nt_dot(grad_attn[rows, :], w_output[...]).astype(BF16)
                self.acc_k[...] = jnp.zeros_like(self.acc_k)
                self.acc_v[...] = jnp.zeros_like(self.acc_v)
            return

        @pl.when(step <= pairs)
        def _():
            here = pl.ds(pl.multiple_of((step - 1) * 128, 128), 128)
            attend_back_pair(
                self.length[0], (step - 1) // 2, queries.at[:, here], keys, values,
                self.heads.at[:, here], cosine, sine, self.grads.at[:, here],
                self.acc_k, self.acc_v,
            )

        @pl.when(step == pairs)
        def _():
            self.grads[:, inner : inner + 128] = rope_back(
                self.acc_k[...], cosine[...], sine[...]
            )
            self.grads[:, inner + 128 :] = self.acc_v[...].astype(BF16)
            self.store_grads().start()

        @pl.when(step == pairs + 1)
        def _():
            self.tokens((0, 1))

        @pl.when(step == pairs + 2)
        def _():
            self.tokens((2, 3))

    def finish(self):
        self.store_grads().wait()
        for band in (2, 3):
            self.store(band).wait()


def heads_ring(job, lengths, grad_attn, w_output, qkv, tables, weights, count, collective_id):
    given = [grad_attn, w_output, *qkv, *tables, *weights]
    rows, width = grad_attn.shape
    inner = qkv[0].shape[1]
    made = [
        jax.ShapeDtypeStruct((rows, inner + 256), BF16),
        jax.ShapeDtypeStruct((rows, width), BF16),
    ]
    spare = [pltpu.VMEM(g.shape, g.dtype) for g in given] + [
        pltpu.VMEM((rows, inner), BF16),
        pltpu.VMEM((rows, inner + 256), BF16),
        pltpu.VMEM((rows, 128), F32),
        pltpu.VMEM((rows, 128), F32),
        pltpu.VMEM((2, rows // 4, width), BF16),
        pltpu.SemaphoreType.DMA((len(given),)),
        pltpu.SemaphoreType.DMA((3,)),
    ]
    specs = [pl.BlockSpec(memory_space=pltpu.SMEM)] + [ANY] * len(given)
    return ring_scatter_dots(
        [job], 2, count, collective_id, (HeadWork, [lengths] + given, specs, made, spare)
    )


def attend_ring_kernel(count, *refs):
    length_ref, shard, sources = refs[0], refs[1], refs[2:9]
    gathered, q_out, k_out, v_out, head_out, part_out = refs[9:15]
    bufs = refs[15:22]
    q_buf, k_buf, v_buf, head_buf, stage, own = refs[22:28]
    send_sems, recv_sems, in_sems, out_sems, local_sem = refs[28:]
    rows_buf, w_query, w_key, w_value, w_output, cosine, sine = bufs
    shape = shard.shape
    me = lax.axis_index("dp")
    loads = [
        pltpu.make_async_copy(source, buf, in_sems.at[k])
        for k, (source, buf) in enumerate(zip(sources, bufs))
    ]
    for load in loads:
        load.start()
    load_own = pltpu.make_async_copy(shard, own, local_sem)
    load_own.start()
    place, neighbours = ring_setup(count)

    def hop(step, side):
        ref = piece(gathered, shape, 0, member_at(place, side, step, count), side, 0, 1)
        return pltpu.make_async_remote_copy(
            src_ref=ref,
            dst_ref=ref,
            send_sem=send_sems.at[side, step],
            recv_sem=recv_sems.at[side, step],
            device_id={"dp": neighbours[side]},
            device_id_type=MESH_ID,
        )

    for side in range(2):
        pltpu.make_async_remote_copy(
            src_ref=piece(shard, shape, None, 0, side, 0, 1),
            dst_ref=piece(gathered, shape, 0, me, side, 0, 1),
            send_sem=send_sems.at[side, 0],
            recv_sem=recv_sems.at[side, 0],
            device_id={"dp": neighbours[side]},
            device_id_type=MESH_ID,
        ).start()

    def pump(step, carry=0):
        for side in range(2):
            hop(step - 1, side).wait_recv()
            hop(step, side).start()
        return carry

    load_own.wait()
    store_own = pltpu.make_async_copy(
        own, gathered.at[pl.ds(pl.multiple_of(me * shape[0], shape[0]), shape[0]), :], local_sem
    )
    store_own.start()
    for load in loads:
        load.wait()

    def projection(band, carry):
        lines = pl.ds(pl.multiple_of(band * 256, 256), 256)
        project_rows(
            rows_buf[lines, :], w_query, w_key, w_value, cosine[lines, :], sine[lines, :],
            q_buf.at[lines, :], k_buf.at[lines, :], v_buf.at[lines, :],
        )
        return carry

    lax.fori_loop(0, LEN // 256, projection, 0)
    stores = [
        pltpu.make_async_copy(buf, out, out_sems.at[k])
        for k, (buf, out) in enumerate(
            ((q_buf, q_out), (k_buf, k_out), (v_buf, v_out), (head_buf, head_out))
        )
    ]
    for store in stores[:3]:
        store.start()
    pump(1)
    pairs = q_buf.shape[1] // 128

    def attention(pair, carry):
        here = pl.ds(pl.multiple_of(pair * 128, 128), 128)
        attend_pair(
            length_ref[0], pair // 2, q_buf.at[:, here], k_buf, v_buf, head_buf.at[:, here]
        )

        @pl.when(pair + 2 <= count - 2)
        def _():
            pump(pair + 2)

        return carry

    lax.fori_loop(0, pairs, attention, 0)
    stores[3].start()

    def store_part(band):
        return pltpu.make_async_copy(
            stage.at[band % 2],
            part_out.at[pl.ds(pl.multiple_of(band * 256, 256), 256), :],
            out_sems.at[4 + band % 2],
        )

    def output(band, carry):
        @pl.when(band >= 2)
        def _():
            store_part(band - 2).wait()

        lines = pl.ds(pl.multiple_of(band * 256, 256), 256)
        for left in range(0, w_output.shape[1], 512):
            cols = slice(left, left + 512)
            stage[band % 2, :, cols] = jnp.dot(
                head_buf[lines, :], w_output[:, cols], preferred_element_type=F32
            ).astype(BF16)
        store_part(band).start()
        return carry

    lax.fori_loop(0, LEN // 256, output, 0)
    lax.fori_loop(min(pairs + 2, count - 1), count - 1, pump, 0)
    for band in (LEN // 256 - 2, LEN // 256 - 1):
        store_part(band).wait()
    for store in stores:
        store.wait()
    store_own.wait()
    for side in range(2):
        hop(count - 2, side).wait_recv()

    def drain(step, carry):
        for side in range(2):
            hop(step, side).wait_send()
        return carry

    lax.fori_loop(0, count - 1, drain, 0)


def attend_ring(shard, lengths, rows_attn, weights, tables, count, collective_id):
    sources = [rows_attn, *weights, *tables]
    rows, width = rows_attn.shape
    inner = weights[0].shape[1]

    def low(*shape):
        return jax.ShapeDtypeStruct(shape, BF16)

    return pl.pallas_call(
        functools.partial(attend_ring_kernel, count),
        out_shape=[
            low(shard.shape[0] * count, shard.shape[1]),
            low(rows, inner),
            low(rows, 128),
            low(rows, 128),
            low(rows, inner),
            low(rows, width),
        ],
        in_specs=[pl.BlockSpec(memory_space=pltpu.SMEM)] + [ANY] * (1 + len(sources)),
        out_specs=[ANY] * 6,
        scratch_shapes=[pltpu.VMEM(source.shape, source.dtype) for source in sources]
        + [
            pltpu.VMEM((rows, inner), BF16),
            pltpu.VMEM((rows, 128), BF16),
            pltpu.VMEM((rows, 128), BF16),
            pltpu.VMEM((rows, inner), BF16),
            pltpu.VMEM((2, 256, width), BF16),
            pltpu.VMEM(shard.shape, BF16),
            pltpu.SemaphoreType.DMA((2, count - 1)),
            pltpu.SemaphoreType.DMA((2, count - 1)),
            pltpu.SemaphoreType.DMA((len(sources),)),
            pltpu.SemaphoreType.DMA((6,)),
            pltpu.SemaphoreType.DMA,
        ],
        compiler_params=pltpu.CompilerParams(
            collective_id=collective_id, has_side_effects=True, vmem_limit_bytes=56 << 20
        ),
        cost_estimate=pl.CostEstimate(
            flops=24 << 30, bytes_accessed=60 << 20, transcendentals=8 << 20
        ),
        name="attend_ring",
    )(lengths, shard, *sources)


def ring_weight_grads(jobs, parts, count, collective_id):
    if all(left.shape[1] // count % 128 == 0 for left, _ in jobs):
        return ring_scatter_dots(jobs, parts, count, collective_id)
    partials = [tn_dot(left, right).astype(BF16) for left, right in jobs]
    num = len(jobs)
    return ring_scatter(partials, [0] * num, [parts] * num, count, collective_id)


def after(value, *deps):
    return lax.optimization_barrier((value,) + deps)[0]


def gather_rows(value):
    return lax.all_gather(value, "tensor", axis=0, tiled=True)


def scatter_rows(value):
    return lax.psum_scatter(value.astype(BF16), "tensor", scatter_dimension=0, tiled=True).astype(
        F32
    )


def share_kernel(count, group, parts_ref, out_ref, first, sums, second, sems):
    row, col = lax.axis_index("dp"), lax.axis_index("tensor")
    barrier = pltpu.get_barrier_semaphore()

    def in_group(shift):
        return {"tensor": (col + shift) % group}

    def in_column(shift):
        return {"dp": (row + shift) % count}

    def greet(device):
        pl.semaphore_signal(barrier, inc=1, device_id=device, device_id_type=MESH_ID)

    for shift in range(1, group):
        greet(in_group(shift))
    for shift in range(1, count):
        greet(in_column(shift))
    pl.semaphore_wait(barrier, group + count - 2)

    def exchange(shift, slot, source, target, device):
        return pltpu.make_async_remote_copy(
            src_ref=source,
            dst_ref=target,
            send_sem=sems.at[0, slot],
            recv_sem=sems.at[1, slot],
            device_id=device,
            device_id_type=MESH_ID,
        )

    moves = [
        exchange(s, s - 1, parts_ref.at[(col + s) % group], first.at[s - 1], in_group(s))
        for s in range(1, group)
    ]
    for move in moves:
        move.start()
    total = parts_ref[col]
    for shift, move in enumerate(moves):
        move.wait()
        total = total + first[shift]
    sums[...] = total
    moves = [
        exchange(
            s, group + s - 2, sums.at[(row + s) % count], second.at[s - 1], in_column(s)
        )
        for s in range(1, count)
    ]
    for move in moves:
        move.start()
    total = sums[row]
    for shift, move in enumerate(moves):
        move.wait()
        total = total + second[shift]
    out_ref[...] = total


def sum_shares(first, second, count, group, collective_id):
    share = first.shape[0] // (count * group)
    pair = jnp.stack([first, second]).reshape(2, count, group, share)
    parts = jnp.transpose(pair, (2, 1, 0, 3)).reshape(group, count, 1, 2 * share)
    width = (2 * share + 127) // 128 * 128
    parts = jnp.pad(parts, ((0, 0), (0, 0), (0, 7), (0, width - 2 * share)))
    tile = (8, width)
    out = pl.pallas_call(
        functools.partial(share_kernel, count, group),
        out_shape=jax.ShapeDtypeStruct(tile, F32),
        in_specs=[pl.BlockSpec(memory_space=pltpu.VMEM)],
        out_specs=pl.BlockSpec(memory_space=pltpu.VMEM),
        scratch_shapes=[
            pltpu.VMEM((group - 1, count) + tile, F32),
            pltpu.VMEM((count,) + tile, F32),
            pltpu.VMEM((count - 1,) + tile, F32),
            pltpu.SemaphoreType.DMA((2, group + count - 2)),
        ],
        compiler_params=pltpu.CompilerParams(collective_id=collective_id, has_side_effects=True),
        name="sum_shares",
    )(parts)
    return out[0, :share], out[0, share : 2 * share]


def dot(left, right):
    return jnp.dot(left, right, preferred_element_type=F32)


def body(
    count,
    group,
    tokens,
    lengths,
    attn_gain,
    w_query,
    w_key,
    w_value,
    w_output,
    mlp_gain,
    w_gate,
    w_up,
    w_down,
    cotangent,
):
    local_rows = tokens.shape[0]
    token_full = tokens.astype(F32)
    gain_attn = attn_gain.astype(F32)
    gain_mlp = mlp_gain.astype(F32)
    row_pos = lax.axis_index("tensor") * local_rows + jnp.arange(local_rows)
    valid_rows = (row_pos < lengths[0]).astype(F32)
    cot_masked = cotangent.astype(F32) * valid_rows[:, None]
    cosine, sine = rope_tables()

    inv_first = lax.rsqrt(jnp.mean(token_full * token_full, axis=1, keepdims=True) + epsilon)
    normed_attn = (token_full * inv_first * gain_attn).astype(BF16)
    rows_attn = gather_rows(normed_attn)
    query_all, key_all, value_all, output_all = ring_gather(
        [after(w_query, normed_attn), w_key, w_value, w_output],
        (0, 0, 0, 1), (1, 1, 1, 1), count, 0,
    )
    grad_branch = gather_rows(after(cot_masked.astype(BF16), rows_attn))
    fused = count == 8
    edge = 3 * w_gate.shape[1] // 8
    gates = []
    if fused:
        first_gate, queries, keys, values, head_out, attn_part = attend_ring(
            w_gate[:, :edge],
            lengths,
            rows_attn,
            (query_all, key_all, value_all, output_all),
            (cosine, sine),
            count,
            9,
        )
        gates.append(first_gate)
    else:
        queries, keys, values = project(rows_attn, query_all, key_all, value_all, cosine, sine)
        head_out = attend(queries, keys, values, lengths)
        attn_part = dot(head_out, output_all).astype(BF16)
    attn_branch = scatter_rows(attn_part)
    rest = w_gate[:, edge:] if fused else w_gate
    (gate_all,) = ring_gather([after(rest, attn_part)], (0,), (2,), count, 1)
    gates.append(gate_all)
    hidden = token_full + attn_branch
    inv_second = lax.rsqrt(jnp.mean(hidden * hidden, axis=1, keepdims=True) + epsilon)
    normed_mlp = (hidden * inv_second * gain_mlp).astype(BF16)
    normed_mlp = after(normed_mlp, gate_all)
    rows_mlp = gather_rows(normed_mlp)
    (up_all,) = ring_gather([after(w_up, normed_mlp)], (0,), (2,), count, 2)
    if fused:
        activated, grad_gate_pre, grad_up_pre, down_all = mlp_ring(
            rows_mlp, gates, after(up_all, rows_mlp), w_down, grad_branch, count, 3
        )
        grad_down, norm_part, mlp_part = down_ring(
            grad_branch, activated, grad_gate_pre, grad_up_pre, gates, up_all, down_all,
            count, 4,
        )
    else:
        gate_proj = dot(rows_mlp, gate_all)
        up_proj = dot(rows_mlp, up_all)
        gate_sig = jax.nn.sigmoid(gate_proj)
        activated = (gate_proj * gate_sig * up_proj).astype(BF16)
        (down_all,) = ring_gather([after(w_down, up_all)], (1,), (2,), count, 3)
        mlp_part = dot(activated, down_all).astype(BF16)
        grad_act = nt_dot(grad_branch, down_all)
        grad_gate_pre = (
            grad_act * up_proj * gate_sig * (1.0 + gate_proj * (1.0 - gate_sig))
        ).astype(BF16)
        grad_up_pre = (grad_act * gate_proj * gate_sig).astype(BF16)
        norm_part = (nt_dot(grad_gate_pre, gate_all) + nt_dot(grad_up_pre, up_all)).astype(BF16)
        (grad_down,) = ring_weight_grads([(grad_branch, activated)], 2, count, 4)
    grad_norm_two = scatter_rows(norm_part)
    (grad_gate,) = ring_weight_grads(
        [(after(rows_mlp, norm_part), grad_gate_pre)], 2, count, 5
    )
    scaled_two = grad_norm_two * gain_mlp
    gain_two_part = jnp.sum(grad_norm_two * hidden * inv_second, axis=0)
    grad_hidden = (
        cot_masked
        + inv_second * scaled_two
        - hidden * inv_second**3 * jnp.mean(scaled_two * hidden, axis=1, keepdims=True)
    )
    grad_hidden = after(grad_hidden, grad_gate)
    grad_attn = gather_rows(grad_hidden.astype(BF16))
    mlp_branch = scatter_rows(after(mlp_part, grad_hidden))
    if fused:
        middle = grad_up_pre.shape[1] // 2
        (up_left,) = ring_weight_grads(
            [(after(rows_mlp, grad_hidden), grad_up_pre[:, :middle])], 2, count, 6
        )
        up_right, grad_qkv, token_part = heads_ring(
            (rows_mlp, grad_up_pre[:, middle:]),
            lengths,
            after(grad_attn, up_left),
            output_all,
            (queries, keys, values),
            (cosine, sine),
            (query_all, key_all, value_all),
            count,
            10,
        )
        grad_up = jnp.concatenate([up_left, up_right], axis=1)
    else:
        (grad_up,) = ring_weight_grads(
            [(after(rows_mlp, grad_hidden), grad_up_pre)], 2, count, 6
        )
        grad_heads = nt_dot(after(grad_attn, grad_up), output_all).astype(BF16)
        grad_qpre, grad_kpre, grad_vpre = attend_back(
            queries, keys, values, grad_heads, lengths, cosine, sine
        )
        token_part = (
            nt_dot(grad_qpre, query_all)
            + nt_dot(grad_kpre, key_all)
            + nt_dot(grad_vpre, value_all)
        ).astype(BF16)
        grad_qkv = jnp.concatenate([grad_qpre, grad_kpre, grad_vpre], axis=1)
    layer_out = (hidden + after(mlp_branch, token_part)).astype(BF16)
    grad_norm_one = scatter_rows(token_part)
    attn_grads, grad_output = ring_weight_grads(
        [(after(rows_attn, token_part), grad_qkv), (grad_attn, head_out)], 1, count, 7
    )
    scaled_one = grad_norm_one * gain_attn
    gain_one_part = jnp.sum(grad_norm_one * token_full * inv_first, axis=0)
    grad_tokens = (
        grad_hidden
        + inv_first * scaled_one
        - token_full * inv_first**3 * jnp.mean(scaled_one * token_full, axis=1, keepdims=True)
    )
    grad_attn_gain, grad_mlp_gain = sum_shares(
        after(gain_one_part, attn_grads), gain_two_part, count, group, 8
    )
    query_cols, key_cols = queries.shape[1], keys.shape[1]
    grad_query = attn_grads[:, :query_cols]
    grad_key = attn_grads[:, query_cols : query_cols + key_cols]
    grad_value = attn_grads[:, query_cols + key_cols :]
    grad_output, grad_down = grad_output.T, grad_down.T
    return (
        layer_out,
        grad_tokens,
        grad_query,
        grad_key,
        grad_value,
        grad_output,
        grad_gate,
        grad_up,
        grad_down,
        grad_attn_gain,
        grad_mlp_gain,
    )


def solution(mesh):
    rows = P(("dp", "tensor"), None)
    tall = P("dp", "tensor")
    wide = P("tensor", "dp")
    share = P(("dp", "tensor"))
    in_specs = (rows, P("dp"), P(), tall, tall, tall, wide, P(), tall, tall, wide, rows)
    out_specs = (rows, rows, tall, tall, tall, wide, tall, tall, wide, share, share)
    return jax.shard_map(
        functools.partial(body, mesh.shape["dp"], mesh.shape["tensor"]),
        mesh=mesh,
        in_specs=in_specs,
        out_specs=out_specs,
        check_vma=False,
    )
```

```python
import functools
from typing import Any, NamedTuple

import jax
import jax.numpy as jnp
from jax import lax
from jax.experimental import pallas as pl
from jax.experimental.pallas import tpu as pltpu
from jax.sharding import PartitionSpec as P

HD = 64
LEN = 1024
QB = 256

epsilon = 1e-05
theta = 500000.0
MESH_ID = pl.DeviceIdType.MESH
BF16 = jnp.bfloat16
ANY = pl.BlockSpec(memory_space=pl.ANY)
F32 = jnp.float32


def rope_frequencies():
    half_size = HD // 2
    base_freq = theta ** (-(jnp.arange(half_size, dtype=jnp.float32) * 2.0) / HD)
    wavelength = 2.0 * jnp.pi / base_freq
    smooth = (8192.0 / wavelength - 1.0) / 3.0
    middle = (1.0 - smooth) * base_freq / 32.0 + smooth * base_freq
    return jnp.where(
        wavelength < 2048.0, base_freq, jnp.where(wavelength > 8192.0, base_freq / 32.0, middle)
    )


def rope_tables():
    steps = jnp.arange(32, dtype=jnp.float32)[:, None]
    frequency = jnp.concatenate([rope_frequencies()] * 4)[None, :]
    low, high = steps * frequency, (32.0 * steps) * frequency
    cos_low, sin_low = jnp.cos(low)[None, :, :], jnp.sin(low)[None, :, :]
    cos_high, sin_high = jnp.cos(high)[:, None, :], jnp.sin(high)[:, None, :]
    sign = jnp.where(jnp.arange(128) % HD < HD // 2, -1.0, 1.0)
    cosine = cos_high * cos_low - sin_high * sin_low
    sine = (sin_high * cos_low + cos_high * sin_low) * sign
    return cosine.reshape(LEN, 128), sine.reshape(LEN, 128)


def lane_index(shape):
    return lax.broadcasted_iota(jnp.int32, shape, 1)


def swap_halves(value):
    low = lane_index(value.shape) % HD < HD // 2
    return jnp.where(low, pltpu.roll(value, 128 - HD // 2, 1), pltpu.roll(value, HD // 2, 1))


def nt_dot(left, right):
    return lax.dot_general(left, right, (((1,), (1,)), ((), ())), preferred_element_type=F32)


def tn_dot(left, right):
    return lax.dot_general(left, right, (((0,), (0,)), ((), ())), preferred_element_type=F32)


def rope(value, cosine, sine):
    return (value * cosine + swap_halves(value) * sine).astype(BF16)


def rope_back(grads, cosine, sine):
    return (grads * cosine - swap_halves(grads) * sine).astype(BF16)


def project_rows(rows, wq_ref, wk_ref, wv_ref, cosine, sine, q_ref, k_ref, v_ref):
    for block in range(q_ref.shape[1] // 256):
        cols = slice(block * 256, (block + 1) * 256)
        value = jnp.dot(rows, wq_ref[:, cols], preferred_element_type=F32)
        for half in range(2):
            start = block * 256 + half * 128
            q_ref[:, start : start + 128] = rope(
                value[:, half * 128 : half * 128 + 128], cosine, sine
            )
    k_ref[...] = rope(jnp.dot(rows, wk_ref[...], preferred_element_type=F32), cosine, sine)
    v_ref[...] = jnp.dot(rows, wv_ref[...], preferred_element_type=F32).astype(BF16)


def project_kernel(x_ref, wq_ref, wk_ref, wv_ref, cos_ref, sin_ref, q_ref, k_ref, v_ref):
    project_rows(
        x_ref[...], wq_ref, wk_ref, wv_ref, cos_ref[...], sin_ref[...], q_ref, k_ref, v_ref
    )


def project(rows, w_query, w_key, w_value, cosine, sine):
    total, width = rows.shape
    block = 256

    def whole(array):
        return pl.BlockSpec(array.shape, lambda i: (0, 0))

    def by_rows(cols):
        return pl.BlockSpec((block, cols), lambda i: (i, 0))

    shapes = [w_query.shape[1], w_key.shape[1], w_value.shape[1]]
    return pl.pallas_call(
        project_kernel,
        grid=(total // block,),
        out_shape=[jax.ShapeDtypeStruct((total, s), BF16) for s in shapes],
        in_specs=[by_rows(width), whole(w_query), whole(w_key), whole(w_value)]
        + [by_rows(128)] * 2,
        out_specs=[by_rows(s) for s in shapes],
        compiler_params=pltpu.CompilerParams(vmem_limit_bytes=32 << 20),
        cost_estimate=pl.CostEstimate(
            flops=2 * total * width * sum(shapes), bytes_accessed=8 << 20, transcendentals=0
        ),
        name="project",
    )(rows, w_query, w_key, w_value, cosine, sine)


def pick_head(pair, which, kv):
    moved = jnp.where(kv == which, pair, pltpu.roll(pair, HD, 1))
    return jnp.where(lane_index(pair.shape) // HD == kv, moved, jnp.zeros_like(moved))


def join_heads(first, second, kv):
    first = jnp.where(kv == 0, first, pltpu.roll(first, HD, 1))
    second = jnp.where(kv == 1, second, pltpu.roll(second, HD, 1))
    return jnp.where(lane_index(first.shape) < HD, first, second)


def attend_pair(length, kv, q_ref, k_ref, v_ref, o_ref):
    square = (QB, QB)
    causal = lax.broadcasted_iota(jnp.int32, square, 1) <= lax.broadcasted_iota(
        jnp.int32, square, 0
    )
    bias = jnp.where(lane_index((1, LEN)) < length, 0.0, -1e30)
    for block in range(LEN // QB):
        start = block * QB
        here = slice(start, start + QB)
        pair = q_ref[here, :].astype(F32) * HD**-0.5
        outs = []
        for which in range(2):
            query = pick_head(pair, which, kv).astype(BF16)
            near = jnp.where(causal, nt_dot(query, k_ref[here, :]), -1e30) + bias[:, here]
            top = jnp.max(near, axis=1, keepdims=True)
            if start:
                far = nt_dot(query, k_ref[:start, :]) + bias[:, :start]
                top = jnp.maximum(top, jnp.max(far, axis=1, keepdims=True))
                far = jnp.exp(far - top)
            near = jnp.exp(near - top)
            total = jnp.sum(near, axis=1, keepdims=True)
            if start:
                total = total + jnp.sum(far, axis=1, keepdims=True)
            inverse = 1.0 / total
            out = jnp.dot(
                (near * inverse).astype(BF16), v_ref[here, :], preferred_element_type=F32
            )
            if start:
                out = out + jnp.dot(
                    (far * inverse).astype(BF16), v_ref[:start, :], preferred_element_type=F32
                )
            outs.append(out)
        o_ref[here, :] = join_heads(outs[0], outs[1], kv).astype(BF16)


def attend_kernel(length_ref, q_ref, k_ref, v_ref, o_ref):
    attend_pair(length_ref[0], pl.program_id(0) // 2, q_ref, k_ref, v_ref, o_ref)


def attend(queries, keys, values, lengths):
    pairs = queries.shape[1] // 128
    whole = pl.BlockSpec((LEN, 128), lambda i: (0, 0))
    paired = pl.BlockSpec((LEN, 128), lambda i: (0, i))
    return pl.pallas_call(
        attend_kernel,
        grid=(pairs,),
        out_shape=jax.ShapeDtypeStruct(queries.shape, BF16),
        in_specs=[pl.BlockSpec(memory_space=pltpu.SMEM), paired, whole, whole],
        out_specs=paired,
        compiler_params=pltpu.CompilerParams(vmem_limit_bytes=48 << 20),
        cost_estimate=pl.CostEstimate(
            flops=12 << 30, bytes_accessed=4 << 20, transcendentals=8 << 20
        ),
        name="attend",
    )(lengths, queries, keys, values)


def attend_back_pair(
    length, kv, q_ref, k_ref, v_ref, g_ref, cos_ref, sin_ref, gq_ref, acc_k, acc_v
):
    for block in range(LEN // QB):
        rows = slice(block * QB, (block + 1) * QB)
        keys = (block + 1) * QB
        pair = q_ref[rows, :].astype(F32) * HD**-0.5
        grad_pair = g_ref[rows, :].astype(F32)
        key_pos = lax.broadcasted_iota(jnp.int32, (keys, QB), 0)
        query_pos = block * QB + lax.broadcasted_iota(jnp.int32, (keys, QB), 1)
        allowed = (key_pos <= query_pos) & (key_pos < length)
        key_vecs = k_ref[:keys, :]
        grad_queries = []
        for which in range(2):
            query = pick_head(pair, which, kv).astype(BF16)
            grad = pick_head(grad_pair, which, kv).astype(BF16)
            scores = jnp.where(allowed, nt_dot(key_vecs, query), -1e30)
            exps = jnp.exp(scores - jnp.max(scores, axis=0, keepdims=True))
            probs = exps * (1.0 / jnp.sum(exps, axis=0, keepdims=True))
            grad_probs = nt_dot(v_ref[:keys, :], grad)
            inner = jnp.sum(probs * grad_probs, axis=0, keepdims=True)
            grad_scores = (probs * (grad_probs - inner)).astype(BF16)
            acc_v[:keys, :] += jnp.dot(probs.astype(BF16), grad, preferred_element_type=F32)
            acc_k[:keys, :] += jnp.dot(grad_scores, query, preferred_element_type=F32)
            grad_queries.append(tn_dot(grad_scores, key_vecs) * HD**-0.5)
        joined = join_heads(grad_queries[0], grad_queries[1], kv)
        gq_ref[rows, :] = rope_back(joined, cos_ref[rows, :], sin_ref[rows, :])


def attend_back_kernel(
    length_ref, q_ref, k_ref, v_ref, g_ref, cos_ref, sin_ref, gq_ref, gk_ref, gv_ref, acc_k, acc_v
):
    pair_index = pl.program_id(0)

    @pl.when(pair_index == 0)
    def _():
        acc_k[...] = jnp.zeros_like(acc_k)
        acc_v[...] = jnp.zeros_like(acc_v)

    attend_back_pair(
        length_ref[0], pair_index // 2, q_ref, k_ref, v_ref, g_ref, cos_ref, sin_ref, gq_ref,
        acc_k, acc_v,
    )

    @pl.when(pair_index == pl.num_programs(0) - 1)
    def _():
        gk_ref[...] = rope_back(acc_k[...], cos_ref[...], sin_ref[...])
        gv_ref[...] = acc_v[...].astype(BF16)


def attend_back(queries, keys, values, grad_heads, lengths, cosine, sine):
    pairs = queries.shape[1] // 128
    whole = pl.BlockSpec((LEN, 128), lambda i: (0, 0))
    paired = pl.BlockSpec((LEN, 128), lambda i: (0, i))
    narrow = jax.ShapeDtypeStruct((LEN, 128), BF16)
    return pl.pallas_call(
        attend_back_kernel,
        grid=(pairs,),
        out_shape=[jax.ShapeDtypeStruct(queries.shape, BF16), narrow, narrow],
        in_specs=[pl.BlockSpec(memory_space=pltpu.SMEM), paired, whole, whole, paired]
        + [whole] * 2,
        out_specs=[paired, whole, whole],
        scratch_shapes=[pltpu.VMEM((LEN, 128), F32)] * 2,
        compiler_params=pltpu.CompilerParams(vmem_limit_bytes=48 << 20),
        cost_estimate=pl.CostEstimate(
            flops=24 << 30, bytes_accessed=8 << 20, transcendentals=8 << 20
        ),
        name="attend_back",
    )(lengths, queries, keys, values, grad_heads, cosine, sine)


def ring_place(index, count):
    odd = index % 2
    return (1 - odd) * (index // 2) + odd * (count - 1 - index // 2)


def ring_member(place, count):
    high = place // (count // 2)
    return (1 - high) * (2 * place) + high * (2 * (count - 1 - place) + 1)


def ring_setup(count, peers=None):
    place = ring_place(lax.axis_index("dp"), count)
    ahead = ring_member((place + 1) % count, count)
    behind = ring_member((place + count - 1) % count, count)
    barrier = pltpu.get_barrier_semaphore()
    peers = peers or [{"dp": ahead}, {"dp": behind}]
    for other in peers:
        pl.semaphore_signal(barrier, inc=1, device_id=other, device_id_type=MESH_ID)
    pl.semaphore_wait(barrier, len(peers))
    return place, (ahead, behind)


def member_at(place, side, steps, count):
    if side == 0:
        return ring_member((place + count - steps) % count, count)
    return ring_member((place + steps) % count, count)


def piece(ref, shape, axis, member, side, part, parts, first=0):
    rows, cols = shape
    sub = rows // (2 * parts)
    start = (side * parts + part) * sub
    if axis is None:
        return ref.at[pl.ds(start, sub), first : first + cols]
    if axis == 0:
        return ref.at[pl.ds(pl.multiple_of(member * rows + start, sub), sub), :]
    return ref.at[pl.ds(start, sub), pl.ds(pl.multiple_of(member * cols, cols), cols)]


def gather_kernel(count, items, *refs):
    num = len(items)
    shards, outs = refs[:num], refs[num : 2 * num]
    stage = refs[2 * num : 3 * num]
    send_sems, recv_sems, local_sem = refs[3 * num :]
    place, neighbours = ring_setup(count)
    me = lax.axis_index("dp")
    slots = [(k, part) for k in range(num) for part in range(items[k][2])]

    def copy(step, side, slot):
        item, part = slots[slot]
        shape, axis, parts, _ = items[item]
        origin = member_at(place, side, step, count)
        target = piece(outs[item], shape, axis, origin, side, part, parts)
        return target, pltpu.make_async_remote_copy(
            src_ref=target,
            dst_ref=target,
            send_sem=send_sems.at[side, step, slot],
            recv_sem=recv_sems.at[side, step, slot],
            device_id={"dp": neighbours[side]},
            device_id_type=MESH_ID,
        )

    for slot, (item, part) in enumerate(slots):
        shape, axis, parts, first = items[item]
        for side in range(2):
            pltpu.make_async_remote_copy(
                src_ref=piece(shards[item], shape, None, 0, side, part, parts, first),
                dst_ref=piece(outs[item], shape, axis, me, side, part, parts),
                send_sem=send_sems.at[side, 0, slot],
                recv_sem=recv_sems.at[side, 0, slot],
                device_id={"dp": neighbours[side]},
                device_id_type=MESH_ID,
            ).start()
    loads = [
        pltpu.make_async_copy(
            shards[k].at[:, items[k][3] : items[k][3] + items[k][0][1]],
            stage[k],
            local_sem.at[k],
        )
        for k in range(num)
    ]
    for load in loads:
        load.start()
    stores = []
    for k in range(num):
        loads[k].wait()
        shape, axis, parts, _ = items[k]
        rows, cols = shape
        if axis == 0:
            own = outs[k].at[pl.ds(pl.multiple_of(me * rows, rows), rows), :]
        else:
            own = outs[k].at[:, pl.ds(pl.multiple_of(me * cols, cols), cols)]
        stores.append(pltpu.make_async_copy(stage[k], own, local_sem.at[k]))
        stores[-1].start()

    def hop(step, carry):
        for slot in range(len(slots)):
            for side in range(2):
                copy(step - 1, side, slot)[1].wait_recv()
                copy(step, side, slot)[1].start()
        return carry

    lax.fori_loop(1, count - 1, hop, 0)
    for slot in range(len(slots)):
        for side in range(2):
            copy(count - 2, side, slot)[1].wait_recv()
    for store in stores:
        store.wait()

    def drain(step, carry):
        for slot in range(len(slots)):
            for side in range(2):
                copy(step, side, slot)[1].wait_send()
        return carry

    lax.fori_loop(0, count - 1, drain, 0)


def ring_gather(shards, axes, parts, count, collective_id, first=0):
    turned = [a == 1 and s.shape[1] % 128 != 0 for s, a in zip(shards, axes)]
    if any(turned):
        shards = [s.T if t else s for s, t in zip(shards, turned)]
        axes = [0 if t else a for a, t in zip(axes, turned)]
        outs = ring_gather(shards, axes, parts, count, collective_id)
        return [o.T if t else o for o, t in zip(outs, turned)]
    shapes = [(s.shape[0], s.shape[1] - first) for s in shards]
    items = tuple((s, a, q, first) for s, a, q in zip(shapes, axes, parts))
    slots = sum(parts)
    outs = [
        jax.ShapeDtypeStruct((s[0] * count, s[1]) if a == 0 else (s[0], s[1] * count), BF16)
        for s, a in zip(shapes, axes)
    ]
    num = len(shards)
    nbytes = sum(s.size * 2 * (count - 1) for s in shards)
    return pl.pallas_call(
        functools.partial(gather_kernel, count, items),
        out_shape=outs,
        in_specs=[pl.BlockSpec(memory_space=pl.ANY)] * num,
        out_specs=[pl.BlockSpec(memory_space=pl.ANY)] * num,
        scratch_shapes=[pltpu.VMEM(s, BF16) for s in shapes]
        + [
            pltpu.SemaphoreType.DMA((2, count - 1, slots)),
            pltpu.SemaphoreType.DMA((2, count - 1, slots)),
            pltpu.SemaphoreType.DMA((num,)),
        ],
        compiler_params=pltpu.CompilerParams(collective_id=collective_id, has_side_effects=True),
        cost_estimate=pl.CostEstimate(flops=0, bytes_accessed=20 * nbytes, transcendentals=0),
        name=f"ring_gather_{collective_id}",
    )(*shards)


def scatter_kernel(count, items, *refs):
    num = len(items)
    partials, outs = refs[:num], refs[num : 2 * num]
    own = refs[2 * num : 3 * num]
    held = refs[3 * num : 4 * num]
    total = refs[4 * num : 5 * num]
    send_sems, recv_sems, load_sems, store_sems = refs[5 * num :]
    slots = [(k, part) for k in range(num) for part in range(items[k][2])]

    def load(step, side, slot, place):
        item, part = slots[slot]
        shape, axis, parts = items[item]
        member = member_at(place, side, step + 1, count)
        return pltpu.make_async_copy(
            piece(partials[item], shape, axis, member, side, part, parts),
            own[item].at[side, step, part],
            load_sems.at[side, step, slot],
        )

    start_place = ring_place(lax.axis_index("dp"), count)

    def load_all(step, carry):
        for slot in range(len(slots)):
            for side in range(2):
                load(step, side, slot, start_place).start()
        return carry

    lax.fori_loop(0, count, load_all, 0)
    place, neighbours = ring_setup(count)

    def send(step, side, slot, source):
        item, part = slots[slot]
        return pltpu.make_async_remote_copy(
            src_ref=source,
            dst_ref=held[item].at[side, step, part],
            send_sem=send_sems.at[side, step, slot],
            recv_sem=recv_sems.at[side, step, slot],
            device_id={"dp": neighbours[side]},
            device_id_type=MESH_ID,
        )

    for slot, (item, part) in enumerate(slots):
        for side in range(2):
            load(0, side, slot, place).wait()
            send(0, side, slot, own[item].at[side, 0, part]).start()

    def hop(step, carry):
        for slot, (item, part) in enumerate(slots):
            for side in range(2):
                load(step, side, slot, place).wait()
                arrived = held[item].at[side, step - 1, part]
                send(step - 1, side, slot, arrived).wait_recv()
                arrived[...] = (
                    arrived[...].astype(jnp.float32)
                    + own[item][side, step, part].astype(jnp.float32)
                ).astype(jnp.bfloat16)
                send(step, side, slot, arrived).start()
        return carry

    lax.fori_loop(1, count - 1, hop, 0)
    last = count - 1
    stores = []
    for slot, (item, part) in enumerate(slots):
        shape, axis, parts = items[item]
        for side in range(2):
            load(last, side, slot, place).wait()
            arrived = held[item].at[side, last - 1, part]
            send(last - 1, side, slot, arrived).wait_recv()
            total[item][side, part] = arrived[...].astype(jnp.float32) + own[item][
                side, last, part
            ].astype(jnp.float32)
            stores.append(
                pltpu.make_async_copy(
                    total[item].at[side, part],
                    piece(outs[item], shape, None, 0, side, part, parts),
                    store_sems.at[side, slot],
                )
            )
            stores[-1].start()
    for store in stores:
        store.wait()

    def drain(step, carry):
        for slot, (item, part) in enumerate(slots):
            for side in range(2):
                send(step, side, slot, held[item].at[side, 0, part]).wait_send()
        return carry

    lax.fori_loop(0, count - 1, drain, 0)


def ring_scatter(partials, axes, parts, count, collective_id):
    turned = [a == 1 and p.shape[1] // count % 128 != 0 for p, a in zip(partials, axes)]
    if any(turned):
        partials = [p.T if t else p for p, t in zip(partials, turned)]
        axes = [0 if t else a for a, t in zip(axes, turned)]
        outs = ring_scatter(partials, axes, parts, count, collective_id)
        return [o.T if t else o for o, t in zip(outs, turned)]
    shapes = [
        (p.shape[0] // count, p.shape[1]) if a == 0 else (p.shape[0], p.shape[1] // count)
        for p, a in zip(partials, axes)
    ]
    items = tuple((s, a, q) for s, a, q in zip(shapes, axes, parts))
    slots = sum(parts)
    num = len(partials)

    def buffers(depth, dtype):
        return [
            pltpu.VMEM((2,) + depth + (q, s[0] // (2 * q), s[1]), dtype)
            for s, q in zip(shapes, parts)
        ]

    nbytes = sum(p.size * 2 for p in partials)
    return pl.pallas_call(
        functools.partial(scatter_kernel, count, items),
        out_shape=[jax.ShapeDtypeStruct(s, jnp.float32) for s in shapes],
        in_specs=[pl.BlockSpec(memory_space=pl.ANY)] * num,
        out_specs=[pl.BlockSpec(memory_space=pl.ANY)] * num,
        scratch_shapes=buffers((count,), jnp.bfloat16)
        + buffers((count - 1,), jnp.bfloat16)
        + buffers((), jnp.float32)
        + [
            pltpu.SemaphoreType.DMA((2, count - 1, slots)),
            pltpu.SemaphoreType.DMA((2, count - 1, slots)),
            pltpu.SemaphoreType.DMA((2, count, slots)),
            pltpu.SemaphoreType.DMA((2, slots)),
        ],
        compiler_params=pltpu.CompilerParams(
            collective_id=collective_id, has_side_effects=True, vmem_limit_bytes=48 << 20
        ),
        cost_estimate=pl.CostEstimate(flops=0, bytes_accessed=20 * nbytes, transcendentals=0),
        name=f"ring_scatter_{collective_id}",
    )(*partials)


class Job(NamedTuple):
    left: Any
    right: Any
    start: int
    cols: int
    into: Any = None
    target: int = 0
    split: bool = False


class Extra(NamedTuple):
    builder: Any
    given: list
    given_specs: list
    made: list
    made_specs: list
    spare: list


def scatter_dot_kernel(count, items, num_outs, num_bases, parts, extra, *refs):
    num = len(items)
    taken = 0

    def take(amount):
        nonlocal taken
        taken += amount
        return refs[taken - amount : taken]

    lefts, rights, _ = take(num), take(num), take(num_bases)
    given = take(len(extra.given) if extra else 0)
    outs = take(num_outs)
    made = take(len(extra.made) if extra else 0)
    left_bufs, right_bufs, firsts, owns, helds, totals = (take(num) for _ in range(6))
    send_sems, recv_sems, left_sems, right_sems, store_sems = take(5)
    beside = extra.builder(count, given, made, refs[taken:], right_bufs) if extra else None
    entry_place = ring_place(lax.axis_index("dp"), count)
    last = count - 1

    def load_right(item):
        _, half, start, _ = items[item]
        return pltpu.make_async_copy(
            rights[item].at[:, start : start + 2 * half], right_bufs[item], right_sems.at[item]
        )

    def load_left(step, side, item, place):
        block = items[item][0]
        member = member_at(place, side, step + 1, count)
        slot = step % 2
        return pltpu.make_async_copy(
            lefts[item].at[:, pl.ds(pl.multiple_of(member * block, block), block)],
            left_bufs[item].at[side, slot],
            left_sems.at[side, slot, item],
        )

    for item in range(num):
        load_right(item).start()
        for side in range(2):
            load_left(0, side, item, entry_place).start()
    if beside:
        beside.begin()
    place, neighbours = ring_setup(count, beside.peers() if beside else None)
    pairs = [(item, side) for item in range(num) for side in range(2)]

    def send(step, side, item, part, source):
        return pltpu.make_async_remote_copy(
            src_ref=source.at[part],
            dst_ref=helds[item].at[side, step, part],
            send_sem=send_sems.at[side, step, item * parts + part],
            recv_sem=recv_sems.at[side, step, item * parts + part],
            device_id={"dp": neighbours[side]},
            device_id_type=MESH_ID,
        )

    def store(item, side, part):
        block, half, _, places = items[item]
        out, column = places[side]
        rows = block // parts
        return pltpu.make_async_copy(
            totals[item].at[side, part],
            outs[out].at[part * rows : (part + 1) * rows, column : column + half],
            store_sems.at[side, item * parts + part],
        )

    for item in range(num):
        load_right(item).wait()

    def turn(step, carry):
        @pl.when(step < last)
        def _():
            for item, side in pairs:
                load_left(step + 1, side, item, place).start()

        for item in range(num):
            half = items[item][1]
            for side in range(2):
                load_left(step, side, item, place).wait()

            def own_sum(side, inner):
                cols = pl.ds(pl.multiple_of(side * half, half), half)
                owns[item][side] = tn_dot(
                    left_bufs[item][side, step % 2], right_bufs[item][:, cols]
                ).reshape(owns[item].shape[1:])
                return inner

            lax.fori_loop(0, 2, own_sum, 0)

        @pl.when(step == 0)
        def _():
            for part in range(parts):
                for item, side in pairs:
                    firsts[item][side, part] = owns[item][side, part].astype(BF16)
                    send(0, side, item, part, firsts[item].at[side]).start()

        if beside:
            beside.compute(step)

        @pl.when((step > 0) & (step < last))
        def _():
            for part in range(parts):
                for item, side in pairs:
                    arrived = helds[item].at[side, step - 1]
                    send(step - 1, side, item, part, arrived).wait_recv()
                    arrived[part] = (
                        arrived[part].astype(F32) + owns[item][side, part]
                    ).astype(BF16)
                    send(step, side, item, part, arrived).start()

        return carry

    lax.fori_loop(0, count, turn, 0)
    for part in range(parts):
        for item, side in pairs:
            arrived = helds[item].at[side, last - 1]
            send(last - 1, side, item, part, arrived).wait_recv()
            totals[item][side, part] = arrived[part].astype(F32) + owns[item][side, part]
            store(item, side, part).start()
    if beside:
        beside.finish()
    for part in range(parts):
        for item, side in pairs:
            store(item, side, part).wait()

    def drain(step, carry):
        for part in range(parts):
            for item, side in pairs:
                send(step, side, item, part, helds[item].at[side, 0]).wait_send()
        return carry

    lax.fori_loop(0, last, drain, 0)


def ring_scatter_dots(jobs, parts, count, collective_id, extra=None):
    rows = jobs[0].left.shape[0]
    items, shapes, bases, aliases = [], [], [], {}
    for job in jobs:
        block, half = job.left.shape[1] // count, job.cols // 2
        if job.split:
            places = ((len(shapes), 0), (len(shapes) + 1, 0))
            shapes += [(block, half)] * 2
        else:
            places = ((len(shapes), job.target), (len(shapes), job.target + half))
            if job.into is None:
                shapes.append((block, job.cols))
            elif isinstance(job.into, int):
                shapes.append((block, job.into))
            else:
                aliases[2 * len(jobs) + len(bases)] = len(shapes)
                bases.append(job.into)
                shapes.append(job.into.shape)
        items.append((block, half, job.start, places))
    num = len(jobs)

    def buffers(depth, dtype):
        return [pltpu.VMEM(depth + (parts, b // parts, h), dtype) for b, h, _, _ in items]

    slots = num * parts
    flops = sum(2 * rows * j.left.shape[1] * j.cols for j in jobs)
    nbytes = sum(2 * j.left.shape[1] * j.cols for j in jobs)
    given, given_specs, made, made_specs, spare = extra[1:] if extra else ([], [], [], [], [])
    return pl.pallas_call(
        functools.partial(
            scatter_dot_kernel, count, items, len(shapes), len(bases), parts, extra
        ),
        out_shape=[jax.ShapeDtypeStruct(s, F32) for s in shapes] + made,
        in_specs=[ANY] * (2 * num + len(bases)) + given_specs,
        out_specs=[ANY] * len(shapes) + made_specs,
        input_output_aliases=aliases,
        scratch_shapes=[pltpu.VMEM((2, 2, rows, i[0]), BF16) for i in items]
        + [pltpu.VMEM((rows, 2 * i[1]), BF16) for i in items]
        + buffers((2,), BF16)
        + buffers((2,), F32)
        + buffers((2, count - 1), BF16)
        + buffers((2,), F32)
        + [
            pltpu.SemaphoreType.DMA((2, count - 1, slots)),
            pltpu.SemaphoreType.DMA((2, count - 1, slots)),
            pltpu.SemaphoreType.DMA((2, 2, num)),
            pltpu.SemaphoreType.DMA((num,)),
            pltpu.SemaphoreType.DMA((2, slots)),
        ]
        + spare,
        compiler_params=pltpu.CompilerParams(
            collective_id=collective_id, has_side_effects=True, vmem_limit_bytes=60 << 20
        ),
        cost_estimate=pl.CostEstimate(
            flops=flops, bytes_accessed=20 * nbytes, transcendentals=0
        ),
        name=f"ring_scatter_{collective_id}",
    )(*[j.left for j in jobs], *[j.right for j in jobs], *bases, *given)


class ShareWork:
    def __init__(self, count, given, made, spare, rights):
        self.given, self.out = given, made[0]
        self.pair, self.first, self.sums, self.second, self.sems = spare
        self.count, self.group = count, self.second.shape[0] + 1
        self.row, self.col = lax.axis_index("dp"), lax.axis_index("tensor")

    def in_column(self, shift):
        return {"dp": (self.row + shift) % self.count}

    def in_group(self, shift):
        return {"tensor": (self.col + shift) % self.group}

    def peers(self):
        return [self.in_column(s) for s in range(1, self.count)] + [
            self.in_group(s) for s in range(1, self.group)
        ]

    def begin(self):
        pass

    def part(self, row):
        width = self.sums.shape[1]
        return pl.ds(pl.multiple_of(row * width, width), width)

    def move(self, stage, shift):
        if stage == 0:
            source = self.pair.at[:, self.part((self.row + shift) % self.count)]
            target, device, slot = self.first.at[shift - 1], self.in_column(shift), shift - 1
        else:
            source, target = self.sums, self.second.at[shift - 1]
            device, slot = self.in_group(shift), self.count + shift - 2
        return pltpu.make_async_remote_copy(
            src_ref=source,
            dst_ref=target,
            send_sem=self.sems.at[0, slot],
            recv_sem=self.sems.at[1, slot],
            device_id=device,
            device_id_type=MESH_ID,
        )

    def compute(self, step):
        @pl.when(step == 0)
        def _():
            self.pair[...] = self.given[0][...]
            self.pair[1:2, :] = self.given[1][...]
            for shift in range(1, self.count):
                self.move(0, shift).start()

        @pl.when(step == 2)
        def _():
            total = self.pair[:, self.part(self.row)]
            for shift in range(1, self.count):
                self.move(0, shift).wait()
                total = total + self.first[shift - 1]
            self.sums[...] = total
            for shift in range(1, self.group):
                self.move(1, shift).start()

    def finish(self):
        total = self.sums[...]
        for shift in range(1, self.group):
            self.move(1, shift).wait()
            total = total + self.second[shift - 1]
        share = total.shape[1] // self.group
        picked = jnp.zeros((8, share), F32)
        for col in range(self.group):
            picked = jnp.where(self.col == col, total[:, col * share : (col + 1) * share], picked)
        self.out[:, :share] = picked


def share_work(first, second, count, group):
    width = first.shape[1] // count
    vmem = pl.BlockSpec(memory_space=pltpu.VMEM)
    return Extra(
        ShareWork,
        [first, second],
        [vmem] * 2,
        [jax.ShapeDtypeStruct((8, 128), F32)],
        [vmem],
        [
            pltpu.VMEM(first.shape, F32),
            pltpu.VMEM((count - 1, 8, width), F32),
            pltpu.VMEM((8, width), F32),
            pltpu.VMEM((group - 1, 8, width), F32),
            pltpu.SemaphoreType.DMA((2, count + group - 2)),
        ],
    )


class NormWork:
    def __init__(self, count, given, made, spare, rights):
        self.grads, self.gates = given[:2], tuple(given[2:4])
        self.up, self.down = given[4:]
        self.outs = made
        self.grad_bufs, self.row_bufs, self.down_bufs, self.stage = spare[0], *spare[1:4]
        self.grad_sems, self.row_sems, self.down_sems, self.out_sems = spare[4:]
        self.act = rights[0]
        self.count = count
        self.block = self.row_bufs.shape[2]

    def load_grad(self, which):
        return pltpu.make_async_copy(
            self.grads[which], self.grad_bufs.at[which], self.grad_sems.at[which]
        )

    def spot(self, step):
        return pl.ds(pl.multiple_of(step * self.block, self.block), self.block)

    def loads(self, step):
        slot = step % 2
        edge = self.gates[0].shape[1]
        gate = self.row_bufs.at[0, slot]
        targets = [gate.at[:, :edge], gate.at[:, edge:], self.row_bufs.at[1, slot]]
        rows = [
            pltpu.make_async_copy(
                source.at[self.spot(step), :], target, self.row_sems.at[which, slot]
            )
            for which, (source, target) in enumerate(zip(self.gates + (self.up,), targets))
        ]
        down = pltpu.make_async_copy(
            self.down.at[:, self.spot(step)], self.down_bufs.at[slot], self.down_sems.at[slot]
        )
        return rows + [down]

    def store(self, which, step):
        slot = step % 2
        return pltpu.make_async_copy(
            self.stage.at[which, slot],
            self.outs[which].at[:, self.spot(step)],
            self.out_sems.at[which, slot],
        )

    def begin(self):
        for which in range(2):
            self.load_grad(which).start()
        for copy in self.loads(0):
            copy.start()

    def peers(self):
        return None

    def compute(self, step):
        @pl.when(step < self.count - 1)
        def _():
            for copy in self.loads(step + 1):
                copy.start()

        @pl.when(step == 0)
        def _():
            for which in range(2):
                self.load_grad(which).wait()

        @pl.when(step >= 2)
        def _():
            for which in range(2):
                self.store(which, step - 2).wait()

        for copy in self.loads(step):
            copy.wait()
        slot = step % 2

        def lines(index, carry):
            band = pl.ds(pl.multiple_of(index * 256, 256), 256)
            norm = nt_dot(self.grad_bufs[0, band, :], self.row_bufs[0, slot])
            norm += nt_dot(self.grad_bufs[1, band, :], self.row_bufs[1, slot])
            self.stage[0, slot, band, :] = norm.astype(BF16)
            value = jnp.dot(
                self.act[band, :], self.down_bufs[slot], preferred_element_type=F32
            )
            self.stage[1, slot, band, :] = value.astype(BF16)
            return carry

        lax.fori_loop(0, self.act.shape[0] // 256, lines, 0)
        for which in range(2):
            self.store(which, step).start()

    def finish(self):
        for step in range(max(self.count - 2, 0), self.count):
            for which in range(2):
                self.store(which, step).wait()


def down_ring(grad_branch, activated, grad_gate, grad_up, gates, up_all, down_all, count, cid):
    rows, hidden = activated.shape
    width = up_all.shape[0]
    block = width // count
    wide = jax.ShapeDtypeStruct((rows, width), BF16)
    spare = [
        pltpu.VMEM((2, rows, hidden), BF16),
        pltpu.VMEM((2, 2, block, hidden), BF16),
        pltpu.VMEM((2, hidden, block), BF16),
        pltpu.VMEM((2, 2, rows, block), BF16),
        pltpu.SemaphoreType.DMA((2,)),
        pltpu.SemaphoreType.DMA((3, 2)),
        pltpu.SemaphoreType.DMA((2,)),
        pltpu.SemaphoreType.DMA((2, 2)),
    ]
    given = [grad_gate, grad_up, *gates, up_all, down_all]
    return ring_scatter_dots(
        [Job(grad_branch, activated, 0, hidden)],
        2,
        count,
        cid,
        Extra(NormWork, given, [ANY] * 6, [wide, wide], [ANY] * 2, spare),
    )


def mlp_kernel(count, *refs):
    x_hbm, wg_hbm, wg_rest, wu_hbm, shard, gb_hbm = refs[:6]
    act_hbm, gg_hbm, gu_hbm, down_all = refs[6:10]
    x_buf, gb_buf, w_bufs, gate_slope, up_slope, acc, half_bufs, stage, own_stage = refs[10:19]
    send_sems, recv_sems, w_sems, in_sems, half_sems, out_sems, local_sem = refs[19:]
    rows, width = x_buf.shape
    hidden = acc.shape[1]
    block = width // count
    cols = w_bufs.shape[-1]
    steps = hidden // cols
    half = hidden // 2
    parts = send_sems.shape[2]
    me = lax.axis_index("dp")

    gate_steps = wg_hbm.shape[1] // cols

    def load_weights(step, which, source=None):
        start = step - gate_steps if source is wg_rest else step
        source = (wg_hbm, wu_hbm)[which] if source is None else source
        return pltpu.make_async_copy(
            source.at[:, pl.ds(pl.multiple_of(start * cols, cols), cols)],
            w_bufs.at[which, step % 2],
            w_sems.at[which, step % 2],
        )

    def fetch(step):
        load_weights(step, 1).start()

        @pl.when(step < gate_steps)
        def _():
            load_weights(step, 0).start()

        @pl.when(step >= gate_steps)
        def _():
            load_weights(step, 0, wg_rest).start()

    load_x = pltpu.make_async_copy(x_hbm, x_buf, in_sems.at[0])
    load_gb = pltpu.make_async_copy(gb_hbm, gb_buf, in_sems.at[1])
    load_own = pltpu.make_async_copy(shard, own_stage, local_sem)
    load_x.start()
    for which in range(2):
        load_weights(0, which).start()
    load_own.start()
    load_gb.start()
    place, neighbours = ring_setup(count)

    def target(ref, member, side, part):
        return piece(ref, (hidden, block), 1, member, side, part, parts)

    def hop(step, side, part):
        ref = target(down_all, member_at(place, side, step, count), side, part)
        return pltpu.make_async_remote_copy(
            src_ref=ref,
            dst_ref=ref,
            send_sem=send_sems.at[side, step, part],
            recv_sem=recv_sems.at[side, step, part],
            device_id={"dp": neighbours[side]},
            device_id_type=MESH_ID,
        )

    for part in range(parts):
        for side in range(2):
            pltpu.make_async_remote_copy(
                src_ref=piece(shard, (hidden, block), None, 0, side, part, parts),
                dst_ref=target(down_all, me, side, part),
                send_sem=send_sems.at[side, 0, part],
                recv_sem=recv_sems.at[side, 0, part],
                device_id={"dp": neighbours[side]},
                device_id_type=MESH_ID,
            ).start()

    def pump(step):
        for part in range(parts):
            for side in range(2):
                hop(step - 1, side, part).wait_recv()
                hop(step, side, part).start()

    load_own.wait()
    store_own = pltpu.make_async_copy(
        own_stage, down_all.at[:, pl.ds(pl.multiple_of(me * block, block), block)], local_sem
    )
    store_own.start()
    load_x.wait()

    def store(ref, which, step):
        return pltpu.make_async_copy(
            stage.at[which, step % 2],
            ref.at[:, pl.ds(pl.multiple_of(step * cols, cols), cols)],
            out_sems.at[which, step % 2],
        )

    def forward(step, carry):
        @pl.when(step + 1 < steps)
        def _():
            fetch(step + 1)

        @pl.when(step >= 2)
        def _():
            store(act_hbm, 0, step - 2).wait()

        load_weights(step, 1).wait()

        @pl.when(step < gate_steps)
        def _():
            load_weights(step, 0).wait()

        @pl.when(step >= gate_steps)
        def _():
            load_weights(step, 0, wg_rest).wait()

        here = pl.ds(pl.multiple_of(step * cols, cols), cols)
        for top in range(0, rows, 256):
            band = pl.ds(top, 256)
            lines = x_buf[band, :]
            gate = jnp.dot(lines, w_bufs[0, step % 2], preferred_element_type=F32)
            up = jnp.dot(lines, w_bufs[1, step % 2], preferred_element_type=F32)
            sig = jax.nn.sigmoid(gate)
            silu = gate * sig
            stage[0, step % 2, band, :] = (silu * up).astype(BF16)
            gate_slope[band, here] = up * sig * (1.0 + gate * (1.0 - sig))
            up_slope[band, here] = silu
            acc[band, here] = jnp.zeros((256, cols), F32)
        store(act_hbm, 0, step).start()

        turn = (step + 1) // 2

        @pl.when((step % 2 == 1) & (turn <= count - 2))
        def _():
            pump(turn)

        return carry

    lax.fori_loop(0, steps, forward, 0)
    for step in range(max(steps - 2, 0), steps):
        store(act_hbm, 0, step).wait()
    pumped = min(steps // 2, count - 2)
    load_gb.wait()

    def load_half(step, side):
        member = member_at(place, side, step, count)
        return pltpu.make_async_copy(
            down_all.at[
                pl.ds(side * half, half), pl.ds(pl.multiple_of(member * block, block), block)
            ],
            half_bufs.at[side],
            half_sems.at[side],
        )

    def backward(step, carry):
        @pl.when((step > pumped) & (step <= count - 2))
        def _():
            pump(step)

        @pl.when(step == count - 1)
        def _():
            for part in range(parts):
                for side in range(2):
                    hop(count - 2, side, part).wait_recv()

        for side in range(2):
            load_half(step, side).start()
        for side in range(2):
            member = member_at(place, side, step, count)
            load_half(step, side).wait()
            here = pl.ds(pl.multiple_of(member * block, block), block)
            spot = pl.ds(side * half, half)

            def lines(index, carry):
                band = pl.ds(pl.multiple_of(index * 256, 256), 256)
                acc[band, spot] += nt_dot(gb_buf[band, here], half_bufs[side])
                return carry

            lax.fori_loop(0, rows // 256, lines, 0)

        return carry

    store_own.wait()
    lax.fori_loop(0, count, backward, 0)

    def slopes(step, carry):
        @pl.when(step >= 2)
        def _():
            store(gg_hbm, 1, step - 2).wait()
            store(gu_hbm, 2, step - 2).wait()

        here = pl.ds(pl.multiple_of(step * cols, cols), cols)

        def lines(index, carry):
            band = pl.ds(pl.multiple_of(index * 256, 256), 256)
            value = acc[band, here]
            stage[1, step % 2, band, :] = (value * gate_slope[band, here]).astype(BF16)
            stage[2, step % 2, band, :] = (value * up_slope[band, here]).astype(BF16)
            return carry

        lax.fori_loop(0, rows // 256, lines, 0)
        store(gg_hbm, 1, step).start()
        store(gu_hbm, 2, step).start()
        return carry

    lax.fori_loop(0, steps, slopes, 0)
    for step in range(max(steps - 2, 0), steps):
        store(gg_hbm, 1, step).wait()
        store(gu_hbm, 2, step).wait()

    def drain(step, carry):
        for part in range(parts):
            for side in range(2):
                hop(step, side, part).wait_send()
        return carry

    lax.fori_loop(0, count - 1, drain, 0)


def mlp_ring(rows_mlp, gates, up_all, w_down, grad_branch, count, collective_id):
    rows, width = rows_mlp.shape
    hidden, block = w_down.shape
    cols, parts = 256, 2
    wide = jax.ShapeDtypeStruct((rows, hidden), BF16)
    return pl.pallas_call(
        functools.partial(mlp_kernel, count),
        out_shape=[wide] * 3 + [jax.ShapeDtypeStruct((hidden, width), BF16)],
        in_specs=[ANY] * 6,
        out_specs=[pl.BlockSpec(memory_space=pl.ANY)] * 4,
        scratch_shapes=[
            pltpu.VMEM((rows, width), BF16),
            pltpu.VMEM((rows, width), BF16),
            pltpu.VMEM((2, 2, width, cols), BF16),
            pltpu.VMEM((rows, hidden), F32),
            pltpu.VMEM((rows, hidden), F32),
            pltpu.VMEM((rows, hidden), F32),
            pltpu.VMEM((2, hidden // 2, block), BF16),
            pltpu.VMEM((3, 2, rows, cols), BF16),
            pltpu.VMEM((hidden, block), BF16),
            pltpu.SemaphoreType.DMA((2, count - 1, parts)),
            pltpu.SemaphoreType.DMA((2, count - 1, parts)),
            pltpu.SemaphoreType.DMA((2, 2)),
            pltpu.SemaphoreType.DMA((2,)),
            pltpu.SemaphoreType.DMA((2,)),
            pltpu.SemaphoreType.DMA((3, 2)),
            pltpu.SemaphoreType.DMA,
        ],
        compiler_params=pltpu.CompilerParams(
            collective_id=collective_id, has_side_effects=True, vmem_limit_bytes=60 << 20
        ),
        cost_estimate=pl.CostEstimate(
            flops=6 * rows * width * hidden,
            bytes_accessed=40 * hidden * width,
            transcendentals=rows * hidden,
        ),
        name="mlp_ring",
    )(rows_mlp, *gates, up_all, w_down, grad_branch)


class HeadWork:
    def __init__(self, count, given, made, spare, rights):
        self.length, self.gain, self.sources = given[0], given[1], given[2:]
        self.grads_out, self.token_out, self.gain_out = made
        num = len(self.sources)
        self.bufs = spare[:num]
        self.heads, self.grads, self.acc_k, self.acc_v, self.stage = spare[num : num + 5]
        self.in_sems, self.out_sems = spare[num + 5 :]

    def peers(self):
        return None

    def load(self, which):
        return pltpu.make_async_copy(
            self.sources[which], self.bufs[which], self.in_sems.at[which]
        )

    def begin(self):
        for which in range(len(self.sources)):
            self.load(which).start()
        self.gain_out[...] = jnp.zeros_like(self.gain_out)
        self.acc_k[...] = jnp.zeros_like(self.acc_k)
        self.acc_v[...] = jnp.zeros_like(self.acc_v)

    def store(self, band):
        rows = self.stage.shape[1]
        return pltpu.make_async_copy(
            self.stage.at[band % 2],
            self.token_out.at[pl.ds(pl.multiple_of(band * rows, rows), rows), :],
            self.out_sems.at[band % 2],
        )

    def store_grads(self):
        return pltpu.make_async_copy(self.grads, self.grads_out, self.out_sems.at[2])

    def tokens(self, band):
        w_query, w_key, w_value, normed = self.bufs[7:]
        rows = self.stage.shape[1]
        inner = w_query.shape[1]

        @pl.when(band >= 2)
        def _():
            self.store(band - 2).wait()

        lines = pl.ds(pl.multiple_of(band * rows, rows), rows)

        def columns(index, carry):
            cols = pl.ds(pl.multiple_of(index * 512, 512), 512)
            value = nt_dot(self.grads[lines, :inner], w_query[cols, :])
            value += nt_dot(self.grads[lines, inner : inner + 128], w_key[cols, :])
            value += nt_dot(self.grads[lines, inner + 128 :], w_value[cols, :])
            self.stage[band % 2, :, cols] = value.astype(BF16)
            scaled = value * normed[lines, cols].astype(F32)
            self.gain_out[0:1, cols] += jnp.sum(scaled, axis=0, keepdims=True)
            return carry

        lax.fori_loop(0, w_query.shape[0] // 512, columns, 0)
        self.store(band).start()

    def compute(self, step):
        grad_attn, w_output, queries, keys, values, cosine, sine = self.bufs[:7]
        inner = queries.shape[1]
        pairs = inner // 128

        @pl.when(step == 0)
        def _():
            for which in range(len(self.sources)):
                self.load(which).wait()

            def band(index, carry):
                rows = pl.ds(pl.multiple_of(index * 256, 256), 256)
                self.heads[rows, :] = nt_dot(grad_attn[rows, :], w_output[...]).astype(BF16)
                return carry

            lax.fori_loop(0, LEN // 256, band, 0)

        @pl.when((step >= 1) & (step <= pairs))
        def _():
            here = pl.ds(pl.multiple_of((step - 1) * 128, 128), 128)
            attend_back_pair(
                self.length[0], (step - 1) // 2, queries.at[:, here], keys, values,
                self.heads.at[:, here], cosine, sine, self.grads.at[:, here],
                self.acc_k, self.acc_v,
            )

        @pl.when(step == pairs)
        def _():
            self.grads[:, inner : inner + 128] = rope_back(
                self.acc_k[...], cosine[...], sine[...]
            )
            self.grads[:, inner + 128 :] = self.acc_v[...].astype(BF16)
            self.store_grads().start()

        @pl.when((step > pairs) & (step <= pairs + 2))
        def _():
            def band(index, carry):
                self.tokens(2 * (step - pairs - 1) + index)
                return carry

            lax.fori_loop(0, 2, band, 0)

    def finish(self):
        self.gain_out[0:1, :] = self.gain_out[0:1, :] / self.gain[...]
        self.store_grads().wait()
        for band in (2, 3):
            self.store(band).wait()


def heads_ring(
    job, lengths, gain, grad_attn, w_output, qkv, tables, weights, rows_attn, count, cid
):
    sources = [grad_attn, w_output, *qkv, *tables, *weights, rows_attn]
    rows, width = grad_attn.shape
    inner = qkv[0].shape[1]
    made = [
        jax.ShapeDtypeStruct((rows, inner + 256), BF16),
        jax.ShapeDtypeStruct((rows, width), BF16),
        jax.ShapeDtypeStruct((8, width), F32),
    ]
    spare = [pltpu.VMEM(g.shape, g.dtype) for g in sources] + [
        pltpu.VMEM((rows, inner), BF16),
        pltpu.VMEM((rows, inner + 256), BF16),
        pltpu.VMEM((rows, 128), F32),
        pltpu.VMEM((rows, 128), F32),
        pltpu.VMEM((2, rows // 4, width), BF16),
        pltpu.SemaphoreType.DMA((len(sources),)),
        pltpu.SemaphoreType.DMA((3,)),
    ]
    vmem = pl.BlockSpec(memory_space=pltpu.VMEM)
    specs = [pl.BlockSpec(memory_space=pltpu.SMEM), vmem] + [ANY] * len(sources)
    return ring_scatter_dots(
        [job],
        2,
        count,
        cid,
        Extra(HeadWork, [lengths, gain] + sources, specs, made, [ANY, ANY, vmem], spare),
    )


def attend_ring_kernel(count, *refs):
    length_ref, shard, sources = refs[0], refs[1], refs[2:9]
    gathered, q_out, k_out, v_out, head_out, part_out = refs[9:15]
    bufs = refs[15:22]
    q_buf, k_buf, v_buf, head_buf, stage, own = refs[22:28]
    send_sems, recv_sems, in_sems, out_sems, local_sem = refs[28:]
    rows_buf, w_query, w_key, w_value, w_output, cosine, sine = bufs
    shape = own.shape
    me = lax.axis_index("dp")
    loads = [
        pltpu.make_async_copy(source, buf, in_sems.at[k])
        for k, (source, buf) in enumerate(zip(sources, bufs))
    ]
    for load in loads:
        load.start()
    load_own = pltpu.make_async_copy(shard.at[:, : shape[1]], own, local_sem)
    load_own.start()
    place, neighbours = ring_setup(count)

    def hop(step, side):
        ref = piece(gathered, shape, 0, member_at(place, side, step, count), side, 0, 1)
        return pltpu.make_async_remote_copy(
            src_ref=ref,
            dst_ref=ref,
            send_sem=send_sems.at[side, step],
            recv_sem=recv_sems.at[side, step],
            device_id={"dp": neighbours[side]},
            device_id_type=MESH_ID,
        )

    for side in range(2):
        pltpu.make_async_remote_copy(
            src_ref=piece(shard, shape, None, 0, side, 0, 1),
            dst_ref=piece(gathered, shape, 0, me, side, 0, 1),
            send_sem=send_sems.at[side, 0],
            recv_sem=recv_sems.at[side, 0],
            device_id={"dp": neighbours[side]},
            device_id_type=MESH_ID,
        ).start()

    def pump(step, carry=0):
        for side in range(2):
            hop(step - 1, side).wait_recv()
            hop(step, side).start()
        return carry

    load_own.wait()
    store_own = pltpu.make_async_copy(
        own, gathered.at[pl.ds(pl.multiple_of(me * shape[0], shape[0]), shape[0]), :], local_sem
    )
    store_own.start()
    for load in loads:
        load.wait()

    def projection(band, carry):
        lines = pl.ds(pl.multiple_of(band * 256, 256), 256)
        project_rows(
            rows_buf[lines, :], w_query, w_key, w_value, cosine[lines, :], sine[lines, :],
            q_buf.at[lines, :], k_buf.at[lines, :], v_buf.at[lines, :],
        )
        return carry

    lax.fori_loop(0, LEN // 256, projection, 0)
    stores = [
        pltpu.make_async_copy(buf, out, out_sems.at[k])
        for k, (buf, out) in enumerate(
            ((q_buf, q_out), (k_buf, k_out), (v_buf, v_out), (head_buf, head_out))
        )
    ]
    for store in stores[:3]:
        store.start()
    pump(1)
    pairs = q_buf.shape[1] // 128

    def attention(pair, carry):
        here = pl.ds(pl.multiple_of(pair * 128, 128), 128)
        attend_pair(
            length_ref[0], pair // 2, q_buf.at[:, here], k_buf, v_buf, head_buf.at[:, here]
        )

        @pl.when(pair + 2 <= count - 2)
        def _():
            pump(pair + 2)

        return carry

    lax.fori_loop(0, pairs, attention, 0)
    stores[3].start()

    def store_part(band):
        return pltpu.make_async_copy(
            stage.at[band % 2],
            part_out.at[pl.ds(pl.multiple_of(band * 256, 256), 256), :],
            out_sems.at[4 + band % 2],
        )

    def output(band, carry):
        @pl.when(band >= 2)
        def _():
            store_part(band - 2).wait()

        lines = pl.ds(pl.multiple_of(band * 256, 256), 256)

        def columns(index, inner):
            cols = pl.ds(pl.multiple_of(index * 512, 512), 512)
            stage[band % 2, :, cols] = jnp.dot(
                head_buf[lines, :], w_output[:, cols], preferred_element_type=F32
            ).astype(BF16)
            return inner

        lax.fori_loop(0, w_output.shape[1] // 512, columns, 0)
        store_part(band).start()
        return carry

    lax.fori_loop(0, LEN // 256, output, 0)
    lax.fori_loop(min(pairs + 2, count - 1), count - 1, pump, 0)
    for band in (LEN // 256 - 2, LEN // 256 - 1):
        store_part(band).wait()
    for store in stores:
        store.wait()
    store_own.wait()
    for side in range(2):
        hop(count - 2, side).wait_recv()

    def drain(step, carry):
        for side in range(2):
            hop(step, side).wait_send()
        return carry

    lax.fori_loop(0, count - 1, drain, 0)


def attend_ring(shard, edge, lengths, rows_attn, weights, tables, count, collective_id):
    sources = [rows_attn, *weights, *tables]
    rows, width = rows_attn.shape
    inner = weights[0].shape[1]

    def low(*shape):
        return jax.ShapeDtypeStruct(shape, BF16)

    return pl.pallas_call(
        functools.partial(attend_ring_kernel, count),
        out_shape=[
            low(shard.shape[0] * count, edge),
            low(rows, inner),
            low(rows, 128),
            low(rows, 128),
            low(rows, inner),
            low(rows, width),
        ],
        in_specs=[pl.BlockSpec(memory_space=pltpu.SMEM)] + [ANY] * (1 + len(sources)),
        out_specs=[ANY] * 6,
        scratch_shapes=[pltpu.VMEM(source.shape, source.dtype) for source in sources]
        + [
            pltpu.VMEM((rows, inner), BF16),
            pltpu.VMEM((rows, 128), BF16),
            pltpu.VMEM((rows, 128), BF16),
            pltpu.VMEM((rows, inner), BF16),
            pltpu.VMEM((2, 256, width), BF16),
            pltpu.VMEM((shard.shape[0], edge), BF16),
            pltpu.SemaphoreType.DMA((2, count - 1)),
            pltpu.SemaphoreType.DMA((2, count - 1)),
            pltpu.SemaphoreType.DMA((len(sources),)),
            pltpu.SemaphoreType.DMA((6,)),
            pltpu.SemaphoreType.DMA,
        ],
        compiler_params=pltpu.CompilerParams(
            collective_id=collective_id, has_side_effects=True, vmem_limit_bytes=56 << 20
        ),
        cost_estimate=pl.CostEstimate(
            flops=24 << 30, bytes_accessed=60 << 20, transcendentals=8 << 20
        ),
        name="attend_ring",
    )(lengths, shard, *sources)


def ring_weight_grads(jobs, parts, count, collective_id):
    if all(left.shape[1] // count % 128 == 0 for left, _ in jobs):
        jobs = [Job(left, right, 0, right.shape[1]) for left, right in jobs]
        return ring_scatter_dots(jobs, parts, count, collective_id)
    partials = [tn_dot(left, right).astype(BF16) for left, right in jobs]
    num = len(jobs)
    return ring_scatter(partials, [0] * num, [parts] * num, count, collective_id)


def after(value, *deps):
    return lax.optimization_barrier((value,) + deps)[0]


def gather_rows(value):
    return lax.all_gather(value, "tensor", axis=0, tiled=True)


def scatter_rows(value):
    return lax.psum_scatter(value.astype(BF16), "tensor", scatter_dimension=0, tiled=True).astype(
        F32
    )


def share_kernel(count, group, parts_ref, out_ref, first, sums, second, sems):
    row, col = lax.axis_index("dp"), lax.axis_index("tensor")
    barrier = pltpu.get_barrier_semaphore()

    def in_group(shift):
        return {"tensor": (col + shift) % group}

    def in_column(shift):
        return {"dp": (row + shift) % count}

    def greet(device):
        pl.semaphore_signal(barrier, inc=1, device_id=device, device_id_type=MESH_ID)

    for shift in range(1, group):
        greet(in_group(shift))
    for shift in range(1, count):
        greet(in_column(shift))
    pl.semaphore_wait(barrier, group + count - 2)

    def exchange(shift, slot, source, target, device):
        return pltpu.make_async_remote_copy(
            src_ref=source,
            dst_ref=target,
            send_sem=sems.at[0, slot],
            recv_sem=sems.at[1, slot],
            device_id=device,
            device_id_type=MESH_ID,
        )

    moves = [
        exchange(s, s - 1, parts_ref.at[(col + s) % group], first.at[s - 1], in_group(s))
        for s in range(1, group)
    ]
    for move in moves:
        move.start()
    total = parts_ref[col]
    for shift, move in enumerate(moves):
        move.wait()
        total = total + first[shift]
    sums[...] = total
    moves = [
        exchange(
            s, group + s - 2, sums.at[(row + s) % count], second.at[s - 1], in_column(s)
        )
        for s in range(1, count)
    ]
    for move in moves:
        move.start()
    total = sums[row]
    for shift, move in enumerate(moves):
        move.wait()
        total = total + second[shift]
    out_ref[...] = total


def sum_shares(first, second, count, group, collective_id):
    share = first.shape[0] // (count * group)
    pair = jnp.stack([first, second]).reshape(2, count, group, share)
    parts = jnp.transpose(pair, (2, 1, 0, 3)).reshape(group, count, 1, 2 * share)
    width = (2 * share + 127) // 128 * 128
    parts = jnp.pad(parts, ((0, 0), (0, 0), (0, 7), (0, width - 2 * share)))
    tile = (8, width)
    out = pl.pallas_call(
        functools.partial(share_kernel, count, group),
        out_shape=jax.ShapeDtypeStruct(tile, F32),
        in_specs=[pl.BlockSpec(memory_space=pltpu.VMEM)],
        out_specs=pl.BlockSpec(memory_space=pltpu.VMEM),
        scratch_shapes=[
            pltpu.VMEM((group - 1, count) + tile, F32),
            pltpu.VMEM((count,) + tile, F32),
            pltpu.VMEM((count - 1,) + tile, F32),
            pltpu.SemaphoreType.DMA((2, group + count - 2)),
        ],
        compiler_params=pltpu.CompilerParams(collective_id=collective_id, has_side_effects=True),
        name="sum_shares",
    )(parts)
    return out[0, :share], out[0, share : 2 * share]


def dot(left, right):
    return jnp.dot(left, right, preferred_element_type=F32)


def body(
    count,
    group,
    tokens,
    lengths,
    attn_gain,
    w_query,
    w_key,
    w_value,
    w_output,
    mlp_gain,
    w_gate,
    w_up,
    w_down,
    cotangent,
):
    local_rows = tokens.shape[0]
    token_full = tokens.astype(F32)
    gain_attn = attn_gain.astype(F32)
    gain_mlp = mlp_gain.astype(F32)
    row_pos = lax.axis_index("tensor") * local_rows + jnp.arange(local_rows)
    valid_rows = (row_pos < lengths[0]).astype(F32)
    cot_masked = cotangent.astype(F32) * valid_rows[:, None]
    cosine, sine = rope_tables()

    inv_first = lax.rsqrt(jnp.mean(token_full * token_full, axis=1, keepdims=True) + epsilon)
    normed_attn = (token_full * inv_first * gain_attn).astype(BF16)
    rows_attn = gather_rows(normed_attn)
    query_all, key_all, value_all, output_all = ring_gather(
        [after(w_query, normed_attn), w_key, w_value, w_output],
        (0, 0, 0, 1), (1, 1, 1, 1), count, 0,
    )
    grad_branch = gather_rows(after(cot_masked.astype(BF16), rows_attn))
    fused = count == 8
    edge = 3 * w_gate.shape[1] // 8
    gates = []
    if fused:
        first_gate, queries, keys, values, head_out, attn_part = attend_ring(
            w_gate,
            edge,
            lengths,
            rows_attn,
            (query_all, key_all, value_all, output_all),
            (cosine, sine),
            count,
            9,
        )
        gates.append(first_gate)
    else:
        queries, keys, values = project(rows_attn, query_all, key_all, value_all, cosine, sine)
        head_out = attend(queries, keys, values, lengths)
        attn_part = dot(head_out, output_all).astype(BF16)
    attn_branch = scatter_rows(attn_part)
    (gate_all,) = ring_gather(
        [after(w_gate, attn_part)], (0,), (2,), count, 1, edge if fused else 0
    )
    gates.append(gate_all)
    hidden = token_full + attn_branch
    inv_second = lax.rsqrt(jnp.mean(hidden * hidden, axis=1, keepdims=True) + epsilon)
    normed_mlp = (hidden * inv_second * gain_mlp).astype(BF16)
    normed_mlp = after(normed_mlp, gate_all)
    rows_mlp = gather_rows(normed_mlp)
    (up_all,) = ring_gather([after(w_up, normed_mlp)], (0,), (2,), count, 2)
    if fused:
        activated, grad_gate_pre, grad_up_pre, down_all = mlp_ring(
            rows_mlp, gates, after(up_all, rows_mlp), w_down, grad_branch, count, 3
        )
        grad_down, norm_part, mlp_part = down_ring(
            grad_branch, activated, grad_gate_pre, grad_up_pre, gates, up_all, down_all,
            count, 4,
        )
    else:
        gate_proj = dot(rows_mlp, gate_all)
        up_proj = dot(rows_mlp, up_all)
        gate_sig = jax.nn.sigmoid(gate_proj)
        activated = (gate_proj * gate_sig * up_proj).astype(BF16)
        (down_all,) = ring_gather([after(w_down, up_all)], (1,), (2,), count, 3)
        mlp_part = dot(activated, down_all).astype(BF16)
        grad_act = nt_dot(grad_branch, down_all)
        grad_gate_pre = (
            grad_act * up_proj * gate_sig * (1.0 + gate_proj * (1.0 - gate_sig))
        ).astype(BF16)
        grad_up_pre = (grad_act * gate_proj * gate_sig).astype(BF16)
        norm_part = (nt_dot(grad_gate_pre, gate_all) + nt_dot(grad_up_pre, up_all)).astype(BF16)
        (grad_down,) = ring_weight_grads([(grad_branch, activated)], 2, count, 4)
    grad_norm_two = scatter_rows(norm_part)
    (grad_gate,) = ring_weight_grads(
        [(after(rows_mlp, norm_part), grad_gate_pre)], 2, count, 5
    )
    scaled_two = grad_norm_two * gain_mlp
    gain_two_part = jnp.sum(grad_norm_two * hidden * inv_second, axis=0)
    grad_hidden = (
        cot_masked
        + inv_second * scaled_two
        - hidden * inv_second**3 * jnp.mean(scaled_two * hidden, axis=1, keepdims=True)
    )
    grad_hidden = after(grad_hidden, grad_gate)
    grad_attn = gather_rows(grad_hidden.astype(BF16))
    mlp_branch = scatter_rows(after(mlp_part, grad_hidden))
    if fused:
        middle = grad_up_pre.shape[1] // 2
        hidden_cols = grad_up_pre.shape[1]
        (grad_up,) = ring_scatter_dots(
            [Job(after(rows_mlp, grad_hidden), grad_up_pre, 0, middle, hidden_cols)],
            2, count, 6,
        )
        grad_up, grad_qkv, token_part, gain_one = heads_ring(
            Job(rows_mlp, grad_up_pre, middle, hidden_cols - middle, grad_up, middle),
            lengths,
            gain_attn[None, :],
            after(grad_attn, grad_up),
            output_all,
            (queries, keys, values),
            (cosine, sine),
            (query_all, key_all, value_all),
            rows_attn,
            count,
            10,
        )
    else:
        (grad_up,) = ring_weight_grads(
            [(after(rows_mlp, grad_hidden), grad_up_pre)], 2, count, 6
        )
        grad_heads = nt_dot(after(grad_attn, grad_up), output_all).astype(BF16)
        grad_qpre, grad_kpre, grad_vpre = attend_back(
            queries, keys, values, grad_heads, lengths, cosine, sine
        )
        token_part = (
            nt_dot(grad_qpre, query_all)
            + nt_dot(grad_kpre, key_all)
            + nt_dot(grad_vpre, value_all)
        ).astype(BF16)
    layer_out = (hidden + after(mlp_branch, token_part)).astype(BF16)
    grad_norm_one = scatter_rows(token_part)
    scaled_one = grad_norm_one * gain_attn
    grad_tokens = (
        grad_hidden
        + inv_first * scaled_one
        - token_full * inv_first**3 * jnp.mean(scaled_one * token_full, axis=1, keepdims=True)
    )
    if fused:
        query_cols, key_cols = queries.shape[1], keys.shape[1]
        rows_late = after(rows_attn, token_part)
        grad_query, grad_key, grad_value, grad_output, shares = ring_scatter_dots(
            [
                Job(rows_late, grad_qkv, 0, query_cols),
                Job(rows_late, grad_qkv, query_cols, 2 * key_cols, split=True),
                Job(grad_attn, head_out, 0, query_cols),
            ],
            1,
            count,
            7,
            share_work(gain_one, gain_two_part[None, :], count, group),
        )
        share = gain_two_part.shape[0] // (count * group)
        grad_attn_gain, grad_mlp_gain = shares[0, :share], shares[1, :share]
    else:
        grad_query, grad_key, grad_value, grad_output = ring_weight_grads(
            [
                (after(rows_attn, token_part), grad_qpre),
                (rows_attn, grad_kpre),
                (rows_attn, grad_vpre),
                (grad_attn, head_out),
            ],
            1, count, 7,
        )
        gain_one_part = jnp.sum(grad_norm_one * token_full * inv_first, axis=0)
        grad_attn_gain, grad_mlp_gain = sum_shares(
            after(gain_one_part, grad_query), gain_two_part, count, group, 8
        )
    grad_output, grad_down = grad_output.T, grad_down.T
    return (
        layer_out,
        grad_tokens,
        grad_query,
        grad_key,
        grad_value,
        grad_output,
        grad_gate,
        grad_up,
        grad_down,
        grad_attn_gain,
        grad_mlp_gain,
    )


def solution(mesh):
    rows = P(("dp", "tensor"), None)
    tall = P("dp", "tensor")
    wide = P("tensor", "dp")
    share = P(("dp", "tensor"))
    in_specs = (rows, P("dp"), P(), tall, tall, tall, wide, P(), tall, tall, wide, rows)
    out_specs = (rows, rows, tall, tall, tall, wide, tall, tall, wide, share, share)
    return jax.shard_map(
        functools.partial(body, mesh.shape["dp"], mesh.shape["tensor"]),
        mesh=mesh,
        in_specs=in_specs,
        out_specs=out_specs,
        check_vma=False,
    )
```

```python
import functools
from typing import Any, NamedTuple

import jax
import jax.numpy as jnp
from jax import lax
from jax.experimental import pallas as pl
from jax.experimental.pallas import tpu as pltpu
from jax.sharding import PartitionSpec as P

HD = 64
LEN = 1024
QB = 256

epsilon = 1e-05
theta = 500000.0
MESH_ID = pl.DeviceIdType.MESH
BF16 = jnp.bfloat16
ANY = pl.BlockSpec(memory_space=pl.ANY)
F32 = jnp.float32


def rope_frequencies():
    half_size = HD // 2
    base_freq = theta ** (-(jnp.arange(half_size, dtype=jnp.float32) * 2.0) / HD)
    wavelength = 2.0 * jnp.pi / base_freq
    smooth = (8192.0 / wavelength - 1.0) / 3.0
    middle = (1.0 - smooth) * base_freq / 32.0 + smooth * base_freq
    return jnp.where(
        wavelength < 2048.0, base_freq, jnp.where(wavelength > 8192.0, base_freq / 32.0, middle)
    )


def rope_tables():
    steps = jnp.arange(32, dtype=jnp.float32)[:, None]
    frequency = jnp.concatenate([rope_frequencies()] * 4)[None, :]
    low, high = steps * frequency, (32.0 * steps) * frequency
    cos_low, sin_low = jnp.cos(low)[None, :, :], jnp.sin(low)[None, :, :]
    cos_high, sin_high = jnp.cos(high)[:, None, :], jnp.sin(high)[:, None, :]
    sign = jnp.where(jnp.arange(128) % HD < HD // 2, -1.0, 1.0)
    cosine = cos_high * cos_low - sin_high * sin_low
    sine = (sin_high * cos_low + cos_high * sin_low) * sign
    return cosine.reshape(LEN, 128), sine.reshape(LEN, 128)


def lane_index(shape):
    return lax.broadcasted_iota(jnp.int32, shape, 1)


def swap_halves(value):
    low = lane_index(value.shape) % HD < HD // 2
    return jnp.where(low, pltpu.roll(value, 128 - HD // 2, 1), pltpu.roll(value, HD // 2, 1))


def nt_dot(left, right):
    return lax.dot_general(left, right, (((1,), (1,)), ((), ())), preferred_element_type=F32)


def tn_dot(left, right):
    return lax.dot_general(left, right, (((0,), (0,)), ((), ())), preferred_element_type=F32)


def rope(value, cosine, sine):
    return (value * cosine + swap_halves(value) * sine).astype(BF16)


def rope_back(grads, cosine, sine):
    return (grads * cosine - swap_halves(grads) * sine).astype(BF16)


def project_rows(rows, wq_ref, wk_ref, wv_ref, cosine, sine, q_ref, k_ref, v_ref):
    for block in range(q_ref.shape[1] // 256):
        cols = slice(block * 256, (block + 1) * 256)
        value = jnp.dot(rows, wq_ref[:, cols], preferred_element_type=F32)
        for half in range(2):
            start = block * 256 + half * 128
            q_ref[:, start : start + 128] = rope(
                value[:, half * 128 : half * 128 + 128], cosine, sine
            )
    k_ref[...] = rope(jnp.dot(rows, wk_ref[...], preferred_element_type=F32), cosine, sine)
    v_ref[...] = jnp.dot(rows, wv_ref[...], preferred_element_type=F32).astype(BF16)


def project_kernel(x_ref, wq_ref, wk_ref, wv_ref, cos_ref, sin_ref, q_ref, k_ref, v_ref):
    project_rows(
        x_ref[...], wq_ref, wk_ref, wv_ref, cos_ref[...], sin_ref[...], q_ref, k_ref, v_ref
    )


def project(rows, w_query, w_key, w_value, cosine, sine):
    total, width = rows.shape
    block = 256

    def whole(array):
        return pl.BlockSpec(array.shape, lambda i: (0, 0))

    def by_rows(cols):
        return pl.BlockSpec((block, cols), lambda i: (i, 0))

    shapes = [w_query.shape[1], w_key.shape[1], w_value.shape[1]]
    return pl.pallas_call(
        project_kernel,
        grid=(total // block,),
        out_shape=[jax.ShapeDtypeStruct((total, s), BF16) for s in shapes],
        in_specs=[by_rows(width), whole(w_query), whole(w_key), whole(w_value)]
        + [by_rows(128)] * 2,
        out_specs=[by_rows(s) for s in shapes],
        compiler_params=pltpu.CompilerParams(vmem_limit_bytes=32 << 20),
        cost_estimate=pl.CostEstimate(
            flops=2 * total * width * sum(shapes), bytes_accessed=8 << 20, transcendentals=0
        ),
        name="project",
    )(rows, w_query, w_key, w_value, cosine, sine)


def pick_head(pair, which, kv):
    moved = jnp.where(kv == which, pair, pltpu.roll(pair, HD, 1))
    return jnp.where(lane_index(pair.shape) // HD == kv, moved, jnp.zeros_like(moved))


def join_heads(first, second, kv):
    first = jnp.where(kv == 0, first, pltpu.roll(first, HD, 1))
    second = jnp.where(kv == 1, second, pltpu.roll(second, HD, 1))
    return jnp.where(lane_index(first.shape) < HD, first, second)


def attend_pair(length, kv, q_ref, k_ref, v_ref, o_ref):
    square = (QB, QB)
    causal = lax.broadcasted_iota(jnp.int32, square, 1) <= lax.broadcasted_iota(
        jnp.int32, square, 0
    )
    bias = jnp.where(lane_index((1, LEN)) < length, 0.0, -1e30)
    for block in range(LEN // QB):
        start = block * QB
        here = slice(start, start + QB)
        pair = q_ref[here, :].astype(F32) * HD**-0.5
        outs = []
        for which in range(2):
            query = pick_head(pair, which, kv).astype(BF16)
            near = jnp.where(causal, nt_dot(query, k_ref[here, :]), -1e30) + bias[:, here]
            top = jnp.max(near, axis=1, keepdims=True)
            if start:
                far = nt_dot(query, k_ref[:start, :]) + bias[:, :start]
                top = jnp.maximum(top, jnp.max(far, axis=1, keepdims=True))
                far = jnp.exp(far - top)
            near = jnp.exp(near - top)
            total = jnp.sum(near, axis=1, keepdims=True)
            if start:
                total = total + jnp.sum(far, axis=1, keepdims=True)
            inverse = 1.0 / total
            out = jnp.dot(
                (near * inverse).astype(BF16), v_ref[here, :], preferred_element_type=F32
            )
            if start:
                out = out + jnp.dot(
                    (far * inverse).astype(BF16), v_ref[:start, :], preferred_element_type=F32
                )
            outs.append(out)
        o_ref[here, :] = join_heads(outs[0], outs[1], kv).astype(BF16)


def attend_kernel(length_ref, q_ref, k_ref, v_ref, o_ref):
    attend_pair(length_ref[0], pl.program_id(0) // 2, q_ref, k_ref, v_ref, o_ref)


def attend(queries, keys, values, lengths):
    pairs = queries.shape[1] // 128
    whole = pl.BlockSpec((LEN, 128), lambda i: (0, 0))
    paired = pl.BlockSpec((LEN, 128), lambda i: (0, i))
    return pl.pallas_call(
        attend_kernel,
        grid=(pairs,),
        out_shape=jax.ShapeDtypeStruct(queries.shape, BF16),
        in_specs=[pl.BlockSpec(memory_space=pltpu.SMEM), paired, whole, whole],
        out_specs=paired,
        compiler_params=pltpu.CompilerParams(vmem_limit_bytes=48 << 20),
        cost_estimate=pl.CostEstimate(
            flops=12 << 30, bytes_accessed=4 << 20, transcendentals=8 << 20
        ),
        name="attend",
    )(lengths, queries, keys, values)


def attend_back_pair(
    length, kv, q_ref, k_ref, v_ref, g_ref, cos_ref, sin_ref, gq_ref, acc_k, acc_v
):
    for block in range(LEN // QB):
        rows = slice(block * QB, (block + 1) * QB)
        keys = (block + 1) * QB
        pair = q_ref[rows, :].astype(F32) * HD**-0.5
        grad_pair = g_ref[rows, :].astype(F32)
        key_pos = lax.broadcasted_iota(jnp.int32, (keys, QB), 0)
        query_pos = block * QB + lax.broadcasted_iota(jnp.int32, (keys, QB), 1)
        allowed = (key_pos <= query_pos) & (key_pos < length)
        key_vecs = k_ref[:keys, :]
        grad_queries = []
        for which in range(2):
            query = pick_head(pair, which, kv).astype(BF16)
            grad = pick_head(grad_pair, which, kv).astype(BF16)
            scores = jnp.where(allowed, nt_dot(key_vecs, query), -1e30)
            exps = jnp.exp(scores - jnp.max(scores, axis=0, keepdims=True))
            probs = exps * (1.0 / jnp.sum(exps, axis=0, keepdims=True))
            grad_probs = nt_dot(v_ref[:keys, :], grad)
            inner = jnp.sum(probs * grad_probs, axis=0, keepdims=True)
            grad_scores = (probs * (grad_probs - inner)).astype(BF16)
            acc_v[:keys, :] += jnp.dot(probs.astype(BF16), grad, preferred_element_type=F32)
            acc_k[:keys, :] += jnp.dot(grad_scores, query, preferred_element_type=F32)
            grad_queries.append(tn_dot(grad_scores, key_vecs) * HD**-0.5)
        joined = join_heads(grad_queries[0], grad_queries[1], kv)
        gq_ref[rows, :] = rope_back(joined, cos_ref[rows, :], sin_ref[rows, :])


def attend_back_kernel(
    length_ref, q_ref, k_ref, v_ref, g_ref, cos_ref, sin_ref, gq_ref, gk_ref, gv_ref, acc_k, acc_v
):
    pair_index = pl.program_id(0)

    @pl.when(pair_index == 0)
    def _():
        acc_k[...] = jnp.zeros_like(acc_k)
        acc_v[...] = jnp.zeros_like(acc_v)

    attend_back_pair(
        length_ref[0], pair_index // 2, q_ref, k_ref, v_ref, g_ref, cos_ref, sin_ref, gq_ref,
        acc_k, acc_v,
    )

    @pl.when(pair_index == pl.num_programs(0) - 1)
    def _():
        gk_ref[...] = rope_back(acc_k[...], cos_ref[...], sin_ref[...])
        gv_ref[...] = acc_v[...].astype(BF16)


def attend_back(queries, keys, values, grad_heads, lengths, cosine, sine):
    pairs = queries.shape[1] // 128
    whole = pl.BlockSpec((LEN, 128), lambda i: (0, 0))
    paired = pl.BlockSpec((LEN, 128), lambda i: (0, i))
    narrow = jax.ShapeDtypeStruct((LEN, 128), BF16)
    return pl.pallas_call(
        attend_back_kernel,
        grid=(pairs,),
        out_shape=[jax.ShapeDtypeStruct(queries.shape, BF16), narrow, narrow],
        in_specs=[pl.BlockSpec(memory_space=pltpu.SMEM), paired, whole, whole, paired]
        + [whole] * 2,
        out_specs=[paired, whole, whole],
        scratch_shapes=[pltpu.VMEM((LEN, 128), F32)] * 2,
        compiler_params=pltpu.CompilerParams(vmem_limit_bytes=48 << 20),
        cost_estimate=pl.CostEstimate(
            flops=24 << 30, bytes_accessed=8 << 20, transcendentals=8 << 20
        ),
        name="attend_back",
    )(lengths, queries, keys, values, grad_heads, cosine, sine)


def ring_place(index, count):
    odd = index % 2
    return (1 - odd) * (index // 2) + odd * (count - 1 - index // 2)


def ring_member(place, count):
    high = place // (count // 2)
    return (1 - high) * (2 * place) + high * (2 * (count - 1 - place) + 1)


def ring_setup(count, peers=None):
    place = ring_place(lax.axis_index("dp"), count)
    ahead = ring_member((place + 1) % count, count)
    behind = ring_member((place + count - 1) % count, count)
    barrier = pltpu.get_barrier_semaphore()
    peers = peers or [{"dp": ahead}, {"dp": behind}]
    for other in peers:
        pl.semaphore_signal(barrier, inc=1, device_id=other, device_id_type=MESH_ID)
    pl.semaphore_wait(barrier, len(peers))
    return place, (ahead, behind)


def member_at(place, side, steps, count):
    if side == 0:
        return ring_member((place + count - steps) % count, count)
    return ring_member((place + steps) % count, count)


def piece(ref, shape, axis, member, side, part, parts, first=0):
    rows, cols = shape
    sub = rows // (2 * parts)
    start = (side * parts + part) * sub
    if axis is None:
        return ref.at[pl.ds(start, sub), first : first + cols]
    if axis == 0:
        return ref.at[pl.ds(pl.multiple_of(member * rows + start, sub), sub), :]
    return ref.at[pl.ds(start, sub), pl.ds(pl.multiple_of(member * cols, cols), cols)]


def gather_kernel(count, items, *refs):
    num = len(items)
    shards, outs = refs[:num], refs[num : 2 * num]
    stage = refs[2 * num : 3 * num]
    send_sems, recv_sems, local_sem = refs[3 * num :]
    place, neighbours = ring_setup(count)
    me = lax.axis_index("dp")
    slots = [(k, part) for k in range(num) for part in range(items[k][2])]

    def copy(step, side, slot):
        item, part = slots[slot]
        shape, axis, parts, _ = items[item]
        origin = member_at(place, side, step, count)
        target = piece(outs[item], shape, axis, origin, side, part, parts)
        return target, pltpu.make_async_remote_copy(
            src_ref=target,
            dst_ref=target,
            send_sem=send_sems.at[side, step, slot],
            recv_sem=recv_sems.at[side, step, slot],
            device_id={"dp": neighbours[side]},
            device_id_type=MESH_ID,
        )

    for slot, (item, part) in enumerate(slots):
        shape, axis, parts, first = items[item]
        for side in range(2):
            pltpu.make_async_remote_copy(
                src_ref=piece(shards[item], shape, None, 0, side, part, parts, first),
                dst_ref=piece(outs[item], shape, axis, me, side, part, parts),
                send_sem=send_sems.at[side, 0, slot],
                recv_sem=recv_sems.at[side, 0, slot],
                device_id={"dp": neighbours[side]},
                device_id_type=MESH_ID,
            ).start()
    loads = [
        pltpu.make_async_copy(
            shards[k].at[:, items[k][3] : items[k][3] + items[k][0][1]],
            stage[k],
            local_sem.at[k],
        )
        for k in range(num)
    ]
    for load in loads:
        load.start()
    stores = []
    for k in range(num):
        loads[k].wait()
        shape, axis, parts, _ = items[k]
        rows, cols = shape
        if axis == 0:
            own = outs[k].at[pl.ds(pl.multiple_of(me * rows, rows), rows), :]
        else:
            own = outs[k].at[:, pl.ds(pl.multiple_of(me * cols, cols), cols)]
        stores.append(pltpu.make_async_copy(stage[k], own, local_sem.at[k]))
        stores[-1].start()

    def hop(step, carry):
        for slot in range(len(slots)):
            for side in range(2):
                copy(step - 1, side, slot)[1].wait_recv()
                copy(step, side, slot)[1].start()
        return carry

    lax.fori_loop(1, count - 1, hop, 0)
    for slot in range(len(slots)):
        for side in range(2):
            copy(count - 2, side, slot)[1].wait_recv()
    for store in stores:
        store.wait()

    def drain(step, carry):
        for slot in range(len(slots)):
            for side in range(2):
                copy(step, side, slot)[1].wait_send()
        return carry

    lax.fori_loop(0, count - 1, drain, 0)


def ring_gather(shards, axes, parts, count, collective_id, first=0):
    turned = [a == 1 and s.shape[1] % 128 != 0 for s, a in zip(shards, axes)]
    if any(turned):
        shards = [s.T if t else s for s, t in zip(shards, turned)]
        axes = [0 if t else a for a, t in zip(axes, turned)]
        outs = ring_gather(shards, axes, parts, count, collective_id)
        return [o.T if t else o for o, t in zip(outs, turned)]
    shapes = [(s.shape[0], s.shape[1] - first) for s in shards]
    items = tuple((s, a, q, first) for s, a, q in zip(shapes, axes, parts))
    slots = sum(parts)
    outs = [
        jax.ShapeDtypeStruct((s[0] * count, s[1]) if a == 0 else (s[0], s[1] * count), BF16)
        for s, a in zip(shapes, axes)
    ]
    num = len(shards)
    nbytes = sum(s.size * 2 * (count - 1) for s in shards)
    return pl.pallas_call(
        functools.partial(gather_kernel, count, items),
        out_shape=outs,
        in_specs=[pl.BlockSpec(memory_space=pl.ANY)] * num,
        out_specs=[pl.BlockSpec(memory_space=pl.ANY)] * num,
        scratch_shapes=[pltpu.VMEM(s, BF16) for s in shapes]
        + [
            pltpu.SemaphoreType.DMA((2, count - 1, slots)),
            pltpu.SemaphoreType.DMA((2, count - 1, slots)),
            pltpu.SemaphoreType.DMA((num,)),
        ],
        compiler_params=pltpu.CompilerParams(collective_id=collective_id, has_side_effects=True),
        cost_estimate=pl.CostEstimate(flops=0, bytes_accessed=20 * nbytes, transcendentals=0),
        name=f"ring_gather_{collective_id}",
    )(*shards)


def scatter_kernel(count, items, *refs):
    num = len(items)
    partials, outs = refs[:num], refs[num : 2 * num]
    own = refs[2 * num : 3 * num]
    held = refs[3 * num : 4 * num]
    total = refs[4 * num : 5 * num]
    send_sems, recv_sems, load_sems, store_sems = refs[5 * num :]
    slots = [(k, part) for k in range(num) for part in range(items[k][2])]

    def load(step, side, slot, place):
        item, part = slots[slot]
        shape, axis, parts = items[item]
        member = member_at(place, side, step + 1, count)
        return pltpu.make_async_copy(
            piece(partials[item], shape, axis, member, side, part, parts),
            own[item].at[side, step, part],
            load_sems.at[side, step, slot],
        )

    start_place = ring_place(lax.axis_index("dp"), count)

    def load_all(step, carry):
        for slot in range(len(slots)):
            for side in range(2):
                load(step, side, slot, start_place).start()
        return carry

    lax.fori_loop(0, count, load_all, 0)
    place, neighbours = ring_setup(count)

    def send(step, side, slot, source):
        item, part = slots[slot]
        return pltpu.make_async_remote_copy(
            src_ref=source,
            dst_ref=held[item].at[side, step, part],
            send_sem=send_sems.at[side, step, slot],
            recv_sem=recv_sems.at[side, step, slot],
            device_id={"dp": neighbours[side]},
            device_id_type=MESH_ID,
        )

    for slot, (item, part) in enumerate(slots):
        for side in range(2):
            load(0, side, slot, place).wait()
            send(0, side, slot, own[item].at[side, 0, part]).start()

    def hop(step, carry):
        for slot, (item, part) in enumerate(slots):
            for side in range(2):
                load(step, side, slot, place).wait()
                arrived = held[item].at[side, step - 1, part]
                send(step - 1, side, slot, arrived).wait_recv()
                arrived[...] = (
                    arrived[...].astype(jnp.float32)
                    + own[item][side, step, part].astype(jnp.float32)
                ).astype(jnp.bfloat16)
                send(step, side, slot, arrived).start()
        return carry

    lax.fori_loop(1, count - 1, hop, 0)
    last = count - 1
    stores = []
    for slot, (item, part) in enumerate(slots):
        shape, axis, parts = items[item]
        for side in range(2):
            load(last, side, slot, place).wait()
            arrived = held[item].at[side, last - 1, part]
            send(last - 1, side, slot, arrived).wait_recv()
            total[item][side, part] = arrived[...].astype(jnp.float32) + own[item][
                side, last, part
            ].astype(jnp.float32)
            stores.append(
                pltpu.make_async_copy(
                    total[item].at[side, part],
                    piece(outs[item], shape, None, 0, side, part, parts),
                    store_sems.at[side, slot],
                )
            )
            stores[-1].start()
    for store in stores:
        store.wait()

    def drain(step, carry):
        for slot, (item, part) in enumerate(slots):
            for side in range(2):
                send(step, side, slot, held[item].at[side, 0, part]).wait_send()
        return carry

    lax.fori_loop(0, count - 1, drain, 0)


def ring_scatter(partials, axes, parts, count, collective_id):
    turned = [a == 1 and p.shape[1] // count % 128 != 0 for p, a in zip(partials, axes)]
    if any(turned):
        partials = [p.T if t else p for p, t in zip(partials, turned)]
        axes = [0 if t else a for a, t in zip(axes, turned)]
        outs = ring_scatter(partials, axes, parts, count, collective_id)
        return [o.T if t else o for o, t in zip(outs, turned)]
    shapes = [
        (p.shape[0] // count, p.shape[1]) if a == 0 else (p.shape[0], p.shape[1] // count)
        for p, a in zip(partials, axes)
    ]
    items = tuple((s, a, q) for s, a, q in zip(shapes, axes, parts))
    slots = sum(parts)
    num = len(partials)

    def buffers(depth, dtype):
        return [
            pltpu.VMEM((2,) + depth + (q, s[0] // (2 * q), s[1]), dtype)
            for s, q in zip(shapes, parts)
        ]

    nbytes = sum(p.size * 2 for p in partials)
    return pl.pallas_call(
        functools.partial(scatter_kernel, count, items),
        out_shape=[jax.ShapeDtypeStruct(s, jnp.float32) for s in shapes],
        in_specs=[pl.BlockSpec(memory_space=pl.ANY)] * num,
        out_specs=[pl.BlockSpec(memory_space=pl.ANY)] * num,
        scratch_shapes=buffers((count,), jnp.bfloat16)
        + buffers((count - 1,), jnp.bfloat16)
        + buffers((), jnp.float32)
        + [
            pltpu.SemaphoreType.DMA((2, count - 1, slots)),
            pltpu.SemaphoreType.DMA((2, count - 1, slots)),
            pltpu.SemaphoreType.DMA((2, count, slots)),
            pltpu.SemaphoreType.DMA((2, slots)),
        ],
        compiler_params=pltpu.CompilerParams(
            collective_id=collective_id, has_side_effects=True, vmem_limit_bytes=48 << 20
        ),
        cost_estimate=pl.CostEstimate(flops=0, bytes_accessed=20 * nbytes, transcendentals=0),
        name=f"ring_scatter_{collective_id}",
    )(*partials)


class Job(NamedTuple):
    left: Any
    right: Any
    start: int
    cols: int
    into: Any = None
    target: int = 0
    pieces: tuple = ()


class Extra(NamedTuple):
    builder: Any
    given: list
    given_specs: list
    made: list
    made_specs: list
    spare: list


def scatter_dot_kernel(count, items, num_outs, num_bases, parts, extra, *refs):
    num = len(items)
    taken = 0

    def take(amount):
        nonlocal taken
        taken += amount
        return refs[taken - amount : taken]

    lefts, rights, _ = take(num), take(num), take(num_bases)
    given = take(len(extra.given) if extra else 0)
    outs = take(num_outs)
    made = take(len(extra.made) if extra else 0)
    left_bufs, right_bufs, firsts, owns, helds, totals = (take(num) for _ in range(6))
    send_sems, recv_sems, left_sems, right_sems, store_sems = take(5)
    beside = extra.builder(count, given, made, refs[taken:], right_bufs) if extra else None
    entry_place = ring_place(lax.axis_index("dp"), count)
    last = count - 1

    def load_right(item):
        _, half, start, _ = items[item]
        return pltpu.make_async_copy(
            rights[item].at[:, start : start + 2 * half], right_bufs[item], right_sems.at[item]
        )

    def load_left(step, side, item, place):
        block = items[item][0]
        member = member_at(place, side, step + 1, count)
        slot = step % 2
        return pltpu.make_async_copy(
            lefts[item].at[:, pl.ds(pl.multiple_of(member * block, block), block)],
            left_bufs[item].at[side, slot],
            left_sems.at[side, slot, item],
        )

    for item in range(num):
        load_right(item).start()
        for side in range(2):
            load_left(0, side, item, entry_place).start()
    if beside:
        beside.begin()
    place, neighbours = ring_setup(count, beside.peers() if beside else None)
    pairs = [(item, side) for item in range(num) for side in range(2)]

    def send(step, side, item, part, source):
        return pltpu.make_async_remote_copy(
            src_ref=source.at[part],
            dst_ref=helds[item].at[side, step, part],
            send_sem=send_sems.at[side, step, item * parts + part],
            recv_sem=recv_sems.at[side, step, item * parts + part],
            device_id={"dp": neighbours[side]},
            device_id_type=MESH_ID,
        )

    def stores(item, side, part):
        block, _, _, places = items[item]
        rows = block // parts
        return [
            pltpu.make_async_copy(
                totals[item].at[side, part, :, source : source + cols],
                outs[out].at[part * rows : (part + 1) * rows, column : column + cols],
                store_sems.at[side, item * parts + part, k],
            )
            for k, (source, cols, out, column) in enumerate(places[side])
        ]

    for item in range(num):
        load_right(item).wait()

    def turn(step, carry):
        @pl.when(step < last)
        def _():
            for item, side in pairs:
                load_left(step + 1, side, item, place).start()

        for item in range(num):
            half = items[item][1]
            for side in range(2):
                load_left(step, side, item, place).wait()

            def own_sum(side, inner):
                cols = pl.ds(pl.multiple_of(side * half, half), half)
                owns[item][side] = tn_dot(
                    left_bufs[item][side, step % 2], right_bufs[item][:, cols]
                ).reshape(owns[item].shape[1:])
                return inner

            lax.fori_loop(0, 2, own_sum, 0)

        @pl.when(step == 0)
        def _():
            for part in range(parts):
                for item, side in pairs:
                    firsts[item][side, part] = owns[item][side, part].astype(BF16)
                    send(0, side, item, part, firsts[item].at[side]).start()

        if beside:
            beside.compute(step)

        @pl.when((step > 0) & (step < last))
        def _():
            for part in range(parts):
                for item, side in pairs:
                    arrived = helds[item].at[side, step - 1]
                    send(step - 1, side, item, part, arrived).wait_recv()
                    arrived[part] = (
                        arrived[part].astype(F32) + owns[item][side, part]
                    ).astype(BF16)
                    send(step, side, item, part, arrived).start()

        return carry

    lax.fori_loop(0, count, turn, 0)
    for part in range(parts):
        for item, side in pairs:
            arrived = helds[item].at[side, last - 1]
            send(last - 1, side, item, part, arrived).wait_recv()
            totals[item][side, part] = arrived[part].astype(F32) + owns[item][side, part]
            for copy in stores(item, side, part):
                copy.start()
    if beside:
        beside.finish()
    for part in range(parts):
        for item, side in pairs:
            for copy in stores(item, side, part):
                copy.wait()

    def drain(step, carry):
        for part in range(parts):
            for item, side in pairs:
                send(step, side, item, part, helds[item].at[side, 0]).wait_send()
        return carry

    lax.fori_loop(0, last, drain, 0)


def ring_scatter_dots(jobs, parts, count, collective_id, extra=None):
    rows = jobs[0].left.shape[0]
    items, shapes, bases, aliases = [], [], [], {}
    for job in jobs:
        block, half = job.left.shape[1] // count, job.cols // 2
        if job.pieces:
            places, column = ([], []), 0
            for cols in job.pieces:
                for side in range(2):
                    low = max(column, side * half)
                    high = min(column + cols, (side + 1) * half)
                    if low < high:
                        places[side].append(
                            (low - side * half, high - low, len(shapes), low - column)
                        )
                column += cols
                shapes.append((block, cols))
        else:
            places = [
                [(0, half, len(shapes), job.target + side * half)] for side in range(2)
            ]
            if job.into is None:
                shapes.append((block, job.cols))
            elif isinstance(job.into, int):
                shapes.append((block, job.into))
            else:
                aliases[2 * len(jobs) + len(bases)] = len(shapes)
                bases.append(job.into)
                shapes.append(job.into.shape)
        items.append((block, half, job.start, places))
    num = len(jobs)

    def buffers(depth, dtype):
        return [pltpu.VMEM(depth + (parts, b // parts, h), dtype) for b, h, _, _ in items]

    slots = num * parts
    flops = sum(2 * rows * j.left.shape[1] * j.cols for j in jobs)
    nbytes = sum(2 * j.left.shape[1] * j.cols for j in jobs)
    given, given_specs, made, made_specs, spare = extra[1:] if extra else ([], [], [], [], [])
    return pl.pallas_call(
        functools.partial(
            scatter_dot_kernel, count, items, len(shapes), len(bases), parts, extra
        ),
        out_shape=[jax.ShapeDtypeStruct(s, F32) for s in shapes] + made,
        in_specs=[ANY] * (2 * num + len(bases)) + given_specs,
        out_specs=[ANY] * len(shapes) + made_specs,
        input_output_aliases=aliases,
        scratch_shapes=[pltpu.VMEM((2, 2, rows, i[0]), BF16) for i in items]
        + [pltpu.VMEM((rows, 2 * i[1]), BF16) for i in items]
        + buffers((2,), BF16)
        + buffers((2,), F32)
        + buffers((2, count - 1), BF16)
        + buffers((2,), F32)
        + [
            pltpu.SemaphoreType.DMA((2, count - 1, slots)),
            pltpu.SemaphoreType.DMA((2, count - 1, slots)),
            pltpu.SemaphoreType.DMA((2, 2, num)),
            pltpu.SemaphoreType.DMA((num,)),
            pltpu.SemaphoreType.DMA((2, slots, 3)),
        ]
        + spare,
        compiler_params=pltpu.CompilerParams(
            collective_id=collective_id, has_side_effects=True, vmem_limit_bytes=60 << 20
        ),
        cost_estimate=pl.CostEstimate(
            flops=flops, bytes_accessed=20 * nbytes, transcendentals=0
        ),
        name=f"ring_scatter_{collective_id}",
    )(*[j.left for j in jobs], *[j.right for j in jobs], *bases, *given)


class ShareWork:
    def __init__(self, count, given, made, spare, rights):
        self.given, self.out = given, made[0]
        self.pair, self.first, self.sums, self.second, self.sems = spare
        self.count, self.group = count, self.second.shape[0] + 1
        self.row, self.col = lax.axis_index("dp"), lax.axis_index("tensor")

    def in_column(self, shift):
        return {"dp": (self.row + shift) % self.count}

    def in_group(self, shift):
        return {"tensor": (self.col + shift) % self.group}

    def peers(self):
        return [self.in_column(s) for s in range(1, self.count)] + [
            self.in_group(s) for s in range(1, self.group)
        ]

    def begin(self):
        pass

    def part(self, row):
        width = self.sums.shape[1]
        return pl.ds(pl.multiple_of(row * width, width), width)

    def move(self, stage, shift):
        if stage == 0:
            source = self.pair.at[:, self.part((self.row + shift) % self.count)]
            target, device, slot = self.first.at[shift - 1], self.in_column(shift), shift - 1
        else:
            source, target = self.sums, self.second.at[shift - 1]
            device, slot = self.in_group(shift), self.count + shift - 2
        return pltpu.make_async_remote_copy(
            src_ref=source,
            dst_ref=target,
            send_sem=self.sems.at[0, slot],
            recv_sem=self.sems.at[1, slot],
            device_id=device,
            device_id_type=MESH_ID,
        )

    def compute(self, step):
        @pl.when(step == 0)
        def _():
            self.pair[...] = self.given[0][...]
            self.pair[1:2, :] = self.given[1][...]
            for shift in range(1, self.count):
                self.move(0, shift).start()

        @pl.when(step == 2)
        def _():
            total = self.pair[:, self.part(self.row)]
            for shift in range(1, self.count):
                self.move(0, shift).wait()
                total = total + self.first[shift - 1]
            self.sums[...] = total
            for shift in range(1, self.group):
                self.move(1, shift).start()

    def finish(self):
        total = self.sums[...]
        for shift in range(1, self.group):
            self.move(1, shift).wait()
            total = total + self.second[shift - 1]
        share = total.shape[1] // self.group
        picked = jnp.zeros((8, share), F32)
        for col in range(self.group):
            picked = jnp.where(self.col == col, total[:, col * share : (col + 1) * share], picked)
        self.out[:, :share] = picked


def share_work(first, second, count, group):
    width = first.shape[1] // count
    vmem = pl.BlockSpec(memory_space=pltpu.VMEM)
    return Extra(
        ShareWork,
        [first, second],
        [vmem] * 2,
        [jax.ShapeDtypeStruct((8, 128), F32)],
        [vmem],
        [
            pltpu.VMEM(first.shape, F32),
            pltpu.VMEM((count - 1, 8, width), F32),
            pltpu.VMEM((8, width), F32),
            pltpu.VMEM((group - 1, 8, width), F32),
            pltpu.SemaphoreType.DMA((2, count + group - 2)),
        ],
    )


class NormWork:
    def __init__(self, count, given, made, spare, rights):
        self.grads, self.gates = given[:2], tuple(given[2:4])
        self.up, self.down = given[4:]
        self.outs = made
        self.grad_bufs, self.row_bufs, self.down_bufs, self.stage = spare[0], *spare[1:4]
        self.grad_sems, self.row_sems, self.down_sems, self.out_sems = spare[4:]
        self.act = rights[0]
        self.count = count
        self.block = self.row_bufs.shape[2]

    def load_grad(self, which):
        return pltpu.make_async_copy(
            self.grads[which], self.grad_bufs.at[which], self.grad_sems.at[which]
        )

    def spot(self, step):
        return pl.ds(pl.multiple_of(step * self.block, self.block), self.block)

    def loads(self, step):
        slot = step % 2
        edge = self.gates[0].shape[1]
        gate = self.row_bufs.at[0, slot]
        targets = [gate.at[:, :edge], gate.at[:, edge:], self.row_bufs.at[1, slot]]
        rows = [
            pltpu.make_async_copy(
                source.at[self.spot(step), :], target, self.row_sems.at[which, slot]
            )
            for which, (source, target) in enumerate(zip(self.gates + (self.up,), targets))
        ]
        down = pltpu.make_async_copy(
            self.down.at[:, self.spot(step)], self.down_bufs.at[slot], self.down_sems.at[slot]
        )
        return rows + [down]

    def store(self, which, step):
        slot = step % 2
        return pltpu.make_async_copy(
            self.stage.at[which, slot],
            self.outs[which].at[:, self.spot(step)],
            self.out_sems.at[which, slot],
        )

    def begin(self):
        for which in range(2):
            self.load_grad(which).start()
        for copy in self.loads(0):
            copy.start()

    def peers(self):
        return None

    def compute(self, step):
        @pl.when(step < self.count - 1)
        def _():
            for copy in self.loads(step + 1):
                copy.start()

        @pl.when(step == 0)
        def _():
            for which in range(2):
                self.load_grad(which).wait()

        @pl.when(step >= 2)
        def _():
            for which in range(2):
                self.store(which, step - 2).wait()

        for copy in self.loads(step):
            copy.wait()
        slot = step % 2

        def lines(index, carry):
            band = pl.ds(pl.multiple_of(index * 256, 256), 256)
            norm = nt_dot(self.grad_bufs[0, band, :], self.row_bufs[0, slot])
            norm += nt_dot(self.grad_bufs[1, band, :], self.row_bufs[1, slot])
            self.stage[0, slot, band, :] = norm.astype(BF16)
            value = jnp.dot(
                self.act[band, :], self.down_bufs[slot], preferred_element_type=F32
            )
            self.stage[1, slot, band, :] = value.astype(BF16)
            return carry

        lax.fori_loop(0, self.act.shape[0] // 256, lines, 0)
        for which in range(2):
            self.store(which, step).start()

    def finish(self):
        for step in range(max(self.count - 2, 0), self.count):
            for which in range(2):
                self.store(which, step).wait()


def down_ring(grad_branch, activated, grad_gate, grad_up, gates, up_all, down_all, count, cid):
    rows, hidden = activated.shape
    width = up_all.shape[0]
    block = width // count
    wide = jax.ShapeDtypeStruct((rows, width), BF16)
    spare = [
        pltpu.VMEM((2, rows, hidden), BF16),
        pltpu.VMEM((2, 2, block, hidden), BF16),
        pltpu.VMEM((2, hidden, block), BF16),
        pltpu.VMEM((2, 2, rows, block), BF16),
        pltpu.SemaphoreType.DMA((2,)),
        pltpu.SemaphoreType.DMA((3, 2)),
        pltpu.SemaphoreType.DMA((2,)),
        pltpu.SemaphoreType.DMA((2, 2)),
    ]
    given = [grad_gate, grad_up, *gates, up_all, down_all]
    return ring_scatter_dots(
        [Job(grad_branch, activated, 0, hidden)],
        2,
        count,
        cid,
        Extra(NormWork, given, [ANY] * 6, [wide, wide], [ANY] * 2, spare),
    )


def mlp_kernel(count, *refs):
    x_hbm, wg_hbm, wg_rest, wu_hbm, shard, gb_hbm = refs[:6]
    act_hbm, gg_hbm, gu_hbm, down_all = refs[6:10]
    x_buf, gb_buf, w_bufs, gate_slope, up_slope, acc, half_bufs, stage, own_stage = refs[10:19]
    send_sems, recv_sems, w_sems, in_sems, half_sems, out_sems, local_sem = refs[19:]
    rows, width = x_buf.shape
    hidden = acc.shape[1]
    block = width // count
    cols = w_bufs.shape[-1]
    steps = hidden // cols
    half = hidden // 2
    parts = send_sems.shape[2]
    me = lax.axis_index("dp")

    gate_steps = wg_hbm.shape[1] // cols

    def load_weights(step, which, source=None):
        start = step - gate_steps if source is wg_rest else step
        source = (wg_hbm, wu_hbm)[which] if source is None else source
        return pltpu.make_async_copy(
            source.at[:, pl.ds(pl.multiple_of(start * cols, cols), cols)],
            w_bufs.at[which, step % 2],
            w_sems.at[which, step % 2],
        )

    def fetch(step):
        load_weights(step, 1).start()

        @pl.when(step < gate_steps)
        def _():
            load_weights(step, 0).start()

        @pl.when(step >= gate_steps)
        def _():
            load_weights(step, 0, wg_rest).start()

    load_x = pltpu.make_async_copy(x_hbm, x_buf, in_sems.at[0])
    load_gb = pltpu.make_async_copy(gb_hbm, gb_buf, in_sems.at[1])
    load_own = pltpu.make_async_copy(shard, own_stage, local_sem)
    load_x.start()
    for which in range(2):
        load_weights(0, which).start()
    load_own.start()
    load_gb.start()
    place, neighbours = ring_setup(count)

    def target(ref, member, side, part):
        return piece(ref, (hidden, block), 1, member, side, part, parts)

    def hop(step, side, part):
        ref = target(down_all, member_at(place, side, step, count), side, part)
        return pltpu.make_async_remote_copy(
            src_ref=ref,
            dst_ref=ref,
            send_sem=send_sems.at[side, step, part],
            recv_sem=recv_sems.at[side, step, part],
            device_id={"dp": neighbours[side]},
            device_id_type=MESH_ID,
        )

    for part in range(parts):
        for side in range(2):
            pltpu.make_async_remote_copy(
                src_ref=piece(shard, (hidden, block), None, 0, side, part, parts),
                dst_ref=target(down_all, me, side, part),
                send_sem=send_sems.at[side, 0, part],
                recv_sem=recv_sems.at[side, 0, part],
                device_id={"dp": neighbours[side]},
                device_id_type=MESH_ID,
            ).start()

    def pump(step):
        for part in range(parts):
            for side in range(2):
                hop(step - 1, side, part).wait_recv()
                hop(step, side, part).start()

    load_own.wait()
    store_own = pltpu.make_async_copy(
        own_stage, down_all.at[:, pl.ds(pl.multiple_of(me * block, block), block)], local_sem
    )
    store_own.start()
    load_x.wait()

    def store(ref, which, step):
        return pltpu.make_async_copy(
            stage.at[which, step % 2],
            ref.at[:, pl.ds(pl.multiple_of(step * cols, cols), cols)],
            out_sems.at[which, step % 2],
        )

    def forward(step, carry):
        @pl.when(step + 1 < steps)
        def _():
            fetch(step + 1)

        @pl.when(step >= 2)
        def _():
            store(act_hbm, 0, step - 2).wait()

        load_weights(step, 1).wait()

        @pl.when(step < gate_steps)
        def _():
            load_weights(step, 0).wait()

        @pl.when(step >= gate_steps)
        def _():
            load_weights(step, 0, wg_rest).wait()

        here = pl.ds(pl.multiple_of(step * cols, cols), cols)
        for top in range(0, rows, 256):
            band = pl.ds(top, 256)
            lines = x_buf[band, :]
            gate = jnp.dot(lines, w_bufs[0, step % 2], preferred_element_type=F32)
            up = jnp.dot(lines, w_bufs[1, step % 2], preferred_element_type=F32)
            sig = jax.nn.sigmoid(gate)
            silu = gate * sig
            stage[0, step % 2, band, :] = (silu * up).astype(BF16)
            gate_slope[band, here] = up * sig * (1.0 + gate * (1.0 - sig))
            up_slope[band, here] = silu
            acc[band, here] = jnp.zeros((256, cols), F32)
        store(act_hbm, 0, step).start()

        turn = (step + 1) // 2

        @pl.when((step % 2 == 1) & (turn <= count - 2))
        def _():
            pump(turn)

        return carry

    lax.fori_loop(0, steps, forward, 0)
    for step in range(max(steps - 2, 0), steps):
        store(act_hbm, 0, step).wait()
    pumped = min(steps // 2, count - 2)
    load_gb.wait()

    def load_half(step, side):
        member = member_at(place, side, step, count)
        return pltpu.make_async_copy(
            down_all.at[
                pl.ds(side * half, half), pl.ds(pl.multiple_of(member * block, block), block)
            ],
            half_bufs.at[side],
            half_sems.at[side],
        )

    def backward(step, carry):
        @pl.when((step > pumped) & (step <= count - 2))
        def _():
            pump(step)

        @pl.when(step == count - 1)
        def _():
            for part in range(parts):
                for side in range(2):
                    hop(count - 2, side, part).wait_recv()

        for side in range(2):
            load_half(step, side).start()
        for side in range(2):
            member = member_at(place, side, step, count)
            load_half(step, side).wait()
            here = pl.ds(pl.multiple_of(member * block, block), block)
            spot = pl.ds(side * half, half)

            def lines(index, carry):
                band = pl.ds(pl.multiple_of(index * 256, 256), 256)
                acc[band, spot] += nt_dot(gb_buf[band, here], half_bufs[side])
                return carry

            lax.fori_loop(0, rows // 256, lines, 0)

        return carry

    store_own.wait()
    lax.fori_loop(0, count, backward, 0)

    def slopes(step, carry):
        @pl.when(step >= 2)
        def _():
            store(gg_hbm, 1, step - 2).wait()
            store(gu_hbm, 2, step - 2).wait()

        here = pl.ds(pl.multiple_of(step * cols, cols), cols)

        def lines(index, carry):
            band = pl.ds(pl.multiple_of(index * 256, 256), 256)
            value = acc[band, here]
            stage[1, step % 2, band, :] = (value * gate_slope[band, here]).astype(BF16)
            stage[2, step % 2, band, :] = (value * up_slope[band, here]).astype(BF16)
            return carry

        lax.fori_loop(0, rows // 256, lines, 0)
        store(gg_hbm, 1, step).start()
        store(gu_hbm, 2, step).start()
        return carry

    lax.fori_loop(0, steps, slopes, 0)
    for step in range(max(steps - 2, 0), steps):
        store(gg_hbm, 1, step).wait()
        store(gu_hbm, 2, step).wait()

    def drain(step, carry):
        for part in range(parts):
            for side in range(2):
                hop(step, side, part).wait_send()
        return carry

    lax.fori_loop(0, count - 1, drain, 0)


def mlp_ring(rows_mlp, gates, up_all, w_down, grad_branch, count, collective_id):
    rows, width = rows_mlp.shape
    hidden, block = w_down.shape
    cols, parts = 256, 2
    wide = jax.ShapeDtypeStruct((rows, hidden), BF16)
    return pl.pallas_call(
        functools.partial(mlp_kernel, count),
        out_shape=[wide] * 3 + [jax.ShapeDtypeStruct((hidden, width), BF16)],
        in_specs=[ANY] * 6,
        out_specs=[pl.BlockSpec(memory_space=pl.ANY)] * 4,
        scratch_shapes=[
            pltpu.VMEM((rows, width), BF16),
            pltpu.VMEM((rows, width), BF16),
            pltpu.VMEM((2, 2, width, cols), BF16),
            pltpu.VMEM((rows, hidden), F32),
            pltpu.VMEM((rows, hidden), F32),
            pltpu.VMEM((rows, hidden), F32),
            pltpu.VMEM((2, hidden // 2, block), BF16),
            pltpu.VMEM((3, 2, rows, cols), BF16),
            pltpu.VMEM((hidden, block), BF16),
            pltpu.SemaphoreType.DMA((2, count - 1, parts)),
            pltpu.SemaphoreType.DMA((2, count - 1, parts)),
            pltpu.SemaphoreType.DMA((2, 2)),
            pltpu.SemaphoreType.DMA((2,)),
            pltpu.SemaphoreType.DMA((2,)),
            pltpu.SemaphoreType.DMA((3, 2)),
            pltpu.SemaphoreType.DMA,
        ],
        compiler_params=pltpu.CompilerParams(
            collective_id=collective_id, has_side_effects=True, vmem_limit_bytes=60 << 20
        ),
        cost_estimate=pl.CostEstimate(
            flops=6 * rows * width * hidden,
            bytes_accessed=40 * hidden * width,
            transcendentals=rows * hidden,
        ),
        name="mlp_ring",
    )(rows_mlp, *gates, up_all, w_down, grad_branch)


class HeadWork:
    def __init__(self, count, given, made, spare, rights):
        self.length, self.gain, self.sources = given[0], given[1], given[2:]
        self.grads_out, self.token_out, self.gain_out = made
        num = len(self.sources)
        self.bufs = spare[:num]
        self.heads, self.grads, self.acc_k, self.acc_v, self.stage = spare[num : num + 5]
        self.in_sems, self.out_sems = spare[num + 5 :]

    def peers(self):
        return None

    def load(self, which):
        return pltpu.make_async_copy(
            self.sources[which], self.bufs[which], self.in_sems.at[which]
        )

    def begin(self):
        for which in range(len(self.sources)):
            self.load(which).start()
        self.gain_out[...] = jnp.zeros_like(self.gain_out)
        self.acc_k[...] = jnp.zeros_like(self.acc_k)
        self.acc_v[...] = jnp.zeros_like(self.acc_v)

    def store(self, band):
        rows = self.stage.shape[1]
        return pltpu.make_async_copy(
            self.stage.at[band % 2],
            self.token_out.at[pl.ds(pl.multiple_of(band * rows, rows), rows), :],
            self.out_sems.at[band % 2],
        )

    def store_grads(self):
        return pltpu.make_async_copy(self.grads, self.grads_out, self.out_sems.at[2])

    def tokens(self, band):
        w_query, w_key, w_value, normed = self.bufs[7:]
        rows = self.stage.shape[1]
        inner = w_query.shape[1]

        @pl.when(band >= 2)
        def _():
            self.store(band - 2).wait()

        lines = pl.ds(pl.multiple_of(band * rows, rows), rows)

        def columns(index, carry):
            cols = pl.ds(pl.multiple_of(index * 512, 512), 512)
            value = nt_dot(self.grads[lines, :inner], w_query[cols, :])
            value += nt_dot(self.grads[lines, inner : inner + 128], w_key[cols, :])
            value += nt_dot(self.grads[lines, inner + 128 :], w_value[cols, :])
            self.stage[band % 2, :, cols] = value.astype(BF16)
            scaled = value * normed[lines, cols].astype(F32)
            self.gain_out[0:1, cols] += jnp.sum(scaled, axis=0, keepdims=True)
            return carry

        lax.fori_loop(0, w_query.shape[0] // 512, columns, 0)
        self.store(band).start()

    def compute(self, step):
        grad_attn, w_output, queries, keys, values, cosine, sine = self.bufs[:7]
        inner = queries.shape[1]
        pairs = inner // 128

        @pl.when(step == 0)
        def _():
            for which in range(2):
                self.load(which).wait()

            def band(index, carry):
                rows = pl.ds(pl.multiple_of(index * 256, 256), 256)
                self.heads[rows, :] = nt_dot(grad_attn[rows, :], w_output[...]).astype(BF16)
                return carry

            lax.fori_loop(0, LEN // 256, band, 0)

        @pl.when(step == 1)
        def _():
            for which in range(2, 7):
                self.load(which).wait()

        @pl.when(step == pairs + 1)
        def _():
            for which in range(7, len(self.sources)):
                self.load(which).wait()

        @pl.when((step >= 1) & (step <= pairs))
        def _():
            here = pl.ds(pl.multiple_of((step - 1) * 128, 128), 128)
            attend_back_pair(
                self.length[0], (step - 1) // 2, queries.at[:, here], keys, values,
                self.heads.at[:, here], cosine, sine, self.grads.at[:, here],
                self.acc_k, self.acc_v,
            )

        @pl.when(step == pairs)
        def _():
            self.grads[:, inner : inner + 128] = rope_back(
                self.acc_k[...], cosine[...], sine[...]
            )
            self.grads[:, inner + 128 :] = self.acc_v[...].astype(BF16)
            self.store_grads().start()

        @pl.when((step > pairs) & (step <= pairs + 2))
        def _():
            def band(index, carry):
                self.tokens(2 * (step - pairs - 1) + index)
                return carry

            lax.fori_loop(0, 2, band, 0)

    def finish(self):
        self.gain_out[0:1, :] = self.gain_out[0:1, :] / self.gain[...]
        self.store_grads().wait()
        for band in (2, 3):
            self.store(band).wait()


def heads_ring(
    job, lengths, gain, grad_attn, w_output, qkv, tables, weights, rows_attn, count, cid
):
    sources = [grad_attn, w_output, *qkv, *tables, *weights, rows_attn]
    rows, width = grad_attn.shape
    inner = qkv[0].shape[1]
    made = [
        jax.ShapeDtypeStruct((rows, inner + 256), BF16),
        jax.ShapeDtypeStruct((rows, width), BF16),
        jax.ShapeDtypeStruct((8, width), F32),
    ]
    spare = [pltpu.VMEM(g.shape, g.dtype) for g in sources] + [
        pltpu.VMEM((rows, inner), BF16),
        pltpu.VMEM((rows, inner + 256), BF16),
        pltpu.VMEM((rows, 128), F32),
        pltpu.VMEM((rows, 128), F32),
        pltpu.VMEM((2, rows // 4, width), BF16),
        pltpu.SemaphoreType.DMA((len(sources),)),
        pltpu.SemaphoreType.DMA((3,)),
    ]
    vmem = pl.BlockSpec(memory_space=pltpu.VMEM)
    specs = [pl.BlockSpec(memory_space=pltpu.SMEM), vmem] + [ANY] * len(sources)
    return ring_scatter_dots(
        [job],
        2,
        count,
        cid,
        Extra(HeadWork, [lengths, gain] + sources, specs, made, [ANY, ANY, vmem], spare),
    )


def attend_ring_kernel(count, *refs):
    length_ref, shard, sources = refs[0], refs[1], refs[2:9]
    gathered, q_out, k_out, v_out, head_out, part_out = refs[9:15]
    bufs = refs[15:22]
    q_buf, k_buf, v_buf, head_buf, stage, own = refs[22:28]
    send_sems, recv_sems, in_sems, out_sems, local_sem = refs[28:]
    rows_buf, w_query, w_key, w_value, w_output, cosine, sine = bufs
    shape = own.shape
    me = lax.axis_index("dp")
    loads = [
        pltpu.make_async_copy(source, buf, in_sems.at[k])
        for k, (source, buf) in enumerate(zip(sources, bufs))
    ]
    for load in loads:
        load.start()
    load_own = pltpu.make_async_copy(shard.at[:, : shape[1]], own, local_sem)
    load_own.start()
    place, neighbours = ring_setup(count)

    def hop(step, side):
        ref = piece(gathered, shape, 0, member_at(place, side, step, count), side, 0, 1)
        return pltpu.make_async_remote_copy(
            src_ref=ref,
            dst_ref=ref,
            send_sem=send_sems.at[side, step],
            recv_sem=recv_sems.at[side, step],
            device_id={"dp": neighbours[side]},
            device_id_type=MESH_ID,
        )

    for side in range(2):
        pltpu.make_async_remote_copy(
            src_ref=piece(shard, shape, None, 0, side, 0, 1),
            dst_ref=piece(gathered, shape, 0, me, side, 0, 1),
            send_sem=send_sems.at[side, 0],
            recv_sem=recv_sems.at[side, 0],
            device_id={"dp": neighbours[side]},
            device_id_type=MESH_ID,
        ).start()

    def pump(step, carry=0):
        for side in range(2):
            hop(step - 1, side).wait_recv()
            hop(step, side).start()
        return carry

    load_own.wait()
    store_own = pltpu.make_async_copy(
        own, gathered.at[pl.ds(pl.multiple_of(me * shape[0], shape[0]), shape[0]), :], local_sem
    )
    store_own.start()
    for k in (0, 1, 2, 3, 5, 6):
        loads[k].wait()

    def projection(band, carry):
        lines = pl.ds(pl.multiple_of(band * 256, 256), 256)
        project_rows(
            rows_buf[lines, :], w_query, w_key, w_value, cosine[lines, :], sine[lines, :],
            q_buf.at[lines, :], k_buf.at[lines, :], v_buf.at[lines, :],
        )
        return carry

    lax.fori_loop(0, LEN // 256, projection, 0)
    stores = [
        pltpu.make_async_copy(buf, out, out_sems.at[k])
        for k, (buf, out) in enumerate(
            ((q_buf, q_out), (k_buf, k_out), (v_buf, v_out), (head_buf, head_out))
        )
    ]
    for store in stores[:3]:
        store.start()
    pump(1)
    pairs = q_buf.shape[1] // 128

    def attention(pair, carry):
        here = pl.ds(pl.multiple_of(pair * 128, 128), 128)
        attend_pair(
            length_ref[0], pair // 2, q_buf.at[:, here], k_buf, v_buf, head_buf.at[:, here]
        )

        @pl.when(pair + 2 <= count - 2)
        def _():
            pump(pair + 2)

        return carry

    lax.fori_loop(0, pairs, attention, 0)
    loads[4].wait()
    stores[3].start()

    def store_part(band):
        return pltpu.make_async_copy(
            stage.at[band % 2],
            part_out.at[pl.ds(pl.multiple_of(band * 256, 256), 256), :],
            out_sems.at[4 + band % 2],
        )

    def output(band, carry):
        @pl.when(band >= 2)
        def _():
            store_part(band - 2).wait()

        lines = pl.ds(pl.multiple_of(band * 256, 256), 256)

        def columns(index, inner):
            cols = pl.ds(pl.multiple_of(index * 512, 512), 512)
            stage[band % 2, :, cols] = jnp.dot(
                head_buf[lines, :], w_output[:, cols], preferred_element_type=F32
            ).astype(BF16)
            return inner

        lax.fori_loop(0, w_output.shape[1] // 512, columns, 0)
        store_part(band).start()

        @pl.when((band == 0) & (pairs + 2 <= count - 2))
        def _():
            pump(pairs + 2)

        return carry

    lax.fori_loop(0, LEN // 256, output, 0)
    lax.fori_loop(min(pairs + 3, count - 1), count - 1, pump, 0)
    for band in (LEN // 256 - 2, LEN // 256 - 1):
        store_part(band).wait()
    for store in stores:
        store.wait()
    store_own.wait()
    for side in range(2):
        hop(count - 2, side).wait_recv()

    def drain(step, carry):
        for side in range(2):
            hop(step, side).wait_send()
        return carry

    lax.fori_loop(0, count - 1, drain, 0)


def attend_ring(shard, edge, lengths, rows_attn, weights, tables, count, collective_id):
    sources = [rows_attn, *weights, *tables]
    rows, width = rows_attn.shape
    inner = weights[0].shape[1]

    def low(*shape):
        return jax.ShapeDtypeStruct(shape, BF16)

    return pl.pallas_call(
        functools.partial(attend_ring_kernel, count),
        out_shape=[
            low(shard.shape[0] * count, edge),
            low(rows, inner),
            low(rows, 128),
            low(rows, 128),
            low(rows, inner),
            low(rows, width),
        ],
        in_specs=[pl.BlockSpec(memory_space=pltpu.SMEM)] + [ANY] * (1 + len(sources)),
        out_specs=[ANY] * 6,
        scratch_shapes=[pltpu.VMEM(source.shape, source.dtype) for source in sources]
        + [
            pltpu.VMEM((rows, inner), BF16),
            pltpu.VMEM((rows, 128), BF16),
            pltpu.VMEM((rows, 128), BF16),
            pltpu.VMEM((rows, inner), BF16),
            pltpu.VMEM((2, 256, width), BF16),
            pltpu.VMEM((shard.shape[0], edge), BF16),
            pltpu.SemaphoreType.DMA((2, count - 1)),
            pltpu.SemaphoreType.DMA((2, count - 1)),
            pltpu.SemaphoreType.DMA((len(sources),)),
            pltpu.SemaphoreType.DMA((6,)),
            pltpu.SemaphoreType.DMA,
        ],
        compiler_params=pltpu.CompilerParams(
            collective_id=collective_id, has_side_effects=True, vmem_limit_bytes=56 << 20
        ),
        cost_estimate=pl.CostEstimate(
            flops=24 << 30, bytes_accessed=60 << 20, transcendentals=8 << 20
        ),
        name="attend_ring",
    )(lengths, shard, *sources)


def ring_weight_grads(jobs, parts, count, collective_id):
    if all(left.shape[1] // count % 128 == 0 for left, _ in jobs):
        jobs = [Job(left, right, 0, right.shape[1]) for left, right in jobs]
        return ring_scatter_dots(jobs, parts, count, collective_id)
    partials = [tn_dot(left, right).astype(BF16) for left, right in jobs]
    num = len(jobs)
    return ring_scatter(partials, [0] * num, [parts] * num, count, collective_id)


def after(value, *deps):
    return lax.optimization_barrier((value,) + deps)[0]


def gather_rows(value):
    return lax.all_gather(value, "tensor", axis=0, tiled=True)


def scatter_rows(value):
    return lax.psum_scatter(value.astype(BF16), "tensor", scatter_dimension=0, tiled=True)


def share_kernel(count, group, parts_ref, out_ref, first, sums, second, sems):
    row, col = lax.axis_index("dp"), lax.axis_index("tensor")
    barrier = pltpu.get_barrier_semaphore()

    def in_group(shift):
        return {"tensor": (col + shift) % group}

    def in_column(shift):
        return {"dp": (row + shift) % count}

    def greet(device):
        pl.semaphore_signal(barrier, inc=1, device_id=device, device_id_type=MESH_ID)

    for shift in range(1, group):
        greet(in_group(shift))
    for shift in range(1, count):
        greet(in_column(shift))
    pl.semaphore_wait(barrier, group + count - 2)

    def exchange(shift, slot, source, target, device):
        return pltpu.make_async_remote_copy(
            src_ref=source,
            dst_ref=target,
            send_sem=sems.at[0, slot],
            recv_sem=sems.at[1, slot],
            device_id=device,
            device_id_type=MESH_ID,
        )

    moves = [
        exchange(s, s - 1, parts_ref.at[(col + s) % group], first.at[s - 1], in_group(s))
        for s in range(1, group)
    ]
    for move in moves:
        move.start()
    total = parts_ref[col]
    for shift, move in enumerate(moves):
        move.wait()
        total = total + first[shift]
    sums[...] = total
    moves = [
        exchange(
            s, group + s - 2, sums.at[(row + s) % count], second.at[s - 1], in_column(s)
        )
        for s in range(1, count)
    ]
    for move in moves:
        move.start()
    total = sums[row]
    for shift, move in enumerate(moves):
        move.wait()
        total = total + second[shift]
    out_ref[...] = total


def sum_shares(first, second, count, group, collective_id):
    share = first.shape[0] // (count * group)
    pair = jnp.stack([first, second]).reshape(2, count, group, share)
    parts = jnp.transpose(pair, (2, 1, 0, 3)).reshape(group, count, 1, 2 * share)
    width = (2 * share + 127) // 128 * 128
    parts = jnp.pad(parts, ((0, 0), (0, 0), (0, 7), (0, width - 2 * share)))
    tile = (8, width)
    out = pl.pallas_call(
        functools.partial(share_kernel, count, group),
        out_shape=jax.ShapeDtypeStruct(tile, F32),
        in_specs=[pl.BlockSpec(memory_space=pltpu.VMEM)],
        out_specs=pl.BlockSpec(memory_space=pltpu.VMEM),
        scratch_shapes=[
            pltpu.VMEM((group - 1, count) + tile, F32),
            pltpu.VMEM((count,) + tile, F32),
            pltpu.VMEM((count - 1,) + tile, F32),
            pltpu.SemaphoreType.DMA((2, group + count - 2)),
        ],
        compiler_params=pltpu.CompilerParams(collective_id=collective_id, has_side_effects=True),
        name="sum_shares",
    )(parts)
    return out[0, :share], out[0, share : 2 * share]


def dot(left, right):
    return jnp.dot(left, right, preferred_element_type=F32)


def body(
    count,
    group,
    tokens,
    lengths,
    attn_gain,
    w_query,
    w_key,
    w_value,
    w_output,
    mlp_gain,
    w_gate,
    w_up,
    w_down,
    cotangent,
):
    local_rows = tokens.shape[0]
    token_full = tokens.astype(F32)
    gain_attn = attn_gain.astype(F32)
    gain_mlp = mlp_gain.astype(F32)
    row_pos = lax.axis_index("tensor") * local_rows + jnp.arange(local_rows)
    valid_rows = (row_pos < lengths[0]).astype(F32)
    cot_masked = cotangent.astype(F32) * valid_rows[:, None]
    cosine, sine = rope_tables()

    inv_first = lax.rsqrt(jnp.mean(token_full * token_full, axis=1, keepdims=True) + epsilon)
    normed_attn = (token_full * inv_first * gain_attn).astype(BF16)
    rows_attn = gather_rows(normed_attn)
    query_all, key_all, value_all, output_all = ring_gather(
        [after(w_query, normed_attn), w_key, w_value, w_output],
        (0, 0, 0, 1), (1, 1, 1, 1), count, 0,
    )
    grad_branch = gather_rows(after(cot_masked.astype(BF16), rows_attn))
    fused = count == 8
    edge = 3 * w_gate.shape[1] // 8
    gates = []
    if fused:
        first_gate, queries, keys, values, head_out, attn_part = attend_ring(
            w_gate,
            edge,
            lengths,
            rows_attn,
            (query_all, key_all, value_all, output_all),
            (cosine, sine),
            count,
            9,
        )
        gates.append(first_gate)
    else:
        queries, keys, values = project(rows_attn, query_all, key_all, value_all, cosine, sine)
        head_out = attend(queries, keys, values, lengths)
        attn_part = dot(head_out, output_all).astype(BF16)
    attn_branch = scatter_rows(attn_part)
    (gate_all,) = ring_gather(
        [after(w_gate, attn_part)], (0,), (2,), count, 1, edge if fused else 0
    )
    gates.append(gate_all)
    hidden = token_full + attn_branch.astype(F32)
    inv_second = lax.rsqrt(jnp.mean(hidden * hidden, axis=1, keepdims=True) + epsilon)
    normed_mlp = (hidden * inv_second * gain_mlp).astype(BF16)
    normed_mlp = after(normed_mlp, gate_all)
    rows_mlp = gather_rows(normed_mlp)
    (up_all,) = ring_gather([after(w_up, normed_mlp)], (0,), (2,), count, 2)
    if fused:
        activated, grad_gate_pre, grad_up_pre, down_all = mlp_ring(
            rows_mlp, gates, after(up_all, rows_mlp), w_down, grad_branch, count, 3
        )
        grad_down, norm_part, mlp_part = down_ring(
            grad_branch, activated, grad_gate_pre, grad_up_pre, gates, up_all, down_all,
            count, 4,
        )
    else:
        gate_proj = dot(rows_mlp, gate_all)
        up_proj = dot(rows_mlp, up_all)
        gate_sig = jax.nn.sigmoid(gate_proj)
        activated = (gate_proj * gate_sig * up_proj).astype(BF16)
        (down_all,) = ring_gather([after(w_down, up_all)], (1,), (2,), count, 3)
        mlp_part = dot(activated, down_all).astype(BF16)
        grad_act = nt_dot(grad_branch, down_all)
        grad_gate_pre = (
            grad_act * up_proj * gate_sig * (1.0 + gate_proj * (1.0 - gate_sig))
        ).astype(BF16)
        grad_up_pre = (grad_act * gate_proj * gate_sig).astype(BF16)
        norm_part = (nt_dot(grad_gate_pre, gate_all) + nt_dot(grad_up_pre, up_all)).astype(BF16)
        (grad_down,) = ring_weight_grads([(grad_branch, activated)], 2, count, 4)
    grad_norm_two = scatter_rows(norm_part).astype(F32)
    (grad_gate,) = ring_weight_grads(
        [(after(rows_mlp, norm_part), grad_gate_pre)], 2, count, 5
    )
    scaled_two = grad_norm_two * gain_mlp
    gain_two_part = jnp.sum(grad_norm_two * hidden * inv_second, axis=0)
    grad_hidden = (
        cot_masked
        + inv_second * scaled_two
        - hidden * inv_second**3 * jnp.mean(scaled_two * hidden, axis=1, keepdims=True)
    )
    grad_hidden = after(grad_hidden, grad_gate)
    grad_attn = gather_rows(grad_hidden.astype(BF16))
    mlp_branch = scatter_rows(after(mlp_part, grad_hidden))
    if fused:
        middle = 5 * grad_up_pre.shape[1] // 8
        hidden_cols = grad_up_pre.shape[1]
        (grad_up,) = ring_scatter_dots(
            [Job(after(rows_mlp, grad_hidden), grad_up_pre, 0, middle, hidden_cols)],
            2, count, 6,
        )
        grad_up, grad_qkv, token_part, gain_one = heads_ring(
            Job(rows_mlp, grad_up_pre, middle, hidden_cols - middle, grad_up, middle),
            lengths,
            gain_attn[None, :],
            after(grad_attn, grad_up),
            output_all,
            (queries, keys, values),
            (cosine, sine),
            (query_all, key_all, value_all),
            rows_attn,
            count,
            10,
        )
    else:
        (grad_up,) = ring_weight_grads(
            [(after(rows_mlp, grad_hidden), grad_up_pre)], 2, count, 6
        )
        grad_heads = nt_dot(after(grad_attn, grad_up), output_all).astype(BF16)
        grad_qpre, grad_kpre, grad_vpre = attend_back(
            queries, keys, values, grad_heads, lengths, cosine, sine
        )
        token_part = (
            nt_dot(grad_qpre, query_all)
            + nt_dot(grad_kpre, key_all)
            + nt_dot(grad_vpre, value_all)
        ).astype(BF16)
    layer_out = (hidden + after(mlp_branch, token_part).astype(F32)).astype(BF16)
    grad_norm_one = scatter_rows(token_part).astype(F32)
    scaled_one = grad_norm_one * gain_attn
    grad_tokens = (
        grad_hidden
        + inv_first * scaled_one
        - token_full * inv_first**3 * jnp.mean(scaled_one * token_full, axis=1, keepdims=True)
    )
    if fused:
        query_cols, key_cols = queries.shape[1], keys.shape[1]
        rows_late = after(rows_attn, token_part)
        grad_query, grad_key, grad_value, grad_output, shares = ring_scatter_dots(
            [
                Job(
                    rows_late,
                    grad_qkv,
                    0,
                    query_cols + 2 * key_cols,
                    pieces=(query_cols, key_cols, key_cols),
                ),
                Job(grad_attn, head_out, 0, query_cols),
            ],
            1,
            count,
            7,
            share_work(gain_one, gain_two_part[None, :], count, group),
        )
        share = gain_two_part.shape[0] // (count * group)
        grad_attn_gain, grad_mlp_gain = shares[0, :share], shares[1, :share]
    else:
        grad_query, grad_key, grad_value, grad_output = ring_weight_grads(
            [
                (after(rows_attn, token_part), grad_qpre),
                (rows_attn, grad_kpre),
                (rows_attn, grad_vpre),
                (grad_attn, head_out),
            ],
            1, count, 7,
        )
        gain_one_part = jnp.sum(grad_norm_one * token_full * inv_first, axis=0)
        grad_attn_gain, grad_mlp_gain = sum_shares(
            after(gain_one_part, grad_query), gain_two_part, count, group, 8
        )
    grad_output, grad_down = grad_output.T, grad_down.T
    return (
        layer_out,
        grad_tokens,
        grad_query,
        grad_key,
        grad_value,
        grad_output,
        grad_gate,
        grad_up,
        grad_down,
        grad_attn_gain,
        grad_mlp_gain,
    )


def solution(mesh):
    rows = P(("dp", "tensor"), None)
    tall = P("dp", "tensor")
    wide = P("tensor", "dp")
    share = P(("dp", "tensor"))
    in_specs = (rows, P("dp"), P(), tall, tall, tall, wide, P(), tall, tall, wide, rows)
    out_specs = (rows, rows, tall, tall, tall, wide, tall, tall, wide, share, share)
    return jax.shard_map(
        functools.partial(body, mesh.shape["dp"], mesh.shape["tensor"]),
        mesh=mesh,
        in_specs=in_specs,
        out_specs=out_specs,
        check_vma=False,
    )
```

```python
import functools
from typing import Any, NamedTuple

import jax
import jax.numpy as jnp
from jax import lax
from jax.experimental import pallas as pl
from jax.experimental.pallas import tpu as pltpu
from jax.sharding import PartitionSpec as P

HD = 64
LEN = 1024
QB = 256

epsilon = 1e-05
theta = 500000.0
MESH_ID = pl.DeviceIdType.MESH
BF16 = jnp.bfloat16
ANY = pl.BlockSpec(memory_space=pl.ANY)
F32 = jnp.float32


def rope_frequencies():
    half_size = HD // 2
    base_freq = theta ** (-(jnp.arange(half_size, dtype=jnp.float32) * 2.0) / HD)
    wavelength = 2.0 * jnp.pi / base_freq
    smooth = (8192.0 / wavelength - 1.0) / 3.0
    middle = (1.0 - smooth) * base_freq / 32.0 + smooth * base_freq
    return jnp.where(
        wavelength < 2048.0, base_freq, jnp.where(wavelength > 8192.0, base_freq / 32.0, middle)
    )


def rope_tables():
    steps = jnp.arange(32, dtype=jnp.float32)[:, None]
    frequency = jnp.concatenate([rope_frequencies()] * 4)[None, :]
    low, high = steps * frequency, (32.0 * steps) * frequency
    cos_low, sin_low = jnp.cos(low)[None, :, :], jnp.sin(low)[None, :, :]
    cos_high, sin_high = jnp.cos(high)[:, None, :], jnp.sin(high)[:, None, :]
    sign = jnp.where(jnp.arange(128) % HD < HD // 2, -1.0, 1.0)
    cosine = cos_high * cos_low - sin_high * sin_low
    sine = (sin_high * cos_low + cos_high * sin_low) * sign
    return cosine.reshape(LEN, 128), sine.reshape(LEN, 128)


def lane_index(shape):
    return lax.broadcasted_iota(jnp.int32, shape, 1)


def swap_halves(value):
    low = lane_index(value.shape) % HD < HD // 2
    return jnp.where(low, pltpu.roll(value, 128 - HD // 2, 1), pltpu.roll(value, HD // 2, 1))


def nt_dot(left, right):
    return lax.dot_general(left, right, (((1,), (1,)), ((), ())), preferred_element_type=F32)


def tn_dot(left, right):
    return lax.dot_general(left, right, (((0,), (0,)), ((), ())), preferred_element_type=F32)


def rope(value, cosine, sine):
    return (value * cosine + swap_halves(value) * sine).astype(BF16)


def rope_back(grads, cosine, sine):
    return (grads * cosine - swap_halves(grads) * sine).astype(BF16)


def project_rows(rows, wq_ref, wk_ref, wv_ref, cosine, sine, q_ref, k_ref, v_ref):
    for block in range(q_ref.shape[1] // 256):
        cols = slice(block * 256, (block + 1) * 256)
        value = jnp.dot(rows, wq_ref[:, cols], preferred_element_type=F32)
        for half in range(2):
            start = block * 256 + half * 128
            q_ref[:, start : start + 128] = rope(
                value[:, half * 128 : half * 128 + 128], cosine, sine
            )
    k_ref[...] = rope(jnp.dot(rows, wk_ref[...], preferred_element_type=F32), cosine, sine)
    v_ref[...] = jnp.dot(rows, wv_ref[...], preferred_element_type=F32).astype(BF16)


def project_kernel(x_ref, wq_ref, wk_ref, wv_ref, cos_ref, sin_ref, q_ref, k_ref, v_ref):
    project_rows(
        x_ref[...], wq_ref, wk_ref, wv_ref, cos_ref[...], sin_ref[...], q_ref, k_ref, v_ref
    )


def project(rows, w_query, w_key, w_value, cosine, sine):
    total, width = rows.shape
    block = 256

    def whole(array):
        return pl.BlockSpec(array.shape, lambda i: (0, 0))

    def by_rows(cols):
        return pl.BlockSpec((block, cols), lambda i: (i, 0))

    shapes = [w_query.shape[1], w_key.shape[1], w_value.shape[1]]
    return pl.pallas_call(
        project_kernel,
        grid=(total // block,),
        out_shape=[jax.ShapeDtypeStruct((total, s), BF16) for s in shapes],
        in_specs=[by_rows(width), whole(w_query), whole(w_key), whole(w_value)]
        + [by_rows(128)] * 2,
        out_specs=[by_rows(s) for s in shapes],
        compiler_params=pltpu.CompilerParams(vmem_limit_bytes=32 << 20),
        cost_estimate=pl.CostEstimate(
            flops=2 * total * width * sum(shapes), bytes_accessed=8 << 20, transcendentals=0
        ),
        name="project",
    )(rows, w_query, w_key, w_value, cosine, sine)


def pick_head(pair, which, kv):
    moved = jnp.where(kv == which, pair, pltpu.roll(pair, HD, 1))
    return jnp.where(lane_index(pair.shape) // HD == kv, moved, jnp.zeros_like(moved))


def join_heads(first, second, kv):
    first = jnp.where(kv == 0, first, pltpu.roll(first, HD, 1))
    second = jnp.where(kv == 1, second, pltpu.roll(second, HD, 1))
    return jnp.where(lane_index(first.shape) < HD, first, second)


def attend_pair(length, pair_index, q_ref, k_ref, v_ref, o_ref, stats_ref=None):
    kv = pair_index // 2
    square = (QB, QB)
    causal = lax.broadcasted_iota(jnp.int32, square, 1) <= lax.broadcasted_iota(
        jnp.int32, square, 0
    )
    bias = jnp.where(lane_index((1, LEN)) < length, 0.0, -1e30)
    for block in range(LEN // QB):
        start = block * QB
        here = slice(start, start + QB)
        pair = q_ref[here, :].astype(F32) * HD**-0.5
        outs = []
        for which in range(2):
            query = pick_head(pair, which, kv).astype(BF16)
            near = jnp.where(causal, nt_dot(query, k_ref[here, :]), -1e30) + bias[:, here]
            top = jnp.max(near, axis=1, keepdims=True)
            if start:
                far = nt_dot(query, k_ref[:start, :]) + bias[:, :start]
                top = jnp.maximum(top, jnp.max(far, axis=1, keepdims=True))
                far = jnp.exp(far - top)
            near = jnp.exp(near - top)
            total = jnp.sum(near, axis=1, keepdims=True)
            if start:
                total = total + jnp.sum(far, axis=1, keepdims=True)
            inverse = 1.0 / total
            if stats_ref is not None:
                kept = stats_ref[here, :]
                mine = lane_index(kept.shape) == 2 * pair_index + which
                stats_ref[here, :] = jnp.where(mine, top + jnp.log(total), kept)
            out = jnp.dot(
                (near * inverse).astype(BF16), v_ref[here, :], preferred_element_type=F32
            )
            if start:
                out = out + jnp.dot(
                    (far * inverse).astype(BF16), v_ref[:start, :], preferred_element_type=F32
                )
            outs.append(out)
        o_ref[here, :] = join_heads(outs[0], outs[1], kv).astype(BF16)


def attend_kernel(length_ref, q_ref, k_ref, v_ref, o_ref):
    attend_pair(length_ref[0], pl.program_id(0), q_ref, k_ref, v_ref, o_ref)


def attend(queries, keys, values, lengths):
    pairs = queries.shape[1] // 128
    whole = pl.BlockSpec((LEN, 128), lambda i: (0, 0))
    paired = pl.BlockSpec((LEN, 128), lambda i: (0, i))
    return pl.pallas_call(
        attend_kernel,
        grid=(pairs,),
        out_shape=jax.ShapeDtypeStruct(queries.shape, BF16),
        in_specs=[pl.BlockSpec(memory_space=pltpu.SMEM), paired, whole, whole],
        out_specs=paired,
        compiler_params=pltpu.CompilerParams(vmem_limit_bytes=48 << 20),
        cost_estimate=pl.CostEstimate(
            flops=12 << 30, bytes_accessed=4 << 20, transcendentals=8 << 20
        ),
        name="attend",
    )(lengths, queries, keys, values)


def attend_back_pair(
    length, kv, q_ref, k_ref, v_ref, g_ref, cos_ref, sin_ref, gq_ref, acc_k, acc_v
):
    for block in range(LEN // QB):
        rows = slice(block * QB, (block + 1) * QB)
        keys = (block + 1) * QB
        pair = q_ref[rows, :].astype(F32) * HD**-0.5
        grad_pair = g_ref[rows, :].astype(F32)
        key_pos = lax.broadcasted_iota(jnp.int32, (keys, QB), 0)
        query_pos = block * QB + lax.broadcasted_iota(jnp.int32, (keys, QB), 1)
        allowed = (key_pos <= query_pos) & (key_pos < length)
        key_vecs = k_ref[:keys, :]
        grad_queries = []
        for which in range(2):
            query = pick_head(pair, which, kv).astype(BF16)
            grad = pick_head(grad_pair, which, kv).astype(BF16)
            scores = jnp.where(allowed, nt_dot(key_vecs, query), -1e30)
            exps = jnp.exp(scores - jnp.max(scores, axis=0, keepdims=True))
            probs = exps * (1.0 / jnp.sum(exps, axis=0, keepdims=True))
            grad_probs = nt_dot(v_ref[:keys, :], grad)
            inner = jnp.sum(probs * grad_probs, axis=0, keepdims=True)
            grad_scores = (probs * (grad_probs - inner)).astype(BF16)
            acc_v[:keys, :] += jnp.dot(probs.astype(BF16), grad, preferred_element_type=F32)
            acc_k[:keys, :] += jnp.dot(grad_scores, query, preferred_element_type=F32)
            grad_queries.append(tn_dot(grad_scores, key_vecs) * HD**-0.5)
        joined = join_heads(grad_queries[0], grad_queries[1], kv)
        gq_ref[rows, :] = rope_back(joined, cos_ref[rows, :], sin_ref[rows, :])


def row_products(grads, outs, pair_index, kept):
    product = grads.astype(F32) * outs.astype(F32)
    lanes = lane_index(product.shape)
    low = jnp.sum(jnp.where(lanes < HD, product, 0.0), axis=1, keepdims=True)
    high = jnp.sum(jnp.where(lanes < HD, 0.0, product), axis=1, keepdims=True)
    kept = jnp.where(lanes == 2 * pair_index, low, kept)
    return jnp.where(lanes == 2 * pair_index + 1, high, kept)


def attend_back_tiles(
    pair_index, q_ref, k_ref, v_ref, g_ref, cos_ref, sin_ref, stats_ref, inner_ref, bias_ref,
    gq_ref, acc_k, acc_v,
):
    kv = pair_index // 2
    square = (QB, QB)
    causal = lax.broadcasted_iota(jnp.int32, square, 0) <= lax.broadcasted_iota(
        jnp.int32, square, 1
    )
    for block in range(LEN // QB):
        rows = slice(block * QB, (block + 1) * QB)
        pair = q_ref[rows, :].astype(F32) * HD**-0.5
        grad_pair = g_ref[rows, :].astype(F32)
        queries, grads, tops, inners = [], [], [], []
        for which in range(2):
            queries.append(pick_head(pair, which, kv).astype(BF16))
            grads.append(pick_head(grad_pair, which, kv).astype(BF16))
            head = pl.ds(2 * pair_index + which, 1)
            tops.append(stats_ref[head, rows])
            inners.append(inner_ref[head, rows])
        grad_queries = [None, None]
        for tile in range(block + 1):
            here = slice(tile * QB, (tile + 1) * QB)
            key_vecs, value_vecs = k_ref[here, :], v_ref[here, :]
            bias = bias_ref[here, :]
            bias = jnp.concatenate([bias] * (QB // 128), axis=1)
            grad_key = grad_value = None
            for which in range(2):
                scores = nt_dot(key_vecs, queries[which]) + bias
                if tile == block:
                    scores = jnp.where(causal, scores, -1e30)
                probs = jnp.exp(scores - tops[which])
                grad_probs = nt_dot(value_vecs, grads[which])
                grad_scores = (probs * (grad_probs - inners[which])).astype(BF16)
                value = jnp.dot(probs.astype(BF16), grads[which], preferred_element_type=F32)
                key = jnp.dot(grad_scores, queries[which], preferred_element_type=F32)
                query = tn_dot(grad_scores, key_vecs)
                grad_value = value if which == 0 else grad_value + value
                grad_key = key if which == 0 else grad_key + key
                grad_queries[which] = query if tile == 0 else grad_queries[which] + query
            acc_v[here, :] += grad_value
            acc_k[here, :] += grad_key
        joined = join_heads(grad_queries[0], grad_queries[1], kv) * HD**-0.5
        gq_ref[rows, :] = rope_back(joined, cos_ref[rows, :], sin_ref[rows, :])


def attend_back_kernel(
    length_ref, q_ref, k_ref, v_ref, g_ref, cos_ref, sin_ref, gq_ref, gk_ref, gv_ref, acc_k, acc_v
):
    pair_index = pl.program_id(0)

    @pl.when(pair_index == 0)
    def _():
        acc_k[...] = jnp.zeros_like(acc_k)
        acc_v[...] = jnp.zeros_like(acc_v)

    attend_back_pair(
        length_ref[0], pair_index // 2, q_ref, k_ref, v_ref, g_ref, cos_ref, sin_ref, gq_ref,
        acc_k, acc_v,
    )

    @pl.when(pair_index == pl.num_programs(0) - 1)
    def _():
        gk_ref[...] = rope_back(acc_k[...], cos_ref[...], sin_ref[...])
        gv_ref[...] = acc_v[...].astype(BF16)


def attend_back(queries, keys, values, grad_heads, lengths, cosine, sine):
    pairs = queries.shape[1] // 128
    whole = pl.BlockSpec((LEN, 128), lambda i: (0, 0))
    paired = pl.BlockSpec((LEN, 128), lambda i: (0, i))
    narrow = jax.ShapeDtypeStruct((LEN, 128), BF16)
    return pl.pallas_call(
        attend_back_kernel,
        grid=(pairs,),
        out_shape=[jax.ShapeDtypeStruct(queries.shape, BF16), narrow, narrow],
        in_specs=[pl.BlockSpec(memory_space=pltpu.SMEM), paired, whole, whole, paired]
        + [whole] * 2,
        out_specs=[paired, whole, whole],
        scratch_shapes=[pltpu.VMEM((LEN, 128), F32)] * 2,
        compiler_params=pltpu.CompilerParams(vmem_limit_bytes=48 << 20),
        cost_estimate=pl.CostEstimate(
            flops=24 << 30, bytes_accessed=8 << 20, transcendentals=8 << 20
        ),
        name="attend_back",
    )(lengths, queries, keys, values, grad_heads, cosine, sine)


def ring_place(index, count):
    odd = index % 2
    return (1 - odd) * (index // 2) + odd * (count - 1 - index // 2)


def ring_member(place, count):
    high = place // (count // 2)
    return (1 - high) * (2 * place) + high * (2 * (count - 1 - place) + 1)


def ring_setup(count, peers=None, more=()):
    place = ring_place(lax.axis_index("dp"), count)
    ahead = ring_member((place + 1) % count, count)
    behind = ring_member((place + count - 1) % count, count)
    barrier = pltpu.get_barrier_semaphore()
    peers = (peers or [{"dp": ahead}, {"dp": behind}]) + list(more)
    for other in peers:
        pl.semaphore_signal(barrier, inc=1, device_id=other, device_id_type=MESH_ID)
    pl.semaphore_wait(barrier, len(peers))
    return place, (ahead, behind)


def member_at(place, side, steps, count):
    if side == 0:
        return ring_member((place + count - steps) % count, count)
    return ring_member((place + steps) % count, count)


def piece(ref, shape, axis, member, side, part, parts, first=0):
    rows, cols = shape
    sub = rows // (2 * parts)
    start = (side * parts + part) * sub
    if axis is None:
        return ref.at[pl.ds(start, sub), first : first + cols]
    if axis == 0:
        return ref.at[pl.ds(pl.multiple_of(member * rows + start, sub), sub), :]
    return ref.at[pl.ds(start, sub), pl.ds(pl.multiple_of(member * cols, cols), cols)]


def gather_kernel(count, items, *refs):
    num = len(items)
    shards, outs = refs[:num], refs[num : 2 * num]
    stage = refs[2 * num : 3 * num]
    send_sems, recv_sems, local_sem = refs[3 * num :]
    place, neighbours = ring_setup(count)
    me = lax.axis_index("dp")
    slots = [(k, part) for k in range(num) for part in range(items[k][2])]

    def copy(step, side, slot):
        item, part = slots[slot]
        shape, axis, parts, _ = items[item]
        origin = member_at(place, side, step, count)
        target = piece(outs[item], shape, axis, origin, side, part, parts)
        return target, pltpu.make_async_remote_copy(
            src_ref=target,
            dst_ref=target,
            send_sem=send_sems.at[side, step, slot],
            recv_sem=recv_sems.at[side, step, slot],
            device_id={"dp": neighbours[side]},
            device_id_type=MESH_ID,
        )

    for slot, (item, part) in enumerate(slots):
        shape, axis, parts, first = items[item]
        for side in range(2):
            pltpu.make_async_remote_copy(
                src_ref=piece(shards[item], shape, None, 0, side, part, parts, first),
                dst_ref=piece(outs[item], shape, axis, me, side, part, parts),
                send_sem=send_sems.at[side, 0, slot],
                recv_sem=recv_sems.at[side, 0, slot],
                device_id={"dp": neighbours[side]},
                device_id_type=MESH_ID,
            ).start()
    loads = [
        pltpu.make_async_copy(
            shards[k].at[:, items[k][3] : items[k][3] + items[k][0][1]],
            stage[k],
            local_sem.at[k],
        )
        for k in range(num)
    ]
    for load in loads:
        load.start()
    stores = []
    for k in range(num):
        loads[k].wait()
        shape, axis, parts, _ = items[k]
        rows, cols = shape
        if axis == 0:
            own = outs[k].at[pl.ds(pl.multiple_of(me * rows, rows), rows), :]
        else:
            own = outs[k].at[:, pl.ds(pl.multiple_of(me * cols, cols), cols)]
        stores.append(pltpu.make_async_copy(stage[k], own, local_sem.at[k]))
        stores[-1].start()

    def hop(step, carry):
        for slot in range(len(slots)):
            for side in range(2):
                copy(step - 1, side, slot)[1].wait_recv()
                copy(step, side, slot)[1].start()
        return carry

    lax.fori_loop(1, count - 1, hop, 0)
    for slot in range(len(slots)):
        for side in range(2):
            copy(count - 2, side, slot)[1].wait_recv()
    for store in stores:
        store.wait()

    def drain(step, carry):
        for slot in range(len(slots)):
            for side in range(2):
                copy(step, side, slot)[1].wait_send()
        return carry

    lax.fori_loop(0, count - 1, drain, 0)


def ring_gather(shards, axes, parts, count, collective_id, first=0):
    turned = [a == 1 and s.shape[1] % 128 != 0 for s, a in zip(shards, axes)]
    if any(turned):
        shards = [s.T if t else s for s, t in zip(shards, turned)]
        axes = [0 if t else a for a, t in zip(axes, turned)]
        outs = ring_gather(shards, axes, parts, count, collective_id)
        return [o.T if t else o for o, t in zip(outs, turned)]
    shapes = [(s.shape[0], s.shape[1] - first) for s in shards]
    items = tuple((s, a, q, first) for s, a, q in zip(shapes, axes, parts))
    slots = sum(parts)
    outs = [
        jax.ShapeDtypeStruct((s[0] * count, s[1]) if a == 0 else (s[0], s[1] * count), BF16)
        for s, a in zip(shapes, axes)
    ]
    num = len(shards)
    nbytes = sum(s.size * 2 * (count - 1) for s in shards)
    return pl.pallas_call(
        functools.partial(gather_kernel, count, items),
        out_shape=outs,
        in_specs=[pl.BlockSpec(memory_space=pl.ANY)] * num,
        out_specs=[pl.BlockSpec(memory_space=pl.ANY)] * num,
        scratch_shapes=[pltpu.VMEM(s, BF16) for s in shapes]
        + [
            pltpu.SemaphoreType.DMA((2, count - 1, slots)),
            pltpu.SemaphoreType.DMA((2, count - 1, slots)),
            pltpu.SemaphoreType.DMA((num,)),
        ],
        compiler_params=pltpu.CompilerParams(collective_id=collective_id, has_side_effects=True),
        cost_estimate=pl.CostEstimate(flops=0, bytes_accessed=20 * nbytes, transcendentals=0),
        name=f"ring_gather_{collective_id}",
    )(*shards)


def scatter_kernel(count, items, *refs):
    num = len(items)
    partials, outs = refs[:num], refs[num : 2 * num]
    own = refs[2 * num : 3 * num]
    held = refs[3 * num : 4 * num]
    total = refs[4 * num : 5 * num]
    send_sems, recv_sems, load_sems, store_sems = refs[5 * num :]
    slots = [(k, part) for k in range(num) for part in range(items[k][2])]

    def load(step, side, slot, place):
        item, part = slots[slot]
        shape, axis, parts = items[item]
        member = member_at(place, side, step + 1, count)
        return pltpu.make_async_copy(
            piece(partials[item], shape, axis, member, side, part, parts),
            own[item].at[side, step, part],
            load_sems.at[side, step, slot],
        )

    start_place = ring_place(lax.axis_index("dp"), count)

    def load_all(step, carry):
        for slot in range(len(slots)):
            for side in range(2):
                load(step, side, slot, start_place).start()
        return carry

    lax.fori_loop(0, count, load_all, 0)
    place, neighbours = ring_setup(count)

    def send(step, side, slot, source):
        item, part = slots[slot]
        return pltpu.make_async_remote_copy(
            src_ref=source,
            dst_ref=held[item].at[side, step, part],
            send_sem=send_sems.at[side, step, slot],
            recv_sem=recv_sems.at[side, step, slot],
            device_id={"dp": neighbours[side]},
            device_id_type=MESH_ID,
        )

    for slot, (item, part) in enumerate(slots):
        for side in range(2):
            load(0, side, slot, place).wait()
            send(0, side, slot, own[item].at[side, 0, part]).start()

    def hop(step, carry):
        for slot, (item, part) in enumerate(slots):
            for side in range(2):
                load(step, side, slot, place).wait()
                arrived = held[item].at[side, step - 1, part]
                send(step - 1, side, slot, arrived).wait_recv()
                arrived[...] = (
                    arrived[...].astype(jnp.float32)
                    + own[item][side, step, part].astype(jnp.float32)
                ).astype(jnp.bfloat16)
                send(step, side, slot, arrived).start()
        return carry

    lax.fori_loop(1, count - 1, hop, 0)
    last = count - 1
    stores = []
    for slot, (item, part) in enumerate(slots):
        shape, axis, parts = items[item]
        for side in range(2):
            load(last, side, slot, place).wait()
            arrived = held[item].at[side, last - 1, part]
            send(last - 1, side, slot, arrived).wait_recv()
            total[item][side, part] = arrived[...].astype(jnp.float32) + own[item][
                side, last, part
            ].astype(jnp.float32)
            stores.append(
                pltpu.make_async_copy(
                    total[item].at[side, part],
                    piece(outs[item], shape, None, 0, side, part, parts),
                    store_sems.at[side, slot],
                )
            )
            stores[-1].start()
    for store in stores:
        store.wait()

    def drain(step, carry):
        for slot, (item, part) in enumerate(slots):
            for side in range(2):
                send(step, side, slot, held[item].at[side, 0, part]).wait_send()
        return carry

    lax.fori_loop(0, count - 1, drain, 0)


def ring_scatter(partials, axes, parts, count, collective_id):
    turned = [a == 1 and p.shape[1] // count % 128 != 0 for p, a in zip(partials, axes)]
    if any(turned):
        partials = [p.T if t else p for p, t in zip(partials, turned)]
        axes = [0 if t else a for a, t in zip(axes, turned)]
        outs = ring_scatter(partials, axes, parts, count, collective_id)
        return [o.T if t else o for o, t in zip(outs, turned)]
    shapes = [
        (p.shape[0] // count, p.shape[1]) if a == 0 else (p.shape[0], p.shape[1] // count)
        for p, a in zip(partials, axes)
    ]
    items = tuple((s, a, q) for s, a, q in zip(shapes, axes, parts))
    slots = sum(parts)
    num = len(partials)

    def buffers(depth, dtype):
        return [
            pltpu.VMEM((2,) + depth + (q, s[0] // (2 * q), s[1]), dtype)
            for s, q in zip(shapes, parts)
        ]

    nbytes = sum(p.size * 2 for p in partials)
    return pl.pallas_call(
        functools.partial(scatter_kernel, count, items),
        out_shape=[jax.ShapeDtypeStruct(s, jnp.float32) for s in shapes],
        in_specs=[pl.BlockSpec(memory_space=pl.ANY)] * num,
        out_specs=[pl.BlockSpec(memory_space=pl.ANY)] * num,
        scratch_shapes=buffers((count,), jnp.bfloat16)
        + buffers((count - 1,), jnp.bfloat16)
        + buffers((), jnp.float32)
        + [
            pltpu.SemaphoreType.DMA((2, count - 1, slots)),
            pltpu.SemaphoreType.DMA((2, count - 1, slots)),
            pltpu.SemaphoreType.DMA((2, count, slots)),
            pltpu.SemaphoreType.DMA((2, slots)),
        ],
        compiler_params=pltpu.CompilerParams(
            collective_id=collective_id, has_side_effects=True, vmem_limit_bytes=48 << 20
        ),
        cost_estimate=pl.CostEstimate(flops=0, bytes_accessed=20 * nbytes, transcendentals=0),
        name=f"ring_scatter_{collective_id}",
    )(*partials)


class Job(NamedTuple):
    left: Any
    right: Any
    start: int
    cols: int
    into: Any = None
    target: int = 0
    pieces: tuple = ()


class Extra(NamedTuple):
    builder: Any
    given: list
    given_specs: list
    made: list
    made_specs: list
    spare: list


def scatter_dot_kernel(count, items, num_outs, num_bases, parts, extra, *refs):
    num = len(items)
    taken = 0

    def take(amount):
        nonlocal taken
        taken += amount
        return refs[taken - amount : taken]

    lefts, rights, _ = take(num), take(num), take(num_bases)
    given = take(len(extra.given) if extra else 0)
    outs = take(num_outs)
    made = take(len(extra.made) if extra else 0)
    left_bufs, right_bufs, firsts, owns, helds, totals = (take(num) for _ in range(6))
    send_sems, recv_sems, left_sems, right_sems, store_sems = take(5)
    beside = extra.builder(count, given, made, refs[taken:], right_bufs) if extra else None
    entry_place = ring_place(lax.axis_index("dp"), count)
    last = count - 1

    def load_right(item):
        _, half, start, _ = items[item]
        return pltpu.make_async_copy(
            rights[item].at[:, start : start + 2 * half], right_bufs[item], right_sems.at[item]
        )

    def load_left(step, side, item, place):
        block = items[item][0]
        member = member_at(place, side, step + 1, count)
        slot = step % 2
        return pltpu.make_async_copy(
            lefts[item].at[:, pl.ds(pl.multiple_of(member * block, block), block)],
            left_bufs[item].at[side, slot],
            left_sems.at[side, slot, item],
        )

    for item in range(num):
        load_right(item).start()
        for side in range(2):
            load_left(0, side, item, entry_place).start()
    if beside:
        beside.begin()
    place, neighbours = ring_setup(count, *(beside.peers() if beside else ()))
    pairs = [(item, side) for item in range(num) for side in range(2)]

    def send(step, side, item, part, source):
        return pltpu.make_async_remote_copy(
            src_ref=source.at[part],
            dst_ref=helds[item].at[side, step, part],
            send_sem=send_sems.at[side, step, item * parts + part],
            recv_sem=recv_sems.at[side, step, item * parts + part],
            device_id={"dp": neighbours[side]},
            device_id_type=MESH_ID,
        )

    def stores(item, side, part):
        block, _, _, places = items[item]
        rows = block // parts
        return [
            pltpu.make_async_copy(
                totals[item].at[side, part, :, source : source + cols],
                outs[out].at[part * rows : (part + 1) * rows, column : column + cols],
                store_sems.at[side, item * parts + part, k],
            )
            for k, (source, cols, out, column) in enumerate(places[side])
        ]

    for item in range(num):
        load_right(item).wait()

    def turn(step, carry):
        @pl.when(step < last)
        def _():
            for item, side in pairs:
                load_left(step + 1, side, item, place).start()

        for item in range(num):
            half = items[item][1]
            for side in range(2):
                load_left(step, side, item, place).wait()

            def own_sum(side, inner):
                cols = pl.ds(pl.multiple_of(side * half, half), half)
                owns[item][side] = tn_dot(
                    left_bufs[item][side, step % 2], right_bufs[item][:, cols]
                ).reshape(owns[item].shape[1:])
                return inner

            lax.fori_loop(0, 2, own_sum, 0)

        @pl.when(step == 0)
        def _():
            for part in range(parts):
                for item, side in pairs:
                    firsts[item][side, part] = owns[item][side, part].astype(BF16)
                    send(0, side, item, part, firsts[item].at[side]).start()

        if beside:
            beside.compute(step)

        @pl.when((step > 0) & (step < last))
        def _():
            for part in range(parts):
                for item, side in pairs:
                    arrived = helds[item].at[side, step - 1]
                    send(step - 1, side, item, part, arrived).wait_recv()
                    arrived[part] = (
                        arrived[part].astype(F32) + owns[item][side, part]
                    ).astype(BF16)
                    send(step, side, item, part, arrived).start()

        return carry

    lax.fori_loop(0, count, turn, 0)
    for part in range(parts):
        for item, side in pairs:
            arrived = helds[item].at[side, last - 1]
            send(last - 1, side, item, part, arrived).wait_recv()
            totals[item][side, part] = arrived[part].astype(F32) + owns[item][side, part]
            for copy in stores(item, side, part):
                copy.start()
    if beside:
        beside.finish()
    for part in range(parts):
        for item, side in pairs:
            for copy in stores(item, side, part):
                copy.wait()

    def drain(step, carry):
        for part in range(parts):
            for item, side in pairs:
                send(step, side, item, part, helds[item].at[side, 0]).wait_send()
        return carry

    lax.fori_loop(0, last, drain, 0)


def ring_scatter_dots(jobs, parts, count, collective_id, extra=None):
    rows = jobs[0].left.shape[0]
    items, shapes, bases, aliases = [], [], [], {}
    for job in jobs:
        block, half = job.left.shape[1] // count, job.cols // 2
        if job.pieces:
            places, column = ([], []), 0
            for cols in job.pieces:
                for side in range(2):
                    low = max(column, side * half)
                    high = min(column + cols, (side + 1) * half)
                    if low < high:
                        places[side].append(
                            (low - side * half, high - low, len(shapes), low - column)
                        )
                column += cols
                shapes.append((block, cols))
        else:
            places = [
                [(0, half, len(shapes), job.target + side * half)] for side in range(2)
            ]
            if job.into is None:
                shapes.append((block, job.cols))
            elif isinstance(job.into, int):
                shapes.append((block, job.into))
            else:
                aliases[2 * len(jobs) + len(bases)] = len(shapes)
                bases.append(job.into)
                shapes.append(job.into.shape)
        items.append((block, half, job.start, places))
    num = len(jobs)

    def buffers(depth, dtype):
        return [pltpu.VMEM(depth + (parts, b // parts, h), dtype) for b, h, _, _ in items]

    slots = num * parts
    flops = sum(2 * rows * j.left.shape[1] * j.cols for j in jobs)
    nbytes = sum(2 * j.left.shape[1] * j.cols for j in jobs)
    given, given_specs, made, made_specs, spare = extra[1:] if extra else ([], [], [], [], [])
    return pl.pallas_call(
        functools.partial(
            scatter_dot_kernel, count, items, len(shapes), len(bases), parts, extra
        ),
        out_shape=[jax.ShapeDtypeStruct(s, F32) for s in shapes] + made,
        in_specs=[ANY] * (2 * num + len(bases)) + given_specs,
        out_specs=[ANY] * len(shapes) + made_specs,
        input_output_aliases=aliases,
        scratch_shapes=[pltpu.VMEM((2, 2, rows, i[0]), BF16) for i in items]
        + [pltpu.VMEM((rows, 2 * i[1]), BF16) for i in items]
        + buffers((2,), BF16)
        + buffers((2,), F32)
        + buffers((2, count - 1), BF16)
        + buffers((2,), F32)
        + [
            pltpu.SemaphoreType.DMA((2, count - 1, slots)),
            pltpu.SemaphoreType.DMA((2, count - 1, slots)),
            pltpu.SemaphoreType.DMA((2, 2, num)),
            pltpu.SemaphoreType.DMA((num,)),
            pltpu.SemaphoreType.DMA((2, slots, 3)),
        ]
        + spare,
        compiler_params=pltpu.CompilerParams(
            collective_id=collective_id, has_side_effects=True, vmem_limit_bytes=60 << 20
        ),
        cost_estimate=pl.CostEstimate(
            flops=flops, bytes_accessed=20 * nbytes, transcendentals=0
        ),
        name=f"ring_scatter_{collective_id}",
    )(*[j.left for j in jobs], *[j.right for j in jobs], *bases, *given)


class ShareWork:
    def __init__(self, count, given, made, spare, rights):
        self.given, self.out = given, made[0]
        self.pair, self.first, self.sums, self.second, self.sems = spare
        self.count, self.group = count, self.second.shape[0] + 1
        self.row, self.col = lax.axis_index("dp"), lax.axis_index("tensor")

    def in_column(self, shift):
        return {"dp": (self.row + shift) % self.count}

    def in_group(self, shift):
        return {"tensor": (self.col + shift) % self.group}

    def peers(self):
        column = [self.in_column(s) for s in range(1, self.count)]
        return column, [self.in_group(s) for s in range(1, self.group)]

    def begin(self):
        pass

    def part(self, row):
        width = self.sums.shape[1]
        return pl.ds(pl.multiple_of(row * width, width), width)

    def move(self, stage, shift):
        if stage == 0:
            source = self.pair.at[:, self.part((self.row + shift) % self.count)]
            target, device, slot = self.first.at[shift - 1], self.in_column(shift), shift - 1
        else:
            source, target = self.sums, self.second.at[shift - 1]
            device, slot = self.in_group(shift), self.count + shift - 2
        return pltpu.make_async_remote_copy(
            src_ref=source,
            dst_ref=target,
            send_sem=self.sems.at[0, slot],
            recv_sem=self.sems.at[1, slot],
            device_id=device,
            device_id_type=MESH_ID,
        )

    def compute(self, step):
        @pl.when(step == 0)
        def _():
            self.pair[...] = self.given[0][...]
            self.pair[1:2, :] = self.given[1][...]
            for shift in range(1, self.count):
                self.move(0, shift).start()

        @pl.when(step == 5)
        def _():
            total = self.pair[:, self.part(self.row)]
            for shift in range(1, self.count):
                self.move(0, shift).wait()
                total = total + self.first[shift - 1]
            self.sums[...] = total
            for shift in range(1, self.group):
                self.move(1, shift).start()

    def finish(self):
        total = self.sums[...]
        for shift in range(1, self.group):
            self.move(1, shift).wait()
            total = total + self.second[shift - 1]
        share = total.shape[1] // self.group
        picked = jnp.zeros((8, share), F32)
        for col in range(self.group):
            picked = jnp.where(self.col == col, total[:, col * share : (col + 1) * share], picked)
        self.out[:, :share] = picked


class GatherWork:
    def __init__(self, count, given, made, spare, rights):
        self.own, self.out = given[0], made[0]
        self.stage, self.sems, self.local = spare
        self.col = lax.axis_index("tensor")
        self.rows = self.own.shape[0]
        self.parts = self.sems.shape[2]

    def core(self):
        return {"tensor": self.col + 1 - 2 * (self.col % 2)}

    def across(self):
        return {"tensor": (self.col + 2) % 4}

    def peers(self):
        return None, [self.core(), self.across()]

    def begin(self):
        pltpu.make_async_copy(self.own, self.stage, self.local).start()

    def spot(self, member, part):
        size = self.rows // self.parts
        return pl.ds(pl.multiple_of(member * self.rows + part * size, size), size)

    def move(self, kind, part):
        size = self.rows // self.parts
        member = (self.col + 2) % 4 if kind == 2 else self.col
        target = self.out.at[self.spot(member, part), :]
        source = target if kind == 2 else self.own.at[part * size : (part + 1) * size, :]
        return pltpu.make_async_remote_copy(
            src_ref=source,
            dst_ref=target,
            send_sem=self.sems.at[0, kind, part],
            recv_sem=self.sems.at[1, kind, part],
            device_id=self.across() if kind == 0 else self.core(),
            device_id_type=MESH_ID,
        )

    def keep(self):
        here = pl.ds(pl.multiple_of(self.col * self.rows, self.rows), self.rows)
        return pltpu.make_async_copy(self.stage, self.out.at[here, :], self.local)

    def compute(self, step):
        @pl.when(step == 0)
        def _():
            for part in range(self.parts):
                self.move(0, part).start()
                self.move(1, part).start()
            pltpu.make_async_copy(self.own, self.stage, self.local).wait()
            self.keep().start()

        for part, turn in enumerate((2, 4, 5, 6)):

            @pl.when(step == turn)
            def _():
                self.move(0, part).wait_recv()
                self.move(2, part).start()

    def finish(self):
        for part in range(self.parts):
            self.move(0, part).wait_send()
            self.move(1, part).wait()
            self.move(2, part).wait()
        self.keep().wait()


def gather_work(own):
    rows, width = own.shape
    return Extra(
        GatherWork,
        [own],
        [ANY],
        [jax.ShapeDtypeStruct((4 * rows, width), BF16)],
        [ANY],
        [
            pltpu.VMEM(own.shape, BF16),
            pltpu.SemaphoreType.DMA((2, 3, 4)),
            pltpu.SemaphoreType.DMA,
        ],
    )


def share_work(first, second, count, group):
    width = first.shape[1] // count
    vmem = pl.BlockSpec(memory_space=pltpu.VMEM)
    return Extra(
        ShareWork,
        [first, second],
        [vmem] * 2,
        [jax.ShapeDtypeStruct((8, 128), F32)],
        [vmem],
        [
            pltpu.VMEM(first.shape, F32),
            pltpu.VMEM((count - 1, 8, width), F32),
            pltpu.VMEM((8, width), F32),
            pltpu.VMEM((group - 1, 8, width), F32),
            pltpu.SemaphoreType.DMA((2, count + group - 2)),
        ],
    )


class NormWork:
    def __init__(self, count, given, made, spare, rights):
        self.grads, self.gates = given[:2], tuple(given[2:4])
        self.up, self.down = given[4:]
        self.outs = made
        self.grad_bufs, self.row_bufs, self.down_bufs, self.stage = spare[0], *spare[1:4]
        self.grad_sems, self.row_sems, self.down_sems, self.out_sems = spare[4:]
        self.act = rights[0]
        self.count = count
        self.block = self.row_bufs.shape[2]

    def load_grad(self, which):
        return pltpu.make_async_copy(
            self.grads[which], self.grad_bufs.at[which], self.grad_sems.at[which]
        )

    def spot(self, step):
        return pl.ds(pl.multiple_of(step * self.block, self.block), self.block)

    def loads(self, step):
        slot = step % 2
        edge = self.gates[0].shape[1]
        gate = self.row_bufs.at[0, slot]
        targets = [gate.at[:, :edge], gate.at[:, edge:], self.row_bufs.at[1, slot]]
        rows = [
            pltpu.make_async_copy(
                source.at[self.spot(step), :], target, self.row_sems.at[which, slot]
            )
            for which, (source, target) in enumerate(zip(self.gates + (self.up,), targets))
        ]
        down = pltpu.make_async_copy(
            self.down.at[:, self.spot(step)], self.down_bufs.at[slot], self.down_sems.at[slot]
        )
        return rows + [down]

    def store(self, which, step):
        slot = step % 2
        return pltpu.make_async_copy(
            self.stage.at[which, slot],
            self.outs[which].at[:, self.spot(step)],
            self.out_sems.at[which, slot],
        )

    def begin(self):
        for which in range(2):
            self.load_grad(which).start()
        for copy in self.loads(0):
            copy.start()

    def peers(self):
        return ()

    def compute(self, step):
        @pl.when(step < self.count - 1)
        def _():
            for copy in self.loads(step + 1):
                copy.start()

        @pl.when(step == 0)
        def _():
            for which in range(2):
                self.load_grad(which).wait()

        @pl.when(step >= 2)
        def _():
            for which in range(2):
                self.store(which, step - 2).wait()

        for copy in self.loads(step):
            copy.wait()
        slot = step % 2

        def lines(index, carry):
            band = pl.ds(pl.multiple_of(index * 256, 256), 256)
            norm = nt_dot(self.grad_bufs[0, band, :], self.row_bufs[0, slot])
            norm += nt_dot(self.grad_bufs[1, band, :], self.row_bufs[1, slot])
            self.stage[0, slot, band, :] = norm.astype(BF16)
            value = jnp.dot(
                self.act[band, :], self.down_bufs[slot], preferred_element_type=F32
            )
            self.stage[1, slot, band, :] = value.astype(BF16)
            return carry

        lax.fori_loop(0, self.act.shape[0] // 256, lines, 0)
        for which in range(2):
            self.store(which, step).start()

    def finish(self):
        for step in range(max(self.count - 2, 0), self.count):
            for which in range(2):
                self.store(which, step).wait()


def down_ring(grad_branch, activated, grad_gate, grad_up, gates, up_all, down_all, count, cid):
    rows, hidden = activated.shape
    width = up_all.shape[0]
    block = width // count
    wide = jax.ShapeDtypeStruct((rows, width), BF16)
    spare = [
        pltpu.VMEM((2, rows, hidden), BF16),
        pltpu.VMEM((2, 2, block, hidden), BF16),
        pltpu.VMEM((2, hidden, block), BF16),
        pltpu.VMEM((2, 2, rows, block), BF16),
        pltpu.SemaphoreType.DMA((2,)),
        pltpu.SemaphoreType.DMA((3, 2)),
        pltpu.SemaphoreType.DMA((2,)),
        pltpu.SemaphoreType.DMA((2, 2)),
    ]
    given = [grad_gate, grad_up, *gates, up_all, down_all]
    return ring_scatter_dots(
        [Job(grad_branch, activated, 0, hidden)],
        2,
        count,
        cid,
        Extra(NormWork, given, [ANY] * 6, [wide, wide], [ANY] * 2, spare),
    )


def mlp_kernel(count, *refs):
    x_hbm, wg_hbm, wg_rest, wu_hbm, shard, gb_hbm = refs[:6]
    act_hbm, gg_hbm, gu_hbm, down_all = refs[6:10]
    x_buf, gb_buf, w_bufs, gate_slope, up_slope, acc, half_bufs, stage, own_stage = refs[10:19]
    send_sems, recv_sems, w_sems, in_sems, half_sems, out_sems, local_sem = refs[19:]
    rows, width = x_buf.shape
    hidden = acc.shape[1]
    block = width // count
    cols = w_bufs.shape[-1]
    steps = hidden // cols
    half = hidden // 2
    parts = send_sems.shape[2]
    me = lax.axis_index("dp")

    gate_steps = wg_hbm.shape[1] // cols

    def load_weights(step, which, source=None):
        start = step - gate_steps if source is wg_rest else step
        source = (wg_hbm, wu_hbm)[which] if source is None else source
        return pltpu.make_async_copy(
            source.at[:, pl.ds(pl.multiple_of(start * cols, cols), cols)],
            w_bufs.at[which, step % 2],
            w_sems.at[which, step % 2],
        )

    def fetch(step):
        load_weights(step, 1).start()

        @pl.when(step < gate_steps)
        def _():
            load_weights(step, 0).start()

        @pl.when(step >= gate_steps)
        def _():
            load_weights(step, 0, wg_rest).start()

    load_x = pltpu.make_async_copy(x_hbm, x_buf, in_sems.at[0])
    load_gb = pltpu.make_async_copy(gb_hbm, gb_buf, in_sems.at[1])
    load_own = pltpu.make_async_copy(shard, own_stage, local_sem)
    load_x.start()
    for which in range(2):
        load_weights(0, which).start()
    load_own.start()
    load_gb.start()
    place, neighbours = ring_setup(count)

    def target(ref, member, side, part):
        return piece(ref, (hidden, block), 1, member, side, part, parts)

    def hop(step, side, part):
        ref = target(down_all, member_at(place, side, step, count), side, part)
        return pltpu.make_async_remote_copy(
            src_ref=ref,
            dst_ref=ref,
            send_sem=send_sems.at[side, step, part],
            recv_sem=recv_sems.at[side, step, part],
            device_id={"dp": neighbours[side]},
            device_id_type=MESH_ID,
        )

    for part in range(parts):
        for side in range(2):
            pltpu.make_async_remote_copy(
                src_ref=piece(shard, (hidden, block), None, 0, side, part, parts),
                dst_ref=target(down_all, me, side, part),
                send_sem=send_sems.at[side, 0, part],
                recv_sem=recv_sems.at[side, 0, part],
                device_id={"dp": neighbours[side]},
                device_id_type=MESH_ID,
            ).start()

    def pump(step):
        for part in range(parts):
            for side in range(2):
                hop(step - 1, side, part).wait_recv()
                hop(step, side, part).start()

    load_own.wait()
    store_own = pltpu.make_async_copy(
        own_stage, down_all.at[:, pl.ds(pl.multiple_of(me * block, block), block)], local_sem
    )
    store_own.start()
    load_x.wait()

    def store(ref, which, step):
        return pltpu.make_async_copy(
            stage.at[which, step % 2],
            ref.at[:, pl.ds(pl.multiple_of(step * cols, cols), cols)],
            out_sems.at[which, step % 2],
        )

    def forward(step, carry):
        @pl.when(step + 1 < steps)
        def _():
            fetch(step + 1)

        @pl.when(step >= 2)
        def _():
            store(act_hbm, 0, step - 2).wait()

        load_weights(step, 1).wait()

        @pl.when(step < gate_steps)
        def _():
            load_weights(step, 0).wait()

        @pl.when(step >= gate_steps)
        def _():
            load_weights(step, 0, wg_rest).wait()

        here = pl.ds(pl.multiple_of(step * cols, cols), cols)
        for top in range(0, rows, 256):
            band = pl.ds(top, 256)
            lines = x_buf[band, :]
            gate = jnp.dot(lines, w_bufs[0, step % 2], preferred_element_type=F32)
            up = jnp.dot(lines, w_bufs[1, step % 2], preferred_element_type=F32)
            sig = jax.nn.sigmoid(gate)
            silu = gate * sig
            stage[0, step % 2, band, :] = (silu * up).astype(BF16)
            gate_slope[band, here] = up * sig * (1.0 + gate * (1.0 - sig))
            up_slope[band, here] = silu
            acc[band, here] = jnp.zeros((256, cols), F32)
        store(act_hbm, 0, step).start()

        turn = (step + 1) // 2

        @pl.when((step % 2 == 1) & (turn <= count - 2))
        def _():
            pump(turn)

        return carry

    lax.fori_loop(0, steps, forward, 0)
    for step in range(max(steps - 2, 0), steps):
        store(act_hbm, 0, step).wait()
    pumped = min(steps // 2, count - 2)
    load_gb.wait()

    def load_half(step, side):
        member = member_at(place, side, step, count)
        return pltpu.make_async_copy(
            down_all.at[
                pl.ds(side * half, half), pl.ds(pl.multiple_of(member * block, block), block)
            ],
            half_bufs.at[side],
            half_sems.at[side],
        )

    def backward(step, carry):
        @pl.when((step > pumped) & (step <= count - 2))
        def _():
            pump(step)

        @pl.when(step == count - 1)
        def _():
            for part in range(parts):
                for side in range(2):
                    hop(count - 2, side, part).wait_recv()

        for side in range(2):
            load_half(step, side).start()
        for side in range(2):
            member = member_at(place, side, step, count)
            load_half(step, side).wait()
            here = pl.ds(pl.multiple_of(member * block, block), block)
            spot = pl.ds(side * half, half)

            def lines(index, carry):
                band = pl.ds(pl.multiple_of(index * 256, 256), 256)
                acc[band, spot] += nt_dot(gb_buf[band, here], half_bufs[side])
                return carry

            lax.fori_loop(0, rows // 256, lines, 0)

        return carry

    store_own.wait()
    lax.fori_loop(0, count, backward, 0)

    def slopes(step, carry):
        @pl.when(step >= 2)
        def _():
            store(gg_hbm, 1, step - 2).wait()
            store(gu_hbm, 2, step - 2).wait()

        here = pl.ds(pl.multiple_of(step * cols, cols), cols)

        def lines(index, carry):
            band = pl.ds(pl.multiple_of(index * 256, 256), 256)
            value = acc[band, here]
            stage[1, step % 2, band, :] = (value * gate_slope[band, here]).astype(BF16)
            stage[2, step % 2, band, :] = (value * up_slope[band, here]).astype(BF16)
            return carry

        lax.fori_loop(0, rows // 256, lines, 0)
        store(gg_hbm, 1, step).start()
        store(gu_hbm, 2, step).start()
        return carry

    lax.fori_loop(0, steps, slopes, 0)
    for step in range(max(steps - 2, 0), steps):
        store(gg_hbm, 1, step).wait()
        store(gu_hbm, 2, step).wait()

    def drain(step, carry):
        for part in range(parts):
            for side in range(2):
                hop(step, side, part).wait_send()
        return carry

    lax.fori_loop(0, count - 1, drain, 0)


def mlp_ring(rows_mlp, gates, up_all, w_down, grad_branch, count, collective_id):
    rows, width = rows_mlp.shape
    hidden, block = w_down.shape
    cols, parts = 256, 2
    wide = jax.ShapeDtypeStruct((rows, hidden), BF16)
    return pl.pallas_call(
        functools.partial(mlp_kernel, count),
        out_shape=[wide] * 3 + [jax.ShapeDtypeStruct((hidden, width), BF16)],
        in_specs=[ANY] * 6,
        out_specs=[pl.BlockSpec(memory_space=pl.ANY)] * 4,
        scratch_shapes=[
            pltpu.VMEM((rows, width), BF16),
            pltpu.VMEM((rows, width), BF16),
            pltpu.VMEM((2, 2, width, cols), BF16),
            pltpu.VMEM((rows, hidden), F32),
            pltpu.VMEM((rows, hidden), F32),
            pltpu.VMEM((rows, hidden), F32),
            pltpu.VMEM((2, hidden // 2, block), BF16),
            pltpu.VMEM((3, 2, rows, cols), BF16),
            pltpu.VMEM((hidden, block), BF16),
            pltpu.SemaphoreType.DMA((2, count - 1, parts)),
            pltpu.SemaphoreType.DMA((2, count - 1, parts)),
            pltpu.SemaphoreType.DMA((2, 2)),
            pltpu.SemaphoreType.DMA((2,)),
            pltpu.SemaphoreType.DMA((2,)),
            pltpu.SemaphoreType.DMA((3, 2)),
            pltpu.SemaphoreType.DMA,
        ],
        compiler_params=pltpu.CompilerParams(
            collective_id=collective_id, has_side_effects=True, vmem_limit_bytes=60 << 20
        ),
        cost_estimate=pl.CostEstimate(
            flops=6 * rows * width * hidden,
            bytes_accessed=40 * hidden * width,
            transcendentals=rows * hidden,
        ),
        name="mlp_ring",
    )(rows_mlp, *gates, up_all, w_down, grad_branch)


class HeadWork:
    def __init__(self, count, given, made, spare, rights):
        self.length, self.gain, self.sources = given[0], given[1], given[2:]
        self.grads_out, self.token_out, self.gain_out = made
        num = len(self.sources)
        self.bufs = spare[:num]
        self.heads, self.grads, self.acc_k, self.acc_v, self.stage = spare[num : num + 5]
        self.stats, self.inner, self.bias = spare[num + 5 : num + 8]
        self.in_sems, self.out_sems = spare[num + 8 :]

    def peers(self):
        return ()

    def load(self, which):
        return pltpu.make_async_copy(
            self.sources[which], self.bufs[which], self.in_sems.at[which]
        )

    def begin(self):
        for which in range(len(self.sources)):
            self.load(which).start()
        self.gain_out[...] = jnp.zeros_like(self.gain_out)
        self.acc_k[...] = jnp.zeros_like(self.acc_k)
        self.acc_v[...] = jnp.zeros_like(self.acc_v)
        key_pos = lax.broadcasted_iota(jnp.int32, self.bias.shape, 0)
        self.bias[...] = jnp.where(key_pos < self.length[0], 0.0, -1e30)

    def store(self, band):
        rows = self.stage.shape[1]
        return pltpu.make_async_copy(
            self.stage.at[band % 2],
            self.token_out.at[pl.ds(pl.multiple_of(band * rows, rows), rows), :],
            self.out_sems.at[band % 2],
        )

    def store_grads(self):
        return pltpu.make_async_copy(self.grads, self.grads_out, self.out_sems.at[2])

    def tokens(self, band):
        w_query, w_key, w_value, normed = self.bufs[9:]
        rows = self.stage.shape[1]
        inner = w_query.shape[1]

        @pl.when(band >= 2)
        def _():
            self.store(band - 2).wait()

        lines = pl.ds(pl.multiple_of(band * rows, rows), rows)

        def columns(index, carry):
            cols = pl.ds(pl.multiple_of(index * 512, 512), 512)
            value = nt_dot(self.grads[lines, :inner], w_query[cols, :])
            value += nt_dot(self.grads[lines, inner : inner + 128], w_key[cols, :])
            value += nt_dot(self.grads[lines, inner + 128 :], w_value[cols, :])
            self.stage[band % 2, :, cols] = value.astype(BF16)
            scaled = value * normed[lines, cols].astype(F32)
            self.gain_out[0:1, cols] += jnp.sum(scaled, axis=0, keepdims=True)
            return carry

        lax.fori_loop(0, w_query.shape[0] // 512, columns, 0)
        self.store(band).start()

    def compute(self, step):
        grad_attn, w_output, queries, keys, values, cosine, sine, outs, stats = self.bufs[:9]
        inner = queries.shape[1]
        pairs = inner // 128

        @pl.when(step == 0)
        def _():
            for which in range(2):
                self.load(which).wait()

            def band(index, carry):
                rows = pl.ds(pl.multiple_of(index * 256, 256), 256)
                self.heads[rows, :] = nt_dot(grad_attn[rows, :], w_output[...]).astype(BF16)
                return carry

            lax.fori_loop(0, LEN // 256, band, 0)

        @pl.when(step == 1)
        def _():
            for which in range(2, 9):
                self.load(which).wait()

            self.stats[...] = jnp.transpose(stats[...])

            def products(index, carry):
                rows = pl.ds(pl.multiple_of(index * 256, 256), 256)
                kept = jnp.zeros((256, 128), F32)
                for pair in range(pairs):
                    cols = slice(pair * 128, (pair + 1) * 128)
                    kept = row_products(self.heads[rows, cols], outs[rows, cols], pair, kept)
                stats[rows, :] = kept
                return carry

            lax.fori_loop(0, LEN // 256, products, 0)
            self.inner[...] = jnp.transpose(stats[...])

        @pl.when(step == pairs + 1)
        def _():
            for which in range(9, len(self.sources)):
                self.load(which).wait()

        @pl.when((step >= 1) & (step <= pairs))
        def _():
            here = pl.ds(pl.multiple_of((step - 1) * 128, 128), 128)
            attend_back_tiles(
                step - 1, queries.at[:, here], keys, values, self.heads.at[:, here], cosine,
                sine, self.stats, self.inner, self.bias, self.grads.at[:, here],
                self.acc_k, self.acc_v,
            )

        @pl.when(step == pairs)
        def _():
            self.grads[:, inner : inner + 128] = rope_back(
                self.acc_k[...], cosine[...], sine[...]
            )
            self.grads[:, inner + 128 :] = self.acc_v[...].astype(BF16)
            self.store_grads().start()

        @pl.when((step > pairs) & (step <= pairs + 2))
        def _():
            def band(index, carry):
                self.tokens(2 * (step - pairs - 1) + index)
                return carry

            lax.fori_loop(0, 2, band, 0)

    def finish(self):
        self.gain_out[0:1, :] = self.gain_out[0:1, :] / self.gain[...]
        self.store_grads().wait()
        for band in (2, 3):
            self.store(band).wait()


def heads_ring(
    job, lengths, gain, grad_attn, w_output, qkv, tables, saved, weights, rows_attn, count, cid
):
    sources = [grad_attn, w_output, *qkv, *tables, *saved, *weights, rows_attn]
    rows, width = grad_attn.shape
    inner = qkv[0].shape[1]
    made = [
        jax.ShapeDtypeStruct((rows, inner + 256), BF16),
        jax.ShapeDtypeStruct((rows, width), BF16),
        jax.ShapeDtypeStruct((8, width), F32),
    ]
    spare = [pltpu.VMEM(g.shape, g.dtype) for g in sources] + [
        pltpu.VMEM((rows, inner), BF16),
        pltpu.VMEM((rows, inner + 256), BF16),
        pltpu.VMEM((rows, 128), F32),
        pltpu.VMEM((rows, 128), F32),
        pltpu.VMEM((2, rows // 4, width), BF16),
        pltpu.VMEM((128, rows), F32),
        pltpu.VMEM((128, rows), F32),
        pltpu.VMEM((rows, 128), F32),
        pltpu.SemaphoreType.DMA((len(sources),)),
        pltpu.SemaphoreType.DMA((3,)),
    ]
    vmem = pl.BlockSpec(memory_space=pltpu.VMEM)
    specs = [pl.BlockSpec(memory_space=pltpu.SMEM), vmem] + [ANY] * len(sources)
    return ring_scatter_dots(
        [job],
        2,
        count,
        cid,
        Extra(HeadWork, [lengths, gain] + sources, specs, made, [ANY, ANY, vmem], spare),
    )


def attend_ring_kernel(count, *refs):
    length_ref, shard, sources = refs[0], refs[1], refs[2:9]
    gathered, q_out, k_out, v_out, head_out, part_out, stats_out = refs[9:16]
    bufs = refs[16:23]
    q_buf, k_buf, v_buf, head_buf, stage, own, stats = refs[23:30]
    send_sems, recv_sems, in_sems, out_sems, local_sem = refs[30:]
    rows_buf, w_query, w_key, w_value, w_output, cosine, sine = bufs
    shape = own.shape
    me = lax.axis_index("dp")
    loads = [
        pltpu.make_async_copy(source, buf, in_sems.at[k])
        for k, (source, buf) in enumerate(zip(sources, bufs))
    ]
    for load in loads:
        load.start()
    load_own = pltpu.make_async_copy(shard.at[:, : shape[1]], own, local_sem)
    load_own.start()
    place, neighbours = ring_setup(count)

    def hop(step, side):
        ref = piece(gathered, shape, 0, member_at(place, side, step, count), side, 0, 1)
        return pltpu.make_async_remote_copy(
            src_ref=ref,
            dst_ref=ref,
            send_sem=send_sems.at[side, step],
            recv_sem=recv_sems.at[side, step],
            device_id={"dp": neighbours[side]},
            device_id_type=MESH_ID,
        )

    for side in range(2):
        pltpu.make_async_remote_copy(
            src_ref=piece(shard, shape, None, 0, side, 0, 1),
            dst_ref=piece(gathered, shape, 0, me, side, 0, 1),
            send_sem=send_sems.at[side, 0],
            recv_sem=recv_sems.at[side, 0],
            device_id={"dp": neighbours[side]},
            device_id_type=MESH_ID,
        ).start()

    def pump(step, carry=0):
        for side in range(2):
            hop(step - 1, side).wait_recv()
            hop(step, side).start()
        return carry

    load_own.wait()
    store_own = pltpu.make_async_copy(
        own, gathered.at[pl.ds(pl.multiple_of(me * shape[0], shape[0]), shape[0]), :], local_sem
    )
    store_own.start()
    for k in (0, 1, 2, 3, 5, 6):
        loads[k].wait()

    stats[...] = jnp.zeros_like(stats)

    def projection(band, carry):
        lines = pl.ds(pl.multiple_of(band * 256, 256), 256)
        project_rows(
            rows_buf[lines, :], w_query, w_key, w_value, cosine[lines, :], sine[lines, :],
            q_buf.at[lines, :], k_buf.at[lines, :], v_buf.at[lines, :],
        )
        return carry

    lax.fori_loop(0, LEN // 256, projection, 0)
    stores = [
        pltpu.make_async_copy(buf, out, out_sems.at[k])
        for k, (buf, out) in enumerate(
            ((q_buf, q_out), (k_buf, k_out), (v_buf, v_out), (head_buf, head_out))
        )
    ]
    for store in stores[:3]:
        store.start()
    pump(1)
    pairs = q_buf.shape[1] // 128

    def attention(pair, carry):
        here = pl.ds(pl.multiple_of(pair * 128, 128), 128)
        attend_pair(
            length_ref[0], pair, q_buf.at[:, here], k_buf, v_buf, head_buf.at[:, here], stats
        )

        @pl.when(pair + 2 <= count - 2)
        def _():
            pump(pair + 2)

        return carry

    lax.fori_loop(0, pairs, attention, 0)
    loads[4].wait()
    stores[3].start()
    store_stats = pltpu.make_async_copy(stats, stats_out, out_sems.at[6])
    store_stats.start()

    def store_part(band):
        return pltpu.make_async_copy(
            stage.at[band % 2],
            part_out.at[pl.ds(pl.multiple_of(band * 256, 256), 256), :],
            out_sems.at[4 + band % 2],
        )

    def output(band, carry):
        @pl.when(band >= 2)
        def _():
            store_part(band - 2).wait()

        lines = pl.ds(pl.multiple_of(band * 256, 256), 256)

        def columns(index, inner):
            cols = pl.ds(pl.multiple_of(index * 512, 512), 512)
            stage[band % 2, :, cols] = jnp.dot(
                head_buf[lines, :], w_output[:, cols], preferred_element_type=F32
            ).astype(BF16)
            return inner

        lax.fori_loop(0, w_output.shape[1] // 512, columns, 0)
        store_part(band).start()

        @pl.when((band == 0) & (pairs + 2 <= count - 2))
        def _():
            pump(pairs + 2)

        return carry

    lax.fori_loop(0, LEN // 256, output, 0)
    lax.fori_loop(min(pairs + 3, count - 1), count - 1, pump, 0)
    for band in (LEN // 256 - 2, LEN // 256 - 1):
        store_part(band).wait()
    for store in stores:
        store.wait()
    store_stats.wait()
    store_own.wait()
    for side in range(2):
        hop(count - 2, side).wait_recv()

    def drain(step, carry):
        for side in range(2):
            hop(step, side).wait_send()
        return carry

    lax.fori_loop(0, count - 1, drain, 0)


def attend_ring(shard, edge, lengths, rows_attn, weights, tables, count, collective_id):
    sources = [rows_attn, *weights, *tables]
    rows, width = rows_attn.shape
    inner = weights[0].shape[1]

    def low(*shape):
        return jax.ShapeDtypeStruct(shape, BF16)

    return pl.pallas_call(
        functools.partial(attend_ring_kernel, count),
        out_shape=[
            low(shard.shape[0] * count, edge),
            low(rows, inner),
            low(rows, 128),
            low(rows, 128),
            low(rows, inner),
            low(rows, width),
            jax.ShapeDtypeStruct((rows, 128), F32),
        ],
        in_specs=[pl.BlockSpec(memory_space=pltpu.SMEM)] + [ANY] * (1 + len(sources)),
        out_specs=[ANY] * 7,
        scratch_shapes=[pltpu.VMEM(source.shape, source.dtype) for source in sources]
        + [
            pltpu.VMEM((rows, inner), BF16),
            pltpu.VMEM((rows, 128), BF16),
            pltpu.VMEM((rows, 128), BF16),
            pltpu.VMEM((rows, inner), BF16),
            pltpu.VMEM((2, 256, width), BF16),
            pltpu.VMEM((shard.shape[0], edge), BF16),
            pltpu.VMEM((rows, 128), F32),
            pltpu.SemaphoreType.DMA((2, count - 1)),
            pltpu.SemaphoreType.DMA((2, count - 1)),
            pltpu.SemaphoreType.DMA((len(sources),)),
            pltpu.SemaphoreType.DMA((7,)),
            pltpu.SemaphoreType.DMA,
        ],
        compiler_params=pltpu.CompilerParams(
            collective_id=collective_id, has_side_effects=True, vmem_limit_bytes=56 << 20
        ),
        cost_estimate=pl.CostEstimate(
            flops=24 << 30, bytes_accessed=60 << 20, transcendentals=8 << 20
        ),
        name="attend_ring",
    )(lengths, shard, *sources)


def ring_weight_grads(jobs, parts, count, collective_id):
    if all(left.shape[1] // count % 128 == 0 for left, _ in jobs):
        jobs = [Job(left, right, 0, right.shape[1]) for left, right in jobs]
        return ring_scatter_dots(jobs, parts, count, collective_id)
    partials = [tn_dot(left, right).astype(BF16) for left, right in jobs]
    num = len(jobs)
    return ring_scatter(partials, [0] * num, [parts] * num, count, collective_id)


def after(value, *deps):
    return lax.optimization_barrier((value,) + deps)[0]


def gather_rows(value):
    return lax.all_gather(value, "tensor", axis=0, tiled=True)


def scatter_rows(value):
    return lax.psum_scatter(value.astype(BF16), "tensor", scatter_dimension=0, tiled=True)


def share_kernel(count, group, parts_ref, out_ref, first, sums, second, sems):
    row, col = lax.axis_index("dp"), lax.axis_index("tensor")
    barrier = pltpu.get_barrier_semaphore()

    def in_group(shift):
        return {"tensor": (col + shift) % group}

    def in_column(shift):
        return {"dp": (row + shift) % count}

    def greet(device):
        pl.semaphore_signal(barrier, inc=1, device_id=device, device_id_type=MESH_ID)

    for shift in range(1, group):
        greet(in_group(shift))
    for shift in range(1, count):
        greet(in_column(shift))
    pl.semaphore_wait(barrier, group + count - 2)

    def exchange(shift, slot, source, target, device):
        return pltpu.make_async_remote_copy(
            src_ref=source,
            dst_ref=target,
            send_sem=sems.at[0, slot],
            recv_sem=sems.at[1, slot],
            device_id=device,
            device_id_type=MESH_ID,
        )

    moves = [
        exchange(s, s - 1, parts_ref.at[(col + s) % group], first.at[s - 1], in_group(s))
        for s in range(1, group)
    ]
    for move in moves:
        move.start()
    total = parts_ref[col]
    for shift, move in enumerate(moves):
        move.wait()
        total = total + first[shift]
    sums[...] = total
    moves = [
        exchange(
            s, group + s - 2, sums.at[(row + s) % count], second.at[s - 1], in_column(s)
        )
        for s in range(1, count)
    ]
    for move in moves:
        move.start()
    total = sums[row]
    for shift, move in enumerate(moves):
        move.wait()
        total = total + second[shift]
    out_ref[...] = total


def sum_shares(first, second, count, group, collective_id):
    share = first.shape[0] // (count * group)
    pair = jnp.stack([first, second]).reshape(2, count, group, share)
    parts = jnp.transpose(pair, (2, 1, 0, 3)).reshape(group, count, 1, 2 * share)
    width = (2 * share + 127) // 128 * 128
    parts = jnp.pad(parts, ((0, 0), (0, 0), (0, 7), (0, width - 2 * share)))
    tile = (8, width)
    out = pl.pallas_call(
        functools.partial(share_kernel, count, group),
        out_shape=jax.ShapeDtypeStruct(tile, F32),
        in_specs=[pl.BlockSpec(memory_space=pltpu.VMEM)],
        out_specs=pl.BlockSpec(memory_space=pltpu.VMEM),
        scratch_shapes=[
            pltpu.VMEM((group - 1, count) + tile, F32),
            pltpu.VMEM((count,) + tile, F32),
            pltpu.VMEM((count - 1,) + tile, F32),
            pltpu.SemaphoreType.DMA((2, group + count - 2)),
        ],
        compiler_params=pltpu.CompilerParams(collective_id=collective_id, has_side_effects=True),
        name="sum_shares",
    )(parts)
    return out[0, :share], out[0, share : 2 * share]


def dot(left, right):
    return jnp.dot(left, right, preferred_element_type=F32)


def body(
    count,
    group,
    tokens,
    lengths,
    attn_gain,
    w_query,
    w_key,
    w_value,
    w_output,
    mlp_gain,
    w_gate,
    w_up,
    w_down,
    cotangent,
):
    local_rows = tokens.shape[0]
    token_full = tokens.astype(F32)
    gain_attn = attn_gain.astype(F32)
    gain_mlp = mlp_gain.astype(F32)
    row_pos = lax.axis_index("tensor") * local_rows + jnp.arange(local_rows)
    valid_rows = (row_pos < lengths[0]).astype(F32)
    cot_masked = cotangent.astype(F32) * valid_rows[:, None]
    cosine, sine = rope_tables()

    inv_first = lax.rsqrt(jnp.mean(token_full * token_full, axis=1, keepdims=True) + epsilon)
    normed_attn = (token_full * inv_first * gain_attn).astype(BF16)
    rows_attn = gather_rows(normed_attn)
    query_all, key_all, value_all, output_all = ring_gather(
        [after(w_query, normed_attn), w_key, w_value, w_output],
        (0, 0, 0, 1), (1, 1, 1, 1), count, 0,
    )
    grad_branch = gather_rows(after(cot_masked.astype(BF16), rows_attn))
    fused = count == 8 and group == 4
    edge = 3 * w_gate.shape[1] // 8
    gates = []
    if fused:
        first_gate, queries, keys, values, head_out, attn_part, stats = attend_ring(
            w_gate,
            edge,
            lengths,
            rows_attn,
            (query_all, key_all, value_all, output_all),
            (cosine, sine),
            count,
            9,
        )
        gates.append(first_gate)
    else:
        queries, keys, values = project(rows_attn, query_all, key_all, value_all, cosine, sine)
        head_out = attend(queries, keys, values, lengths)
        attn_part = dot(head_out, output_all).astype(BF16)
    attn_branch = scatter_rows(attn_part)
    (gate_all,) = ring_gather(
        [after(w_gate, attn_part)], (0,), (2,), count, 1, edge if fused else 0
    )
    gates.append(gate_all)
    hidden = token_full + attn_branch.astype(F32)
    inv_second = lax.rsqrt(jnp.mean(hidden * hidden, axis=1, keepdims=True) + epsilon)
    normed_mlp = (hidden * inv_second * gain_mlp).astype(BF16)
    normed_mlp = after(normed_mlp, gate_all)
    rows_mlp = gather_rows(normed_mlp)
    (up_all,) = ring_gather([after(w_up, normed_mlp)], (0,), (2,), count, 2)
    if fused:
        activated, grad_gate_pre, grad_up_pre, down_all = mlp_ring(
            rows_mlp, gates, after(up_all, rows_mlp), w_down, grad_branch, count, 3
        )
        grad_down, norm_part, mlp_part = down_ring(
            grad_branch, activated, grad_gate_pre, grad_up_pre, gates, up_all, down_all,
            count, 4,
        )
    else:
        gate_proj = dot(rows_mlp, gate_all)
        up_proj = dot(rows_mlp, up_all)
        gate_sig = jax.nn.sigmoid(gate_proj)
        activated = (gate_proj * gate_sig * up_proj).astype(BF16)
        (down_all,) = ring_gather([after(w_down, up_all)], (1,), (2,), count, 3)
        mlp_part = dot(activated, down_all).astype(BF16)
        grad_act = nt_dot(grad_branch, down_all)
        grad_gate_pre = (
            grad_act * up_proj * gate_sig * (1.0 + gate_proj * (1.0 - gate_sig))
        ).astype(BF16)
        grad_up_pre = (grad_act * gate_proj * gate_sig).astype(BF16)
        norm_part = (nt_dot(grad_gate_pre, gate_all) + nt_dot(grad_up_pre, up_all)).astype(BF16)
        (grad_down,) = ring_weight_grads([(grad_branch, activated)], 2, count, 4)
    grad_norm_two = scatter_rows(norm_part).astype(F32)
    (grad_gate,) = ring_weight_grads(
        [(after(rows_mlp, norm_part), grad_gate_pre)], 2, count, 5
    )
    scaled_two = grad_norm_two * gain_mlp
    gain_two_part = jnp.sum(grad_norm_two * hidden * inv_second, axis=0)
    grad_hidden = (
        cot_masked
        + inv_second * scaled_two
        - hidden * inv_second**3 * jnp.mean(scaled_two * hidden, axis=1, keepdims=True)
    )
    grad_hidden = after(grad_hidden, grad_gate)
    if fused:
        middle = 3 * grad_up_pre.shape[1] // 8
        hidden_cols = grad_up_pre.shape[1]
        grad_up, grad_attn = ring_scatter_dots(
            [Job(rows_mlp, grad_up_pre, 0, middle, hidden_cols)],
            2, count, 6, gather_work(grad_hidden.astype(BF16)),
        )
        mlp_branch = scatter_rows(after(mlp_part, grad_attn))
        grad_up, grad_qkv, token_part, gain_one = heads_ring(
            Job(rows_mlp, grad_up_pre, middle, hidden_cols - middle, grad_up, middle),
            lengths,
            gain_attn[None, :],
            grad_attn,
            output_all,
            (queries, keys, values),
            (cosine, sine),
            (head_out, stats),
            (query_all, key_all, value_all),
            rows_attn,
            count,
            10,
        )
    else:
        grad_attn = gather_rows(grad_hidden.astype(BF16))
        mlp_branch = scatter_rows(after(mlp_part, grad_hidden))
        (grad_up,) = ring_weight_grads(
            [(after(rows_mlp, grad_hidden), grad_up_pre)], 2, count, 6
        )
        grad_heads = nt_dot(after(grad_attn, grad_up), output_all).astype(BF16)
        grad_qpre, grad_kpre, grad_vpre = attend_back(
            queries, keys, values, grad_heads, lengths, cosine, sine
        )
        token_part = (
            nt_dot(grad_qpre, query_all)
            + nt_dot(grad_kpre, key_all)
            + nt_dot(grad_vpre, value_all)
        ).astype(BF16)
    layer_out = (hidden + after(mlp_branch, token_part).astype(F32)).astype(BF16)
    grad_norm_one = scatter_rows(token_part).astype(F32)
    scaled_one = grad_norm_one * gain_attn
    grad_tokens = (
        grad_hidden
        + inv_first * scaled_one
        - token_full * inv_first**3 * jnp.mean(scaled_one * token_full, axis=1, keepdims=True)
    )
    if fused:
        query_cols, key_cols = queries.shape[1], keys.shape[1]
        rows_late = after(rows_attn, token_part)
        grad_query, grad_key, grad_value, grad_output, shares = ring_scatter_dots(
            [
                Job(
                    rows_late,
                    grad_qkv,
                    0,
                    query_cols + 2 * key_cols,
                    pieces=(query_cols, key_cols, key_cols),
                ),
                Job(grad_attn, head_out, 0, query_cols),
            ],
            1,
            count,
            7,
            share_work(gain_one, gain_two_part[None, :], count, group),
        )
        share = gain_two_part.shape[0] // (count * group)
        grad_attn_gain, grad_mlp_gain = shares[0, :share], shares[1, :share]
    else:
        grad_query, grad_key, grad_value, grad_output = ring_weight_grads(
            [
                (after(rows_attn, token_part), grad_qpre),
                (rows_attn, grad_kpre),
                (rows_attn, grad_vpre),
                (grad_attn, head_out),
            ],
            1, count, 7,
        )
        gain_one_part = jnp.sum(grad_norm_one * token_full * inv_first, axis=0)
        grad_attn_gain, grad_mlp_gain = sum_shares(
            after(gain_one_part, grad_query), gain_two_part, count, group, 8
        )
    grad_output, grad_down = grad_output.T, grad_down.T
    return (
        layer_out,
        grad_tokens,
        grad_query,
        grad_key,
        grad_value,
        grad_output,
        grad_gate,
        grad_up,
        grad_down,
        grad_attn_gain,
        grad_mlp_gain,
    )


def solution(mesh):
    rows = P(("dp", "tensor"), None)
    tall = P("dp", "tensor")
    wide = P("tensor", "dp")
    share = P(("dp", "tensor"))
    in_specs = (rows, P("dp"), P(), tall, tall, tall, wide, P(), tall, tall, wide, rows)
    out_specs = (rows, rows, tall, tall, tall, wide, tall, tall, wide, share, share)
    return jax.shard_map(
        functools.partial(body, mesh.shape["dp"], mesh.shape["tensor"]),
        mesh=mesh,
        in_specs=in_specs,
        out_specs=out_specs,
        check_vma=False,
    )
```

```python
import functools
from typing import Any, NamedTuple

import jax
import jax.numpy as jnp
from jax import lax
from jax.experimental import pallas as pl
from jax.experimental.pallas import tpu as pltpu
from jax.sharding import PartitionSpec as P

HD = 64
LEN = 1024
QB = 256

epsilon = 1e-05
theta = 500000.0
MESH_ID = pl.DeviceIdType.MESH
BF16 = jnp.bfloat16
ANY = pl.BlockSpec(memory_space=pl.ANY)
F32 = jnp.float32


def rope_frequencies():
    half_size = HD // 2
    base_freq = theta ** (-(jnp.arange(half_size, dtype=jnp.float32) * 2.0) / HD)
    wavelength = 2.0 * jnp.pi / base_freq
    smooth = (8192.0 / wavelength - 1.0) / 3.0
    middle = (1.0 - smooth) * base_freq / 32.0 + smooth * base_freq
    return jnp.where(
        wavelength < 2048.0, base_freq, jnp.where(wavelength > 8192.0, base_freq / 32.0, middle)
    )


def rope_tables():
    steps = jnp.arange(32, dtype=jnp.float32)[:, None]
    frequency = jnp.concatenate([rope_frequencies()] * 4)[None, :]
    low, high = steps * frequency, (32.0 * steps) * frequency
    cos_low, sin_low = jnp.cos(low)[None, :, :], jnp.sin(low)[None, :, :]
    cos_high, sin_high = jnp.cos(high)[:, None, :], jnp.sin(high)[:, None, :]
    sign = jnp.where(jnp.arange(128) % HD < HD // 2, -1.0, 1.0)
    cosine = cos_high * cos_low - sin_high * sin_low
    sine = (sin_high * cos_low + cos_high * sin_low) * sign
    return cosine.reshape(LEN, 128), sine.reshape(LEN, 128)


def lane_index(shape):
    return lax.broadcasted_iota(jnp.int32, shape, 1)


def swap_halves(value):
    low = lane_index(value.shape) % HD < HD // 2
    return jnp.where(low, pltpu.roll(value, 128 - HD // 2, 1), pltpu.roll(value, HD // 2, 1))


def nt_dot(left, right):
    return lax.dot_general(left, right, (((1,), (1,)), ((), ())), preferred_element_type=F32)


def tn_dot(left, right):
    return lax.dot_general(left, right, (((0,), (0,)), ((), ())), preferred_element_type=F32)


def rope(value, cosine, sine):
    return (value * cosine + swap_halves(value) * sine).astype(BF16)


def rope_back(grads, cosine, sine):
    return (grads * cosine - swap_halves(grads) * sine).astype(BF16)


def project_rows(rows, wq_ref, wk_ref, wv_ref, cosine, sine, q_ref, k_ref, v_ref):
    for block in range(q_ref.shape[1] // 256):
        cols = slice(block * 256, (block + 1) * 256)
        value = jnp.dot(rows, wq_ref[:, cols], preferred_element_type=F32)
        for half in range(2):
            start = block * 256 + half * 128
            q_ref[:, start : start + 128] = rope(
                value[:, half * 128 : half * 128 + 128], cosine, sine
            )
    k_ref[...] = rope(jnp.dot(rows, wk_ref[...], preferred_element_type=F32), cosine, sine)
    v_ref[...] = jnp.dot(rows, wv_ref[...], preferred_element_type=F32).astype(BF16)


def project_kernel(x_ref, wq_ref, wk_ref, wv_ref, cos_ref, sin_ref, q_ref, k_ref, v_ref):
    project_rows(
        x_ref[...], wq_ref, wk_ref, wv_ref, cos_ref[...], sin_ref[...], q_ref, k_ref, v_ref
    )


def project(rows, w_query, w_key, w_value, cosine, sine):
    total, width = rows.shape
    block = 256

    def whole(array):
        return pl.BlockSpec(array.shape, lambda i: (0, 0))

    def by_rows(cols):
        return pl.BlockSpec((block, cols), lambda i: (i, 0))

    shapes = [w_query.shape[1], w_key.shape[1], w_value.shape[1]]
    return pl.pallas_call(
        project_kernel,
        grid=(total // block,),
        out_shape=[jax.ShapeDtypeStruct((total, s), BF16) for s in shapes],
        in_specs=[by_rows(width), whole(w_query), whole(w_key), whole(w_value)]
        + [by_rows(128)] * 2,
        out_specs=[by_rows(s) for s in shapes],
        compiler_params=pltpu.CompilerParams(vmem_limit_bytes=32 << 20),
        cost_estimate=pl.CostEstimate(
            flops=2 * total * width * sum(shapes), bytes_accessed=8 << 20, transcendentals=0
        ),
        name="project",
    )(rows, w_query, w_key, w_value, cosine, sine)


def pick_head(pair, which, kv):
    moved = jnp.where(kv == which, pair, pltpu.roll(pair, HD, 1))
    return jnp.where(lane_index(pair.shape) // HD == kv, moved, jnp.zeros_like(moved))


def join_heads(first, second, kv):
    first = jnp.where(kv == 0, first, pltpu.roll(first, HD, 1))
    second = jnp.where(kv == 1, second, pltpu.roll(second, HD, 1))
    return jnp.where(lane_index(first.shape) < HD, first, second)


def attend_pair(length, pair_index, q_ref, k_ref, v_ref, o_ref, stats_ref=None):
    kv = pair_index // 2
    square = (QB, QB)
    causal = lax.broadcasted_iota(jnp.int32, square, 1) <= lax.broadcasted_iota(
        jnp.int32, square, 0
    )
    bias = jnp.where(lane_index((1, LEN)) < length, 0.0, -1e30)
    for block in range(LEN // QB):
        start = block * QB
        here = slice(start, start + QB)
        pair = q_ref[here, :].astype(F32) * HD**-0.5
        outs = []
        for which in range(2):
            query = pick_head(pair, which, kv).astype(BF16)
            near = jnp.where(causal, nt_dot(query, k_ref[here, :]), -1e30) + bias[:, here]
            top = jnp.max(near, axis=1, keepdims=True)
            if start:
                far = nt_dot(query, k_ref[:start, :]) + bias[:, :start]
                top = jnp.maximum(top, jnp.max(far, axis=1, keepdims=True))
                far = jnp.exp(far - top)
            near = jnp.exp(near - top)
            total = jnp.sum(near, axis=1, keepdims=True)
            if start:
                total = total + jnp.sum(far, axis=1, keepdims=True)
            inverse = 1.0 / total
            if stats_ref is not None:
                kept = stats_ref[here, :]
                mine = lane_index(kept.shape) == 2 * pair_index + which
                stats_ref[here, :] = jnp.where(mine, top + jnp.log(total), kept)
            out = jnp.dot(
                (near * inverse).astype(BF16), v_ref[here, :], preferred_element_type=F32
            )
            if start:
                out = out + jnp.dot(
                    (far * inverse).astype(BF16), v_ref[:start, :], preferred_element_type=F32
                )
            outs.append(out)
        o_ref[here, :] = join_heads(outs[0], outs[1], kv).astype(BF16)


def attend_kernel(length_ref, q_ref, k_ref, v_ref, o_ref):
    attend_pair(length_ref[0], pl.program_id(0), q_ref, k_ref, v_ref, o_ref)


def attend(queries, keys, values, lengths):
    pairs = queries.shape[1] // 128
    whole = pl.BlockSpec((LEN, 128), lambda i: (0, 0))
    paired = pl.BlockSpec((LEN, 128), lambda i: (0, i))
    return pl.pallas_call(
        attend_kernel,
        grid=(pairs,),
        out_shape=jax.ShapeDtypeStruct(queries.shape, BF16),
        in_specs=[pl.BlockSpec(memory_space=pltpu.SMEM), paired, whole, whole],
        out_specs=paired,
        compiler_params=pltpu.CompilerParams(vmem_limit_bytes=48 << 20),
        cost_estimate=pl.CostEstimate(
            flops=12 << 30, bytes_accessed=4 << 20, transcendentals=8 << 20
        ),
        name="attend",
    )(lengths, queries, keys, values)


def attend_back_pair(
    length, kv, q_ref, k_ref, v_ref, g_ref, cos_ref, sin_ref, gq_ref, acc_k, acc_v
):
    for block in range(LEN // QB):
        rows = slice(block * QB, (block + 1) * QB)
        keys = (block + 1) * QB
        pair = q_ref[rows, :].astype(F32) * HD**-0.5
        grad_pair = g_ref[rows, :].astype(F32)
        key_pos = lax.broadcasted_iota(jnp.int32, (keys, QB), 0)
        query_pos = block * QB + lax.broadcasted_iota(jnp.int32, (keys, QB), 1)
        allowed = (key_pos <= query_pos) & (key_pos < length)
        key_vecs = k_ref[:keys, :]
        grad_queries = []
        for which in range(2):
            query = pick_head(pair, which, kv).astype(BF16)
            grad = pick_head(grad_pair, which, kv).astype(BF16)
            scores = jnp.where(allowed, nt_dot(key_vecs, query), -1e30)
            exps = jnp.exp(scores - jnp.max(scores, axis=0, keepdims=True))
            probs = exps * (1.0 / jnp.sum(exps, axis=0, keepdims=True))
            grad_probs = nt_dot(v_ref[:keys, :], grad)
            inner = jnp.sum(probs * grad_probs, axis=0, keepdims=True)
            grad_scores = (probs * (grad_probs - inner)).astype(BF16)
            acc_v[:keys, :] += jnp.dot(probs.astype(BF16), grad, preferred_element_type=F32)
            acc_k[:keys, :] += jnp.dot(grad_scores, query, preferred_element_type=F32)
            grad_queries.append(tn_dot(grad_scores, key_vecs) * HD**-0.5)
        joined = join_heads(grad_queries[0], grad_queries[1], kv)
        gq_ref[rows, :] = rope_back(joined, cos_ref[rows, :], sin_ref[rows, :])


def row_products(grads, outs, pair_index, kept):
    product = grads.astype(F32) * outs.astype(F32)
    lanes = lane_index(product.shape)
    low = jnp.sum(jnp.where(lanes < HD, product, 0.0), axis=1, keepdims=True)
    high = jnp.sum(jnp.where(lanes < HD, 0.0, product), axis=1, keepdims=True)
    kept = jnp.where(lanes == 2 * pair_index, low, kept)
    return jnp.where(lanes == 2 * pair_index + 1, high, kept)


def attend_back_tiles(
    pair_index, q_ref, k_ref, v_ref, g_ref, cos_ref, sin_ref, stats_ref, inner_ref, bias_ref,
    gq_ref, acc_k, acc_v,
):
    kv = pair_index // 2
    square = (QB, QB)
    causal = lax.broadcasted_iota(jnp.int32, square, 0) <= lax.broadcasted_iota(
        jnp.int32, square, 1
    )
    for block in range(LEN // QB):
        rows = slice(block * QB, (block + 1) * QB)
        pair = q_ref[rows, :].astype(F32) * HD**-0.5
        grad_pair = g_ref[rows, :].astype(F32)
        queries, grads, tops, inners = [], [], [], []
        for which in range(2):
            queries.append(pick_head(pair, which, kv).astype(BF16))
            grads.append(pick_head(grad_pair, which, kv).astype(BF16))
            head = pl.ds(2 * pair_index + which, 1)
            tops.append(stats_ref[head, rows])
            inners.append(inner_ref[head, rows])
        grad_queries = [None, None]
        for tile in range(block + 1):
            here = slice(tile * QB, (tile + 1) * QB)
            key_vecs, value_vecs = k_ref[here, :], v_ref[here, :]
            bias = bias_ref[here, :]
            bias = jnp.concatenate([bias] * (QB // 128), axis=1)
            grad_key = grad_value = None
            for which in range(2):
                scores = nt_dot(key_vecs, queries[which]) + bias
                if tile == block:
                    scores = jnp.where(causal, scores, -1e30)
                probs = jnp.exp(scores - tops[which])
                grad_probs = nt_dot(value_vecs, grads[which])
                grad_scores = (probs * (grad_probs - inners[which])).astype(BF16)
                value = jnp.dot(probs.astype(BF16), grads[which], preferred_element_type=F32)
                key = jnp.dot(grad_scores, queries[which], preferred_element_type=F32)
                query = tn_dot(grad_scores, key_vecs)
                grad_value = value if which == 0 else grad_value + value
                grad_key = key if which == 0 else grad_key + key
                grad_queries[which] = query if tile == 0 else grad_queries[which] + query
            acc_v[here, :] += grad_value
            acc_k[here, :] += grad_key
        joined = join_heads(grad_queries[0], grad_queries[1], kv) * HD**-0.5
        gq_ref[rows, :] = rope_back(joined, cos_ref[rows, :], sin_ref[rows, :])


def attend_back_kernel(
    length_ref, q_ref, k_ref, v_ref, g_ref, cos_ref, sin_ref, gq_ref, gk_ref, gv_ref, acc_k, acc_v
):
    pair_index = pl.program_id(0)

    @pl.when(pair_index == 0)
    def _():
        acc_k[...] = jnp.zeros_like(acc_k)
        acc_v[...] = jnp.zeros_like(acc_v)

    attend_back_pair(
        length_ref[0], pair_index // 2, q_ref, k_ref, v_ref, g_ref, cos_ref, sin_ref, gq_ref,
        acc_k, acc_v,
    )

    @pl.when(pair_index == pl.num_programs(0) - 1)
    def _():
        gk_ref[...] = rope_back(acc_k[...], cos_ref[...], sin_ref[...])
        gv_ref[...] = acc_v[...].astype(BF16)


def attend_back(queries, keys, values, grad_heads, lengths, cosine, sine):
    pairs = queries.shape[1] // 128
    whole = pl.BlockSpec((LEN, 128), lambda i: (0, 0))
    paired = pl.BlockSpec((LEN, 128), lambda i: (0, i))
    narrow = jax.ShapeDtypeStruct((LEN, 128), BF16)
    return pl.pallas_call(
        attend_back_kernel,
        grid=(pairs,),
        out_shape=[jax.ShapeDtypeStruct(queries.shape, BF16), narrow, narrow],
        in_specs=[pl.BlockSpec(memory_space=pltpu.SMEM), paired, whole, whole, paired]
        + [whole] * 2,
        out_specs=[paired, whole, whole],
        scratch_shapes=[pltpu.VMEM((LEN, 128), F32)] * 2,
        compiler_params=pltpu.CompilerParams(vmem_limit_bytes=48 << 20),
        cost_estimate=pl.CostEstimate(
            flops=24 << 30, bytes_accessed=8 << 20, transcendentals=8 << 20
        ),
        name="attend_back",
    )(lengths, queries, keys, values, grad_heads, cosine, sine)


def ring_place(index, count):
    odd = index % 2
    return (1 - odd) * (index // 2) + odd * (count - 1 - index // 2)


def ring_member(place, count):
    high = place // (count // 2)
    return (1 - high) * (2 * place) + high * (2 * (count - 1 - place) + 1)


def ring_setup(count, peers=None, more=()):
    place = ring_place(lax.axis_index("dp"), count)
    ahead = ring_member((place + 1) % count, count)
    behind = ring_member((place + count - 1) % count, count)
    barrier = pltpu.get_barrier_semaphore()
    peers = (peers or [{"dp": ahead}, {"dp": behind}]) + list(more)
    for other in peers:
        pl.semaphore_signal(barrier, inc=1, device_id=other, device_id_type=MESH_ID)
    pl.semaphore_wait(barrier, len(peers))
    return place, (ahead, behind)


def member_at(place, side, steps, count):
    if side == 0:
        return ring_member((place + count - steps) % count, count)
    return ring_member((place + steps) % count, count)


def piece(ref, shape, axis, member, side, part, parts, first=0):
    rows, cols = shape
    sub = rows // (2 * parts)
    start = (side * parts + part) * sub
    if axis is None:
        return ref.at[pl.ds(start, sub), first : first + cols]
    if axis == 0:
        return ref.at[pl.ds(pl.multiple_of(member * rows + start, sub), sub), :]
    return ref.at[pl.ds(start, sub), pl.ds(pl.multiple_of(member * cols, cols), cols)]


def gather_kernel(count, items, *refs):
    num = len(items)
    shards, outs = refs[:num], refs[num : 2 * num]
    stage = refs[2 * num : 3 * num]
    send_sems, recv_sems, local_sem = refs[3 * num :]
    place, neighbours = ring_setup(count)
    me = lax.axis_index("dp")
    slots = [(k, part) for k in range(num) for part in range(items[k][2])]

    def copy(step, side, slot):
        item, part = slots[slot]
        shape, axis, parts, _ = items[item]
        origin = member_at(place, side, step, count)
        target = piece(outs[item], shape, axis, origin, side, part, parts)
        return target, pltpu.make_async_remote_copy(
            src_ref=target,
            dst_ref=target,
            send_sem=send_sems.at[side, step, slot],
            recv_sem=recv_sems.at[side, step, slot],
            device_id={"dp": neighbours[side]},
            device_id_type=MESH_ID,
        )

    for slot, (item, part) in enumerate(slots):
        shape, axis, parts, first = items[item]
        for side in range(2):
            pltpu.make_async_remote_copy(
                src_ref=piece(shards[item], shape, None, 0, side, part, parts, first),
                dst_ref=piece(outs[item], shape, axis, me, side, part, parts),
                send_sem=send_sems.at[side, 0, slot],
                recv_sem=recv_sems.at[side, 0, slot],
                device_id={"dp": neighbours[side]},
                device_id_type=MESH_ID,
            ).start()
    loads = [
        pltpu.make_async_copy(
            shards[k].at[:, items[k][3] : items[k][3] + items[k][0][1]],
            stage[k],
            local_sem.at[k],
        )
        for k in range(num)
    ]
    for load in loads:
        load.start()
    stores = []
    for k in range(num):
        loads[k].wait()
        shape, axis, parts, _ = items[k]
        rows, cols = shape
        if axis == 0:
            own = outs[k].at[pl.ds(pl.multiple_of(me * rows, rows), rows), :]
        else:
            own = outs[k].at[:, pl.ds(pl.multiple_of(me * cols, cols), cols)]
        stores.append(pltpu.make_async_copy(stage[k], own, local_sem.at[k]))
        stores[-1].start()

    def hop(step, carry):
        for slot in range(len(slots)):
            for side in range(2):
                copy(step - 1, side, slot)[1].wait_recv()
                copy(step, side, slot)[1].start()
        return carry

    lax.fori_loop(1, count - 1, hop, 0)
    for slot in range(len(slots)):
        for side in range(2):
            copy(count - 2, side, slot)[1].wait_recv()
    for store in stores:
        store.wait()

    def drain(step, carry):
        for slot in range(len(slots)):
            for side in range(2):
                copy(step, side, slot)[1].wait_send()
        return carry

    lax.fori_loop(0, count - 1, drain, 0)


def ring_gather(shards, axes, parts, count, collective_id, first=0):
    turned = [a == 1 and s.shape[1] % 128 != 0 for s, a in zip(shards, axes)]
    if any(turned):
        shards = [s.T if t else s for s, t in zip(shards, turned)]
        axes = [0 if t else a for a, t in zip(axes, turned)]
        outs = ring_gather(shards, axes, parts, count, collective_id)
        return [o.T if t else o for o, t in zip(outs, turned)]
    shapes = [(s.shape[0], s.shape[1] - first) for s in shards]
    items = tuple((s, a, q, first) for s, a, q in zip(shapes, axes, parts))
    slots = sum(parts)
    outs = [
        jax.ShapeDtypeStruct((s[0] * count, s[1]) if a == 0 else (s[0], s[1] * count), BF16)
        for s, a in zip(shapes, axes)
    ]
    num = len(shards)
    nbytes = sum(s.size * 2 * (count - 1) for s in shards)
    return pl.pallas_call(
        functools.partial(gather_kernel, count, items),
        out_shape=outs,
        in_specs=[pl.BlockSpec(memory_space=pl.ANY)] * num,
        out_specs=[pl.BlockSpec(memory_space=pl.ANY)] * num,
        scratch_shapes=[pltpu.VMEM(s, BF16) for s in shapes]
        + [
            pltpu.SemaphoreType.DMA((2, count - 1, slots)),
            pltpu.SemaphoreType.DMA((2, count - 1, slots)),
            pltpu.SemaphoreType.DMA((num,)),
        ],
        compiler_params=pltpu.CompilerParams(collective_id=collective_id, has_side_effects=True),
        cost_estimate=pl.CostEstimate(flops=0, bytes_accessed=20 * nbytes, transcendentals=0),
        name=f"ring_gather_{collective_id}",
    )(*shards)


def scatter_kernel(count, items, *refs):
    num = len(items)
    partials, outs = refs[:num], refs[num : 2 * num]
    own = refs[2 * num : 3 * num]
    held = refs[3 * num : 4 * num]
    total = refs[4 * num : 5 * num]
    send_sems, recv_sems, load_sems, store_sems = refs[5 * num :]
    slots = [(k, part) for k in range(num) for part in range(items[k][2])]

    def load(step, side, slot, place):
        item, part = slots[slot]
        shape, axis, parts = items[item]
        member = member_at(place, side, step + 1, count)
        return pltpu.make_async_copy(
            piece(partials[item], shape, axis, member, side, part, parts),
            own[item].at[side, step, part],
            load_sems.at[side, step, slot],
        )

    start_place = ring_place(lax.axis_index("dp"), count)

    def load_all(step, carry):
        for slot in range(len(slots)):
            for side in range(2):
                load(step, side, slot, start_place).start()
        return carry

    lax.fori_loop(0, count, load_all, 0)
    place, neighbours = ring_setup(count)

    def send(step, side, slot, source):
        item, part = slots[slot]
        return pltpu.make_async_remote_copy(
            src_ref=source,
            dst_ref=held[item].at[side, step, part],
            send_sem=send_sems.at[side, step, slot],
            recv_sem=recv_sems.at[side, step, slot],
            device_id={"dp": neighbours[side]},
            device_id_type=MESH_ID,
        )

    for slot, (item, part) in enumerate(slots):
        for side in range(2):
            load(0, side, slot, place).wait()
            send(0, side, slot, own[item].at[side, 0, part]).start()

    def hop(step, carry):
        for slot, (item, part) in enumerate(slots):
            for side in range(2):
                load(step, side, slot, place).wait()
                arrived = held[item].at[side, step - 1, part]
                send(step - 1, side, slot, arrived).wait_recv()
                arrived[...] = (
                    arrived[...].astype(jnp.float32)
                    + own[item][side, step, part].astype(jnp.float32)
                ).astype(jnp.bfloat16)
                send(step, side, slot, arrived).start()
        return carry

    lax.fori_loop(1, count - 1, hop, 0)
    last = count - 1
    stores = []
    for slot, (item, part) in enumerate(slots):
        shape, axis, parts = items[item]
        for side in range(2):
            load(last, side, slot, place).wait()
            arrived = held[item].at[side, last - 1, part]
            send(last - 1, side, slot, arrived).wait_recv()
            total[item][side, part] = arrived[...].astype(jnp.float32) + own[item][
                side, last, part
            ].astype(jnp.float32)
            stores.append(
                pltpu.make_async_copy(
                    total[item].at[side, part],
                    piece(outs[item], shape, None, 0, side, part, parts),
                    store_sems.at[side, slot],
                )
            )
            stores[-1].start()
    for store in stores:
        store.wait()

    def drain(step, carry):
        for slot, (item, part) in enumerate(slots):
            for side in range(2):
                send(step, side, slot, held[item].at[side, 0, part]).wait_send()
        return carry

    lax.fori_loop(0, count - 1, drain, 0)


def ring_scatter(partials, axes, parts, count, collective_id):
    turned = [a == 1 and p.shape[1] // count % 128 != 0 for p, a in zip(partials, axes)]
    if any(turned):
        partials = [p.T if t else p for p, t in zip(partials, turned)]
        axes = [0 if t else a for a, t in zip(axes, turned)]
        outs = ring_scatter(partials, axes, parts, count, collective_id)
        return [o.T if t else o for o, t in zip(outs, turned)]
    shapes = [
        (p.shape[0] // count, p.shape[1]) if a == 0 else (p.shape[0], p.shape[1] // count)
        for p, a in zip(partials, axes)
    ]
    items = tuple((s, a, q) for s, a, q in zip(shapes, axes, parts))
    slots = sum(parts)
    num = len(partials)

    def buffers(depth, dtype):
        return [
            pltpu.VMEM((2,) + depth + (q, s[0] // (2 * q), s[1]), dtype)
            for s, q in zip(shapes, parts)
        ]

    nbytes = sum(p.size * 2 for p in partials)
    return pl.pallas_call(
        functools.partial(scatter_kernel, count, items),
        out_shape=[jax.ShapeDtypeStruct(s, jnp.float32) for s in shapes],
        in_specs=[pl.BlockSpec(memory_space=pl.ANY)] * num,
        out_specs=[pl.BlockSpec(memory_space=pl.ANY)] * num,
        scratch_shapes=buffers((count,), jnp.bfloat16)
        + buffers((count - 1,), jnp.bfloat16)
        + buffers((), jnp.float32)
        + [
            pltpu.SemaphoreType.DMA((2, count - 1, slots)),
            pltpu.SemaphoreType.DMA((2, count - 1, slots)),
            pltpu.SemaphoreType.DMA((2, count, slots)),
            pltpu.SemaphoreType.DMA((2, slots)),
        ],
        compiler_params=pltpu.CompilerParams(
            collective_id=collective_id, has_side_effects=True, vmem_limit_bytes=48 << 20
        ),
        cost_estimate=pl.CostEstimate(flops=0, bytes_accessed=20 * nbytes, transcendentals=0),
        name=f"ring_scatter_{collective_id}",
    )(*partials)


class Job(NamedTuple):
    left: Any
    right: Any
    start: int
    cols: int
    into: Any = None
    target: int = 0
    pieces: tuple = ()


class Extra(NamedTuple):
    builder: Any
    given: list
    given_specs: list
    made: list
    made_specs: list
    spare: list


def scatter_dot_kernel(count, items, num_outs, num_bases, parts, extra, *refs):
    num = len(items)
    taken = 0

    def take(amount):
        nonlocal taken
        taken += amount
        return refs[taken - amount : taken]

    lefts, rights, _ = take(num), take(num), take(num_bases)
    given = take(len(extra.given) if extra else 0)
    outs = take(num_outs)
    made = take(len(extra.made) if extra else 0)
    left_bufs, right_bufs, firsts, owns, helds, totals = (take(num) for _ in range(6))
    send_sems, recv_sems, left_sems, right_sems, store_sems = take(5)
    beside = (
        extra.builder(count, given, made, refs[taken:], (left_bufs, right_bufs)) if extra else None
    )
    entry_place = ring_place(lax.axis_index("dp"), count)
    last = count - 1

    ready = [buf.shape[0] == 8 for buf in right_bufs]

    def load_right(item):
        _, half, start, _ = items[item]
        return pltpu.make_async_copy(
            rights[item].at[:, start : start + 2 * half], right_bufs[item], right_sems.at[item]
        )

    def load_left(step, side, item, place):
        block = items[item][0]
        member = member_at(place, side, step + 1, count)
        slot = step % 2
        here = pl.ds(pl.multiple_of(member * block, block), block)
        if ready[item]:
            half = items[item][1]
            source = lefts[item].at[here, side * half : (side + 1) * half]
        else:
            source = lefts[item].at[:, here]
        return pltpu.make_async_copy(
            source, left_bufs[item].at[side, slot], left_sems.at[side, slot, item]
        )

    for item in range(num):
        if not ready[item]:
            load_right(item).start()
        for side in range(2):
            load_left(0, side, item, entry_place).start()
    if beside:
        beside.begin()
    place, neighbours = ring_setup(count, *(beside.peers() if beside else ()))
    pairs = [(item, side) for item in range(num) for side in range(2)]

    def send(step, side, item, part, source):
        return pltpu.make_async_remote_copy(
            src_ref=source.at[part],
            dst_ref=helds[item].at[side, step, part],
            send_sem=send_sems.at[side, step, item * parts + part],
            recv_sem=recv_sems.at[side, step, item * parts + part],
            device_id={"dp": neighbours[side]},
            device_id_type=MESH_ID,
        )

    def stores(item, side, part):
        block, _, _, places = items[item]
        rows = block // parts
        return [
            pltpu.make_async_copy(
                totals[item].at[side, part, :, source : source + cols],
                outs[out].at[part * rows : (part + 1) * rows, column : column + cols],
                store_sems.at[side, item * parts + part, k],
            )
            for k, (source, cols, out, column) in enumerate(places[side])
        ]

    for item in range(num):
        if not ready[item]:
            load_right(item).wait()

    def turn(step, carry):
        @pl.when(step < last)
        def _():
            for item, side in pairs:
                load_left(step + 1, side, item, place).start()

        for item in range(num):
            half = items[item][1]
            for side in range(2):
                load_left(step, side, item, place).wait()

            if ready[item]:
                for side in range(2):
                    owns[item][side] = (
                        left_bufs[item][side, step % 2].astype(F32).reshape(owns[item].shape[1:])
                    )
                continue

            def own_sum(side, inner):
                cols = pl.ds(pl.multiple_of(side * half, half), half)
                owns[item][side] = tn_dot(
                    left_bufs[item][side, step % 2], right_bufs[item][:, cols]
                ).reshape(owns[item].shape[1:])
                return inner

            lax.fori_loop(0, 2, own_sum, 0)

        @pl.when(step == 0)
        def _():
            for part in range(parts):
                for item, side in pairs:
                    firsts[item][side, part] = owns[item][side, part].astype(BF16)
                    send(0, side, item, part, firsts[item].at[side]).start()

        if beside:
            beside.compute(step)

        @pl.when((step > 0) & (step < last))
        def _():
            for part in range(parts):
                for item, side in pairs:
                    arrived = helds[item].at[side, step - 1]
                    send(step - 1, side, item, part, arrived).wait_recv()
                    arrived[part] = (
                        arrived[part].astype(F32) + owns[item][side, part]
                    ).astype(BF16)
                    send(step, side, item, part, arrived).start()

        return carry

    lax.fori_loop(0, count, turn, 0)
    for part in range(parts):
        for item, side in pairs:
            arrived = helds[item].at[side, last - 1]
            send(last - 1, side, item, part, arrived).wait_recv()
            totals[item][side, part] = arrived[part].astype(F32) + owns[item][side, part]
            for copy in stores(item, side, part):
                copy.start()
    if beside:
        beside.finish()
    for part in range(parts):
        for item, side in pairs:
            for copy in stores(item, side, part):
                copy.wait()

    def drain(step, carry):
        for part in range(parts):
            for item, side in pairs:
                send(step, side, item, part, helds[item].at[side, 0]).wait_send()
        return carry

    lax.fori_loop(0, last, drain, 0)


def ring_scatter_dots(jobs, parts, count, collective_id, extra=None):
    rows = next((j.left.shape[0] for j in jobs if j.right is not None), 0)
    items, shapes, bases, aliases = [], [], [], {}
    for job in jobs:
        width = job.left.shape[1] if job.right is not None else job.left.shape[0]
        block, half = width // count, job.cols // 2
        if job.pieces:
            places, column = ([], []), 0
            for cols in job.pieces:
                for side in range(2):
                    low = max(column, side * half)
                    high = min(column + cols, (side + 1) * half)
                    if low < high:
                        places[side].append(
                            (low - side * half, high - low, len(shapes), low - column)
                        )
                column += cols
                shapes.append((block, cols))
        else:
            places = [
                [(0, half, len(shapes), job.target + side * half)] for side in range(2)
            ]
            if job.into is None:
                shapes.append((block, job.cols))
            elif isinstance(job.into, int):
                shapes.append((block, job.into))
            else:
                aliases[2 * len(jobs) + len(bases)] = len(shapes)
                bases.append(job.into)
                shapes.append(job.into.shape)
        items.append((block, half, job.start, places))
    num = len(jobs)

    def buffers(depth, dtype):
        return [pltpu.VMEM(depth + (parts, b // parts, h), dtype) for b, h, _, _ in items]

    slots = num * parts
    flops = sum(2 * rows * count * i[0] * 2 * i[1] for i in items)
    nbytes = sum(2 * count * i[0] * 2 * i[1] for i in items)
    dots = [j.right is not None for j in jobs]
    given, given_specs, made, made_specs, spare = extra[1:] if extra else ([], [], [], [], [])
    return pl.pallas_call(
        functools.partial(
            scatter_dot_kernel, count, items, len(shapes), len(bases), parts, extra
        ),
        out_shape=[jax.ShapeDtypeStruct(s, F32) for s in shapes] + made,
        in_specs=[ANY] * (2 * num + len(bases)) + given_specs,
        out_specs=[ANY] * len(shapes) + made_specs,
        input_output_aliases=aliases,
        scratch_shapes=[
            pltpu.VMEM((2, 2) + ((rows, i[0]) if dot_job else (i[0], i[1])), BF16)
            for i, dot_job in zip(items, dots)
        ]
        + [
            pltpu.VMEM((rows, 2 * i[1]) if dot_job else (8, 128), BF16)
            for i, dot_job in zip(items, dots)
        ]
        + buffers((2,), BF16)
        + buffers((2,), F32)
        + buffers((2, count - 1), BF16)
        + buffers((2,), F32)
        + [
            pltpu.SemaphoreType.DMA((2, count - 1, slots)),
            pltpu.SemaphoreType.DMA((2, count - 1, slots)),
            pltpu.SemaphoreType.DMA((2, 2, num)),
            pltpu.SemaphoreType.DMA((num,)),
            pltpu.SemaphoreType.DMA((2, slots, 3)),
        ]
        + spare,
        compiler_params=pltpu.CompilerParams(
            collective_id=collective_id, has_side_effects=True, vmem_limit_bytes=60 << 20
        ),
        cost_estimate=pl.CostEstimate(
            flops=flops, bytes_accessed=20 * nbytes, transcendentals=0
        ),
        name=f"ring_scatter_{collective_id}",
    )(
        *[j.left for j in jobs],
        *[j.left if j.right is None else j.right for j in jobs],
        *bases,
        *given,
    )


class ShareWork:
    def __init__(self, count, given, made, spare, bufs):
        self.given, self.out = given, made[0]
        self.pair, self.first, self.sums, self.second, self.sems = spare
        self.count, self.group = count, self.second.shape[0] + 1
        self.row, self.col = lax.axis_index("dp"), lax.axis_index("tensor")

    def in_column(self, shift):
        return {"dp": (self.row + shift) % self.count}

    def in_group(self, shift):
        return {"tensor": (self.col + shift) % self.group}

    def peers(self):
        column = [self.in_column(s) for s in range(1, self.count)]
        return column, [self.in_group(s) for s in range(1, self.group)]

    def begin(self):
        pass

    def part(self, row):
        width = self.sums.shape[1]
        return pl.ds(pl.multiple_of(row * width, width), width)

    def move(self, stage, shift):
        if stage == 0:
            source = self.pair.at[:, self.part((self.row + shift) % self.count)]
            target, device, slot = self.first.at[shift - 1], self.in_column(shift), shift - 1
        else:
            source, target = self.sums, self.second.at[shift - 1]
            device, slot = self.in_group(shift), self.count + shift - 2
        return pltpu.make_async_remote_copy(
            src_ref=source,
            dst_ref=target,
            send_sem=self.sems.at[0, slot],
            recv_sem=self.sems.at[1, slot],
            device_id=device,
            device_id_type=MESH_ID,
        )

    def compute(self, step):
        @pl.when(step == 0)
        def _():
            self.pair[...] = self.given[0][...]
            self.pair[1:2, :] = self.given[1][...]
            for shift in range(1, self.count):
                self.move(0, shift).start()

        @pl.when(step == 5)
        def _():
            total = self.pair[:, self.part(self.row)]
            for shift in range(1, self.count):
                self.move(0, shift).wait()
                total = total + self.first[shift - 1]
            self.sums[...] = total
            for shift in range(1, self.group):
                self.move(1, shift).start()

    def finish(self):
        total = self.sums[...]
        for shift in range(1, self.group):
            self.move(1, shift).wait()
            total = total + self.second[shift - 1]
        share = total.shape[1] // self.group
        picked = jnp.zeros((8, share), F32)
        for col in range(self.group):
            picked = jnp.where(self.col == col, total[:, col * share : (col + 1) * share], picked)
        self.out[:, :share] = picked


class ProductWork:
    def __init__(self, count, given, made, spare, bufs):
        self.right, self.out = given[0], made[0]
        self.right_buf, self.stage, self.load_sem, self.sems = spare
        self.left, self.count = bufs[0][0], count
        self.place = ring_place(lax.axis_index("dp"), count)
        self.start = self.right.shape[1] - self.right_buf.shape[1]

    def peers(self):
        return ()

    def load(self):
        return pltpu.make_async_copy(
            self.right.at[:, self.start :], self.right_buf, self.load_sem
        )

    def begin(self):
        self.load().start()

    def store(self, step):
        block = self.stage.shape[1]
        member = member_at(self.place, 0, step + 1, self.count)
        return pltpu.make_async_copy(
            self.stage.at[step % 2],
            self.out.at[pl.ds(pl.multiple_of(member * block, block), block), :],
            self.sems.at[step % 2],
        )

    def compute(self, step):
        @pl.when(step == 0)
        def _():
            self.load().wait()

        @pl.when(step >= 2)
        def _():
            self.store(step - 2).wait()

        self.stage[step % 2] = tn_dot(self.left[0, step % 2], self.right_buf[...]).astype(BF16)
        self.store(step).start()

    def finish(self):
        for step in (self.count - 2, self.count - 1):
            self.store(step).wait()


def product_work(right, start, count, width):
    rows, cols = right.shape[0], right.shape[1] - start
    return Extra(
        ProductWork,
        [right],
        [ANY],
        [jax.ShapeDtypeStruct((width, cols), BF16)],
        [ANY],
        [
            pltpu.VMEM((rows, cols), BF16),
            pltpu.VMEM((2, width // count, cols), BF16),
            pltpu.SemaphoreType.DMA,
            pltpu.SemaphoreType.DMA((2,)),
        ],
    )


class GatherWork:
    def __init__(self, count, given, made, spare, bufs):
        self.own, self.out = given[0], made[0]
        self.stage, self.sems, self.local = spare
        self.col = lax.axis_index("tensor")
        self.rows = self.own.shape[0]
        self.parts = self.sems.shape[2]

    def core(self):
        return {"tensor": self.col + 1 - 2 * (self.col % 2)}

    def across(self):
        return {"tensor": (self.col + 2) % 4}

    def peers(self):
        return None, [self.core(), self.across()]

    def begin(self):
        pltpu.make_async_copy(self.own, self.stage, self.local).start()

    def spot(self, member, part):
        size = self.rows // self.parts
        return pl.ds(pl.multiple_of(member * self.rows + part * size, size), size)

    def move(self, kind, part):
        size = self.rows // self.parts
        member = (self.col + 2) % 4 if kind == 2 else self.col
        target = self.out.at[self.spot(member, part), :]
        source = target if kind == 2 else self.own.at[part * size : (part + 1) * size, :]
        return pltpu.make_async_remote_copy(
            src_ref=source,
            dst_ref=target,
            send_sem=self.sems.at[0, kind, part],
            recv_sem=self.sems.at[1, kind, part],
            device_id=self.across() if kind == 0 else self.core(),
            device_id_type=MESH_ID,
        )

    def keep(self):
        here = pl.ds(pl.multiple_of(self.col * self.rows, self.rows), self.rows)
        return pltpu.make_async_copy(self.stage, self.out.at[here, :], self.local)

    def compute(self, step):
        @pl.when(step == 0)
        def _():
            for part in range(self.parts):
                self.move(0, part).start()
                self.move(1, part).start()
            pltpu.make_async_copy(self.own, self.stage, self.local).wait()
            self.keep().start()

        for part, turn in enumerate((2, 4, 5, 6)):

            @pl.when(step == turn)
            def _():
                self.move(0, part).wait_recv()
                self.move(2, part).start()

    def finish(self):
        for part in range(self.parts):
            self.move(0, part).wait_send()
            self.move(1, part).wait()
            self.move(2, part).wait()
        self.keep().wait()


def gather_work(own):
    rows, width = own.shape
    return Extra(
        GatherWork,
        [own],
        [ANY],
        [jax.ShapeDtypeStruct((4 * rows, width), BF16)],
        [ANY],
        [
            pltpu.VMEM(own.shape, BF16),
            pltpu.SemaphoreType.DMA((2, 3, 4)),
            pltpu.SemaphoreType.DMA,
        ],
    )


def share_work(first, second, count, group):
    width = first.shape[1] // count
    vmem = pl.BlockSpec(memory_space=pltpu.VMEM)
    return Extra(
        ShareWork,
        [first, second],
        [vmem] * 2,
        [jax.ShapeDtypeStruct((8, 128), F32)],
        [vmem],
        [
            pltpu.VMEM(first.shape, F32),
            pltpu.VMEM((count - 1, 8, width), F32),
            pltpu.VMEM((8, width), F32),
            pltpu.VMEM((group - 1, 8, width), F32),
            pltpu.SemaphoreType.DMA((2, count + group - 2)),
        ],
    )


class NormWork:
    def __init__(self, count, given, made, spare, bufs):
        self.grads, self.gates = given[:2], tuple(given[2:4])
        self.up, self.down = given[4:]
        self.outs = made
        self.grad_bufs, self.row_bufs, self.down_bufs, self.stage = spare[0], *spare[1:4]
        self.grad_sems, self.row_sems, self.down_sems, self.out_sems = spare[4:]
        self.act = bufs[1][0]
        self.count = count
        self.block = self.row_bufs.shape[2]

    def load_grad(self, which):
        return pltpu.make_async_copy(
            self.grads[which], self.grad_bufs.at[which], self.grad_sems.at[which]
        )

    def spot(self, step):
        return pl.ds(pl.multiple_of(step * self.block, self.block), self.block)

    def loads(self, step):
        slot = step % 2
        edge = self.gates[0].shape[1]
        gate = self.row_bufs.at[0, slot]
        targets = [gate.at[:, :edge], gate.at[:, edge:], self.row_bufs.at[1, slot]]
        rows = [
            pltpu.make_async_copy(
                source.at[self.spot(step), :], target, self.row_sems.at[which, slot]
            )
            for which, (source, target) in enumerate(zip(self.gates + (self.up,), targets))
        ]
        down = pltpu.make_async_copy(
            self.down.at[:, self.spot(step)], self.down_bufs.at[slot], self.down_sems.at[slot]
        )
        return rows + [down]

    def store(self, which, step):
        slot = step % 2
        return pltpu.make_async_copy(
            self.stage.at[which, slot],
            self.outs[which].at[:, self.spot(step)],
            self.out_sems.at[which, slot],
        )

    def begin(self):
        for which in range(2):
            self.load_grad(which).start()
        for copy in self.loads(0):
            copy.start()

    def peers(self):
        return ()

    def compute(self, step):
        @pl.when(step < self.count - 1)
        def _():
            for copy in self.loads(step + 1):
                copy.start()

        @pl.when(step == 0)
        def _():
            for which in range(2):
                self.load_grad(which).wait()

        @pl.when(step >= 2)
        def _():
            for which in range(2):
                self.store(which, step - 2).wait()

        for copy in self.loads(step):
            copy.wait()
        slot = step % 2

        def lines(index, carry):
            band = pl.ds(pl.multiple_of(index * 256, 256), 256)
            norm = nt_dot(self.grad_bufs[0, band, :], self.row_bufs[0, slot])
            norm += nt_dot(self.grad_bufs[1, band, :], self.row_bufs[1, slot])
            self.stage[0, slot, band, :] = norm.astype(BF16)
            value = jnp.dot(
                self.act[band, :], self.down_bufs[slot], preferred_element_type=F32
            )
            self.stage[1, slot, band, :] = value.astype(BF16)
            return carry

        lax.fori_loop(0, self.act.shape[0] // 256, lines, 0)
        for which in range(2):
            self.store(which, step).start()

    def finish(self):
        for step in range(max(self.count - 2, 0), self.count):
            for which in range(2):
                self.store(which, step).wait()


def down_ring(grad_branch, activated, grad_gate, grad_up, gates, up_all, down_all, count, cid):
    rows, hidden = activated.shape
    width = up_all.shape[0]
    block = width // count
    wide = jax.ShapeDtypeStruct((rows, width), BF16)
    spare = [
        pltpu.VMEM((2, rows, hidden), BF16),
        pltpu.VMEM((2, 2, block, hidden), BF16),
        pltpu.VMEM((2, hidden, block), BF16),
        pltpu.VMEM((2, 2, rows, block), BF16),
        pltpu.SemaphoreType.DMA((2,)),
        pltpu.SemaphoreType.DMA((3, 2)),
        pltpu.SemaphoreType.DMA((2,)),
        pltpu.SemaphoreType.DMA((2, 2)),
    ]
    given = [grad_gate, grad_up, *gates, up_all, down_all]
    return ring_scatter_dots(
        [Job(grad_branch, activated, 0, hidden)],
        2,
        count,
        cid,
        Extra(NormWork, given, [ANY] * 6, [wide, wide], [ANY] * 2, spare),
    )


def mlp_kernel(count, *refs):
    x_hbm, wg_hbm, wg_rest, wu_hbm, shard, gb_hbm = refs[:6]
    act_hbm, gg_hbm, gu_hbm, down_all = refs[6:10]
    x_buf, gb_buf, w_bufs, gate_slope, up_slope, acc, half_bufs, stage, own_stage = refs[10:19]
    send_sems, recv_sems, w_sems, in_sems, half_sems, out_sems, local_sem = refs[19:]
    rows, width = x_buf.shape
    hidden = acc.shape[1]
    block = width // count
    cols = w_bufs.shape[-1]
    steps = hidden // cols
    half = hidden // 2
    parts = send_sems.shape[2]
    me = lax.axis_index("dp")

    gate_steps = wg_hbm.shape[1] // cols

    def load_weights(step, which, source=None):
        start = step - gate_steps if source is wg_rest else step
        source = (wg_hbm, wu_hbm)[which] if source is None else source
        return pltpu.make_async_copy(
            source.at[:, pl.ds(pl.multiple_of(start * cols, cols), cols)],
            w_bufs.at[which, step % 2],
            w_sems.at[which, step % 2],
        )

    def fetch(step):
        load_weights(step, 1).start()

        @pl.when(step < gate_steps)
        def _():
            load_weights(step, 0).start()

        @pl.when(step >= gate_steps)
        def _():
            load_weights(step, 0, wg_rest).start()

    load_x = pltpu.make_async_copy(x_hbm, x_buf, in_sems.at[0])
    load_gb = pltpu.make_async_copy(gb_hbm, gb_buf, in_sems.at[1])
    load_own = pltpu.make_async_copy(shard, own_stage, local_sem)
    load_x.start()
    for which in range(2):
        load_weights(0, which).start()
    load_own.start()
    load_gb.start()
    place, neighbours = ring_setup(count)

    def target(ref, member, side, part):
        return piece(ref, (hidden, block), 1, member, side, part, parts)

    def hop(step, side, part):
        ref = target(down_all, member_at(place, side, step, count), side, part)
        return pltpu.make_async_remote_copy(
            src_ref=ref,
            dst_ref=ref,
            send_sem=send_sems.at[side, step, part],
            recv_sem=recv_sems.at[side, step, part],
            device_id={"dp": neighbours[side]},
            device_id_type=MESH_ID,
        )

    for part in range(parts):
        for side in range(2):
            pltpu.make_async_remote_copy(
                src_ref=piece(shard, (hidden, block), None, 0, side, part, parts),
                dst_ref=target(down_all, me, side, part),
                send_sem=send_sems.at[side, 0, part],
                recv_sem=recv_sems.at[side, 0, part],
                device_id={"dp": neighbours[side]},
                device_id_type=MESH_ID,
            ).start()

    def pump(step):
        for part in range(parts):
            for side in range(2):
                hop(step - 1, side, part).wait_recv()
                hop(step, side, part).start()

    load_own.wait()
    store_own = pltpu.make_async_copy(
        own_stage, down_all.at[:, pl.ds(pl.multiple_of(me * block, block), block)], local_sem
    )
    store_own.start()
    load_x.wait()

    def store(ref, which, step):
        return pltpu.make_async_copy(
            stage.at[which, step % 2],
            ref.at[:, pl.ds(pl.multiple_of(step * cols, cols), cols)],
            out_sems.at[which, step % 2],
        )

    def forward(step, carry):
        @pl.when(step + 1 < steps)
        def _():
            fetch(step + 1)

        @pl.when(step >= 2)
        def _():
            store(act_hbm, 0, step - 2).wait()

        load_weights(step, 1).wait()

        @pl.when(step < gate_steps)
        def _():
            load_weights(step, 0).wait()

        @pl.when(step >= gate_steps)
        def _():
            load_weights(step, 0, wg_rest).wait()

        here = pl.ds(pl.multiple_of(step * cols, cols), cols)
        for top in range(0, rows, 256):
            band = pl.ds(top, 256)
            lines = x_buf[band, :]
            gate = jnp.dot(lines, w_bufs[0, step % 2], preferred_element_type=F32)
            up = jnp.dot(lines, w_bufs[1, step % 2], preferred_element_type=F32)
            sig = jax.nn.sigmoid(gate)
            silu = gate * sig
            stage[0, step % 2, band, :] = (silu * up).astype(BF16)
            gate_slope[band, here] = up * sig * (1.0 + gate * (1.0 - sig))
            up_slope[band, here] = silu
            acc[band, here] = jnp.zeros((256, cols), F32)
        store(act_hbm, 0, step).start()

        turn = (step + 1) // 2

        @pl.when((step % 2 == 1) & (turn <= count - 2))
        def _():
            pump(turn)

        return carry

    lax.fori_loop(0, steps, forward, 0)
    for step in range(max(steps - 2, 0), steps):
        store(act_hbm, 0, step).wait()
    pumped = min(steps // 2, count - 2)
    load_gb.wait()

    def load_half(step, side):
        member = member_at(place, side, step, count)
        return pltpu.make_async_copy(
            down_all.at[
                pl.ds(side * half, half), pl.ds(pl.multiple_of(member * block, block), block)
            ],
            half_bufs.at[side],
            half_sems.at[side],
        )

    def backward(step, carry):
        @pl.when((step > pumped) & (step <= count - 2))
        def _():
            pump(step)

        @pl.when(step == count - 1)
        def _():
            for part in range(parts):
                for side in range(2):
                    hop(count - 2, side, part).wait_recv()

        for side in range(2):
            load_half(step, side).start()
        for side in range(2):
            member = member_at(place, side, step, count)
            load_half(step, side).wait()
            here = pl.ds(pl.multiple_of(member * block, block), block)
            spot = pl.ds(side * half, half)

            def lines(index, carry):
                band = pl.ds(pl.multiple_of(index * 256, 256), 256)
                acc[band, spot] += nt_dot(gb_buf[band, here], half_bufs[side])
                return carry

            lax.fori_loop(0, rows // 256, lines, 0)

        return carry

    store_own.wait()
    lax.fori_loop(0, count, backward, 0)

    def slopes(step, carry):
        @pl.when(step >= 2)
        def _():
            store(gg_hbm, 1, step - 2).wait()
            store(gu_hbm, 2, step - 2).wait()

        here = pl.ds(pl.multiple_of(step * cols, cols), cols)

        def lines(index, carry):
            band = pl.ds(pl.multiple_of(index * 256, 256), 256)
            value = acc[band, here]
            stage[1, step % 2, band, :] = (value * gate_slope[band, here]).astype(BF16)
            stage[2, step % 2, band, :] = (value * up_slope[band, here]).astype(BF16)
            return carry

        lax.fori_loop(0, rows // 256, lines, 0)
        store(gg_hbm, 1, step).start()
        store(gu_hbm, 2, step).start()
        return carry

    lax.fori_loop(0, steps, slopes, 0)
    for step in range(max(steps - 2, 0), steps):
        store(gg_hbm, 1, step).wait()
        store(gu_hbm, 2, step).wait()

    def drain(step, carry):
        for part in range(parts):
            for side in range(2):
                hop(step, side, part).wait_send()
        return carry

    lax.fori_loop(0, count - 1, drain, 0)


def mlp_ring(rows_mlp, gates, up_all, w_down, grad_branch, count, collective_id):
    rows, width = rows_mlp.shape
    hidden, block = w_down.shape
    cols, parts = 256, 2
    wide = jax.ShapeDtypeStruct((rows, hidden), BF16)
    return pl.pallas_call(
        functools.partial(mlp_kernel, count),
        out_shape=[wide] * 3 + [jax.ShapeDtypeStruct((hidden, width), BF16)],
        in_specs=[ANY] * 6,
        out_specs=[pl.BlockSpec(memory_space=pl.ANY)] * 4,
        scratch_shapes=[
            pltpu.VMEM((rows, width), BF16),
            pltpu.VMEM((rows, width), BF16),
            pltpu.VMEM((2, 2, width, cols), BF16),
            pltpu.VMEM((rows, hidden), F32),
            pltpu.VMEM((rows, hidden), F32),
            pltpu.VMEM((rows, hidden), F32),
            pltpu.VMEM((2, hidden // 2, block), BF16),
            pltpu.VMEM((3, 2, rows, cols), BF16),
            pltpu.VMEM((hidden, block), BF16),
            pltpu.SemaphoreType.DMA((2, count - 1, parts)),
            pltpu.SemaphoreType.DMA((2, count - 1, parts)),
            pltpu.SemaphoreType.DMA((2, 2)),
            pltpu.SemaphoreType.DMA((2,)),
            pltpu.SemaphoreType.DMA((2,)),
            pltpu.SemaphoreType.DMA((3, 2)),
            pltpu.SemaphoreType.DMA,
        ],
        compiler_params=pltpu.CompilerParams(
            collective_id=collective_id, has_side_effects=True, vmem_limit_bytes=60 << 20
        ),
        cost_estimate=pl.CostEstimate(
            flops=6 * rows * width * hidden,
            bytes_accessed=40 * hidden * width,
            transcendentals=rows * hidden,
        ),
        name="mlp_ring",
    )(rows_mlp, *gates, up_all, w_down, grad_branch)


class HeadWork:
    def __init__(self, count, given, made, spare, bufs):
        self.length, self.gain, self.sources = given[0], given[1], given[2:]
        self.grads_out, self.token_out, self.gain_out = made
        num = len(self.sources)
        self.bufs = spare[:num]
        self.heads, self.grads, self.acc_k, self.acc_v, self.stage = spare[num : num + 5]
        self.stats, self.inner, self.bias = spare[num + 5 : num + 8]
        self.in_sems, self.out_sems = spare[num + 8 :]

    def peers(self):
        return ()

    def load(self, which):
        return pltpu.make_async_copy(
            self.sources[which], self.bufs[which], self.in_sems.at[which]
        )

    def begin(self):
        for which in range(len(self.sources)):
            self.load(which).start()
        self.gain_out[...] = jnp.zeros_like(self.gain_out)
        self.acc_k[...] = jnp.zeros_like(self.acc_k)
        self.acc_v[...] = jnp.zeros_like(self.acc_v)
        key_pos = lax.broadcasted_iota(jnp.int32, self.bias.shape, 0)
        self.bias[...] = jnp.where(key_pos < self.length[0], 0.0, -1e30)

    def store(self, band):
        rows = self.stage.shape[1]
        return pltpu.make_async_copy(
            self.stage.at[band % 2],
            self.token_out.at[pl.ds(pl.multiple_of(band * rows, rows), rows), :],
            self.out_sems.at[band % 2],
        )

    def store_grads(self):
        return pltpu.make_async_copy(self.grads, self.grads_out, self.out_sems.at[2])

    def tokens(self, band):
        w_query, w_key, w_value, normed = self.bufs[9:]
        rows = self.stage.shape[1]
        inner = w_query.shape[1]

        @pl.when(band >= 2)
        def _():
            self.store(band - 2).wait()

        lines = pl.ds(pl.multiple_of(band * rows, rows), rows)

        def columns(index, carry):
            cols = pl.ds(pl.multiple_of(index * 512, 512), 512)
            value = nt_dot(self.grads[lines, :inner], w_query[cols, :])
            value += nt_dot(self.grads[lines, inner : inner + 128], w_key[cols, :])
            value += nt_dot(self.grads[lines, inner + 128 :], w_value[cols, :])
            self.stage[band % 2, :, cols] = value.astype(BF16)
            scaled = value * normed[lines, cols].astype(F32)
            self.gain_out[0:1, cols] += jnp.sum(scaled, axis=0, keepdims=True)
            return carry

        lax.fori_loop(0, w_query.shape[0] // 512, columns, 0)
        self.store(band).start()

    def compute(self, step):
        grad_attn, w_output, queries, keys, values, cosine, sine, outs, stats = self.bufs[:9]
        inner = queries.shape[1]
        pairs = inner // 128

        @pl.when(step == 0)
        def _():
            for which in range(2):
                self.load(which).wait()

            def band(index, carry):
                rows = pl.ds(pl.multiple_of(index * 256, 256), 256)
                self.heads[rows, :] = nt_dot(grad_attn[rows, :], w_output[...]).astype(BF16)
                return carry

            lax.fori_loop(0, LEN // 256, band, 0)

        @pl.when(step == 1)
        def _():
            for which in range(2, 9):
                self.load(which).wait()

            self.stats[...] = jnp.transpose(stats[...])

            def products(index, carry):
                rows = pl.ds(pl.multiple_of(index * 256, 256), 256)
                kept = jnp.zeros((256, 128), F32)
                for pair in range(pairs):
                    cols = slice(pair * 128, (pair + 1) * 128)
                    kept = row_products(self.heads[rows, cols], outs[rows, cols], pair, kept)
                stats[rows, :] = kept
                return carry

            lax.fori_loop(0, LEN // 256, products, 0)
            self.inner[...] = jnp.transpose(stats[...])

        @pl.when(step == pairs + 1)
        def _():
            for which in range(9, len(self.sources)):
                self.load(which).wait()

        @pl.when((step >= 1) & (step <= pairs))
        def _():
            here = pl.ds(pl.multiple_of((step - 1) * 128, 128), 128)
            attend_back_tiles(
                step - 1, queries.at[:, here], keys, values, self.heads.at[:, here], cosine,
                sine, self.stats, self.inner, self.bias, self.grads.at[:, here],
                self.acc_k, self.acc_v,
            )

        @pl.when(step == pairs)
        def _():
            self.grads[:, inner : inner + 128] = rope_back(
                self.acc_k[...], cosine[...], sine[...]
            )
            self.grads[:, inner + 128 :] = self.acc_v[...].astype(BF16)
            self.store_grads().start()

        @pl.when((step > pairs) & (step <= pairs + 2))
        def _():
            def band(index, carry):
                self.tokens(2 * (step - pairs - 1) + index)
                return carry

            lax.fori_loop(0, 2, band, 0)

    def finish(self):
        self.gain_out[0:1, :] = self.gain_out[0:1, :] / self.gain[...]
        self.store_grads().wait()
        for band in (2, 3):
            self.store(band).wait()


def heads_ring(
    job, lengths, gain, grad_attn, w_output, qkv, tables, saved, weights, rows_attn, count, cid
):
    sources = [grad_attn, w_output, *qkv, *tables, *saved, *weights, rows_attn]
    rows, width = grad_attn.shape
    inner = qkv[0].shape[1]
    made = [
        jax.ShapeDtypeStruct((rows, inner + 256), BF16),
        jax.ShapeDtypeStruct((rows, width), BF16),
        jax.ShapeDtypeStruct((8, width), F32),
    ]
    spare = [pltpu.VMEM(g.shape, g.dtype) for g in sources] + [
        pltpu.VMEM((rows, inner), BF16),
        pltpu.VMEM((rows, inner + 256), BF16),
        pltpu.VMEM((rows, 128), F32),
        pltpu.VMEM((rows, 128), F32),
        pltpu.VMEM((2, rows // 4, width), BF16),
        pltpu.VMEM((128, rows), F32),
        pltpu.VMEM((128, rows), F32),
        pltpu.VMEM((rows, 128), F32),
        pltpu.SemaphoreType.DMA((len(sources),)),
        pltpu.SemaphoreType.DMA((3,)),
    ]
    vmem = pl.BlockSpec(memory_space=pltpu.VMEM)
    specs = [pl.BlockSpec(memory_space=pltpu.SMEM), vmem] + [ANY] * len(sources)
    return ring_scatter_dots(
        [job],
        4,
        count,
        cid,
        Extra(HeadWork, [lengths, gain] + sources, specs, made, [ANY, ANY, vmem], spare),
    )


def attend_ring_kernel(count, *refs):
    length_ref, shard, sources = refs[0], refs[1], refs[2:9]
    gathered, q_out, k_out, v_out, head_out, part_out, stats_out = refs[9:16]
    bufs = refs[16:23]
    q_buf, k_buf, v_buf, head_buf, stage, own, stats = refs[23:30]
    send_sems, recv_sems, in_sems, out_sems, local_sem = refs[30:]
    rows_buf, w_query, w_key, w_value, w_output, cosine, sine = bufs
    shape = own.shape
    me = lax.axis_index("dp")
    loads = [
        pltpu.make_async_copy(source, buf, in_sems.at[k])
        for k, (source, buf) in enumerate(zip(sources, bufs))
    ]
    for load in loads:
        load.start()
    load_own = pltpu.make_async_copy(shard.at[:, : shape[1]], own, local_sem)
    load_own.start()
    place, neighbours = ring_setup(count)

    def hop(step, side):
        ref = piece(gathered, shape, 0, member_at(place, side, step, count), side, 0, 1)
        return pltpu.make_async_remote_copy(
            src_ref=ref,
            dst_ref=ref,
            send_sem=send_sems.at[side, step],
            recv_sem=recv_sems.at[side, step],
            device_id={"dp": neighbours[side]},
            device_id_type=MESH_ID,
        )

    for side in range(2):
        pltpu.make_async_remote_copy(
            src_ref=piece(shard, shape, None, 0, side, 0, 1),
            dst_ref=piece(gathered, shape, 0, me, side, 0, 1),
            send_sem=send_sems.at[side, 0],
            recv_sem=recv_sems.at[side, 0],
            device_id={"dp": neighbours[side]},
            device_id_type=MESH_ID,
        ).start()

    def pump(step, carry=0):
        for side in range(2):
            hop(step - 1, side).wait_recv()
            hop(step, side).start()
        return carry

    load_own.wait()
    store_own = pltpu.make_async_copy(
        own, gathered.at[pl.ds(pl.multiple_of(me * shape[0], shape[0]), shape[0]), :], local_sem
    )
    store_own.start()
    for k in (0, 1, 2, 3, 5, 6):
        loads[k].wait()

    stats[...] = jnp.zeros_like(stats)

    def projection(band, carry):
        lines = pl.ds(pl.multiple_of(band * 256, 256), 256)
        project_rows(
            rows_buf[lines, :], w_query, w_key, w_value, cosine[lines, :], sine[lines, :],
            q_buf.at[lines, :], k_buf.at[lines, :], v_buf.at[lines, :],
        )
        return carry

    lax.fori_loop(0, LEN // 256, projection, 0)
    stores = [
        pltpu.make_async_copy(buf, out, out_sems.at[k])
        for k, (buf, out) in enumerate(
            ((q_buf, q_out), (k_buf, k_out), (v_buf, v_out), (head_buf, head_out))
        )
    ]
    for store in stores[:3]:
        store.start()
    pump(1)
    pairs = q_buf.shape[1] // 128

    def attention(pair, carry):
        here = pl.ds(pl.multiple_of(pair * 128, 128), 128)
        attend_pair(
            length_ref[0], pair, q_buf.at[:, here], k_buf, v_buf, head_buf.at[:, here], stats
        )

        @pl.when(pair + 2 <= count - 2)
        def _():
            pump(pair + 2)

        return carry

    lax.fori_loop(0, pairs, attention, 0)
    loads[4].wait()
    stores[3].start()
    store_stats = pltpu.make_async_copy(stats, stats_out, out_sems.at[6])
    store_stats.start()

    def store_part(band):
        return pltpu.make_async_copy(
            stage.at[band % 2],
            part_out.at[pl.ds(pl.multiple_of(band * 256, 256), 256), :],
            out_sems.at[4 + band % 2],
        )

    def output(band, carry):
        @pl.when(band >= 2)
        def _():
            store_part(band - 2).wait()

        lines = pl.ds(pl.multiple_of(band * 256, 256), 256)

        def columns(index, inner):
            cols = pl.ds(pl.multiple_of(index * 512, 512), 512)
            stage[band % 2, :, cols] = jnp.dot(
                head_buf[lines, :], w_output[:, cols], preferred_element_type=F32
            ).astype(BF16)
            return inner

        lax.fori_loop(0, w_output.shape[1] // 512, columns, 0)
        store_part(band).start()

        @pl.when((band == 0) & (pairs + 2 <= count - 2))
        def _():
            pump(pairs + 2)

        return carry

    lax.fori_loop(0, LEN // 256, output, 0)
    lax.fori_loop(min(pairs + 3, count - 1), count - 1, pump, 0)
    for band in (LEN // 256 - 2, LEN // 256 - 1):
        store_part(band).wait()
    for store in stores:
        store.wait()
    store_stats.wait()
    store_own.wait()
    for side in range(2):
        hop(count - 2, side).wait_recv()

    def drain(step, carry):
        for side in range(2):
            hop(step, side).wait_send()
        return carry

    lax.fori_loop(0, count - 1, drain, 0)


def attend_ring(shard, edge, lengths, rows_attn, weights, tables, count, collective_id):
    sources = [rows_attn, *weights, *tables]
    rows, width = rows_attn.shape
    inner = weights[0].shape[1]

    def low(*shape):
        return jax.ShapeDtypeStruct(shape, BF16)

    return pl.pallas_call(
        functools.partial(attend_ring_kernel, count),
        out_shape=[
            low(shard.shape[0] * count, edge),
            low(rows, inner),
            low(rows, 128),
            low(rows, 128),
            low(rows, inner),
            low(rows, width),
            jax.ShapeDtypeStruct((rows, 128), F32),
        ],
        in_specs=[pl.BlockSpec(memory_space=pltpu.SMEM)] + [ANY] * (1 + len(sources)),
        out_specs=[ANY] * 7,
        scratch_shapes=[pltpu.VMEM(source.shape, source.dtype) for source in sources]
        + [
            pltpu.VMEM((rows, inner), BF16),
            pltpu.VMEM((rows, 128), BF16),
            pltpu.VMEM((rows, 128), BF16),
            pltpu.VMEM((rows, inner), BF16),
            pltpu.VMEM((2, 256, width), BF16),
            pltpu.VMEM((shard.shape[0], edge), BF16),
            pltpu.VMEM((rows, 128), F32),
            pltpu.SemaphoreType.DMA((2, count - 1)),
            pltpu.SemaphoreType.DMA((2, count - 1)),
            pltpu.SemaphoreType.DMA((len(sources),)),
            pltpu.SemaphoreType.DMA((7,)),
            pltpu.SemaphoreType.DMA,
        ],
        compiler_params=pltpu.CompilerParams(
            collective_id=collective_id, has_side_effects=True, vmem_limit_bytes=56 << 20
        ),
        cost_estimate=pl.CostEstimate(
            flops=24 << 30, bytes_accessed=60 << 20, transcendentals=8 << 20
        ),
        name="attend_ring",
    )(lengths, shard, *sources)


def ring_weight_grads(jobs, parts, count, collective_id):
    if all(left.shape[1] // count % 128 == 0 for left, _ in jobs):
        jobs = [Job(left, right, 0, right.shape[1]) for left, right in jobs]
        return ring_scatter_dots(jobs, parts, count, collective_id)
    partials = [tn_dot(left, right).astype(BF16) for left, right in jobs]
    num = len(jobs)
    return ring_scatter(partials, [0] * num, [parts] * num, count, collective_id)


def after(value, *deps):
    return lax.optimization_barrier((value,) + deps)[0]


def gather_rows(value):
    return lax.all_gather(value, "tensor", axis=0, tiled=True)


def scatter_rows(value):
    return lax.psum_scatter(value.astype(BF16), "tensor", scatter_dimension=0, tiled=True)


def share_kernel(count, group, parts_ref, out_ref, first, sums, second, sems):
    row, col = lax.axis_index("dp"), lax.axis_index("tensor")
    barrier = pltpu.get_barrier_semaphore()

    def in_group(shift):
        return {"tensor": (col + shift) % group}

    def in_column(shift):
        return {"dp": (row + shift) % count}

    def greet(device):
        pl.semaphore_signal(barrier, inc=1, device_id=device, device_id_type=MESH_ID)

    for shift in range(1, group):
        greet(in_group(shift))
    for shift in range(1, count):
        greet(in_column(shift))
    pl.semaphore_wait(barrier, group + count - 2)

    def exchange(shift, slot, source, target, device):
        return pltpu.make_async_remote_copy(
            src_ref=source,
            dst_ref=target,
            send_sem=sems.at[0, slot],
            recv_sem=sems.at[1, slot],
            device_id=device,
            device_id_type=MESH_ID,
        )

    moves = [
        exchange(s, s - 1, parts_ref.at[(col + s) % group], first.at[s - 1], in_group(s))
        for s in range(1, group)
    ]
    for move in moves:
        move.start()
    total = parts_ref[col]
    for shift, move in enumerate(moves):
        move.wait()
        total = total + first[shift]
    sums[...] = total
    moves = [
        exchange(
            s, group + s - 2, sums.at[(row + s) % count], second.at[s - 1], in_column(s)
        )
        for s in range(1, count)
    ]
    for move in moves:
        move.start()
    total = sums[row]
    for shift, move in enumerate(moves):
        move.wait()
        total = total + second[shift]
    out_ref[...] = total


def sum_shares(first, second, count, group, collective_id):
    share = first.shape[0] // (count * group)
    pair = jnp.stack([first, second]).reshape(2, count, group, share)
    parts = jnp.transpose(pair, (2, 1, 0, 3)).reshape(group, count, 1, 2 * share)
    width = (2 * share + 127) // 128 * 128
    parts = jnp.pad(parts, ((0, 0), (0, 0), (0, 7), (0, width - 2 * share)))
    tile = (8, width)
    out = pl.pallas_call(
        functools.partial(share_kernel, count, group),
        out_shape=jax.ShapeDtypeStruct(tile, F32),
        in_specs=[pl.BlockSpec(memory_space=pltpu.VMEM)],
        out_specs=pl.BlockSpec(memory_space=pltpu.VMEM),
        scratch_shapes=[
            pltpu.VMEM((group - 1, count) + tile, F32),
            pltpu.VMEM((count,) + tile, F32),
            pltpu.VMEM((count - 1,) + tile, F32),
            pltpu.SemaphoreType.DMA((2, group + count - 2)),
        ],
        compiler_params=pltpu.CompilerParams(collective_id=collective_id, has_side_effects=True),
        name="sum_shares",
    )(parts)
    return out[0, :share], out[0, share : 2 * share]


def dot(left, right):
    return jnp.dot(left, right, preferred_element_type=F32)


def body(
    count,
    group,
    tokens,
    lengths,
    attn_gain,
    w_query,
    w_key,
    w_value,
    w_output,
    mlp_gain,
    w_gate,
    w_up,
    w_down,
    cotangent,
):
    local_rows = tokens.shape[0]
    token_full = tokens.astype(F32)
    gain_attn = attn_gain.astype(F32)
    gain_mlp = mlp_gain.astype(F32)
    row_pos = lax.axis_index("tensor") * local_rows + jnp.arange(local_rows)
    valid_rows = (row_pos < lengths[0]).astype(F32)
    cot_masked = cotangent.astype(F32) * valid_rows[:, None]
    cosine, sine = rope_tables()

    inv_first = lax.rsqrt(jnp.mean(token_full * token_full, axis=1, keepdims=True) + epsilon)
    normed_attn = (token_full * inv_first * gain_attn).astype(BF16)
    rows_attn = gather_rows(normed_attn)
    query_all, key_all, value_all, output_all = ring_gather(
        [after(w_query, normed_attn), w_key, w_value, w_output],
        (0, 0, 0, 1), (1, 1, 1, 1), count, 0,
    )
    grad_branch = gather_rows(after(cot_masked.astype(BF16), rows_attn))
    fused = count == 8 and group == 4
    edge = 3 * w_gate.shape[1] // 8
    gates = []
    if fused:
        first_gate, queries, keys, values, head_out, attn_part, stats = attend_ring(
            w_gate,
            edge,
            lengths,
            rows_attn,
            (query_all, key_all, value_all, output_all),
            (cosine, sine),
            count,
            9,
        )
        gates.append(first_gate)
    else:
        queries, keys, values = project(rows_attn, query_all, key_all, value_all, cosine, sine)
        head_out = attend(queries, keys, values, lengths)
        attn_part = dot(head_out, output_all).astype(BF16)
    attn_branch = scatter_rows(attn_part)
    (gate_all,) = ring_gather(
        [after(w_gate, attn_part)], (0,), (2,), count, 1, edge if fused else 0
    )
    gates.append(gate_all)
    hidden = token_full + attn_branch.astype(F32)
    inv_second = lax.rsqrt(jnp.mean(hidden * hidden, axis=1, keepdims=True) + epsilon)
    normed_mlp = (hidden * inv_second * gain_mlp).astype(BF16)
    normed_mlp = after(normed_mlp, gate_all)
    rows_mlp = gather_rows(normed_mlp)
    (up_all,) = ring_gather([after(w_up, normed_mlp)], (0,), (2,), count, 2)
    if fused:
        activated, grad_gate_pre, grad_up_pre, down_all = mlp_ring(
            rows_mlp, gates, after(up_all, rows_mlp), w_down, grad_branch, count, 3
        )
        grad_down, norm_part, mlp_part = down_ring(
            grad_branch, activated, grad_gate_pre, grad_up_pre, gates, up_all, down_all,
            count, 4,
        )
    else:
        gate_proj = dot(rows_mlp, gate_all)
        up_proj = dot(rows_mlp, up_all)
        gate_sig = jax.nn.sigmoid(gate_proj)
        activated = (gate_proj * gate_sig * up_proj).astype(BF16)
        (down_all,) = ring_gather([after(w_down, up_all)], (1,), (2,), count, 3)
        mlp_part = dot(activated, down_all).astype(BF16)
        grad_act = nt_dot(grad_branch, down_all)
        grad_gate_pre = (
            grad_act * up_proj * gate_sig * (1.0 + gate_proj * (1.0 - gate_sig))
        ).astype(BF16)
        grad_up_pre = (grad_act * gate_proj * gate_sig).astype(BF16)
        norm_part = (nt_dot(grad_gate_pre, gate_all) + nt_dot(grad_up_pre, up_all)).astype(BF16)
        (grad_down,) = ring_weight_grads([(grad_branch, activated)], 2, count, 4)
    grad_norm_two = scatter_rows(norm_part).astype(F32)
    middle = 3 * grad_up_pre.shape[1] // 8
    if fused:
        grad_gate, up_part = ring_scatter_dots(
            [Job(after(rows_mlp, norm_part), grad_gate_pre, 0, grad_gate_pre.shape[1])],
            2, count, 5, product_work(grad_up_pre, middle, count, rows_mlp.shape[1]),
        )
    else:
        (grad_gate,) = ring_weight_grads(
            [(after(rows_mlp, norm_part), grad_gate_pre)], 2, count, 5
        )
    scaled_two = grad_norm_two * gain_mlp
    gain_two_part = jnp.sum(grad_norm_two * hidden * inv_second, axis=0)
    grad_hidden = (
        cot_masked
        + inv_second * scaled_two
        - hidden * inv_second**3 * jnp.mean(scaled_two * hidden, axis=1, keepdims=True)
    )
    grad_hidden = after(grad_hidden, grad_gate)
    if fused:
        hidden_cols = grad_up_pre.shape[1]
        grad_up, grad_attn = ring_scatter_dots(
            [Job(rows_mlp, grad_up_pre, 0, middle, hidden_cols)],
            4, count, 6, gather_work(grad_hidden.astype(BF16)),
        )
        mlp_branch = scatter_rows(after(mlp_part, grad_attn))
        grad_up, grad_qkv, token_part, gain_one = heads_ring(
            Job(up_part, None, 0, hidden_cols - middle, grad_up, middle),
            lengths,
            gain_attn[None, :],
            grad_attn,
            output_all,
            (queries, keys, values),
            (cosine, sine),
            (head_out, stats),
            (query_all, key_all, value_all),
            rows_attn,
            count,
            10,
        )
    else:
        grad_attn = gather_rows(grad_hidden.astype(BF16))
        mlp_branch = scatter_rows(after(mlp_part, grad_hidden))
        (grad_up,) = ring_weight_grads(
            [(after(rows_mlp, grad_hidden), grad_up_pre)], 2, count, 6
        )
        grad_heads = nt_dot(after(grad_attn, grad_up), output_all).astype(BF16)
        grad_qpre, grad_kpre, grad_vpre = attend_back(
            queries, keys, values, grad_heads, lengths, cosine, sine
        )
        token_part = (
            nt_dot(grad_qpre, query_all)
            + nt_dot(grad_kpre, key_all)
            + nt_dot(grad_vpre, value_all)
        ).astype(BF16)
    layer_out = (hidden + after(mlp_branch, token_part).astype(F32)).astype(BF16)
    grad_norm_one = scatter_rows(token_part).astype(F32)
    scaled_one = grad_norm_one * gain_attn
    grad_tokens = (
        grad_hidden
        + inv_first * scaled_one
        - token_full * inv_first**3 * jnp.mean(scaled_one * token_full, axis=1, keepdims=True)
    )
    if fused:
        query_cols, key_cols = queries.shape[1], keys.shape[1]
        rows_late = after(rows_attn, token_part)
        grad_query, grad_key, grad_value, grad_output, shares = ring_scatter_dots(
            [
                Job(
                    rows_late,
                    grad_qkv,
                    0,
                    query_cols + 2 * key_cols,
                    pieces=(query_cols, key_cols, key_cols),
                ),
                Job(grad_attn, head_out, 0, query_cols),
            ],
            1,
            count,
            7,
            share_work(gain_one, gain_two_part[None, :], count, group),
        )
        share = gain_two_part.shape[0] // (count * group)
        grad_attn_gain, grad_mlp_gain = shares[0, :share], shares[1, :share]
    else:
        grad_query, grad_key, grad_value, grad_output = ring_weight_grads(
            [
                (after(rows_attn, token_part), grad_qpre),
                (rows_attn, grad_kpre),
                (rows_attn, grad_vpre),
                (grad_attn, head_out),
            ],
            1, count, 7,
        )
        gain_one_part = jnp.sum(grad_norm_one * token_full * inv_first, axis=0)
        grad_attn_gain, grad_mlp_gain = sum_shares(
            after(gain_one_part, grad_query), gain_two_part, count, group, 8
        )
    grad_output, grad_down = grad_output.T, grad_down.T
    return (
        layer_out,
        grad_tokens,
        grad_query,
        grad_key,
        grad_value,
        grad_output,
        grad_gate,
        grad_up,
        grad_down,
        grad_attn_gain,
        grad_mlp_gain,
    )


def solution(mesh):
    rows = P(("dp", "tensor"), None)
    tall = P("dp", "tensor")
    wide = P("tensor", "dp")
    share = P(("dp", "tensor"))
    in_specs = (rows, P("dp"), P(), tall, tall, tall, wide, P(), tall, tall, wide, rows)
    out_specs = (rows, rows, tall, tall, tall, wide, tall, tall, wide, share, share)
    return jax.shard_map(
        functools.partial(body, mesh.shape["dp"], mesh.shape["tensor"]),
        mesh=mesh,
        in_specs=in_specs,
        out_specs=out_specs,
        check_vma=False,
    )
```

```python
import functools
from typing import Any, NamedTuple

import jax
import jax.numpy as jnp
from jax import lax
from jax.experimental import pallas as pl
from jax.experimental.pallas import tpu as pltpu
from jax.sharding import PartitionSpec as P

HD = 64
LEN = 1024
QB = 256

epsilon = 1e-05
theta = 500000.0
MESH_ID = pl.DeviceIdType.MESH
BF16 = jnp.bfloat16
ANY = pl.BlockSpec(memory_space=pl.ANY)
F32 = jnp.float32


def rope_frequencies():
    half_size = HD // 2
    base_freq = theta ** (-(jnp.arange(half_size, dtype=jnp.float32) * 2.0) / HD)
    wavelength = 2.0 * jnp.pi / base_freq
    smooth = (8192.0 / wavelength - 1.0) / 3.0
    middle = (1.0 - smooth) * base_freq / 32.0 + smooth * base_freq
    return jnp.where(
        wavelength < 2048.0, base_freq, jnp.where(wavelength > 8192.0, base_freq / 32.0, middle)
    )


def rope_tables():
    steps = jnp.arange(32, dtype=jnp.float32)[:, None]
    frequency = jnp.concatenate([rope_frequencies()] * 4)[None, :]
    low, high = steps * frequency, (32.0 * steps) * frequency
    cos_low, sin_low = jnp.cos(low)[None, :, :], jnp.sin(low)[None, :, :]
    cos_high, sin_high = jnp.cos(high)[:, None, :], jnp.sin(high)[:, None, :]
    sign = jnp.where(jnp.arange(128) % HD < HD // 2, -1.0, 1.0)
    cosine = cos_high * cos_low - sin_high * sin_low
    sine = (sin_high * cos_low + cos_high * sin_low) * sign
    return cosine.reshape(LEN, 128), sine.reshape(LEN, 128)


def lane_index(shape):
    return lax.broadcasted_iota(jnp.int32, shape, 1)


def swap_halves(value):
    low = lane_index(value.shape) % HD < HD // 2
    return jnp.where(low, pltpu.roll(value, 128 - HD // 2, 1), pltpu.roll(value, HD // 2, 1))


def nt_dot(left, right):
    return lax.dot_general(left, right, (((1,), (1,)), ((), ())), preferred_element_type=F32)


def tn_dot(left, right):
    return lax.dot_general(left, right, (((0,), (0,)), ((), ())), preferred_element_type=F32)


def rope(value, cosine, sine):
    return (value * cosine + swap_halves(value) * sine).astype(BF16)


def rope_back(grads, cosine, sine):
    return (grads * cosine - swap_halves(grads) * sine).astype(BF16)


def project_rows(rows, wq_ref, wk_ref, wv_ref, cosine, sine, q_ref, k_ref, v_ref):
    for block in range(q_ref.shape[1] // 256):
        cols = slice(block * 256, (block + 1) * 256)
        value = jnp.dot(rows, wq_ref[:, cols], preferred_element_type=F32)
        for half in range(2):
            start = block * 256 + half * 128
            q_ref[:, start : start + 128] = rope(
                value[:, half * 128 : half * 128 + 128], cosine, sine
            )
    k_ref[...] = rope(jnp.dot(rows, wk_ref[...], preferred_element_type=F32), cosine, sine)
    v_ref[...] = jnp.dot(rows, wv_ref[...], preferred_element_type=F32).astype(BF16)


def project_kernel(x_ref, wq_ref, wk_ref, wv_ref, cos_ref, sin_ref, q_ref, k_ref, v_ref):
    project_rows(
        x_ref[...], wq_ref, wk_ref, wv_ref, cos_ref[...], sin_ref[...], q_ref, k_ref, v_ref
    )


def project(rows, w_query, w_key, w_value, cosine, sine):
    total, width = rows.shape
    block = 256

    def whole(array):
        return pl.BlockSpec(array.shape, lambda i: (0, 0))

    def by_rows(cols):
        return pl.BlockSpec((block, cols), lambda i: (i, 0))

    shapes = [w_query.shape[1], w_key.shape[1], w_value.shape[1]]
    return pl.pallas_call(
        project_kernel,
        grid=(total // block,),
        out_shape=[jax.ShapeDtypeStruct((total, s), BF16) for s in shapes],
        in_specs=[by_rows(width), whole(w_query), whole(w_key), whole(w_value)]
        + [by_rows(128)] * 2,
        out_specs=[by_rows(s) for s in shapes],
        compiler_params=pltpu.CompilerParams(vmem_limit_bytes=32 << 20),
        cost_estimate=pl.CostEstimate(
            flops=2 * total * width * sum(shapes), bytes_accessed=8 << 20, transcendentals=0
        ),
        name="project",
    )(rows, w_query, w_key, w_value, cosine, sine)


def pick_head(pair, which, kv):
    moved = jnp.where(kv == which, pair, pltpu.roll(pair, HD, 1))
    return jnp.where(lane_index(pair.shape) // HD == kv, moved, jnp.zeros_like(moved))


def join_heads(first, second, kv):
    first = jnp.where(kv == 0, first, pltpu.roll(first, HD, 1))
    second = jnp.where(kv == 1, second, pltpu.roll(second, HD, 1))
    return jnp.where(lane_index(first.shape) < HD, first, second)


def attend_pair(length, pair_index, q_ref, k_ref, v_ref, o_ref, stats_ref=None):
    kv = pair_index // 2
    square = (QB, QB)
    causal = lax.broadcasted_iota(jnp.int32, square, 1) <= lax.broadcasted_iota(
        jnp.int32, square, 0
    )
    bias = jnp.where(lane_index((1, LEN)) < length, 0.0, -1e30)
    for block in range(LEN // QB):
        start = block * QB
        here = slice(start, start + QB)
        pair = q_ref[here, :].astype(F32) * HD**-0.5
        outs = []
        for which in range(2):
            query = pick_head(pair, which, kv).astype(BF16)
            near = jnp.where(causal, nt_dot(query, k_ref[here, :]), -1e30) + bias[:, here]
            top = jnp.max(near, axis=1, keepdims=True)
            if start:
                far = nt_dot(query, k_ref[:start, :]) + bias[:, :start]
                top = jnp.maximum(top, jnp.max(far, axis=1, keepdims=True))
                far = jnp.exp(far - top)
            near = jnp.exp(near - top)
            total = jnp.sum(near, axis=1, keepdims=True)
            if start:
                total = total + jnp.sum(far, axis=1, keepdims=True)
            inverse = 1.0 / total
            if stats_ref is not None:
                kept = stats_ref[here, :]
                mine = lane_index(kept.shape) == 2 * pair_index + which
                stats_ref[here, :] = jnp.where(mine, top + jnp.log(total), kept)
            out = jnp.dot(
                (near * inverse).astype(BF16), v_ref[here, :], preferred_element_type=F32
            )
            if start:
                out = out + jnp.dot(
                    (far * inverse).astype(BF16), v_ref[:start, :], preferred_element_type=F32
                )
            outs.append(out)
        o_ref[here, :] = join_heads(outs[0], outs[1], kv).astype(BF16)


def attend_kernel(length_ref, q_ref, k_ref, v_ref, o_ref):
    attend_pair(length_ref[0], pl.program_id(0), q_ref, k_ref, v_ref, o_ref)


def attend(queries, keys, values, lengths):
    pairs = queries.shape[1] // 128
    whole = pl.BlockSpec((LEN, 128), lambda i: (0, 0))
    paired = pl.BlockSpec((LEN, 128), lambda i: (0, i))
    return pl.pallas_call(
        attend_kernel,
        grid=(pairs,),
        out_shape=jax.ShapeDtypeStruct(queries.shape, BF16),
        in_specs=[pl.BlockSpec(memory_space=pltpu.SMEM), paired, whole, whole],
        out_specs=paired,
        compiler_params=pltpu.CompilerParams(vmem_limit_bytes=48 << 20),
        cost_estimate=pl.CostEstimate(
            flops=12 << 30, bytes_accessed=4 << 20, transcendentals=8 << 20
        ),
        name="attend",
    )(lengths, queries, keys, values)


def attend_back_pair(
    length, kv, q_ref, k_ref, v_ref, g_ref, cos_ref, sin_ref, gq_ref, acc_k, acc_v
):
    for block in range(LEN // QB):
        rows = slice(block * QB, (block + 1) * QB)
        keys = (block + 1) * QB
        pair = q_ref[rows, :].astype(F32) * HD**-0.5
        grad_pair = g_ref[rows, :].astype(F32)
        key_pos = lax.broadcasted_iota(jnp.int32, (keys, QB), 0)
        query_pos = block * QB + lax.broadcasted_iota(jnp.int32, (keys, QB), 1)
        allowed = (key_pos <= query_pos) & (key_pos < length)
        key_vecs = k_ref[:keys, :]
        grad_queries = []
        for which in range(2):
            query = pick_head(pair, which, kv).astype(BF16)
            grad = pick_head(grad_pair, which, kv).astype(BF16)
            scores = jnp.where(allowed, nt_dot(key_vecs, query), -1e30)
            exps = jnp.exp(scores - jnp.max(scores, axis=0, keepdims=True))
            probs = exps * (1.0 / jnp.sum(exps, axis=0, keepdims=True))
            grad_probs = nt_dot(v_ref[:keys, :], grad)
            inner = jnp.sum(probs * grad_probs, axis=0, keepdims=True)
            grad_scores = (probs * (grad_probs - inner)).astype(BF16)
            acc_v[:keys, :] += jnp.dot(probs.astype(BF16), grad, preferred_element_type=F32)
            acc_k[:keys, :] += jnp.dot(grad_scores, query, preferred_element_type=F32)
            grad_queries.append(tn_dot(grad_scores, key_vecs) * HD**-0.5)
        joined = join_heads(grad_queries[0], grad_queries[1], kv)
        gq_ref[rows, :] = rope_back(joined, cos_ref[rows, :], sin_ref[rows, :])


def row_products(grads, outs, pair_index, kept):
    product = grads.astype(F32) * outs.astype(F32)
    lanes = lane_index(product.shape)
    low = jnp.sum(jnp.where(lanes < HD, product, 0.0), axis=1, keepdims=True)
    high = jnp.sum(jnp.where(lanes < HD, 0.0, product), axis=1, keepdims=True)
    kept = jnp.where(lanes == 2 * pair_index, low, kept)
    return jnp.where(lanes == 2 * pair_index + 1, high, kept)


def attend_back_tiles(
    pair_index, q_ref, k_ref, v_ref, g_ref, cos_ref, sin_ref, stats_ref, inner_ref, bias_ref,
    gq_ref, acc_k, acc_v, blocks,
):
    kv = pair_index // 2
    square = (QB, QB)
    causal = lax.broadcasted_iota(jnp.int32, square, 0) <= lax.broadcasted_iota(
        jnp.int32, square, 1
    )
    for block in blocks:
        rows = slice(block * QB, (block + 1) * QB)
        pair = q_ref[rows, :].astype(F32) * HD**-0.5
        grad_pair = g_ref[rows, :].astype(F32)
        queries, grads, tops, inners = [], [], [], []
        for which in range(2):
            queries.append(pick_head(pair, which, kv).astype(BF16))
            grads.append(pick_head(grad_pair, which, kv).astype(BF16))
            head = pl.ds(2 * pair_index + which, 1)
            tops.append(stats_ref[head, rows])
            inners.append(inner_ref[head, rows])
        grad_queries = [None, None]
        for tile in range(block + 1):
            here = slice(tile * QB, (tile + 1) * QB)
            key_vecs, value_vecs = k_ref[here, :], v_ref[here, :]
            bias = bias_ref[here, :]
            bias = jnp.concatenate([bias] * (QB // 128), axis=1)
            grad_key = grad_value = None
            for which in range(2):
                scores = nt_dot(key_vecs, queries[which]) + bias
                if tile == block:
                    scores = jnp.where(causal, scores, -1e30)
                probs = jnp.exp(scores - tops[which])
                grad_probs = nt_dot(value_vecs, grads[which])
                grad_scores = (probs * (grad_probs - inners[which])).astype(BF16)
                value = jnp.dot(probs.astype(BF16), grads[which], preferred_element_type=F32)
                key = jnp.dot(grad_scores, queries[which], preferred_element_type=F32)
                query = tn_dot(grad_scores, key_vecs)
                grad_value = value if which == 0 else grad_value + value
                grad_key = key if which == 0 else grad_key + key
                grad_queries[which] = query if tile == 0 else grad_queries[which] + query
            acc_v[here, :] += grad_value
            acc_k[here, :] += grad_key
        joined = join_heads(grad_queries[0], grad_queries[1], kv) * HD**-0.5
        gq_ref[rows, :] = rope_back(joined, cos_ref[rows, :], sin_ref[rows, :])


def attend_back_kernel(
    length_ref, q_ref, k_ref, v_ref, g_ref, cos_ref, sin_ref, gq_ref, gk_ref, gv_ref, acc_k, acc_v
):
    pair_index = pl.program_id(0)

    @pl.when(pair_index == 0)
    def _():
        acc_k[...] = jnp.zeros_like(acc_k)
        acc_v[...] = jnp.zeros_like(acc_v)

    attend_back_pair(
        length_ref[0], pair_index // 2, q_ref, k_ref, v_ref, g_ref, cos_ref, sin_ref, gq_ref,
        acc_k, acc_v,
    )

    @pl.when(pair_index == pl.num_programs(0) - 1)
    def _():
        gk_ref[...] = rope_back(acc_k[...], cos_ref[...], sin_ref[...])
        gv_ref[...] = acc_v[...].astype(BF16)


def attend_back(queries, keys, values, grad_heads, lengths, cosine, sine):
    pairs = queries.shape[1] // 128
    whole = pl.BlockSpec((LEN, 128), lambda i: (0, 0))
    paired = pl.BlockSpec((LEN, 128), lambda i: (0, i))
    narrow = jax.ShapeDtypeStruct((LEN, 128), BF16)
    return pl.pallas_call(
        attend_back_kernel,
        grid=(pairs,),
        out_shape=[jax.ShapeDtypeStruct(queries.shape, BF16), narrow, narrow],
        in_specs=[pl.BlockSpec(memory_space=pltpu.SMEM), paired, whole, whole, paired]
        + [whole] * 2,
        out_specs=[paired, whole, whole],
        scratch_shapes=[pltpu.VMEM((LEN, 128), F32)] * 2,
        compiler_params=pltpu.CompilerParams(vmem_limit_bytes=48 << 20),
        cost_estimate=pl.CostEstimate(
            flops=24 << 30, bytes_accessed=8 << 20, transcendentals=8 << 20
        ),
        name="attend_back",
    )(lengths, queries, keys, values, grad_heads, cosine, sine)


def ring_place(index, count):
    odd = index % 2
    return (1 - odd) * (index // 2) + odd * (count - 1 - index // 2)


def ring_member(place, count):
    high = place // (count // 2)
    return (1 - high) * (2 * place) + high * (2 * (count - 1 - place) + 1)


def ring_setup(count, peers=None, more=()):
    place = ring_place(lax.axis_index("dp"), count)
    ahead = ring_member((place + 1) % count, count)
    behind = ring_member((place + count - 1) % count, count)
    barrier = pltpu.get_barrier_semaphore()
    peers = (peers or [{"dp": ahead}, {"dp": behind}]) + list(more)
    for other in peers:
        pl.semaphore_signal(barrier, inc=1, device_id=other, device_id_type=MESH_ID)
    pl.semaphore_wait(barrier, len(peers))
    return place, (ahead, behind)


def member_at(place, side, steps, count):
    if side == 0:
        return ring_member((place + count - steps) % count, count)
    return ring_member((place + steps) % count, count)


def piece(ref, shape, axis, member, side, part, parts, first=0):
    rows, cols = shape
    sub = rows // (2 * parts)
    start = (side * parts + part) * sub
    if axis is None:
        return ref.at[pl.ds(start, sub), first : first + cols]
    if axis == 0:
        return ref.at[pl.ds(pl.multiple_of(member * rows + start, sub), sub), :]
    return ref.at[pl.ds(start, sub), pl.ds(pl.multiple_of(member * cols, cols), cols)]


def gather_kernel(count, items, *refs):
    num = len(items)
    shards, outs = refs[:num], refs[num : 2 * num]
    stage = refs[2 * num : 3 * num]
    send_sems, recv_sems, local_sem = refs[3 * num :]
    place, neighbours = ring_setup(count)
    me = lax.axis_index("dp")
    slots = [(k, part) for k in range(num) for part in range(items[k][2])]

    def copy(step, side, slot):
        item, part = slots[slot]
        shape, axis, parts, _ = items[item]
        origin = member_at(place, side, step, count)
        target = piece(outs[item], shape, axis, origin, side, part, parts)
        return target, pltpu.make_async_remote_copy(
            src_ref=target,
            dst_ref=target,
            send_sem=send_sems.at[side, step, slot],
            recv_sem=recv_sems.at[side, step, slot],
            device_id={"dp": neighbours[side]},
            device_id_type=MESH_ID,
        )

    for slot, (item, part) in enumerate(slots):
        shape, axis, parts, first = items[item]
        for side in range(2):
            pltpu.make_async_remote_copy(
                src_ref=piece(shards[item], shape, None, 0, side, part, parts, first),
                dst_ref=piece(outs[item], shape, axis, me, side, part, parts),
                send_sem=send_sems.at[side, 0, slot],
                recv_sem=recv_sems.at[side, 0, slot],
                device_id={"dp": neighbours[side]},
                device_id_type=MESH_ID,
            ).start()
    loads = [
        pltpu.make_async_copy(
            shards[k].at[:, items[k][3] : items[k][3] + items[k][0][1]],
            stage[k],
            local_sem.at[k],
        )
        for k in range(num)
    ]
    for load in loads:
        load.start()
    stores = []
    for k in range(num):
        loads[k].wait()
        shape, axis, parts, _ = items[k]
        rows, cols = shape
        if axis == 0:
            own = outs[k].at[pl.ds(pl.multiple_of(me * rows, rows), rows), :]
        else:
            own = outs[k].at[:, pl.ds(pl.multiple_of(me * cols, cols), cols)]
        stores.append(pltpu.make_async_copy(stage[k], own, local_sem.at[k]))
        stores[-1].start()

    def hop(step, carry):
        for slot in range(len(slots)):
            for side in range(2):
                copy(step - 1, side, slot)[1].wait_recv()
                copy(step, side, slot)[1].start()
        return carry

    lax.fori_loop(1, count - 1, hop, 0)
    for slot in range(len(slots)):
        for side in range(2):
            copy(count - 2, side, slot)[1].wait_recv()
    for store in stores:
        store.wait()

    def drain(step, carry):
        for slot in range(len(slots)):
            for side in range(2):
                copy(step, side, slot)[1].wait_send()
        return carry

    lax.fori_loop(0, count - 1, drain, 0)


def ring_gather(shards, axes, parts, count, collective_id, first=0):
    turned = [a == 1 and s.shape[1] % 128 != 0 for s, a in zip(shards, axes)]
    if any(turned):
        shards = [s.T if t else s for s, t in zip(shards, turned)]
        axes = [0 if t else a for a, t in zip(axes, turned)]
        outs = ring_gather(shards, axes, parts, count, collective_id)
        return [o.T if t else o for o, t in zip(outs, turned)]
    shapes = [(s.shape[0], s.shape[1] - first) for s in shards]
    items = tuple((s, a, q, first) for s, a, q in zip(shapes, axes, parts))
    slots = sum(parts)
    outs = [
        jax.ShapeDtypeStruct((s[0] * count, s[1]) if a == 0 else (s[0], s[1] * count), BF16)
        for s, a in zip(shapes, axes)
    ]
    num = len(shards)
    nbytes = sum(s.size * 2 * (count - 1) for s in shards)
    return pl.pallas_call(
        functools.partial(gather_kernel, count, items),
        out_shape=outs,
        in_specs=[pl.BlockSpec(memory_space=pl.ANY)] * num,
        out_specs=[pl.BlockSpec(memory_space=pl.ANY)] * num,
        scratch_shapes=[pltpu.VMEM(s, BF16) for s in shapes]
        + [
            pltpu.SemaphoreType.DMA((2, count - 1, slots)),
            pltpu.SemaphoreType.DMA((2, count - 1, slots)),
            pltpu.SemaphoreType.DMA((num,)),
        ],
        compiler_params=pltpu.CompilerParams(collective_id=collective_id, has_side_effects=True),
        cost_estimate=pl.CostEstimate(flops=0, bytes_accessed=20 * nbytes, transcendentals=0),
        name=f"ring_gather_{collective_id}",
    )(*shards)


def scatter_kernel(count, items, *refs):
    num = len(items)
    partials, outs = refs[:num], refs[num : 2 * num]
    own = refs[2 * num : 3 * num]
    held = refs[3 * num : 4 * num]
    total = refs[4 * num : 5 * num]
    send_sems, recv_sems, load_sems, store_sems = refs[5 * num :]
    slots = [(k, part) for k in range(num) for part in range(items[k][2])]

    def load(step, side, slot, place):
        item, part = slots[slot]
        shape, axis, parts = items[item]
        member = member_at(place, side, step + 1, count)
        return pltpu.make_async_copy(
            piece(partials[item], shape, axis, member, side, part, parts),
            own[item].at[side, step, part],
            load_sems.at[side, step, slot],
        )

    start_place = ring_place(lax.axis_index("dp"), count)

    def load_all(step, carry):
        for slot in range(len(slots)):
            for side in range(2):
                load(step, side, slot, start_place).start()
        return carry

    lax.fori_loop(0, count, load_all, 0)
    place, neighbours = ring_setup(count)

    def send(step, side, slot, source):
        item, part = slots[slot]
        return pltpu.make_async_remote_copy(
            src_ref=source,
            dst_ref=held[item].at[side, step, part],
            send_sem=send_sems.at[side, step, slot],
            recv_sem=recv_sems.at[side, step, slot],
            device_id={"dp": neighbours[side]},
            device_id_type=MESH_ID,
        )

    for slot, (item, part) in enumerate(slots):
        for side in range(2):
            load(0, side, slot, place).wait()
            send(0, side, slot, own[item].at[side, 0, part]).start()

    def hop(step, carry):
        for slot, (item, part) in enumerate(slots):
            for side in range(2):
                load(step, side, slot, place).wait()
                arrived = held[item].at[side, step - 1, part]
                send(step - 1, side, slot, arrived).wait_recv()
                arrived[...] = (
                    arrived[...].astype(jnp.float32)
                    + own[item][side, step, part].astype(jnp.float32)
                ).astype(jnp.bfloat16)
                send(step, side, slot, arrived).start()
        return carry

    lax.fori_loop(1, count - 1, hop, 0)
    last = count - 1
    stores = []
    for slot, (item, part) in enumerate(slots):
        shape, axis, parts = items[item]
        for side in range(2):
            load(last, side, slot, place).wait()
            arrived = held[item].at[side, last - 1, part]
            send(last - 1, side, slot, arrived).wait_recv()
            total[item][side, part] = arrived[...].astype(jnp.float32) + own[item][
                side, last, part
            ].astype(jnp.float32)
            stores.append(
                pltpu.make_async_copy(
                    total[item].at[side, part],
                    piece(outs[item], shape, None, 0, side, part, parts),
                    store_sems.at[side, slot],
                )
            )
            stores[-1].start()
    for store in stores:
        store.wait()

    def drain(step, carry):
        for slot, (item, part) in enumerate(slots):
            for side in range(2):
                send(step, side, slot, held[item].at[side, 0, part]).wait_send()
        return carry

    lax.fori_loop(0, count - 1, drain, 0)


def ring_scatter(partials, axes, parts, count, collective_id):
    turned = [a == 1 and p.shape[1] // count % 128 != 0 for p, a in zip(partials, axes)]
    if any(turned):
        partials = [p.T if t else p for p, t in zip(partials, turned)]
        axes = [0 if t else a for a, t in zip(axes, turned)]
        outs = ring_scatter(partials, axes, parts, count, collective_id)
        return [o.T if t else o for o, t in zip(outs, turned)]
    shapes = [
        (p.shape[0] // count, p.shape[1]) if a == 0 else (p.shape[0], p.shape[1] // count)
        for p, a in zip(partials, axes)
    ]
    items = tuple((s, a, q) for s, a, q in zip(shapes, axes, parts))
    slots = sum(parts)
    num = len(partials)

    def buffers(depth, dtype):
        return [
            pltpu.VMEM((2,) + depth + (q, s[0] // (2 * q), s[1]), dtype)
            for s, q in zip(shapes, parts)
        ]

    nbytes = sum(p.size * 2 for p in partials)
    return pl.pallas_call(
        functools.partial(scatter_kernel, count, items),
        out_shape=[jax.ShapeDtypeStruct(s, jnp.float32) for s in shapes],
        in_specs=[pl.BlockSpec(memory_space=pl.ANY)] * num,
        out_specs=[pl.BlockSpec(memory_space=pl.ANY)] * num,
        scratch_shapes=buffers((count,), jnp.bfloat16)
        + buffers((count - 1,), jnp.bfloat16)
        + buffers((), jnp.float32)
        + [
            pltpu.SemaphoreType.DMA((2, count - 1, slots)),
            pltpu.SemaphoreType.DMA((2, count - 1, slots)),
            pltpu.SemaphoreType.DMA((2, count, slots)),
            pltpu.SemaphoreType.DMA((2, slots)),
        ],
        compiler_params=pltpu.CompilerParams(
            collective_id=collective_id, has_side_effects=True, vmem_limit_bytes=48 << 20
        ),
        cost_estimate=pl.CostEstimate(flops=0, bytes_accessed=20 * nbytes, transcendentals=0),
        name=f"ring_scatter_{collective_id}",
    )(*partials)


class Job(NamedTuple):
    left: Any
    right: Any
    start: int
    cols: int
    into: Any = None
    target: int = 0
    pieces: tuple = ()


class Extra(NamedTuple):
    builder: Any
    given: list
    given_specs: list
    made: list
    made_specs: list
    spare: list


def scatter_dot_kernel(count, items, num_outs, num_bases, parts, extra, *refs):
    num = len(items)
    taken = 0

    def take(amount):
        nonlocal taken
        taken += amount
        return refs[taken - amount : taken]

    lefts, rights, _ = take(num), take(num), take(num_bases)
    given = take(len(extra.given) if extra else 0)
    outs = take(num_outs)
    made = take(len(extra.made) if extra else 0)
    left_bufs, right_bufs, firsts, owns, helds, totals = (take(num) for _ in range(6))
    send_sems, recv_sems, left_sems, right_sems, store_sems = take(5)
    beside = (
        extra.builder(count, given, made, refs[taken:], (left_bufs, right_bufs)) if extra else None
    )
    entry_place = ring_place(lax.axis_index("dp"), count)
    last = count - 1

    ready = [buf.shape[0] == 8 for buf in right_bufs]

    def load_right(item):
        _, half, start, _ = items[item]
        return pltpu.make_async_copy(
            rights[item].at[:, start : start + 2 * half], right_bufs[item], right_sems.at[item]
        )

    def load_left(step, side, item, place):
        block = items[item][0]
        member = member_at(place, side, step + 1, count)
        slot = step % 2
        here = pl.ds(pl.multiple_of(member * block, block), block)
        if ready[item]:
            half = items[item][1]
            source = lefts[item].at[here, side * half : (side + 1) * half]
        else:
            source = lefts[item].at[:, here]
        return pltpu.make_async_copy(
            source, left_bufs[item].at[side, slot], left_sems.at[side, slot, item]
        )

    for item in range(num):
        if not ready[item]:
            load_right(item).start()
        for side in range(2):
            load_left(0, side, item, entry_place).start()
    if beside:
        beside.begin()
    place, neighbours = ring_setup(count, *(beside.peers() if beside else ()))
    pairs = [(item, side) for item in range(num) for side in range(2)]

    def send(step, side, item, part, source):
        return pltpu.make_async_remote_copy(
            src_ref=source.at[part],
            dst_ref=helds[item].at[side, step, part],
            send_sem=send_sems.at[side, step, item * parts + part],
            recv_sem=recv_sems.at[side, step, item * parts + part],
            device_id={"dp": neighbours[side]},
            device_id_type=MESH_ID,
        )

    def stores(item, side, part):
        block, _, _, places = items[item]
        rows = block // parts
        return [
            pltpu.make_async_copy(
                totals[item].at[side, part, :, source : source + cols],
                outs[out].at[part * rows : (part + 1) * rows, column : column + cols],
                store_sems.at[side, item * parts + part, k],
            )
            for k, (source, cols, out, column) in enumerate(places[side])
        ]

    for item in range(num):
        if not ready[item]:
            load_right(item).wait()

    def turn(step, carry):
        @pl.when(step < last)
        def _():
            for item, side in pairs:
                load_left(step + 1, side, item, place).start()

        for item in range(num):
            half = items[item][1]
            for side in range(2):
                load_left(step, side, item, place).wait()

            if ready[item]:
                for side in range(2):
                    owns[item][side] = (
                        left_bufs[item][side, step % 2].astype(F32).reshape(owns[item].shape[1:])
                    )
                continue

            def own_sum(side, inner):
                cols = pl.ds(pl.multiple_of(side * half, half), half)
                owns[item][side] = tn_dot(
                    left_bufs[item][side, step % 2], right_bufs[item][:, cols]
                ).reshape(owns[item].shape[1:])
                return inner

            lax.fori_loop(0, 2, own_sum, 0)

        @pl.when(step == 0)
        def _():
            for part in range(parts):
                for item, side in pairs:
                    firsts[item][side, part] = owns[item][side, part].astype(BF16)
                    send(0, side, item, part, firsts[item].at[side]).start()

        if beside:
            beside.compute(step)

        @pl.when((step > 0) & (step < last))
        def _():
            for part in range(parts):
                for item, side in pairs:
                    arrived = helds[item].at[side, step - 1]
                    send(step - 1, side, item, part, arrived).wait_recv()
                    arrived[part] = (
                        arrived[part].astype(F32) + owns[item][side, part]
                    ).astype(BF16)
                    send(step, side, item, part, arrived).start()

        return carry

    lax.fori_loop(0, count, turn, 0)
    for part in range(parts):
        for item, side in pairs:
            arrived = helds[item].at[side, last - 1]
            send(last - 1, side, item, part, arrived).wait_recv()
            totals[item][side, part] = arrived[part].astype(F32) + owns[item][side, part]
            for copy in stores(item, side, part):
                copy.start()
    if beside:
        beside.finish()
    for part in range(parts):
        for item, side in pairs:
            for copy in stores(item, side, part):
                copy.wait()

    def drain(step, carry):
        for part in range(parts):
            for item, side in pairs:
                send(step, side, item, part, helds[item].at[side, 0]).wait_send()
        return carry

    lax.fori_loop(0, last, drain, 0)


def ring_scatter_dots(jobs, parts, count, collective_id, extra=None):
    rows = next((j.left.shape[0] for j in jobs if j.right is not None), 0)
    items, shapes, bases, aliases = [], [], [], {}
    for job in jobs:
        width = job.left.shape[1] if job.right is not None else job.left.shape[0]
        block, half = width // count, job.cols // 2
        if job.pieces:
            places, column = ([], []), 0
            for cols in job.pieces:
                for side in range(2):
                    low = max(column, side * half)
                    high = min(column + cols, (side + 1) * half)
                    if low < high:
                        places[side].append(
                            (low - side * half, high - low, len(shapes), low - column)
                        )
                column += cols
                shapes.append((block, cols))
        else:
            places = [
                [(0, half, len(shapes), job.target + side * half)] for side in range(2)
            ]
            if job.into is None:
                shapes.append((block, job.cols))
            elif isinstance(job.into, int):
                shapes.append((block, job.into))
            else:
                aliases[2 * len(jobs) + len(bases)] = len(shapes)
                bases.append(job.into)
                shapes.append(job.into.shape)
        items.append((block, half, job.start, places))
    num = len(jobs)

    def buffers(depth, dtype):
        return [pltpu.VMEM(depth + (parts, b // parts, h), dtype) for b, h, _, _ in items]

    slots = num * parts
    flops = sum(2 * rows * count * i[0] * 2 * i[1] for i in items)
    nbytes = sum(2 * count * i[0] * 2 * i[1] for i in items)
    dots = [j.right is not None for j in jobs]
    given, given_specs, made, made_specs, spare = extra[1:] if extra else ([], [], [], [], [])
    return pl.pallas_call(
        functools.partial(
            scatter_dot_kernel, count, items, len(shapes), len(bases), parts, extra
        ),
        out_shape=[jax.ShapeDtypeStruct(s, F32) for s in shapes] + made,
        in_specs=[ANY] * (2 * num + len(bases)) + given_specs,
        out_specs=[ANY] * len(shapes) + made_specs,
        input_output_aliases=aliases,
        scratch_shapes=[
            pltpu.VMEM((2, 2) + ((rows, i[0]) if dot_job else (i[0], i[1])), BF16)
            for i, dot_job in zip(items, dots)
        ]
        + [
            pltpu.VMEM((rows, 2 * i[1]) if dot_job else (8, 128), BF16)
            for i, dot_job in zip(items, dots)
        ]
        + buffers((2,), BF16)
        + buffers((2,), F32)
        + buffers((2, count - 1), BF16)
        + buffers((2,), F32)
        + [
            pltpu.SemaphoreType.DMA((2, count - 1, slots)),
            pltpu.SemaphoreType.DMA((2, count - 1, slots)),
            pltpu.SemaphoreType.DMA((2, 2, num)),
            pltpu.SemaphoreType.DMA((num,)),
            pltpu.SemaphoreType.DMA((2, slots, 3)),
        ]
        + spare,
        compiler_params=pltpu.CompilerParams(
            collective_id=collective_id, has_side_effects=True, vmem_limit_bytes=60 << 20
        ),
        cost_estimate=pl.CostEstimate(
            flops=flops, bytes_accessed=20 * nbytes, transcendentals=0
        ),
        name=f"ring_scatter_{collective_id}",
    )(
        *[j.left for j in jobs],
        *[j.left if j.right is None else j.right for j in jobs],
        *bases,
        *given,
    )


class ShareWork:
    def __init__(self, count, given, made, spare, bufs):
        self.given, self.out = given, made[0]
        self.pair, self.first, self.sums, self.second, self.sems = spare
        self.count, self.group = count, self.second.shape[0] + 1
        self.row, self.col = lax.axis_index("dp"), lax.axis_index("tensor")

    def in_column(self, shift):
        return {"dp": (self.row + shift) % self.count}

    def in_group(self, shift):
        return {"tensor": (self.col + shift) % self.group}

    def peers(self):
        column = [self.in_column(s) for s in range(1, self.count)]
        return column, [self.in_group(s) for s in range(1, self.group)]

    def begin(self):
        pass

    def part(self, row):
        width = self.sums.shape[1]
        return pl.ds(pl.multiple_of(row * width, width), width)

    def move(self, stage, shift):
        if stage == 0:
            source = self.pair.at[:, self.part((self.row + shift) % self.count)]
            target, device, slot = self.first.at[shift - 1], self.in_column(shift), shift - 1
        else:
            source, target = self.sums, self.second.at[shift - 1]
            device, slot = self.in_group(shift), self.count + shift - 2
        return pltpu.make_async_remote_copy(
            src_ref=source,
            dst_ref=target,
            send_sem=self.sems.at[0, slot],
            recv_sem=self.sems.at[1, slot],
            device_id=device,
            device_id_type=MESH_ID,
        )

    def compute(self, step):
        @pl.when(step == 0)
        def _():
            self.pair[...] = self.given[0][...]
            self.pair[1:2, :] = self.given[1][...]
            for shift in range(1, self.count):
                self.move(0, shift).start()

        @pl.when(step == 5)
        def _():
            total = self.pair[:, self.part(self.row)]
            for shift in range(1, self.count):
                self.move(0, shift).wait()
                total = total + self.first[shift - 1]
            self.sums[...] = total
            for shift in range(1, self.group):
                self.move(1, shift).start()

    def finish(self):
        total = self.sums[...]
        for shift in range(1, self.group):
            self.move(1, shift).wait()
            total = total + self.second[shift - 1]
        share = total.shape[1] // self.group
        picked = jnp.zeros((8, share), F32)
        for col in range(self.group):
            picked = jnp.where(self.col == col, total[:, col * share : (col + 1) * share], picked)
        self.out[:, :share] = picked


class ProductWork:
    def __init__(self, count, given, made, spare, bufs):
        self.right, self.out = given[0], made[0]
        self.right_buf, self.stage, self.load_sem, self.sems = spare
        self.left, self.count = bufs[0][0], count
        self.place = ring_place(lax.axis_index("dp"), count)
        self.start = self.right.shape[1] - self.right_buf.shape[1]

    def peers(self):
        return ()

    def load(self):
        return pltpu.make_async_copy(
            self.right.at[:, self.start :], self.right_buf, self.load_sem
        )

    def begin(self):
        self.load().start()

    def store(self, step):
        block = self.stage.shape[1]
        member = member_at(self.place, 0, step + 1, self.count)
        return pltpu.make_async_copy(
            self.stage.at[step % 2],
            self.out.at[pl.ds(pl.multiple_of(member * block, block), block), :],
            self.sems.at[step % 2],
        )

    def compute(self, step):
        @pl.when(step == 0)
        def _():
            self.load().wait()

        @pl.when(step >= 2)
        def _():
            self.store(step - 2).wait()

        self.stage[step % 2] = tn_dot(self.left[0, step % 2], self.right_buf[...]).astype(BF16)
        self.store(step).start()

    def finish(self):
        for step in (self.count - 2, self.count - 1):
            self.store(step).wait()


def product_work(right, start, count, width):
    rows, cols = right.shape[0], right.shape[1] - start
    return Extra(
        ProductWork,
        [right],
        [ANY],
        [jax.ShapeDtypeStruct((width, cols), BF16)],
        [ANY],
        [
            pltpu.VMEM((rows, cols), BF16),
            pltpu.VMEM((2, width // count, cols), BF16),
            pltpu.SemaphoreType.DMA,
            pltpu.SemaphoreType.DMA((2,)),
        ],
    )


class GatherWork:
    def __init__(self, count, given, made, spare, bufs):
        self.own, self.out = given[0], made[0]
        self.stage, self.sems, self.local = spare
        self.col = lax.axis_index("tensor")
        self.rows = self.own.shape[0]
        self.parts = self.sems.shape[2]

    def core(self):
        return {"tensor": self.col + 1 - 2 * (self.col % 2)}

    def across(self):
        return {"tensor": (self.col + 2) % 4}

    def peers(self):
        return None, [self.core(), self.across()]

    def begin(self):
        pltpu.make_async_copy(self.own, self.stage, self.local).start()

    def spot(self, member, part):
        size = self.rows // self.parts
        return pl.ds(pl.multiple_of(member * self.rows + part * size, size), size)

    def move(self, kind, part):
        size = self.rows // self.parts
        member = (self.col + 2) % 4 if kind == 2 else self.col
        target = self.out.at[self.spot(member, part), :]
        source = target if kind == 2 else self.own.at[part * size : (part + 1) * size, :]
        return pltpu.make_async_remote_copy(
            src_ref=source,
            dst_ref=target,
            send_sem=self.sems.at[0, kind, part],
            recv_sem=self.sems.at[1, kind, part],
            device_id=self.across() if kind == 0 else self.core(),
            device_id_type=MESH_ID,
        )

    def keep(self):
        here = pl.ds(pl.multiple_of(self.col * self.rows, self.rows), self.rows)
        return pltpu.make_async_copy(self.stage, self.out.at[here, :], self.local)

    def compute(self, step):
        @pl.when(step == 0)
        def _():
            for part in range(self.parts):
                self.move(0, part).start()
                self.move(1, part).start()
            pltpu.make_async_copy(self.own, self.stage, self.local).wait()
            self.keep().start()

        for part, turn in enumerate((2, 4, 5, 6)):

            @pl.when(step == turn)
            def _():
                self.move(0, part).wait_recv()
                self.move(2, part).start()

    def finish(self):
        for part in range(self.parts):
            self.move(0, part).wait_send()
            self.move(1, part).wait()
            self.move(2, part).wait()
        self.keep().wait()


def gather_work(own):
    rows, width = own.shape
    return Extra(
        GatherWork,
        [own],
        [ANY],
        [jax.ShapeDtypeStruct((4 * rows, width), BF16)],
        [ANY],
        [
            pltpu.VMEM(own.shape, BF16),
            pltpu.SemaphoreType.DMA((2, 3, 4)),
            pltpu.SemaphoreType.DMA,
        ],
    )


def share_work(first, second, count, group):
    width = first.shape[1] // count
    vmem = pl.BlockSpec(memory_space=pltpu.VMEM)
    return Extra(
        ShareWork,
        [first, second],
        [vmem] * 2,
        [jax.ShapeDtypeStruct((8, 128), F32)],
        [vmem],
        [
            pltpu.VMEM(first.shape, F32),
            pltpu.VMEM((count - 1, 8, width), F32),
            pltpu.VMEM((8, width), F32),
            pltpu.VMEM((group - 1, 8, width), F32),
            pltpu.SemaphoreType.DMA((2, count + group - 2)),
        ],
    )


class NormWork:
    def __init__(self, count, given, made, spare, bufs):
        self.grads, self.gates = given[:2], tuple(given[2:4])
        self.up, self.down = given[4:]
        self.outs = made
        self.grad_bufs, self.row_bufs, self.down_bufs, self.stage = spare[0], *spare[1:4]
        self.grad_sems, self.row_sems, self.down_sems, self.out_sems = spare[4:]
        self.act = bufs[1][0]
        self.count = count
        self.block = self.row_bufs.shape[2]

    def load_grad(self, which):
        return pltpu.make_async_copy(
            self.grads[which], self.grad_bufs.at[which], self.grad_sems.at[which]
        )

    def spot(self, step):
        return pl.ds(pl.multiple_of(step * self.block, self.block), self.block)

    def loads(self, step):
        slot = step % 2
        edge = self.gates[0].shape[1]
        gate = self.row_bufs.at[0, slot]
        targets = [gate.at[:, :edge], gate.at[:, edge:], self.row_bufs.at[1, slot]]
        rows = [
            pltpu.make_async_copy(
                source.at[self.spot(step), :], target, self.row_sems.at[which, slot]
            )
            for which, (source, target) in enumerate(zip(self.gates + (self.up,), targets))
        ]
        down = pltpu.make_async_copy(
            self.down.at[:, self.spot(step)], self.down_bufs.at[slot], self.down_sems.at[slot]
        )
        return rows + [down]

    def store(self, which, step):
        slot = step % 2
        return pltpu.make_async_copy(
            self.stage.at[which, slot],
            self.outs[which].at[:, self.spot(step)],
            self.out_sems.at[which, slot],
        )

    def begin(self):
        for which in range(2):
            self.load_grad(which).start()
        for copy in self.loads(0):
            copy.start()

    def peers(self):
        return ()

    def compute(self, step):
        @pl.when(step < self.count - 1)
        def _():
            for copy in self.loads(step + 1):
                copy.start()

        @pl.when(step == 0)
        def _():
            for which in range(2):
                self.load_grad(which).wait()

        @pl.when(step >= 2)
        def _():
            for which in range(2):
                self.store(which, step - 2).wait()

        for copy in self.loads(step):
            copy.wait()
        slot = step % 2

        def lines(index, carry):
            band = pl.ds(pl.multiple_of(index * 256, 256), 256)
            norm = nt_dot(self.grad_bufs[0, band, :], self.row_bufs[0, slot])
            norm += nt_dot(self.grad_bufs[1, band, :], self.row_bufs[1, slot])
            self.stage[0, slot, band, :] = norm.astype(BF16)
            value = jnp.dot(
                self.act[band, :], self.down_bufs[slot], preferred_element_type=F32
            )
            self.stage[1, slot, band, :] = value.astype(BF16)
            return carry

        lax.fori_loop(0, self.act.shape[0] // 256, lines, 0)
        for which in range(2):
            self.store(which, step).start()

    def finish(self):
        for step in range(max(self.count - 2, 0), self.count):
            for which in range(2):
                self.store(which, step).wait()


def down_ring(grad_branch, activated, grad_gate, grad_up, gates, up_all, down_all, count, cid):
    rows, hidden = activated.shape
    width = up_all.shape[0]
    block = width // count
    wide = jax.ShapeDtypeStruct((rows, width), BF16)
    spare = [
        pltpu.VMEM((2, rows, hidden), BF16),
        pltpu.VMEM((2, 2, block, hidden), BF16),
        pltpu.VMEM((2, hidden, block), BF16),
        pltpu.VMEM((2, 2, rows, block), BF16),
        pltpu.SemaphoreType.DMA((2,)),
        pltpu.SemaphoreType.DMA((3, 2)),
        pltpu.SemaphoreType.DMA((2,)),
        pltpu.SemaphoreType.DMA((2, 2)),
    ]
    given = [grad_gate, grad_up, *gates, up_all, down_all]
    return ring_scatter_dots(
        [Job(grad_branch, activated, 0, hidden)],
        2,
        count,
        cid,
        Extra(NormWork, given, [ANY] * 6, [wide, wide], [ANY] * 2, spare),
    )


def mlp_kernel(count, *refs):
    x_hbm, wg_hbm, wg_rest, wu_hbm, shard, gb_hbm = refs[:6]
    act_hbm, gg_hbm, gu_hbm, down_all = refs[6:10]
    x_buf, gb_buf, w_bufs, gate_slope, up_slope, acc, half_bufs, stage, own_stage = refs[10:19]
    send_sems, recv_sems, w_sems, in_sems, half_sems, out_sems, local_sem = refs[19:]
    rows, width = x_buf.shape
    hidden = acc.shape[1]
    block = width // count
    cols = w_bufs.shape[-1]
    steps = hidden // cols
    half = hidden // 2
    parts = send_sems.shape[2]
    me = lax.axis_index("dp")

    gate_steps = wg_hbm.shape[1] // cols

    def load_weights(step, which, source=None):
        start = step - gate_steps if source is wg_rest else step
        source = (wg_hbm, wu_hbm)[which] if source is None else source
        return pltpu.make_async_copy(
            source.at[:, pl.ds(pl.multiple_of(start * cols, cols), cols)],
            w_bufs.at[which, step % 2],
            w_sems.at[which, step % 2],
        )

    def fetch(step):
        load_weights(step, 1).start()

        @pl.when(step < gate_steps)
        def _():
            load_weights(step, 0).start()

        @pl.when(step >= gate_steps)
        def _():
            load_weights(step, 0, wg_rest).start()

    load_x = pltpu.make_async_copy(x_hbm, x_buf, in_sems.at[0])
    load_gb = pltpu.make_async_copy(gb_hbm, gb_buf, in_sems.at[1])
    load_own = pltpu.make_async_copy(shard, own_stage, local_sem)
    load_x.start()
    for which in range(2):
        load_weights(0, which).start()
    load_own.start()
    load_gb.start()
    place, neighbours = ring_setup(count)

    def target(ref, member, side, part):
        return piece(ref, (hidden, block), 1, member, side, part, parts)

    def hop(step, side, part):
        ref = target(down_all, member_at(place, side, step, count), side, part)
        return pltpu.make_async_remote_copy(
            src_ref=ref,
            dst_ref=ref,
            send_sem=send_sems.at[side, step, part],
            recv_sem=recv_sems.at[side, step, part],
            device_id={"dp": neighbours[side]},
            device_id_type=MESH_ID,
        )

    for part in range(parts):
        for side in range(2):
            pltpu.make_async_remote_copy(
                src_ref=piece(shard, (hidden, block), None, 0, side, part, parts),
                dst_ref=target(down_all, me, side, part),
                send_sem=send_sems.at[side, 0, part],
                recv_sem=recv_sems.at[side, 0, part],
                device_id={"dp": neighbours[side]},
                device_id_type=MESH_ID,
            ).start()

    def pump(step):
        for part in range(parts):
            for side in range(2):
                hop(step - 1, side, part).wait_recv()
                hop(step, side, part).start()

    load_own.wait()
    store_own = pltpu.make_async_copy(
        own_stage, down_all.at[:, pl.ds(pl.multiple_of(me * block, block), block)], local_sem
    )
    store_own.start()
    load_x.wait()

    def store(ref, which, step):
        return pltpu.make_async_copy(
            stage.at[which, step % 2],
            ref.at[:, pl.ds(pl.multiple_of(step * cols, cols), cols)],
            out_sems.at[which, step % 2],
        )

    def forward(step, carry):
        @pl.when(step + 1 < steps)
        def _():
            fetch(step + 1)

        @pl.when(step >= 2)
        def _():
            store(act_hbm, 0, step - 2).wait()

        load_weights(step, 1).wait()

        @pl.when(step < gate_steps)
        def _():
            load_weights(step, 0).wait()

        @pl.when(step >= gate_steps)
        def _():
            load_weights(step, 0, wg_rest).wait()

        here = pl.ds(pl.multiple_of(step * cols, cols), cols)
        for top in range(0, rows, 256):
            band = pl.ds(top, 256)
            lines = x_buf[band, :]
            gate = jnp.dot(lines, w_bufs[0, step % 2], preferred_element_type=F32)
            up = jnp.dot(lines, w_bufs[1, step % 2], preferred_element_type=F32)
            sig = jax.nn.sigmoid(gate)
            silu = gate * sig
            stage[0, step % 2, band, :] = (silu * up).astype(BF16)
            gate_slope[band, here] = up * sig * (1.0 + gate * (1.0 - sig))
            up_slope[band, here] = silu
            acc[band, here] = jnp.zeros((256, cols), F32)
        store(act_hbm, 0, step).start()

        turn = (step + 1) // 2

        @pl.when((step % 2 == 1) & (turn <= count - 2))
        def _():
            pump(turn)

        return carry

    lax.fori_loop(0, steps, forward, 0)
    for step in range(max(steps - 2, 0), steps):
        store(act_hbm, 0, step).wait()
    pumped = min(steps // 2, count - 2)
    load_gb.wait()

    def load_half(step, side):
        member = member_at(place, side, step, count)
        return pltpu.make_async_copy(
            down_all.at[
                pl.ds(side * half, half), pl.ds(pl.multiple_of(member * block, block), block)
            ],
            half_bufs.at[side],
            half_sems.at[side],
        )

    def backward(step, carry):
        @pl.when((step > pumped) & (step <= count - 2))
        def _():
            pump(step)

        @pl.when(step == count - 1)
        def _():
            for part in range(parts):
                for side in range(2):
                    hop(count - 2, side, part).wait_recv()

        for side in range(2):
            load_half(step, side).start()
        for side in range(2):
            member = member_at(place, side, step, count)
            load_half(step, side).wait()
            here = pl.ds(pl.multiple_of(member * block, block), block)
            spot = pl.ds(side * half, half)

            def lines(index, carry):
                band = pl.ds(pl.multiple_of(index * 256, 256), 256)
                acc[band, spot] += nt_dot(gb_buf[band, here], half_bufs[side])
                return carry

            lax.fori_loop(0, rows // 256, lines, 0)

        return carry

    store_own.wait()
    lax.fori_loop(0, count, backward, 0)

    def slopes(step, carry):
        @pl.when(step >= 2)
        def _():
            store(gg_hbm, 1, step - 2).wait()
            store(gu_hbm, 2, step - 2).wait()

        here = pl.ds(pl.multiple_of(step * cols, cols), cols)

        def lines(index, carry):
            band = pl.ds(pl.multiple_of(index * 256, 256), 256)
            value = acc[band, here]
            stage[1, step % 2, band, :] = (value * gate_slope[band, here]).astype(BF16)
            stage[2, step % 2, band, :] = (value * up_slope[band, here]).astype(BF16)
            return carry

        lax.fori_loop(0, rows // 256, lines, 0)
        store(gg_hbm, 1, step).start()
        store(gu_hbm, 2, step).start()
        return carry

    lax.fori_loop(0, steps, slopes, 0)
    for step in range(max(steps - 2, 0), steps):
        store(gg_hbm, 1, step).wait()
        store(gu_hbm, 2, step).wait()

    def drain(step, carry):
        for part in range(parts):
            for side in range(2):
                hop(step, side, part).wait_send()
        return carry

    lax.fori_loop(0, count - 1, drain, 0)


def mlp_ring(rows_mlp, gates, up_all, w_down, grad_branch, count, collective_id):
    rows, width = rows_mlp.shape
    hidden, block = w_down.shape
    cols, parts = 256, 2
    wide = jax.ShapeDtypeStruct((rows, hidden), BF16)
    return pl.pallas_call(
        functools.partial(mlp_kernel, count),
        out_shape=[wide] * 3 + [jax.ShapeDtypeStruct((hidden, width), BF16)],
        in_specs=[ANY] * 6,
        out_specs=[pl.BlockSpec(memory_space=pl.ANY)] * 4,
        scratch_shapes=[
            pltpu.VMEM((rows, width), BF16),
            pltpu.VMEM((rows, width), BF16),
            pltpu.VMEM((2, 2, width, cols), BF16),
            pltpu.VMEM((rows, hidden), F32),
            pltpu.VMEM((rows, hidden), F32),
            pltpu.VMEM((rows, hidden), F32),
            pltpu.VMEM((2, hidden // 2, block), BF16),
            pltpu.VMEM((3, 2, rows, cols), BF16),
            pltpu.VMEM((hidden, block), BF16),
            pltpu.SemaphoreType.DMA((2, count - 1, parts)),
            pltpu.SemaphoreType.DMA((2, count - 1, parts)),
            pltpu.SemaphoreType.DMA((2, 2)),
            pltpu.SemaphoreType.DMA((2,)),
            pltpu.SemaphoreType.DMA((2,)),
            pltpu.SemaphoreType.DMA((3, 2)),
            pltpu.SemaphoreType.DMA,
        ],
        compiler_params=pltpu.CompilerParams(
            collective_id=collective_id, has_side_effects=True, vmem_limit_bytes=60 << 20
        ),
        cost_estimate=pl.CostEstimate(
            flops=6 * rows * width * hidden,
            bytes_accessed=40 * hidden * width,
            transcendentals=rows * hidden,
        ),
        name="mlp_ring",
    )(rows_mlp, *gates, up_all, w_down, grad_branch)


class HeadWork:
    def __init__(self, count, given, made, spare, bufs):
        self.length, self.gain, self.sources = given[0], given[1], given[2:]
        self.grads_out, self.token_out, self.gain_out = made
        num = len(self.sources)
        self.bufs = spare[:num]
        self.heads, self.grads, self.acc_k, self.acc_v, self.stage = spare[num : num + 5]
        self.stats, self.inner, self.bias = spare[num + 5 : num + 8]
        self.in_sems, self.out_sems = spare[num + 8 :]

    def peers(self):
        return ()

    def load(self, which):
        return pltpu.make_async_copy(
            self.sources[which], self.bufs[which], self.in_sems.at[which]
        )

    def begin(self):
        for which in range(len(self.sources)):
            self.load(which).start()
        self.gain_out[...] = jnp.zeros_like(self.gain_out)
        self.acc_k[...] = jnp.zeros_like(self.acc_k)
        self.acc_v[...] = jnp.zeros_like(self.acc_v)
        key_pos = lax.broadcasted_iota(jnp.int32, self.bias.shape, 0)
        self.bias[...] = jnp.where(key_pos < self.length[0], 0.0, -1e30)

    def store(self, band):
        rows = self.stage.shape[1]
        return pltpu.make_async_copy(
            self.stage.at[band % 2],
            self.token_out.at[pl.ds(pl.multiple_of(band * rows, rows), rows), :],
            self.out_sems.at[band % 2],
        )

    def store_grads(self):
        return pltpu.make_async_copy(self.grads, self.grads_out, self.out_sems.at[2])

    def tokens(self, band):
        w_query, w_key, w_value, normed = self.bufs[9:]
        rows = self.stage.shape[1]
        inner = w_query.shape[1]

        @pl.when(band >= 2)
        def _():
            self.store(band - 2).wait()

        lines = pl.ds(pl.multiple_of(band * rows, rows), rows)

        def columns(index, carry):
            cols = pl.ds(pl.multiple_of(index * 512, 512), 512)
            value = nt_dot(self.grads[lines, :inner], w_query[cols, :])
            value += nt_dot(self.grads[lines, inner : inner + 128], w_key[cols, :])
            value += nt_dot(self.grads[lines, inner + 128 :], w_value[cols, :])
            self.stage[band % 2, :, cols] = value.astype(BF16)
            scaled = value * normed[lines, cols].astype(F32)
            self.gain_out[0:1, cols] += jnp.sum(scaled, axis=0, keepdims=True)
            return carry

        lax.fori_loop(0, w_query.shape[0] // 512, columns, 0)
        self.store(band).start()

    def compute(self, step):
        grad_attn, w_output, queries, keys, values, cosine, sine, outs, stats = self.bufs[:9]
        inner = queries.shape[1]
        pairs = inner // 128

        @pl.when(step == 0)
        def _():
            for which in range(2):
                self.load(which).wait()

            def band(index, carry):
                rows = pl.ds(pl.multiple_of(index * 256, 256), 256)
                self.heads[rows, :] = nt_dot(grad_attn[rows, :], w_output[...]).astype(BF16)
                return carry

            lax.fori_loop(0, LEN // 256, band, 0)

        @pl.when(step == 1)
        def _():
            for which in range(2, 9):
                self.load(which).wait()

            self.stats[...] = jnp.transpose(stats[...])

            def products(index, carry):
                rows = pl.ds(pl.multiple_of(index * 256, 256), 256)
                kept = jnp.zeros((256, 128), F32)
                for pair in range(pairs):
                    cols = slice(pair * 128, (pair + 1) * 128)
                    kept = row_products(self.heads[rows, cols], outs[rows, cols], pair, kept)
                stats[rows, :] = kept
                return carry

            lax.fori_loop(0, LEN // 256, products, 0)
            self.inner[...] = jnp.transpose(stats[...])

        def tiles(pair, blocks):
            here = pl.ds(pl.multiple_of(pair * 128, 128), 128)
            attend_back_tiles(
                pair, queries.at[:, here], keys, values, self.heads.at[:, here], cosine, sine,
                self.stats, self.inner, self.bias, self.grads.at[:, here], self.acc_k,
                self.acc_v, blocks,
            )

        @pl.when((step >= 1) & (step <= pairs))
        def _():
            tiles(step - 1, (2, 3))

        @pl.when((step > pairs) & (step <= pairs + 2))
        def _():
            def early(index, carry):
                tiles(pairs // 2 * (step - pairs - 1) + index, (0, 1))
                return carry

            lax.fori_loop(0, pairs // 2, early, 0)

        @pl.when(step == pairs + 3)
        def _():
            self.grads[:, inner : inner + 128] = rope_back(
                self.acc_k[...], cosine[...], sine[...]
            )
            self.grads[:, inner + 128 :] = self.acc_v[...].astype(BF16)
            self.store_grads().start()
            for which in range(9, len(self.sources)):
                self.load(which).wait()

            def band(index, carry):
                self.tokens(index)
                return carry

            lax.fori_loop(0, 4, band, 0)

    def finish(self):
        self.gain_out[0:1, :] = self.gain_out[0:1, :] / self.gain[...]
        self.store_grads().wait()
        for band in (2, 3):
            self.store(band).wait()


def heads_ring(
    job, lengths, gain, grad_attn, w_output, qkv, tables, saved, weights, rows_attn, count, cid
):
    sources = [grad_attn, w_output, *qkv, *tables, *saved, *weights, rows_attn]
    rows, width = grad_attn.shape
    inner = qkv[0].shape[1]
    made = [
        jax.ShapeDtypeStruct((rows, inner + 256), BF16),
        jax.ShapeDtypeStruct((rows, width), BF16),
        jax.ShapeDtypeStruct((8, width), F32),
    ]
    spare = [pltpu.VMEM(g.shape, g.dtype) for g in sources] + [
        pltpu.VMEM((rows, inner), BF16),
        pltpu.VMEM((rows, inner + 256), BF16),
        pltpu.VMEM((rows, 128), F32),
        pltpu.VMEM((rows, 128), F32),
        pltpu.VMEM((2, rows // 4, width), BF16),
        pltpu.VMEM((128, rows), F32),
        pltpu.VMEM((128, rows), F32),
        pltpu.VMEM((rows, 128), F32),
        pltpu.SemaphoreType.DMA((len(sources),)),
        pltpu.SemaphoreType.DMA((3,)),
    ]
    vmem = pl.BlockSpec(memory_space=pltpu.VMEM)
    specs = [pl.BlockSpec(memory_space=pltpu.SMEM), vmem] + [ANY] * len(sources)
    return ring_scatter_dots(
        [job],
        4,
        count,
        cid,
        Extra(HeadWork, [lengths, gain] + sources, specs, made, [ANY, ANY, vmem], spare),
    )


def attend_ring_kernel(count, *refs):
    length_ref, shard, sources = refs[0], refs[1], refs[2:9]
    gathered, q_out, k_out, v_out, head_out, part_out, stats_out = refs[9:16]
    bufs = refs[16:23]
    q_buf, k_buf, v_buf, head_buf, stage, own, stats = refs[23:30]
    send_sems, recv_sems, in_sems, out_sems, local_sem = refs[30:]
    rows_buf, w_query, w_key, w_value, w_output, cosine, sine = bufs
    shape = own.shape
    me = lax.axis_index("dp")
    loads = [
        pltpu.make_async_copy(source, buf, in_sems.at[k])
        for k, (source, buf) in enumerate(zip(sources, bufs))
    ]
    for load in loads:
        load.start()
    load_own = pltpu.make_async_copy(shard.at[:, : shape[1]], own, local_sem)
    load_own.start()
    place, neighbours = ring_setup(count)

    def hop(step, side):
        ref = piece(gathered, shape, 0, member_at(place, side, step, count), side, 0, 1)
        return pltpu.make_async_remote_copy(
            src_ref=ref,
            dst_ref=ref,
            send_sem=send_sems.at[side, step],
            recv_sem=recv_sems.at[side, step],
            device_id={"dp": neighbours[side]},
            device_id_type=MESH_ID,
        )

    for side in range(2):
        pltpu.make_async_remote_copy(
            src_ref=piece(shard, shape, None, 0, side, 0, 1),
            dst_ref=piece(gathered, shape, 0, me, side, 0, 1),
            send_sem=send_sems.at[side, 0],
            recv_sem=recv_sems.at[side, 0],
            device_id={"dp": neighbours[side]},
            device_id_type=MESH_ID,
        ).start()

    def pump(step, carry=0):
        for side in range(2):
            hop(step - 1, side).wait_recv()
            hop(step, side).start()
        return carry

    load_own.wait()
    store_own = pltpu.make_async_copy(
        own, gathered.at[pl.ds(pl.multiple_of(me * shape[0], shape[0]), shape[0]), :], local_sem
    )
    store_own.start()
    for k in (0, 1, 2, 3, 5, 6):
        loads[k].wait()

    stats[...] = jnp.zeros_like(stats)

    def projection(band, carry):
        lines = pl.ds(pl.multiple_of(band * 256, 256), 256)
        project_rows(
            rows_buf[lines, :], w_query, w_key, w_value, cosine[lines, :], sine[lines, :],
            q_buf.at[lines, :], k_buf.at[lines, :], v_buf.at[lines, :],
        )
        return carry

    lax.fori_loop(0, LEN // 256, projection, 0)
    stores = [
        pltpu.make_async_copy(buf, out, out_sems.at[k])
        for k, (buf, out) in enumerate(
            ((q_buf, q_out), (k_buf, k_out), (v_buf, v_out), (head_buf, head_out))
        )
    ]
    for store in stores[:3]:
        store.start()
    pump(1)
    pairs = q_buf.shape[1] // 128

    def attention(pair, carry):
        here = pl.ds(pl.multiple_of(pair * 128, 128), 128)
        attend_pair(
            length_ref[0], pair, q_buf.at[:, here], k_buf, v_buf, head_buf.at[:, here], stats
        )

        @pl.when(pair + 2 <= count - 2)
        def _():
            pump(pair + 2)

        return carry

    lax.fori_loop(0, pairs, attention, 0)
    loads[4].wait()
    stores[3].start()
    store_stats = pltpu.make_async_copy(stats, stats_out, out_sems.at[6])
    store_stats.start()

    def store_part(band):
        return pltpu.make_async_copy(
            stage.at[band % 2],
            part_out.at[pl.ds(pl.multiple_of(band * 256, 256), 256), :],
            out_sems.at[4 + band % 2],
        )

    def output(band, carry):
        @pl.when(band >= 2)
        def _():
            store_part(band - 2).wait()

        lines = pl.ds(pl.multiple_of(band * 256, 256), 256)

        def columns(index, inner):
            cols = pl.ds(pl.multiple_of(index * 512, 512), 512)
            stage[band % 2, :, cols] = jnp.dot(
                head_buf[lines, :], w_output[:, cols], preferred_element_type=F32
            ).astype(BF16)
            return inner

        lax.fori_loop(0, w_output.shape[1] // 512, columns, 0)
        store_part(band).start()

        @pl.when((band == 0) & (pairs + 2 <= count - 2))
        def _():
            pump(pairs + 2)

        return carry

    lax.fori_loop(0, LEN // 256, output, 0)
    lax.fori_loop(min(pairs + 3, count - 1), count - 1, pump, 0)
    for band in (LEN // 256 - 2, LEN // 256 - 1):
        store_part(band).wait()
    for store in stores:
        store.wait()
    store_stats.wait()
    store_own.wait()
    for side in range(2):
        hop(count - 2, side).wait_recv()

    def drain(step, carry):
        for side in range(2):
            hop(step, side).wait_send()
        return carry

    lax.fori_loop(0, count - 1, drain, 0)


def attend_ring(shard, edge, lengths, rows_attn, weights, tables, count, collective_id):
    sources = [rows_attn, *weights, *tables]
    rows, width = rows_attn.shape
    inner = weights[0].shape[1]

    def low(*shape):
        return jax.ShapeDtypeStruct(shape, BF16)

    return pl.pallas_call(
        functools.partial(attend_ring_kernel, count),
        out_shape=[
            low(shard.shape[0] * count, edge),
            low(rows, inner),
            low(rows, 128),
            low(rows, 128),
            low(rows, inner),
            low(rows, width),
            jax.ShapeDtypeStruct((rows, 128), F32),
        ],
        in_specs=[pl.BlockSpec(memory_space=pltpu.SMEM)] + [ANY] * (1 + len(sources)),
        out_specs=[ANY] * 7,
        scratch_shapes=[pltpu.VMEM(source.shape, source.dtype) for source in sources]
        + [
            pltpu.VMEM((rows, inner), BF16),
            pltpu.VMEM((rows, 128), BF16),
            pltpu.VMEM((rows, 128), BF16),
            pltpu.VMEM((rows, inner), BF16),
            pltpu.VMEM((2, 256, width), BF16),
            pltpu.VMEM((shard.shape[0], edge), BF16),
            pltpu.VMEM((rows, 128), F32),
            pltpu.SemaphoreType.DMA((2, count - 1)),
            pltpu.SemaphoreType.DMA((2, count - 1)),
            pltpu.SemaphoreType.DMA((len(sources),)),
            pltpu.SemaphoreType.DMA((7,)),
            pltpu.SemaphoreType.DMA,
        ],
        compiler_params=pltpu.CompilerParams(
            collective_id=collective_id, has_side_effects=True, vmem_limit_bytes=56 << 20
        ),
        cost_estimate=pl.CostEstimate(
            flops=24 << 30, bytes_accessed=60 << 20, transcendentals=8 << 20
        ),
        name="attend_ring",
    )(lengths, shard, *sources)


def ring_weight_grads(jobs, parts, count, collective_id):
    if all(left.shape[1] // count % 128 == 0 for left, _ in jobs):
        jobs = [Job(left, right, 0, right.shape[1]) for left, right in jobs]
        return ring_scatter_dots(jobs, parts, count, collective_id)
    partials = [tn_dot(left, right).astype(BF16) for left, right in jobs]
    num = len(jobs)
    return ring_scatter(partials, [0] * num, [parts] * num, count, collective_id)


def after(value, *deps):
    return lax.optimization_barrier((value,) + deps)[0]


def gather_rows(value):
    return lax.all_gather(value, "tensor", axis=0, tiled=True)


def scatter_rows(value):
    return lax.psum_scatter(value.astype(BF16), "tensor", scatter_dimension=0, tiled=True)


def share_kernel(count, group, parts_ref, out_ref, first, sums, second, sems):
    row, col = lax.axis_index("dp"), lax.axis_index("tensor")
    barrier = pltpu.get_barrier_semaphore()

    def in_group(shift):
        return {"tensor": (col + shift) % group}

    def in_column(shift):
        return {"dp": (row + shift) % count}

    def greet(device):
        pl.semaphore_signal(barrier, inc=1, device_id=device, device_id_type=MESH_ID)

    for shift in range(1, group):
        greet(in_group(shift))
    for shift in range(1, count):
        greet(in_column(shift))
    pl.semaphore_wait(barrier, group + count - 2)

    def exchange(shift, slot, source, target, device):
        return pltpu.make_async_remote_copy(
            src_ref=source,
            dst_ref=target,
            send_sem=sems.at[0, slot],
            recv_sem=sems.at[1, slot],
            device_id=device,
            device_id_type=MESH_ID,
        )

    moves = [
        exchange(s, s - 1, parts_ref.at[(col + s) % group], first.at[s - 1], in_group(s))
        for s in range(1, group)
    ]
    for move in moves:
        move.start()
    total = parts_ref[col]
    for shift, move in enumerate(moves):
        move.wait()
        total = total + first[shift]
    sums[...] = total
    moves = [
        exchange(
            s, group + s - 2, sums.at[(row + s) % count], second.at[s - 1], in_column(s)
        )
        for s in range(1, count)
    ]
    for move in moves:
        move.start()
    total = sums[row]
    for shift, move in enumerate(moves):
        move.wait()
        total = total + second[shift]
    out_ref[...] = total


def sum_shares(first, second, count, group, collective_id):
    share = first.shape[0] // (count * group)
    pair = jnp.stack([first, second]).reshape(2, count, group, share)
    parts = jnp.transpose(pair, (2, 1, 0, 3)).reshape(group, count, 1, 2 * share)
    width = (2 * share + 127) // 128 * 128
    parts = jnp.pad(parts, ((0, 0), (0, 0), (0, 7), (0, width - 2 * share)))
    tile = (8, width)
    out = pl.pallas_call(
        functools.partial(share_kernel, count, group),
        out_shape=jax.ShapeDtypeStruct(tile, F32),
        in_specs=[pl.BlockSpec(memory_space=pltpu.VMEM)],
        out_specs=pl.BlockSpec(memory_space=pltpu.VMEM),
        scratch_shapes=[
            pltpu.VMEM((group - 1, count) + tile, F32),
            pltpu.VMEM((count,) + tile, F32),
            pltpu.VMEM((count - 1,) + tile, F32),
            pltpu.SemaphoreType.DMA((2, group + count - 2)),
        ],
        compiler_params=pltpu.CompilerParams(collective_id=collective_id, has_side_effects=True),
        name="sum_shares",
    )(parts)
    return out[0, :share], out[0, share : 2 * share]


def dot(left, right):
    return jnp.dot(left, right, preferred_element_type=F32)


def body(
    count,
    group,
    tokens,
    lengths,
    attn_gain,
    w_query,
    w_key,
    w_value,
    w_output,
    mlp_gain,
    w_gate,
    w_up,
    w_down,
    cotangent,
):
    local_rows = tokens.shape[0]
    token_full = tokens.astype(F32)
    gain_attn = attn_gain.astype(F32)
    gain_mlp = mlp_gain.astype(F32)
    row_pos = lax.axis_index("tensor") * local_rows + jnp.arange(local_rows)
    valid_rows = (row_pos < lengths[0]).astype(F32)
    cot_masked = cotangent.astype(F32) * valid_rows[:, None]
    cosine, sine = rope_tables()

    inv_first = lax.rsqrt(jnp.mean(token_full * token_full, axis=1, keepdims=True) + epsilon)
    normed_attn = (token_full * inv_first * gain_attn).astype(BF16)
    rows_attn = gather_rows(normed_attn)
    query_all, key_all, value_all, output_all = ring_gather(
        [after(w_query, normed_attn), w_key, w_value, w_output],
        (0, 0, 0, 1), (1, 1, 1, 1), count, 0,
    )
    grad_branch = gather_rows(after(cot_masked.astype(BF16), rows_attn))
    fused = count == 8 and group == 4
    edge = 3 * w_gate.shape[1] // 8
    gates = []
    if fused:
        first_gate, queries, keys, values, head_out, attn_part, stats = attend_ring(
            w_gate,
            edge,
            lengths,
            rows_attn,
            (query_all, key_all, value_all, output_all),
            (cosine, sine),
            count,
            9,
        )
        gates.append(first_gate)
    else:
        queries, keys, values = project(rows_attn, query_all, key_all, value_all, cosine, sine)
        head_out = attend(queries, keys, values, lengths)
        attn_part = dot(head_out, output_all).astype(BF16)
    attn_branch = scatter_rows(attn_part)
    (gate_all,) = ring_gather(
        [after(w_gate, attn_part)], (0,), (2,), count, 1, edge if fused else 0
    )
    gates.append(gate_all)
    hidden = token_full + attn_branch.astype(F32)
    inv_second = lax.rsqrt(jnp.mean(hidden * hidden, axis=1, keepdims=True) + epsilon)
    normed_mlp = (hidden * inv_second * gain_mlp).astype(BF16)
    normed_mlp = after(normed_mlp, gate_all)
    rows_mlp = gather_rows(normed_mlp)
    (up_all,) = ring_gather([after(w_up, normed_mlp)], (0,), (2,), count, 2)
    if fused:
        activated, grad_gate_pre, grad_up_pre, down_all = mlp_ring(
            rows_mlp, gates, after(up_all, rows_mlp), w_down, grad_branch, count, 3
        )
        grad_down, norm_part, mlp_part = down_ring(
            grad_branch, activated, grad_gate_pre, grad_up_pre, gates, up_all, down_all,
            count, 4,
        )
    else:
        gate_proj = dot(rows_mlp, gate_all)
        up_proj = dot(rows_mlp, up_all)
        gate_sig = jax.nn.sigmoid(gate_proj)
        activated = (gate_proj * gate_sig * up_proj).astype(BF16)
        (down_all,) = ring_gather([after(w_down, up_all)], (1,), (2,), count, 3)
        mlp_part = dot(activated, down_all).astype(BF16)
        grad_act = nt_dot(grad_branch, down_all)
        grad_gate_pre = (
            grad_act * up_proj * gate_sig * (1.0 + gate_proj * (1.0 - gate_sig))
        ).astype(BF16)
        grad_up_pre = (grad_act * gate_proj * gate_sig).astype(BF16)
        norm_part = (nt_dot(grad_gate_pre, gate_all) + nt_dot(grad_up_pre, up_all)).astype(BF16)
        (grad_down,) = ring_weight_grads([(grad_branch, activated)], 2, count, 4)
    grad_norm_two = scatter_rows(norm_part).astype(F32)
    middle = 3 * grad_up_pre.shape[1] // 8
    if fused:
        grad_gate, up_part = ring_scatter_dots(
            [Job(after(rows_mlp, norm_part), grad_gate_pre, 0, grad_gate_pre.shape[1])],
            2, count, 5, product_work(grad_up_pre, middle, count, rows_mlp.shape[1]),
        )
    else:
        (grad_gate,) = ring_weight_grads(
            [(after(rows_mlp, norm_part), grad_gate_pre)], 2, count, 5
        )
    scaled_two = grad_norm_two * gain_mlp
    gain_two_part = jnp.sum(grad_norm_two * hidden * inv_second, axis=0)
    grad_hidden = (
        cot_masked
        + inv_second * scaled_two
        - hidden * inv_second**3 * jnp.mean(scaled_two * hidden, axis=1, keepdims=True)
    )
    grad_hidden = after(grad_hidden, grad_gate)
    if fused:
        hidden_cols = grad_up_pre.shape[1]
        grad_up, grad_attn = ring_scatter_dots(
            [Job(rows_mlp, grad_up_pre, 0, middle, hidden_cols)],
            4, count, 6, gather_work(grad_hidden.astype(BF16)),
        )
        mlp_branch = scatter_rows(after(mlp_part, grad_attn))
        grad_up, grad_qkv, token_part, gain_one = heads_ring(
            Job(up_part, None, 0, hidden_cols - middle, grad_up, middle),
            lengths,
            gain_attn[None, :],
            grad_attn,
            output_all,
            (queries, keys, values),
            (cosine, sine),
            (head_out, stats),
            (query_all, key_all, value_all),
            rows_attn,
            count,
            10,
        )
    else:
        grad_attn = gather_rows(grad_hidden.astype(BF16))
        mlp_branch = scatter_rows(after(mlp_part, grad_hidden))
        (grad_up,) = ring_weight_grads(
            [(after(rows_mlp, grad_hidden), grad_up_pre)], 2, count, 6
        )
        grad_heads = nt_dot(after(grad_attn, grad_up), output_all).astype(BF16)
        grad_qpre, grad_kpre, grad_vpre = attend_back(
            queries, keys, values, grad_heads, lengths, cosine, sine
        )
        token_part = (
            nt_dot(grad_qpre, query_all)
            + nt_dot(grad_kpre, key_all)
            + nt_dot(grad_vpre, value_all)
        ).astype(BF16)
    layer_out = (hidden + after(mlp_branch, token_part).astype(F32)).astype(BF16)
    grad_norm_one = scatter_rows(token_part).astype(F32)
    scaled_one = grad_norm_one * gain_attn
    grad_tokens = (
        grad_hidden
        + inv_first * scaled_one
        - token_full * inv_first**3 * jnp.mean(scaled_one * token_full, axis=1, keepdims=True)
    )
    if fused:
        query_cols, key_cols = queries.shape[1], keys.shape[1]
        rows_late = after(rows_attn, token_part)
        grad_query, grad_key, grad_value, grad_output, shares = ring_scatter_dots(
            [
                Job(
                    rows_late,
                    grad_qkv,
                    0,
                    query_cols + 2 * key_cols,
                    pieces=(query_cols, key_cols, key_cols),
                ),
                Job(grad_attn, head_out, 0, query_cols),
            ],
            1,
            count,
            7,
            share_work(gain_one, gain_two_part[None, :], count, group),
        )
        share = gain_two_part.shape[0] // (count * group)
        grad_attn_gain, grad_mlp_gain = shares[0, :share], shares[1, :share]
    else:
        grad_query, grad_key, grad_value, grad_output = ring_weight_grads(
            [
                (after(rows_attn, token_part), grad_qpre),
                (rows_attn, grad_kpre),
                (rows_attn, grad_vpre),
                (grad_attn, head_out),
            ],
            1, count, 7,
        )
        gain_one_part = jnp.sum(grad_norm_one * token_full * inv_first, axis=0)
        grad_attn_gain, grad_mlp_gain = sum_shares(
            after(gain_one_part, grad_query), gain_two_part, count, group, 8
        )
    grad_output, grad_down = grad_output.T, grad_down.T
    return (
        layer_out,
        grad_tokens,
        grad_query,
        grad_key,
        grad_value,
        grad_output,
        grad_gate,
        grad_up,
        grad_down,
        grad_attn_gain,
        grad_mlp_gain,
    )


def solution(mesh):
    rows = P(("dp", "tensor"), None)
    tall = P("dp", "tensor")
    wide = P("tensor", "dp")
    share = P(("dp", "tensor"))
    in_specs = (rows, P("dp"), P(), tall, tall, tall, wide, P(), tall, tall, wide, rows)
    out_specs = (rows, rows, tall, tall, tall, wide, tall, tall, wide, share, share)
    return jax.shard_map(
        functools.partial(body, mesh.shape["dp"], mesh.shape["tensor"]),
        mesh=mesh,
        in_specs=in_specs,
        out_specs=out_specs,
        check_vma=False,
    )
```

```python
import functools
from typing import Any, NamedTuple

import jax
import jax.numpy as jnp
from jax import lax
from jax.experimental import pallas as pl
from jax.experimental.pallas import tpu as pltpu
from jax.sharding import PartitionSpec as P

HD = 64
LEN = 1024
QB = 256

epsilon = 1e-05
theta = 500000.0
MESH_ID = pl.DeviceIdType.MESH
BF16 = jnp.bfloat16
ANY = pl.BlockSpec(memory_space=pl.ANY)
F32 = jnp.float32


def rope_frequencies():
    half_size = HD // 2
    base_freq = theta ** (-(jnp.arange(half_size, dtype=jnp.float32) * 2.0) / HD)
    wavelength = 2.0 * jnp.pi / base_freq
    smooth = (8192.0 / wavelength - 1.0) / 3.0
    middle = (1.0 - smooth) * base_freq / 32.0 + smooth * base_freq
    return jnp.where(
        wavelength < 2048.0, base_freq, jnp.where(wavelength > 8192.0, base_freq / 32.0, middle)
    )


def rope_tables():
    steps = jnp.arange(32, dtype=jnp.float32)[:, None]
    frequency = jnp.concatenate([rope_frequencies()] * 4)[None, :]
    low, high = steps * frequency, (32.0 * steps) * frequency
    cos_low, sin_low = jnp.cos(low)[None, :, :], jnp.sin(low)[None, :, :]
    cos_high, sin_high = jnp.cos(high)[:, None, :], jnp.sin(high)[:, None, :]
    sign = jnp.where(jnp.arange(128) % HD < HD // 2, -1.0, 1.0)
    cosine = cos_high * cos_low - sin_high * sin_low
    sine = (sin_high * cos_low + cos_high * sin_low) * sign
    return cosine.reshape(LEN, 128), sine.reshape(LEN, 128)


def lane_index(shape):
    return lax.broadcasted_iota(jnp.int32, shape, 1)


def swap_halves(value):
    low = lane_index(value.shape) % HD < HD // 2
    return jnp.where(low, pltpu.roll(value, 128 - HD // 2, 1), pltpu.roll(value, HD // 2, 1))


def nt_dot(left, right):
    return lax.dot_general(left, right, (((1,), (1,)), ((), ())), preferred_element_type=F32)


def tn_dot(left, right):
    return lax.dot_general(left, right, (((0,), (0,)), ((), ())), preferred_element_type=F32)


def rope(value, cosine, sine):
    return (value * cosine + swap_halves(value) * sine).astype(BF16)


def rope_back(grads, cosine, sine):
    return (grads * cosine - swap_halves(grads) * sine).astype(BF16)


def project_rows(rows, wq_ref, wk_ref, wv_ref, cosine, sine, q_ref, k_ref, v_ref):
    for block in range(q_ref.shape[1] // 256):
        cols = slice(block * 256, (block + 1) * 256)
        value = jnp.dot(rows, wq_ref[:, cols], preferred_element_type=F32)
        for half in range(2):
            start = block * 256 + half * 128
            q_ref[:, start : start + 128] = rope(
                value[:, half * 128 : half * 128 + 128], cosine, sine
            )
    k_ref[...] = rope(jnp.dot(rows, wk_ref[...], preferred_element_type=F32), cosine, sine)
    v_ref[...] = jnp.dot(rows, wv_ref[...], preferred_element_type=F32).astype(BF16)


def project_kernel(x_ref, wq_ref, wk_ref, wv_ref, cos_ref, sin_ref, q_ref, k_ref, v_ref):
    project_rows(
        x_ref[...], wq_ref, wk_ref, wv_ref, cos_ref[...], sin_ref[...], q_ref, k_ref, v_ref
    )


def project(rows, w_query, w_key, w_value, cosine, sine):
    total, width = rows.shape
    block = 256

    def whole(array):
        return pl.BlockSpec(array.shape, lambda i: (0, 0))

    def by_rows(cols):
        return pl.BlockSpec((block, cols), lambda i: (i, 0))

    shapes = [w_query.shape[1], w_key.shape[1], w_value.shape[1]]
    return pl.pallas_call(
        project_kernel,
        grid=(total // block,),
        out_shape=[jax.ShapeDtypeStruct((total, s), BF16) for s in shapes],
        in_specs=[by_rows(width), whole(w_query), whole(w_key), whole(w_value)]
        + [by_rows(128)] * 2,
        out_specs=[by_rows(s) for s in shapes],
        compiler_params=pltpu.CompilerParams(vmem_limit_bytes=32 << 20),
        cost_estimate=pl.CostEstimate(
            flops=2 * total * width * sum(shapes), bytes_accessed=8 << 20, transcendentals=0
        ),
        name="project",
    )(rows, w_query, w_key, w_value, cosine, sine)


def pick_head(pair, which, kv):
    moved = jnp.where(kv == which, pair, pltpu.roll(pair, HD, 1))
    return jnp.where(lane_index(pair.shape) // HD == kv, moved, jnp.zeros_like(moved))


def join_heads(first, second, kv):
    first = jnp.where(kv == 0, first, pltpu.roll(first, HD, 1))
    second = jnp.where(kv == 1, second, pltpu.roll(second, HD, 1))
    return jnp.where(lane_index(first.shape) < HD, first, second)


def attend_pair(length, pair_index, q_ref, k_ref, v_ref, o_ref, stats_ref=None):
    kv = pair_index // 2
    square = (QB, QB)
    causal = lax.broadcasted_iota(jnp.int32, square, 1) <= lax.broadcasted_iota(
        jnp.int32, square, 0
    )
    bias = jnp.where(lane_index((1, LEN)) < length, 0.0, -1e30)
    for block in range(LEN // QB):
        start = block * QB
        here = slice(start, start + QB)
        pair = q_ref[here, :].astype(F32) * HD**-0.5
        outs = []
        for which in range(2):
            query = pick_head(pair, which, kv).astype(BF16)
            near = jnp.where(causal, nt_dot(query, k_ref[here, :]), -1e30) + bias[:, here]
            top = jnp.max(near, axis=1, keepdims=True)
            if start:
                far = nt_dot(query, k_ref[:start, :]) + bias[:, :start]
                top = jnp.maximum(top, jnp.max(far, axis=1, keepdims=True))
                far = jnp.exp(far - top)
            near = jnp.exp(near - top)
            total = jnp.sum(near, axis=1, keepdims=True)
            if start:
                total = total + jnp.sum(far, axis=1, keepdims=True)
            inverse = 1.0 / total
            if stats_ref is not None:
                kept = stats_ref[here, :]
                mine = lane_index(kept.shape) == 2 * pair_index + which
                stats_ref[here, :] = jnp.where(mine, top + jnp.log(total), kept)
            out = jnp.dot(
                (near * inverse).astype(BF16), v_ref[here, :], preferred_element_type=F32
            )
            if start:
                out = out + jnp.dot(
                    (far * inverse).astype(BF16), v_ref[:start, :], preferred_element_type=F32
                )
            outs.append(out)
        o_ref[here, :] = join_heads(outs[0], outs[1], kv).astype(BF16)


def attend_kernel(length_ref, q_ref, k_ref, v_ref, o_ref):
    attend_pair(length_ref[0], pl.program_id(0), q_ref, k_ref, v_ref, o_ref)


def attend(queries, keys, values, lengths):
    pairs = queries.shape[1] // 128
    whole = pl.BlockSpec((LEN, 128), lambda i: (0, 0))
    paired = pl.BlockSpec((LEN, 128), lambda i: (0, i))
    return pl.pallas_call(
        attend_kernel,
        grid=(pairs,),
        out_shape=jax.ShapeDtypeStruct(queries.shape, BF16),
        in_specs=[pl.BlockSpec(memory_space=pltpu.SMEM), paired, whole, whole],
        out_specs=paired,
        compiler_params=pltpu.CompilerParams(vmem_limit_bytes=48 << 20),
        cost_estimate=pl.CostEstimate(
            flops=12 << 30, bytes_accessed=4 << 20, transcendentals=8 << 20
        ),
        name="attend",
    )(lengths, queries, keys, values)


def attend_back_pair(
    length, kv, q_ref, k_ref, v_ref, g_ref, cos_ref, sin_ref, gq_ref, acc_k, acc_v
):
    for block in range(LEN // QB):
        rows = slice(block * QB, (block + 1) * QB)
        keys = (block + 1) * QB
        pair = q_ref[rows, :].astype(F32) * HD**-0.5
        grad_pair = g_ref[rows, :].astype(F32)
        key_pos = lax.broadcasted_iota(jnp.int32, (keys, QB), 0)
        query_pos = block * QB + lax.broadcasted_iota(jnp.int32, (keys, QB), 1)
        allowed = (key_pos <= query_pos) & (key_pos < length)
        key_vecs = k_ref[:keys, :]
        grad_queries = []
        for which in range(2):
            query = pick_head(pair, which, kv).astype(BF16)
            grad = pick_head(grad_pair, which, kv).astype(BF16)
            scores = jnp.where(allowed, nt_dot(key_vecs, query), -1e30)
            exps = jnp.exp(scores - jnp.max(scores, axis=0, keepdims=True))
            probs = exps * (1.0 / jnp.sum(exps, axis=0, keepdims=True))
            grad_probs = nt_dot(v_ref[:keys, :], grad)
            inner = jnp.sum(probs * grad_probs, axis=0, keepdims=True)
            grad_scores = (probs * (grad_probs - inner)).astype(BF16)
            acc_v[:keys, :] += jnp.dot(probs.astype(BF16), grad, preferred_element_type=F32)
            acc_k[:keys, :] += jnp.dot(grad_scores, query, preferred_element_type=F32)
            grad_queries.append(tn_dot(grad_scores, key_vecs) * HD**-0.5)
        joined = join_heads(grad_queries[0], grad_queries[1], kv)
        gq_ref[rows, :] = rope_back(joined, cos_ref[rows, :], sin_ref[rows, :])


def row_products(grads, outs, pair_index, kept):
    product = grads.astype(F32) * outs.astype(F32)
    lanes = lane_index(product.shape)
    low = jnp.sum(jnp.where(lanes < HD, product, 0.0), axis=1, keepdims=True)
    high = jnp.sum(jnp.where(lanes < HD, 0.0, product), axis=1, keepdims=True)
    kept = jnp.where(lanes == 2 * pair_index, low, kept)
    return jnp.where(lanes == 2 * pair_index + 1, high, kept)


def attend_back_tiles(
    pair_index, q_ref, k_ref, v_ref, g_ref, cos_ref, sin_ref, stats_ref, inner_ref, bias_ref,
    gq_ref, acc_k, acc_v,
):
    kv = pair_index // 2
    square = (QB, QB)
    causal = lax.broadcasted_iota(jnp.int32, square, 0) <= lax.broadcasted_iota(
        jnp.int32, square, 1
    )
    for block in range(LEN // QB):
        rows = slice(block * QB, (block + 1) * QB)
        pair = q_ref[rows, :].astype(F32) * HD**-0.5
        grad_pair = g_ref[rows, :].astype(F32)
        queries, grads, tops, inners = [], [], [], []
        for which in range(2):
            queries.append(pick_head(pair, which, kv).astype(BF16))
            grads.append(pick_head(grad_pair, which, kv).astype(BF16))
            head = pl.ds(2 * pair_index + which, 1)
            tops.append(stats_ref[head, rows])
            inners.append(inner_ref[head, rows])
        grad_queries = [None, None]
        for tile in range(block + 1):
            here = slice(tile * QB, (tile + 1) * QB)
            key_vecs, value_vecs = k_ref[here, :], v_ref[here, :]
            bias = bias_ref[here, :]
            bias = jnp.concatenate([bias] * (QB // 128), axis=1)
            grad_key = grad_value = None
            for which in range(2):
                scores = nt_dot(key_vecs, queries[which]) + bias
                if tile == block:
                    scores = jnp.where(causal, scores, -1e30)
                probs = jnp.exp(scores - tops[which])
                grad_probs = nt_dot(value_vecs, grads[which])
                grad_scores = (probs * (grad_probs - inners[which])).astype(BF16)
                value = jnp.dot(probs.astype(BF16), grads[which], preferred_element_type=F32)
                key = jnp.dot(grad_scores, queries[which], preferred_element_type=F32)
                query = tn_dot(grad_scores, key_vecs)
                grad_value = value if which == 0 else grad_value + value
                grad_key = key if which == 0 else grad_key + key
                grad_queries[which] = query if tile == 0 else grad_queries[which] + query
            acc_v[here, :] += grad_value
            acc_k[here, :] += grad_key
        joined = join_heads(grad_queries[0], grad_queries[1], kv) * HD**-0.5
        gq_ref[rows, :] = rope_back(joined, cos_ref[rows, :], sin_ref[rows, :])


def attend_back_kernel(
    length_ref, q_ref, k_ref, v_ref, g_ref, cos_ref, sin_ref, gq_ref, gk_ref, gv_ref, acc_k, acc_v
):
    pair_index = pl.program_id(0)

    @pl.when(pair_index == 0)
    def _():
        acc_k[...] = jnp.zeros_like(acc_k)
        acc_v[...] = jnp.zeros_like(acc_v)

    attend_back_pair(
        length_ref[0], pair_index // 2, q_ref, k_ref, v_ref, g_ref, cos_ref, sin_ref, gq_ref,
        acc_k, acc_v,
    )

    @pl.when(pair_index == pl.num_programs(0) - 1)
    def _():
        gk_ref[...] = rope_back(acc_k[...], cos_ref[...], sin_ref[...])
        gv_ref[...] = acc_v[...].astype(BF16)


def attend_back(queries, keys, values, grad_heads, lengths, cosine, sine):
    pairs = queries.shape[1] // 128
    whole = pl.BlockSpec((LEN, 128), lambda i: (0, 0))
    paired = pl.BlockSpec((LEN, 128), lambda i: (0, i))
    narrow = jax.ShapeDtypeStruct((LEN, 128), BF16)
    return pl.pallas_call(
        attend_back_kernel,
        grid=(pairs,),
        out_shape=[jax.ShapeDtypeStruct(queries.shape, BF16), narrow, narrow],
        in_specs=[pl.BlockSpec(memory_space=pltpu.SMEM), paired, whole, whole, paired]
        + [whole] * 2,
        out_specs=[paired, whole, whole],
        scratch_shapes=[pltpu.VMEM((LEN, 128), F32)] * 2,
        compiler_params=pltpu.CompilerParams(vmem_limit_bytes=48 << 20),
        cost_estimate=pl.CostEstimate(
            flops=24 << 30, bytes_accessed=8 << 20, transcendentals=8 << 20
        ),
        name="attend_back",
    )(lengths, queries, keys, values, grad_heads, cosine, sine)


def ring_place(index, count):
    odd = index % 2
    return (1 - odd) * (index // 2) + odd * (count - 1 - index // 2)


def ring_member(place, count):
    high = place // (count // 2)
    return (1 - high) * (2 * place) + high * (2 * (count - 1 - place) + 1)


def ring_setup(count, peers=None, more=()):
    place = ring_place(lax.axis_index("dp"), count)
    ahead = ring_member((place + 1) % count, count)
    behind = ring_member((place + count - 1) % count, count)
    barrier = pltpu.get_barrier_semaphore()
    peers = (peers or [{"dp": ahead}, {"dp": behind}]) + list(more)
    for other in peers:
        pl.semaphore_signal(barrier, inc=1, device_id=other, device_id_type=MESH_ID)
    pl.semaphore_wait(barrier, len(peers))
    return place, (ahead, behind)


def member_at(place, side, steps, count):
    if side == 0:
        return ring_member((place + count - steps) % count, count)
    return ring_member((place + steps) % count, count)


def piece(ref, shape, axis, member, side, part, parts, first=0):
    rows, cols = shape
    sub = rows // (2 * parts)
    start = (side * parts + part) * sub
    if axis is None:
        return ref.at[pl.ds(start, sub), first : first + cols]
    if axis == 0:
        return ref.at[pl.ds(pl.multiple_of(member * rows + start, sub), sub), :]
    return ref.at[pl.ds(start, sub), pl.ds(pl.multiple_of(member * cols, cols), cols)]


def gather_kernel(count, items, *refs):
    num = len(items)
    shards, outs = refs[:num], refs[num : 2 * num]
    stage = refs[2 * num : 3 * num]
    send_sems, recv_sems, local_sem = refs[3 * num :]
    place, neighbours = ring_setup(count)
    me = lax.axis_index("dp")
    slots = [(k, part) for k in range(num) for part in range(items[k][2])]

    def copy(step, side, slot):
        item, part = slots[slot]
        shape, axis, parts, _ = items[item]
        origin = member_at(place, side, step, count)
        target = piece(outs[item], shape, axis, origin, side, part, parts)
        return target, pltpu.make_async_remote_copy(
            src_ref=target,
            dst_ref=target,
            send_sem=send_sems.at[side, step, slot],
            recv_sem=recv_sems.at[side, step, slot],
            device_id={"dp": neighbours[side]},
            device_id_type=MESH_ID,
        )

    for slot, (item, part) in enumerate(slots):
        shape, axis, parts, first = items[item]
        for side in range(2):
            pltpu.make_async_remote_copy(
                src_ref=piece(shards[item], shape, None, 0, side, part, parts, first),
                dst_ref=piece(outs[item], shape, axis, me, side, part, parts),
                send_sem=send_sems.at[side, 0, slot],
                recv_sem=recv_sems.at[side, 0, slot],
                device_id={"dp": neighbours[side]},
                device_id_type=MESH_ID,
            ).start()
    loads = [
        pltpu.make_async_copy(
            shards[k].at[:, items[k][3] : items[k][3] + items[k][0][1]],
            stage[k],
            local_sem.at[k],
        )
        for k in range(num)
    ]
    for load in loads:
        load.start()
    stores = []
    for k in range(num):
        loads[k].wait()
        shape, axis, parts, _ = items[k]
        rows, cols = shape
        if axis == 0:
            own = outs[k].at[pl.ds(pl.multiple_of(me * rows, rows), rows), :]
        else:
            own = outs[k].at[:, pl.ds(pl.multiple_of(me * cols, cols), cols)]
        stores.append(pltpu.make_async_copy(stage[k], own, local_sem.at[k]))
        stores[-1].start()

    def hop(step, carry):
        for slot in range(len(slots)):
            for side in range(2):
                copy(step - 1, side, slot)[1].wait_recv()
                copy(step, side, slot)[1].start()
        return carry

    lax.fori_loop(1, count - 1, hop, 0)
    for slot in range(len(slots)):
        for side in range(2):
            copy(count - 2, side, slot)[1].wait_recv()
    for store in stores:
        store.wait()

    def drain(step, carry):
        for slot in range(len(slots)):
            for side in range(2):
                copy(step, side, slot)[1].wait_send()
        return carry

    lax.fori_loop(0, count - 1, drain, 0)


def ring_gather(shards, axes, parts, count, collective_id, first=0):
    turned = [a == 1 and s.shape[1] % 128 != 0 for s, a in zip(shards, axes)]
    if any(turned):
        shards = [s.T if t else s for s, t in zip(shards, turned)]
        axes = [0 if t else a for a, t in zip(axes, turned)]
        outs = ring_gather(shards, axes, parts, count, collective_id)
        return [o.T if t else o for o, t in zip(outs, turned)]
    shapes = [(s.shape[0], s.shape[1] - first) for s in shards]
    items = tuple((s, a, q, first) for s, a, q in zip(shapes, axes, parts))
    slots = sum(parts)
    outs = [
        jax.ShapeDtypeStruct((s[0] * count, s[1]) if a == 0 else (s[0], s[1] * count), BF16)
        for s, a in zip(shapes, axes)
    ]
    num = len(shards)
    nbytes = sum(s.size * 2 * (count - 1) for s in shards)
    return pl.pallas_call(
        functools.partial(gather_kernel, count, items),
        out_shape=outs,
        in_specs=[pl.BlockSpec(memory_space=pl.ANY)] * num,
        out_specs=[pl.BlockSpec(memory_space=pl.ANY)] * num,
        scratch_shapes=[pltpu.VMEM(s, BF16) for s in shapes]
        + [
            pltpu.SemaphoreType.DMA((2, count - 1, slots)),
            pltpu.SemaphoreType.DMA((2, count - 1, slots)),
            pltpu.SemaphoreType.DMA((num,)),
        ],
        compiler_params=pltpu.CompilerParams(collective_id=collective_id, has_side_effects=True),
        cost_estimate=pl.CostEstimate(flops=0, bytes_accessed=20 * nbytes, transcendentals=0),
        name=f"ring_gather_{collective_id}",
    )(*shards)


def scatter_kernel(count, items, *refs):
    num = len(items)
    partials, outs = refs[:num], refs[num : 2 * num]
    own = refs[2 * num : 3 * num]
    held = refs[3 * num : 4 * num]
    total = refs[4 * num : 5 * num]
    send_sems, recv_sems, load_sems, store_sems = refs[5 * num :]
    slots = [(k, part) for k in range(num) for part in range(items[k][2])]

    def load(step, side, slot, place):
        item, part = slots[slot]
        shape, axis, parts = items[item]
        member = member_at(place, side, step + 1, count)
        return pltpu.make_async_copy(
            piece(partials[item], shape, axis, member, side, part, parts),
            own[item].at[side, step, part],
            load_sems.at[side, step, slot],
        )

    start_place = ring_place(lax.axis_index("dp"), count)

    def load_all(step, carry):
        for slot in range(len(slots)):
            for side in range(2):
                load(step, side, slot, start_place).start()
        return carry

    lax.fori_loop(0, count, load_all, 0)
    place, neighbours = ring_setup(count)

    def send(step, side, slot, source):
        item, part = slots[slot]
        return pltpu.make_async_remote_copy(
            src_ref=source,
            dst_ref=held[item].at[side, step, part],
            send_sem=send_sems.at[side, step, slot],
            recv_sem=recv_sems.at[side, step, slot],
            device_id={"dp": neighbours[side]},
            device_id_type=MESH_ID,
        )

    for slot, (item, part) in enumerate(slots):
        for side in range(2):
            load(0, side, slot, place).wait()
            send(0, side, slot, own[item].at[side, 0, part]).start()

    def hop(step, carry):
        for slot, (item, part) in enumerate(slots):
            for side in range(2):
                load(step, side, slot, place).wait()
                arrived = held[item].at[side, step - 1, part]
                send(step - 1, side, slot, arrived).wait_recv()
                arrived[...] = (
                    arrived[...].astype(jnp.float32)
                    + own[item][side, step, part].astype(jnp.float32)
                ).astype(jnp.bfloat16)
                send(step, side, slot, arrived).start()
        return carry

    lax.fori_loop(1, count - 1, hop, 0)
    last = count - 1
    stores = []
    for slot, (item, part) in enumerate(slots):
        shape, axis, parts = items[item]
        for side in range(2):
            load(last, side, slot, place).wait()
            arrived = held[item].at[side, last - 1, part]
            send(last - 1, side, slot, arrived).wait_recv()
            total[item][side, part] = arrived[...].astype(jnp.float32) + own[item][
                side, last, part
            ].astype(jnp.float32)
            stores.append(
                pltpu.make_async_copy(
                    total[item].at[side, part],
                    piece(outs[item], shape, None, 0, side, part, parts),
                    store_sems.at[side, slot],
                )
            )
            stores[-1].start()
    for store in stores:
        store.wait()

    def drain(step, carry):
        for slot, (item, part) in enumerate(slots):
            for side in range(2):
                send(step, side, slot, held[item].at[side, 0, part]).wait_send()
        return carry

    lax.fori_loop(0, count - 1, drain, 0)


def ring_scatter(partials, axes, parts, count, collective_id):
    turned = [a == 1 and p.shape[1] // count % 128 != 0 for p, a in zip(partials, axes)]
    if any(turned):
        partials = [p.T if t else p for p, t in zip(partials, turned)]
        axes = [0 if t else a for a, t in zip(axes, turned)]
        outs = ring_scatter(partials, axes, parts, count, collective_id)
        return [o.T if t else o for o, t in zip(outs, turned)]
    shapes = [
        (p.shape[0] // count, p.shape[1]) if a == 0 else (p.shape[0], p.shape[1] // count)
        for p, a in zip(partials, axes)
    ]
    items = tuple((s, a, q) for s, a, q in zip(shapes, axes, parts))
    slots = sum(parts)
    num = len(partials)

    def buffers(depth, dtype):
        return [
            pltpu.VMEM((2,) + depth + (q, s[0] // (2 * q), s[1]), dtype)
            for s, q in zip(shapes, parts)
        ]

    nbytes = sum(p.size * 2 for p in partials)
    return pl.pallas_call(
        functools.partial(scatter_kernel, count, items),
        out_shape=[jax.ShapeDtypeStruct(s, jnp.float32) for s in shapes],
        in_specs=[pl.BlockSpec(memory_space=pl.ANY)] * num,
        out_specs=[pl.BlockSpec(memory_space=pl.ANY)] * num,
        scratch_shapes=buffers((count,), jnp.bfloat16)
        + buffers((count - 1,), jnp.bfloat16)
        + buffers((), jnp.float32)
        + [
            pltpu.SemaphoreType.DMA((2, count - 1, slots)),
            pltpu.SemaphoreType.DMA((2, count - 1, slots)),
            pltpu.SemaphoreType.DMA((2, count, slots)),
            pltpu.SemaphoreType.DMA((2, slots)),
        ],
        compiler_params=pltpu.CompilerParams(
            collective_id=collective_id, has_side_effects=True, vmem_limit_bytes=48 << 20
        ),
        cost_estimate=pl.CostEstimate(flops=0, bytes_accessed=20 * nbytes, transcendentals=0),
        name=f"ring_scatter_{collective_id}",
    )(*partials)


class Job(NamedTuple):
    left: Any
    right: Any
    start: int
    cols: int
    into: Any = None
    target: int = 0
    pieces: tuple = ()


class Extra(NamedTuple):
    builder: Any
    given: list
    given_specs: list
    made: list
    made_specs: list
    spare: list


def scatter_dot_kernel(count, items, num_outs, num_bases, parts, extra, *refs):
    num = len(items)
    taken = 0

    def take(amount):
        nonlocal taken
        taken += amount
        return refs[taken - amount : taken]

    lefts, rights, _ = take(num), take(num), take(num_bases)
    given = take(len(extra.given) if extra else 0)
    outs = take(num_outs)
    made = take(len(extra.made) if extra else 0)
    left_bufs, right_bufs, firsts, owns, helds, totals = (take(num) for _ in range(6))
    send_sems, recv_sems, left_sems, right_sems, store_sems = take(5)
    beside = (
        extra.builder(count, given, made, refs[taken:], (left_bufs, right_bufs)) if extra else None
    )
    entry_place = ring_place(lax.axis_index("dp"), count)
    last = count - 1

    ready = [buf.shape[0] == 8 for buf in right_bufs]

    def load_right(item):
        _, half, start, _ = items[item]
        return pltpu.make_async_copy(
            rights[item].at[:, start : start + 2 * half], right_bufs[item], right_sems.at[item]
        )

    def load_left(step, side, item, place):
        block = items[item][0]
        member = member_at(place, side, step + 1, count)
        slot = step % 2
        here = pl.ds(pl.multiple_of(member * block, block), block)
        if ready[item]:
            half = items[item][1]
            source = lefts[item].at[here, side * half : (side + 1) * half]
        else:
            source = lefts[item].at[:, here]
        return pltpu.make_async_copy(
            source, left_bufs[item].at[side, slot], left_sems.at[side, slot, item]
        )

    for item in range(num):
        if not ready[item]:
            load_right(item).start()
        for side in range(2):
            load_left(0, side, item, entry_place).start()
    if beside:
        beside.begin()
    place, neighbours = ring_setup(count, *(beside.peers() if beside else ()))
    pairs = [(item, side) for item in range(num) for side in range(2)]

    def send(step, side, item, part, source):
        return pltpu.make_async_remote_copy(
            src_ref=source.at[part],
            dst_ref=helds[item].at[side, step, part],
            send_sem=send_sems.at[side, step, item * parts + part],
            recv_sem=recv_sems.at[side, step, item * parts + part],
            device_id={"dp": neighbours[side]},
            device_id_type=MESH_ID,
        )

    def stores(item, side, part):
        block, _, _, places = items[item]
        rows = block // parts
        return [
            pltpu.make_async_copy(
                totals[item].at[side, part, :, source : source + cols],
                outs[out].at[part * rows : (part + 1) * rows, column : column + cols],
                store_sems.at[side, item * parts + part, k],
            )
            for k, (source, cols, out, column) in enumerate(places[side])
        ]

    for item in range(num):
        if not ready[item]:
            load_right(item).wait()

    def turn(step, carry):
        @pl.when(step < last)
        def _():
            for item, side in pairs:
                load_left(step + 1, side, item, place).start()

        for item in range(num):
            half = items[item][1]
            for side in range(2):
                load_left(step, side, item, place).wait()

            if ready[item]:
                for side in range(2):
                    owns[item][side] = (
                        left_bufs[item][side, step % 2].astype(F32).reshape(owns[item].shape[1:])
                    )
                continue

            def own_sum(side, inner):
                cols = pl.ds(pl.multiple_of(side * half, half), half)
                owns[item][side] = tn_dot(
                    left_bufs[item][side, step % 2], right_bufs[item][:, cols]
                ).reshape(owns[item].shape[1:])
                return inner

            lax.fori_loop(0, 2, own_sum, 0)

        @pl.when(step == 0)
        def _():
            for part in range(parts):
                for item, side in pairs:
                    firsts[item][side, part] = owns[item][side, part].astype(BF16)
                    send(0, side, item, part, firsts[item].at[side]).start()

        if beside:
            beside.compute(step)

        @pl.when((step > 0) & (step < last))
        def _():
            for part in range(parts):
                for item, side in pairs:
                    arrived = helds[item].at[side, step - 1]
                    send(step - 1, side, item, part, arrived).wait_recv()
                    arrived[part] = (
                        arrived[part].astype(F32) + owns[item][side, part]
                    ).astype(BF16)
                    send(step, side, item, part, arrived).start()

        return carry

    lax.fori_loop(0, count, turn, 0)
    for part in range(parts):
        for item, side in pairs:
            arrived = helds[item].at[side, last - 1]
            send(last - 1, side, item, part, arrived).wait_recv()
            totals[item][side, part] = arrived[part].astype(F32) + owns[item][side, part]
            for copy in stores(item, side, part):
                copy.start()
    if beside:
        beside.finish()
    for part in range(parts):
        for item, side in pairs:
            for copy in stores(item, side, part):
                copy.wait()

    def drain(step, carry):
        for part in range(parts):
            for item, side in pairs:
                send(step, side, item, part, helds[item].at[side, 0]).wait_send()
        return carry

    lax.fori_loop(0, last, drain, 0)


def ring_scatter_dots(jobs, parts, count, collective_id, extra=None):
    rows = next((j.left.shape[0] for j in jobs if j.right is not None), 0)
    items, shapes, bases, aliases = [], [], [], {}
    for job in jobs:
        width = job.left.shape[1] if job.right is not None else job.left.shape[0]
        block, half = width // count, job.cols // 2
        if job.pieces:
            places, column = ([], []), 0
            for cols in job.pieces:
                for side in range(2):
                    low = max(column, side * half)
                    high = min(column + cols, (side + 1) * half)
                    if low < high:
                        places[side].append(
                            (low - side * half, high - low, len(shapes), low - column)
                        )
                column += cols
                shapes.append((block, cols))
        else:
            places = [
                [(0, half, len(shapes), job.target + side * half)] for side in range(2)
            ]
            if job.into is None:
                shapes.append((block, job.cols))
            elif isinstance(job.into, int):
                shapes.append((block, job.into))
            else:
                aliases[2 * len(jobs) + len(bases)] = len(shapes)
                bases.append(job.into)
                shapes.append(job.into.shape)
        items.append((block, half, job.start, places))
    num = len(jobs)

    def buffers(depth, dtype):
        return [pltpu.VMEM(depth + (parts, b // parts, h), dtype) for b, h, _, _ in items]

    slots = num * parts
    flops = sum(2 * rows * count * i[0] * 2 * i[1] for i in items)
    nbytes = sum(2 * count * i[0] * 2 * i[1] for i in items)
    dots = [j.right is not None for j in jobs]
    given, given_specs, made, made_specs, spare = extra[1:] if extra else ([], [], [], [], [])
    return pl.pallas_call(
        functools.partial(
            scatter_dot_kernel, count, items, len(shapes), len(bases), parts, extra
        ),
        out_shape=[jax.ShapeDtypeStruct(s, F32) for s in shapes] + made,
        in_specs=[ANY] * (2 * num + len(bases)) + given_specs,
        out_specs=[ANY] * len(shapes) + made_specs,
        input_output_aliases=aliases,
        scratch_shapes=[
            pltpu.VMEM((2, 2) + ((rows, i[0]) if dot_job else (i[0], i[1])), BF16)
            for i, dot_job in zip(items, dots)
        ]
        + [
            pltpu.VMEM((rows, 2 * i[1]) if dot_job else (8, 128), BF16)
            for i, dot_job in zip(items, dots)
        ]
        + buffers((2,), BF16)
        + buffers((2,), F32)
        + buffers((2, count - 1), BF16)
        + buffers((2,), F32)
        + [
            pltpu.SemaphoreType.DMA((2, count - 1, slots)),
            pltpu.SemaphoreType.DMA((2, count - 1, slots)),
            pltpu.SemaphoreType.DMA((2, 2, num)),
            pltpu.SemaphoreType.DMA((num,)),
            pltpu.SemaphoreType.DMA((2, slots, 3)),
        ]
        + spare,
        compiler_params=pltpu.CompilerParams(
            collective_id=collective_id, has_side_effects=True, vmem_limit_bytes=60 << 20
        ),
        cost_estimate=pl.CostEstimate(
            flops=flops, bytes_accessed=20 * nbytes, transcendentals=0
        ),
        name=f"ring_scatter_{collective_id}",
    )(
        *[j.left for j in jobs],
        *[j.left if j.right is None else j.right for j in jobs],
        *bases,
        *given,
    )


class ShareWork:
    def __init__(self, count, given, made, spare, bufs):
        self.given, self.out = given, made[0]
        self.pair, self.first, self.sums, self.second, self.sems = spare
        self.count, self.group = count, self.second.shape[0] + 1
        self.row, self.col = lax.axis_index("dp"), lax.axis_index("tensor")

    def in_column(self, shift):
        return {"dp": (self.row + shift) % self.count}

    def in_group(self, shift):
        return {"tensor": (self.col + shift) % self.group}

    def peers(self):
        column = [self.in_column(s) for s in range(1, self.count)]
        return column, [self.in_group(s) for s in range(1, self.group)]

    def begin(self):
        pass

    def part(self, row):
        width = self.sums.shape[1]
        return pl.ds(pl.multiple_of(row * width, width), width)

    def move(self, stage, shift):
        if stage == 0:
            source = self.pair.at[:, self.part((self.row + shift) % self.count)]
            target, device, slot = self.first.at[shift - 1], self.in_column(shift), shift - 1
        else:
            source, target = self.sums, self.second.at[shift - 1]
            device, slot = self.in_group(shift), self.count + shift - 2
        return pltpu.make_async_remote_copy(
            src_ref=source,
            dst_ref=target,
            send_sem=self.sems.at[0, slot],
            recv_sem=self.sems.at[1, slot],
            device_id=device,
            device_id_type=MESH_ID,
        )

    def compute(self, step):
        @pl.when(step == 0)
        def _():
            self.pair[...] = self.given[0][...]
            self.pair[1:2, :] = self.given[1][...]
            for shift in range(1, self.count):
                self.move(0, shift).start()

        @pl.when(step == 5)
        def _():
            total = self.pair[:, self.part(self.row)]
            for shift in range(1, self.count):
                self.move(0, shift).wait()
                total = total + self.first[shift - 1]
            self.sums[...] = total
            for shift in range(1, self.group):
                self.move(1, shift).start()

    def finish(self):
        total = self.sums[...]
        for shift in range(1, self.group):
            self.move(1, shift).wait()
            total = total + self.second[shift - 1]
        share = total.shape[1] // self.group
        picked = jnp.zeros((8, share), F32)
        for col in range(self.group):
            picked = jnp.where(self.col == col, total[:, col * share : (col + 1) * share], picked)
        self.out[:, :share] = picked


class ProductWork:
    def __init__(self, count, given, made, spare, bufs):
        self.right, self.out = given[0], made[0]
        self.right_buf, self.stage, self.load_sem, self.sems = spare
        self.left, self.count = bufs[0][0], count
        self.place = ring_place(lax.axis_index("dp"), count)
        self.start = self.right.shape[1] - self.right_buf.shape[1]

    def peers(self):
        return ()

    def load(self):
        return pltpu.make_async_copy(
            self.right.at[:, self.start :], self.right_buf, self.load_sem
        )

    def begin(self):
        self.load().start()

    def store(self, step):
        block = self.stage.shape[1]
        member = member_at(self.place, 0, step + 1, self.count)
        return pltpu.make_async_copy(
            self.stage.at[step % 2],
            self.out.at[pl.ds(pl.multiple_of(member * block, block), block), :],
            self.sems.at[step % 2],
        )

    def compute(self, step):
        @pl.when(step == 0)
        def _():
            self.load().wait()

        @pl.when(step >= 2)
        def _():
            self.store(step - 2).wait()

        self.stage[step % 2] = tn_dot(self.left[0, step % 2], self.right_buf[...]).astype(BF16)
        self.store(step).start()

    def finish(self):
        for step in (self.count - 2, self.count - 1):
            self.store(step).wait()


def product_work(right, start, count, width):
    rows, cols = right.shape[0], right.shape[1] - start
    return Extra(
        ProductWork,
        [right],
        [ANY],
        [jax.ShapeDtypeStruct((width, cols), BF16)],
        [ANY],
        [
            pltpu.VMEM((rows, cols), BF16),
            pltpu.VMEM((2, width // count, cols), BF16),
            pltpu.SemaphoreType.DMA,
            pltpu.SemaphoreType.DMA((2,)),
        ],
    )


class GatherWork:
    def __init__(self, count, given, made, spare, bufs):
        self.own, self.out = given[0], made[0]
        self.stage, self.sems, self.local = spare
        self.col = lax.axis_index("tensor")
        self.rows = self.own.shape[0]
        self.parts = self.sems.shape[2]

    def core(self):
        return {"tensor": self.col + 1 - 2 * (self.col % 2)}

    def across(self):
        return {"tensor": (self.col + 2) % 4}

    def peers(self):
        return None, [self.core(), self.across()]

    def begin(self):
        pltpu.make_async_copy(self.own, self.stage, self.local).start()

    def spot(self, member, part):
        size = self.rows // self.parts
        return pl.ds(pl.multiple_of(member * self.rows + part * size, size), size)

    def move(self, kind, part):
        size = self.rows // self.parts
        member = (self.col + 2) % 4 if kind == 2 else self.col
        target = self.out.at[self.spot(member, part), :]
        source = target if kind == 2 else self.own.at[part * size : (part + 1) * size, :]
        return pltpu.make_async_remote_copy(
            src_ref=source,
            dst_ref=target,
            send_sem=self.sems.at[0, kind, part],
            recv_sem=self.sems.at[1, kind, part],
            device_id=self.across() if kind == 0 else self.core(),
            device_id_type=MESH_ID,
        )

    def keep(self):
        here = pl.ds(pl.multiple_of(self.col * self.rows, self.rows), self.rows)
        return pltpu.make_async_copy(self.stage, self.out.at[here, :], self.local)

    def compute(self, step):
        @pl.when(step == 0)
        def _():
            for part in range(self.parts):
                self.move(0, part).start()
                self.move(1, part).start()
            pltpu.make_async_copy(self.own, self.stage, self.local).wait()
            self.keep().start()

        for part, turn in enumerate((2, 4, 5, 6)):

            @pl.when(step == turn)
            def _():
                self.move(0, part).wait_recv()
                self.move(2, part).start()

    def finish(self):
        for part in range(self.parts):
            self.move(0, part).wait_send()
            self.move(1, part).wait()
            self.move(2, part).wait()
        self.keep().wait()


def gather_work(own):
    rows, width = own.shape
    return Extra(
        GatherWork,
        [own],
        [ANY],
        [jax.ShapeDtypeStruct((4 * rows, width), BF16)],
        [ANY],
        [
            pltpu.VMEM(own.shape, BF16),
            pltpu.SemaphoreType.DMA((2, 3, 4)),
            pltpu.SemaphoreType.DMA,
        ],
    )


def share_work(first, second, count, group):
    width = first.shape[1] // count
    vmem = pl.BlockSpec(memory_space=pltpu.VMEM)
    return Extra(
        ShareWork,
        [first, second],
        [vmem] * 2,
        [jax.ShapeDtypeStruct((8, 128), F32)],
        [vmem],
        [
            pltpu.VMEM(first.shape, F32),
            pltpu.VMEM((count - 1, 8, width), F32),
            pltpu.VMEM((8, width), F32),
            pltpu.VMEM((group - 1, 8, width), F32),
            pltpu.SemaphoreType.DMA((2, count + group - 2)),
        ],
    )


class NormWork:
    def __init__(self, count, given, made, spare, bufs):
        self.grads, self.gates = given[:2], tuple(given[2:4])
        self.up, self.down = given[4:]
        self.outs = made
        self.grad_bufs, self.row_bufs, self.down_bufs, self.stage = spare[0], *spare[1:4]
        self.grad_sems, self.row_sems, self.down_sems, self.out_sems = spare[4:]
        self.act = bufs[1][0]
        self.count = count
        self.block = self.row_bufs.shape[2]

    def load_grad(self, which):
        return pltpu.make_async_copy(
            self.grads[which], self.grad_bufs.at[which], self.grad_sems.at[which]
        )

    def spot(self, step):
        return pl.ds(pl.multiple_of(step * self.block, self.block), self.block)

    def loads(self, step):
        slot = step % 2
        edge = self.gates[0].shape[1]
        gate = self.row_bufs.at[0, slot]
        targets = [gate.at[:, :edge], gate.at[:, edge:], self.row_bufs.at[1, slot]]
        rows = [
            pltpu.make_async_copy(
                source.at[self.spot(step), :], target, self.row_sems.at[which, slot]
            )
            for which, (source, target) in enumerate(zip(self.gates + (self.up,), targets))
        ]
        down = pltpu.make_async_copy(
            self.down.at[:, self.spot(step)], self.down_bufs.at[slot], self.down_sems.at[slot]
        )
        return rows + [down]

    def store(self, which, step):
        slot = step % 2
        return pltpu.make_async_copy(
            self.stage.at[which, slot],
            self.outs[which].at[:, self.spot(step)],
            self.out_sems.at[which, slot],
        )

    def begin(self):
        for which in range(2):
            self.load_grad(which).start()
        for copy in self.loads(0):
            copy.start()

    def peers(self):
        return ()

    def compute(self, step):
        @pl.when(step < self.count - 1)
        def _():
            for copy in self.loads(step + 1):
                copy.start()

        @pl.when(step == 0)
        def _():
            for which in range(2):
                self.load_grad(which).wait()

        @pl.when(step >= 2)
        def _():
            for which in range(2):
                self.store(which, step - 2).wait()

        for copy in self.loads(step):
            copy.wait()
        slot = step % 2

        def lines(index, carry):
            band = pl.ds(pl.multiple_of(index * 256, 256), 256)
            norm = nt_dot(self.grad_bufs[0, band, :], self.row_bufs[0, slot])
            norm += nt_dot(self.grad_bufs[1, band, :], self.row_bufs[1, slot])
            self.stage[0, slot, band, :] = norm.astype(BF16)
            value = jnp.dot(
                self.act[band, :], self.down_bufs[slot], preferred_element_type=F32
            )
            self.stage[1, slot, band, :] = value.astype(BF16)
            return carry

        lax.fori_loop(0, self.act.shape[0] // 256, lines, 0)
        for which in range(2):
            self.store(which, step).start()

    def finish(self):
        for step in range(max(self.count - 2, 0), self.count):
            for which in range(2):
                self.store(which, step).wait()


def down_ring(grad_branch, activated, grad_gate, grad_up, gates, up_all, down_all, count, cid):
    rows, hidden = activated.shape
    width = up_all.shape[0]
    block = width // count
    wide = jax.ShapeDtypeStruct((rows, width), BF16)
    spare = [
        pltpu.VMEM((2, rows, hidden), BF16),
        pltpu.VMEM((2, 2, block, hidden), BF16),
        pltpu.VMEM((2, hidden, block), BF16),
        pltpu.VMEM((2, 2, rows, block), BF16),
        pltpu.SemaphoreType.DMA((2,)),
        pltpu.SemaphoreType.DMA((3, 2)),
        pltpu.SemaphoreType.DMA((2,)),
        pltpu.SemaphoreType.DMA((2, 2)),
    ]
    given = [grad_gate, grad_up, *gates, up_all, down_all]
    return ring_scatter_dots(
        [Job(grad_branch, activated, 0, hidden)],
        2,
        count,
        cid,
        Extra(NormWork, given, [ANY] * 6, [wide, wide], [ANY] * 2, spare),
    )


def mlp_kernel(count, *refs):
    x_hbm, wg_hbm, wg_rest, wu_hbm, shard, gb_hbm = refs[:6]
    act_hbm, gg_hbm, gu_hbm, down_all = refs[6:10]
    x_buf, gb_buf, w_bufs, gate_slope, up_slope, acc, half_bufs, stage, own_stage = refs[10:19]
    send_sems, recv_sems, w_sems, in_sems, half_sems, out_sems, local_sem = refs[19:]
    rows, width = x_buf.shape
    hidden = acc.shape[1]
    block = width // count
    cols = w_bufs.shape[-1]
    steps = hidden // cols
    half = hidden // 2
    parts = send_sems.shape[2]
    me = lax.axis_index("dp")

    gate_steps = wg_hbm.shape[1] // cols

    def load_weights(step, which, source=None):
        start = step - gate_steps if source is wg_rest else step
        source = (wg_hbm, wu_hbm)[which] if source is None else source
        return pltpu.make_async_copy(
            source.at[:, pl.ds(pl.multiple_of(start * cols, cols), cols)],
            w_bufs.at[which, step % 2],
            w_sems.at[which, step % 2],
        )

    def fetch(step):
        load_weights(step, 1).start()

        @pl.when(step < gate_steps)
        def _():
            load_weights(step, 0).start()

        @pl.when(step >= gate_steps)
        def _():
            load_weights(step, 0, wg_rest).start()

    load_x = pltpu.make_async_copy(x_hbm, x_buf, in_sems.at[0])
    load_gb = pltpu.make_async_copy(gb_hbm, gb_buf, in_sems.at[1])
    load_own = pltpu.make_async_copy(shard, own_stage, local_sem)
    load_x.start()
    for which in range(2):
        load_weights(0, which).start()
    load_own.start()
    load_gb.start()
    place, neighbours = ring_setup(count)

    def target(ref, member, side, part):
        return piece(ref, (hidden, block), 1, member, side, part, parts)

    def hop(step, side, part):
        ref = target(down_all, member_at(place, side, step, count), side, part)
        return pltpu.make_async_remote_copy(
            src_ref=ref,
            dst_ref=ref,
            send_sem=send_sems.at[side, step, part],
            recv_sem=recv_sems.at[side, step, part],
            device_id={"dp": neighbours[side]},
            device_id_type=MESH_ID,
        )

    for part in range(parts):
        for side in range(2):
            pltpu.make_async_remote_copy(
                src_ref=piece(shard, (hidden, block), None, 0, side, part, parts),
                dst_ref=target(down_all, me, side, part),
                send_sem=send_sems.at[side, 0, part],
                recv_sem=recv_sems.at[side, 0, part],
                device_id={"dp": neighbours[side]},
                device_id_type=MESH_ID,
            ).start()

    def pump(step):
        for part in range(parts):
            for side in range(2):
                hop(step - 1, side, part).wait_recv()
                hop(step, side, part).start()

    load_own.wait()
    store_own = pltpu.make_async_copy(
        own_stage, down_all.at[:, pl.ds(pl.multiple_of(me * block, block), block)], local_sem
    )
    store_own.start()
    load_x.wait()

    def store(ref, which, step):
        return pltpu.make_async_copy(
            stage.at[which, step % 2],
            ref.at[:, pl.ds(pl.multiple_of(step * cols, cols), cols)],
            out_sems.at[which, step % 2],
        )

    def forward(step, carry):
        @pl.when(step + 1 < steps)
        def _():
            fetch(step + 1)

        @pl.when(step >= 2)
        def _():
            store(act_hbm, 0, step - 2).wait()

        load_weights(step, 1).wait()

        @pl.when(step < gate_steps)
        def _():
            load_weights(step, 0).wait()

        @pl.when(step >= gate_steps)
        def _():
            load_weights(step, 0, wg_rest).wait()

        here = pl.ds(pl.multiple_of(step * cols, cols), cols)
        for top in range(0, rows, 256):
            band = pl.ds(top, 256)
            lines = x_buf[band, :]
            gate = jnp.dot(lines, w_bufs[0, step % 2], preferred_element_type=F32)
            up = jnp.dot(lines, w_bufs[1, step % 2], preferred_element_type=F32)
            sig = jax.nn.sigmoid(gate)
            silu = gate * sig
            stage[0, step % 2, band, :] = (silu * up).astype(BF16)
            gate_slope[band, here] = up * sig * (1.0 + gate * (1.0 - sig))
            up_slope[band, here] = silu
            acc[band, here] = jnp.zeros((256, cols), F32)
        store(act_hbm, 0, step).start()

        turn = (step + 1) // 2

        @pl.when((step % 2 == 1) & (turn <= count - 2))
        def _():
            pump(turn)

        return carry

    lax.fori_loop(0, steps, forward, 0)
    for step in range(max(steps - 2, 0), steps):
        store(act_hbm, 0, step).wait()
    pumped = min(steps // 2, count - 2)
    load_gb.wait()

    def load_half(step, side):
        member = member_at(place, side, step, count)
        return pltpu.make_async_copy(
            down_all.at[
                pl.ds(side * half, half), pl.ds(pl.multiple_of(member * block, block), block)
            ],
            half_bufs.at[side],
            half_sems.at[side],
        )

    def backward(step, carry):
        @pl.when((step > pumped) & (step <= count - 2))
        def _():
            pump(step)

        @pl.when(step == count - 1)
        def _():
            for part in range(parts):
                for side in range(2):
                    hop(count - 2, side, part).wait_recv()

        for side in range(2):
            load_half(step, side).start()
        for side in range(2):
            member = member_at(place, side, step, count)
            load_half(step, side).wait()
            here = pl.ds(pl.multiple_of(member * block, block), block)
            spot = pl.ds(side * half, half)

            def lines(index, carry):
                band = pl.ds(pl.multiple_of(index * 256, 256), 256)
                acc[band, spot] += nt_dot(gb_buf[band, here], half_bufs[side])
                return carry

            lax.fori_loop(0, rows // 256, lines, 0)

        return carry

    store_own.wait()
    lax.fori_loop(0, count, backward, 0)

    def slopes(step, carry):
        @pl.when(step >= 2)
        def _():
            store(gg_hbm, 1, step - 2).wait()
            store(gu_hbm, 2, step - 2).wait()

        here = pl.ds(pl.multiple_of(step * cols, cols), cols)

        def lines(index, carry):
            band = pl.ds(pl.multiple_of(index * 256, 256), 256)
            value = acc[band, here]
            stage[1, step % 2, band, :] = (value * gate_slope[band, here]).astype(BF16)
            stage[2, step % 2, band, :] = (value * up_slope[band, here]).astype(BF16)
            return carry

        lax.fori_loop(0, rows // 256, lines, 0)
        store(gg_hbm, 1, step).start()
        store(gu_hbm, 2, step).start()
        return carry

    lax.fori_loop(0, steps, slopes, 0)
    for step in range(max(steps - 2, 0), steps):
        store(gg_hbm, 1, step).wait()
        store(gu_hbm, 2, step).wait()

    def drain(step, carry):
        for part in range(parts):
            for side in range(2):
                hop(step, side, part).wait_send()
        return carry

    lax.fori_loop(0, count - 1, drain, 0)


def mlp_ring(rows_mlp, gates, up_all, w_down, grad_branch, count, collective_id):
    rows, width = rows_mlp.shape
    hidden, block = w_down.shape
    cols, parts = 256, 2
    wide = jax.ShapeDtypeStruct((rows, hidden), BF16)
    return pl.pallas_call(
        functools.partial(mlp_kernel, count),
        out_shape=[wide] * 3 + [jax.ShapeDtypeStruct((hidden, width), BF16)],
        in_specs=[ANY] * 6,
        out_specs=[pl.BlockSpec(memory_space=pl.ANY)] * 4,
        scratch_shapes=[
            pltpu.VMEM((rows, width), BF16),
            pltpu.VMEM((rows, width), BF16),
            pltpu.VMEM((2, 2, width, cols), BF16),
            pltpu.VMEM((rows, hidden), F32),
            pltpu.VMEM((rows, hidden), F32),
            pltpu.VMEM((rows, hidden), F32),
            pltpu.VMEM((2, hidden // 2, block), BF16),
            pltpu.VMEM((3, 2, rows, cols), BF16),
            pltpu.VMEM((hidden, block), BF16),
            pltpu.SemaphoreType.DMA((2, count - 1, parts)),
            pltpu.SemaphoreType.DMA((2, count - 1, parts)),
            pltpu.SemaphoreType.DMA((2, 2)),
            pltpu.SemaphoreType.DMA((2,)),
            pltpu.SemaphoreType.DMA((2,)),
            pltpu.SemaphoreType.DMA((3, 2)),
            pltpu.SemaphoreType.DMA,
        ],
        compiler_params=pltpu.CompilerParams(
            collective_id=collective_id, has_side_effects=True, vmem_limit_bytes=60 << 20
        ),
        cost_estimate=pl.CostEstimate(
            flops=6 * rows * width * hidden,
            bytes_accessed=40 * hidden * width,
            transcendentals=rows * hidden,
        ),
        name="mlp_ring",
    )(rows_mlp, *gates, up_all, w_down, grad_branch)


class HeadWork:
    def __init__(self, count, given, made, spare, bufs):
        self.length, self.gain, self.sources = given[0], given[1], given[2:]
        self.grads_out, self.token_out, self.gain_out = made
        num = len(self.sources)
        self.bufs = spare[:num]
        self.heads, self.grads, self.acc_k, self.acc_v, self.stage = spare[num : num + 5]
        self.stats, self.inner, self.bias = spare[num + 5 : num + 8]
        self.in_sems, self.out_sems = spare[num + 8 :]

    def peers(self):
        return ()

    def load(self, which):
        return pltpu.make_async_copy(
            self.sources[which], self.bufs[which], self.in_sems.at[which]
        )

    def begin(self):
        for which in range(len(self.sources)):
            self.load(which).start()
        self.gain_out[...] = jnp.zeros_like(self.gain_out)
        self.acc_k[...] = jnp.zeros_like(self.acc_k)
        self.acc_v[...] = jnp.zeros_like(self.acc_v)
        key_pos = lax.broadcasted_iota(jnp.int32, self.bias.shape, 0)
        self.bias[...] = jnp.where(key_pos < self.length[0], 0.0, -1e30)

    def store(self, band):
        rows = self.stage.shape[1]
        return pltpu.make_async_copy(
            self.stage.at[band % 2],
            self.token_out.at[pl.ds(pl.multiple_of(band * rows, rows), rows), :],
            self.out_sems.at[band % 2],
        )

    def store_grads(self):
        return pltpu.make_async_copy(self.grads, self.grads_out, self.out_sems.at[2])

    def tokens(self, band):
        w_query, w_key, w_value, normed = self.bufs[9:]
        rows = self.stage.shape[1]
        inner = w_query.shape[1]

        @pl.when(band >= 2)
        def _():
            self.store(band - 2).wait()

        lines = pl.ds(pl.multiple_of(band * rows, rows), rows)

        def columns(index, carry):
            cols = pl.ds(pl.multiple_of(index * 512, 512), 512)
            value = nt_dot(self.grads[lines, :inner], w_query[cols, :])
            value += nt_dot(self.grads[lines, inner : inner + 128], w_key[cols, :])
            value += nt_dot(self.grads[lines, inner + 128 :], w_value[cols, :])
            self.stage[band % 2, :, cols] = value.astype(BF16)
            scaled = value * normed[lines, cols].astype(F32)
            self.gain_out[0:1, cols] += jnp.sum(scaled, axis=0, keepdims=True)
            return carry

        lax.fori_loop(0, w_query.shape[0] // 512, columns, 0)
        self.store(band).start()

    def compute(self, step):
        grad_attn, w_output, queries, keys, values, cosine, sine, outs, stats = self.bufs[:9]
        inner = queries.shape[1]
        pairs = inner // 128

        @pl.when(step == 0)
        def _():
            for which in range(2):
                self.load(which).wait()

            def band(index, carry):
                rows = pl.ds(pl.multiple_of(index * 256, 256), 256)
                self.heads[rows, :] = nt_dot(grad_attn[rows, :], w_output[...]).astype(BF16)
                return carry

            lax.fori_loop(0, LEN // 256, band, 0)

        @pl.when(step == 1)
        def _():
            for which in range(2, 9):
                self.load(which).wait()

            self.stats[...] = jnp.transpose(stats[...])

            def products(index, carry):
                rows = pl.ds(pl.multiple_of(index * 256, 256), 256)
                kept = jnp.zeros((256, 128), F32)
                for pair in range(pairs):
                    cols = slice(pair * 128, (pair + 1) * 128)
                    kept = row_products(self.heads[rows, cols], outs[rows, cols], pair, kept)
                stats[rows, :] = kept
                return carry

            lax.fori_loop(0, LEN // 256, products, 0)
            self.inner[...] = jnp.transpose(stats[...])

        @pl.when(step == pairs + 1)
        def _():
            for which in range(9, len(self.sources)):
                self.load(which).wait()

        @pl.when((step >= 1) & (step <= pairs))
        def _():
            here = pl.ds(pl.multiple_of((step - 1) * 128, 128), 128)
            attend_back_tiles(
                step - 1, queries.at[:, here], keys, values, self.heads.at[:, here], cosine,
                sine, self.stats, self.inner, self.bias, self.grads.at[:, here],
                self.acc_k, self.acc_v,
            )

        @pl.when(step == pairs)
        def _():
            self.grads[:, inner : inner + 128] = rope_back(
                self.acc_k[...], cosine[...], sine[...]
            )
            self.grads[:, inner + 128 :] = self.acc_v[...].astype(BF16)
            self.store_grads().start()

        @pl.when((step > pairs) & (step <= pairs + 2))
        def _():
            def band(index, carry):
                self.tokens(2 * (step - pairs - 1) + index)
                return carry

            lax.fori_loop(0, 2, band, 0)

    def finish(self):
        self.gain_out[0:1, :] = self.gain_out[0:1, :] / self.gain[...]
        self.store_grads().wait()
        for band in (2, 3):
            self.store(band).wait()


def heads_ring(
    job, lengths, gain, grad_attn, w_output, qkv, tables, saved, weights, rows_attn, count, cid
):
    sources = [grad_attn, w_output, *qkv, *tables, *saved, *weights, rows_attn]
    rows, width = grad_attn.shape
    inner = qkv[0].shape[1]
    made = [
        jax.ShapeDtypeStruct((rows, inner + 256), BF16),
        jax.ShapeDtypeStruct((rows, width), BF16),
        jax.ShapeDtypeStruct((8, width), F32),
    ]
    spare = [pltpu.VMEM(g.shape, g.dtype) for g in sources] + [
        pltpu.VMEM((rows, inner), BF16),
        pltpu.VMEM((rows, inner + 256), BF16),
        pltpu.VMEM((rows, 128), F32),
        pltpu.VMEM((rows, 128), F32),
        pltpu.VMEM((2, rows // 4, width), BF16),
        pltpu.VMEM((128, rows), F32),
        pltpu.VMEM((128, rows), F32),
        pltpu.VMEM((rows, 128), F32),
        pltpu.SemaphoreType.DMA((len(sources),)),
        pltpu.SemaphoreType.DMA((3,)),
    ]
    vmem = pl.BlockSpec(memory_space=pltpu.VMEM)
    specs = [pl.BlockSpec(memory_space=pltpu.SMEM), vmem] + [ANY] * len(sources)
    return ring_scatter_dots(
        [job],
        4,
        count,
        cid,
        Extra(HeadWork, [lengths, gain] + sources, specs, made, [ANY, ANY, vmem], spare),
    )


def attend_ring_kernel(count, *refs):
    length_ref, shard, sources = refs[0], refs[1], refs[2:9]
    gathered, q_out, k_out, v_out, head_out, part_out, stats_out = refs[9:16]
    bufs = refs[16:23]
    q_buf, k_buf, v_buf, head_buf, stage, own, stats = refs[23:30]
    send_sems, recv_sems, in_sems, out_sems, local_sem = refs[30:]
    rows_buf, w_query, w_key, w_value, w_output, cosine, sine = bufs
    shape = own.shape
    me = lax.axis_index("dp")
    loads = [
        pltpu.make_async_copy(source, buf, in_sems.at[k])
        for k, (source, buf) in enumerate(zip(sources, bufs))
    ]
    for load in loads:
        load.start()
    load_own = pltpu.make_async_copy(shard.at[:, : shape[1]], own, local_sem)
    load_own.start()
    place, neighbours = ring_setup(count)

    def hop(step, side):
        ref = piece(gathered, shape, 0, member_at(place, side, step, count), side, 0, 1)
        return pltpu.make_async_remote_copy(
            src_ref=ref,
            dst_ref=ref,
            send_sem=send_sems.at[side, step],
            recv_sem=recv_sems.at[side, step],
            device_id={"dp": neighbours[side]},
            device_id_type=MESH_ID,
        )

    for side in range(2):
        pltpu.make_async_remote_copy(
            src_ref=piece(shard, shape, None, 0, side, 0, 1),
            dst_ref=piece(gathered, shape, 0, me, side, 0, 1),
            send_sem=send_sems.at[side, 0],
            recv_sem=recv_sems.at[side, 0],
            device_id={"dp": neighbours[side]},
            device_id_type=MESH_ID,
        ).start()

    def pump(step, carry=0):
        for side in range(2):
            hop(step - 1, side).wait_recv()
            hop(step, side).start()
        return carry

    load_own.wait()
    store_own = pltpu.make_async_copy(
        own, gathered.at[pl.ds(pl.multiple_of(me * shape[0], shape[0]), shape[0]), :], local_sem
    )
    store_own.start()
    for k in (0, 1, 2, 3, 5, 6):
        loads[k].wait()

    stats[...] = jnp.zeros_like(stats)

    def projection(band, carry):
        lines = pl.ds(pl.multiple_of(band * 256, 256), 256)
        project_rows(
            rows_buf[lines, :], w_query, w_key, w_value, cosine[lines, :], sine[lines, :],
            q_buf.at[lines, :], k_buf.at[lines, :], v_buf.at[lines, :],
        )
        return carry

    lax.fori_loop(0, LEN // 256, projection, 0)
    stores = [
        pltpu.make_async_copy(buf, out, out_sems.at[k])
        for k, (buf, out) in enumerate(
            ((q_buf, q_out), (k_buf, k_out), (v_buf, v_out), (head_buf, head_out))
        )
    ]
    for store in stores[:3]:
        store.start()
    pump(1)
    pairs = q_buf.shape[1] // 128

    def attention(pair, carry):
        here = pl.ds(pl.multiple_of(pair * 128, 128), 128)
        attend_pair(
            length_ref[0], pair, q_buf.at[:, here], k_buf, v_buf, head_buf.at[:, here], stats
        )

        @pl.when(pair + 2 <= count - 2)
        def _():
            pump(pair + 2)

        return carry

    lax.fori_loop(0, pairs, attention, 0)
    loads[4].wait()
    stores[3].start()
    store_stats = pltpu.make_async_copy(stats, stats_out, out_sems.at[6])
    store_stats.start()

    def store_part(band):
        return pltpu.make_async_copy(
            stage.at[band % 2],
            part_out.at[pl.ds(pl.multiple_of(band * 256, 256), 256), :],
            out_sems.at[4 + band % 2],
        )

    def output(band, carry):
        @pl.when(band >= 2)
        def _():
            store_part(band - 2).wait()

        lines = pl.ds(pl.multiple_of(band * 256, 256), 256)

        def columns(index, inner):
            cols = pl.ds(pl.multiple_of(index * 512, 512), 512)
            stage[band % 2, :, cols] = jnp.dot(
                head_buf[lines, :], w_output[:, cols], preferred_element_type=F32
            ).astype(BF16)
            return inner

        lax.fori_loop(0, w_output.shape[1] // 512, columns, 0)
        store_part(band).start()

        @pl.when((band == 0) & (pairs + 2 <= count - 2))
        def _():
            pump(pairs + 2)

        return carry

    lax.fori_loop(0, LEN // 256, output, 0)
    lax.fori_loop(min(pairs + 3, count - 1), count - 1, pump, 0)
    for band in (LEN // 256 - 2, LEN // 256 - 1):
        store_part(band).wait()
    for store in stores:
        store.wait()
    store_stats.wait()
    store_own.wait()
    for side in range(2):
        hop(count - 2, side).wait_recv()

    def drain(step, carry):
        for side in range(2):
            hop(step, side).wait_send()
        return carry

    lax.fori_loop(0, count - 1, drain, 0)


def attend_ring(shard, edge, lengths, rows_attn, weights, tables, count, collective_id):
    sources = [rows_attn, *weights, *tables]
    rows, width = rows_attn.shape
    inner = weights[0].shape[1]

    def low(*shape):
        return jax.ShapeDtypeStruct(shape, BF16)

    return pl.pallas_call(
        functools.partial(attend_ring_kernel, count),
        out_shape=[
            low(shard.shape[0] * count, edge),
            low(rows, inner),
            low(rows, 128),
            low(rows, 128),
            low(rows, inner),
            low(rows, width),
            jax.ShapeDtypeStruct((rows, 128), F32),
        ],
        in_specs=[pl.BlockSpec(memory_space=pltpu.SMEM)] + [ANY] * (1 + len(sources)),
        out_specs=[ANY] * 7,
        scratch_shapes=[pltpu.VMEM(source.shape, source.dtype) for source in sources]
        + [
            pltpu.VMEM((rows, inner), BF16),
            pltpu.VMEM((rows, 128), BF16),
            pltpu.VMEM((rows, 128), BF16),
            pltpu.VMEM((rows, inner), BF16),
            pltpu.VMEM((2, 256, width), BF16),
            pltpu.VMEM((shard.shape[0], edge), BF16),
            pltpu.VMEM((rows, 128), F32),
            pltpu.SemaphoreType.DMA((2, count - 1)),
            pltpu.SemaphoreType.DMA((2, count - 1)),
            pltpu.SemaphoreType.DMA((len(sources),)),
            pltpu.SemaphoreType.DMA((7,)),
            pltpu.SemaphoreType.DMA,
        ],
        compiler_params=pltpu.CompilerParams(
            collective_id=collective_id, has_side_effects=True, vmem_limit_bytes=56 << 20
        ),
        cost_estimate=pl.CostEstimate(
            flops=24 << 30, bytes_accessed=60 << 20, transcendentals=8 << 20
        ),
        name="attend_ring",
    )(lengths, shard, *sources)


def ring_weight_grads(jobs, parts, count, collective_id):
    if all(left.shape[1] // count % 128 == 0 for left, _ in jobs):
        jobs = [Job(left, right, 0, right.shape[1]) for left, right in jobs]
        return ring_scatter_dots(jobs, parts, count, collective_id)
    partials = [tn_dot(left, right).astype(BF16) for left, right in jobs]
    num = len(jobs)
    return ring_scatter(partials, [0] * num, [parts] * num, count, collective_id)


def after(value, *deps):
    return lax.optimization_barrier((value,) + deps)[0]


def gather_rows(value):
    return lax.all_gather(value, "tensor", axis=0, tiled=True)


def scatter_rows(value):
    return lax.psum_scatter(value.astype(BF16), "tensor", scatter_dimension=0, tiled=True)


def share_kernel(count, group, parts_ref, out_ref, first, sums, second, sems):
    row, col = lax.axis_index("dp"), lax.axis_index("tensor")
    barrier = pltpu.get_barrier_semaphore()

    def in_group(shift):
        return {"tensor": (col + shift) % group}

    def in_column(shift):
        return {"dp": (row + shift) % count}

    def greet(device):
        pl.semaphore_signal(barrier, inc=1, device_id=device, device_id_type=MESH_ID)

    for shift in range(1, group):
        greet(in_group(shift))
    for shift in range(1, count):
        greet(in_column(shift))
    pl.semaphore_wait(barrier, group + count - 2)

    def exchange(shift, slot, source, target, device):
        return pltpu.make_async_remote_copy(
            src_ref=source,
            dst_ref=target,
            send_sem=sems.at[0, slot],
            recv_sem=sems.at[1, slot],
            device_id=device,
            device_id_type=MESH_ID,
        )

    moves = [
        exchange(s, s - 1, parts_ref.at[(col + s) % group], first.at[s - 1], in_group(s))
        for s in range(1, group)
    ]
    for move in moves:
        move.start()
    total = parts_ref[col]
    for shift, move in enumerate(moves):
        move.wait()
        total = total + first[shift]
    sums[...] = total
    moves = [
        exchange(
            s, group + s - 2, sums.at[(row + s) % count], second.at[s - 1], in_column(s)
        )
        for s in range(1, count)
    ]
    for move in moves:
        move.start()
    total = sums[row]
    for shift, move in enumerate(moves):
        move.wait()
        total = total + second[shift]
    out_ref[...] = total


def sum_shares(first, second, count, group, collective_id):
    share = first.shape[0] // (count * group)
    pair = jnp.stack([first, second]).reshape(2, count, group, share)
    parts = jnp.transpose(pair, (2, 1, 0, 3)).reshape(group, count, 1, 2 * share)
    width = (2 * share + 127) // 128 * 128
    parts = jnp.pad(parts, ((0, 0), (0, 0), (0, 7), (0, width - 2 * share)))
    tile = (8, width)
    out = pl.pallas_call(
        functools.partial(share_kernel, count, group),
        out_shape=jax.ShapeDtypeStruct(tile, F32),
        in_specs=[pl.BlockSpec(memory_space=pltpu.VMEM)],
        out_specs=pl.BlockSpec(memory_space=pltpu.VMEM),
        scratch_shapes=[
            pltpu.VMEM((group - 1, count) + tile, F32),
            pltpu.VMEM((count,) + tile, F32),
            pltpu.VMEM((count - 1,) + tile, F32),
            pltpu.SemaphoreType.DMA((2, group + count - 2)),
        ],
        compiler_params=pltpu.CompilerParams(collective_id=collective_id, has_side_effects=True),
        name="sum_shares",
    )(parts)
    return out[0, :share], out[0, share : 2 * share]


def dot(left, right):
    return jnp.dot(left, right, preferred_element_type=F32)


def body(
    count,
    group,
    tokens,
    lengths,
    attn_gain,
    w_query,
    w_key,
    w_value,
    w_output,
    mlp_gain,
    w_gate,
    w_up,
    w_down,
    cotangent,
):
    local_rows = tokens.shape[0]
    token_full = tokens.astype(F32)
    gain_attn = attn_gain.astype(F32)
    gain_mlp = mlp_gain.astype(F32)
    row_pos = lax.axis_index("tensor") * local_rows + jnp.arange(local_rows)
    valid_rows = (row_pos < lengths[0]).astype(F32)
    cot_masked = cotangent.astype(F32) * valid_rows[:, None]
    cosine, sine = rope_tables()

    inv_first = lax.rsqrt(jnp.mean(token_full * token_full, axis=1, keepdims=True) + epsilon)
    normed_attn = (token_full * inv_first * gain_attn).astype(BF16)
    rows_attn = gather_rows(normed_attn)
    query_all, key_all, value_all, output_all = ring_gather(
        [after(w_query, normed_attn), w_key, w_value, w_output],
        (0, 0, 0, 1), (1, 1, 1, 1), count, 0,
    )
    grad_branch = gather_rows(after(cot_masked.astype(BF16), rows_attn))
    fused = count == 8 and group == 4
    edge = 3 * w_gate.shape[1] // 8
    gates = []
    if fused:
        first_gate, queries, keys, values, head_out, attn_part, stats = attend_ring(
            w_gate,
            edge,
            lengths,
            rows_attn,
            (query_all, key_all, value_all, output_all),
            (cosine, sine),
            count,
            9,
        )
        gates.append(first_gate)
    else:
        queries, keys, values = project(rows_attn, query_all, key_all, value_all, cosine, sine)
        head_out = attend(queries, keys, values, lengths)
        attn_part = dot(head_out, output_all).astype(BF16)
    attn_branch = scatter_rows(attn_part)
    (gate_all,) = ring_gather(
        [after(w_gate, attn_part)], (0,), (2,), count, 1, edge if fused else 0
    )
    gates.append(gate_all)
    hidden = token_full + attn_branch.astype(F32)
    inv_second = lax.rsqrt(jnp.mean(hidden * hidden, axis=1, keepdims=True) + epsilon)
    normed_mlp = (hidden * inv_second * gain_mlp).astype(BF16)
    normed_mlp = after(normed_mlp, gate_all)
    rows_mlp = gather_rows(normed_mlp)
    (up_all,) = ring_gather([after(w_up, normed_mlp)], (0,), (2,), count, 2)
    if fused:
        activated, grad_gate_pre, grad_up_pre, down_all = mlp_ring(
            rows_mlp, gates, after(up_all, rows_mlp), w_down, grad_branch, count, 3
        )
        grad_down, norm_part, mlp_part = down_ring(
            grad_branch, activated, grad_gate_pre, grad_up_pre, gates, up_all, down_all,
            count, 4,
        )
    else:
        gate_proj = dot(rows_mlp, gate_all)
        up_proj = dot(rows_mlp, up_all)
        gate_sig = jax.nn.sigmoid(gate_proj)
        activated = (gate_proj * gate_sig * up_proj).astype(BF16)
        (down_all,) = ring_gather([after(w_down, up_all)], (1,), (2,), count, 3)
        mlp_part = dot(activated, down_all).astype(BF16)
        grad_act = nt_dot(grad_branch, down_all)
        grad_gate_pre = (
            grad_act * up_proj * gate_sig * (1.0 + gate_proj * (1.0 - gate_sig))
        ).astype(BF16)
        grad_up_pre = (grad_act * gate_proj * gate_sig).astype(BF16)
        norm_part = (nt_dot(grad_gate_pre, gate_all) + nt_dot(grad_up_pre, up_all)).astype(BF16)
        (grad_down,) = ring_weight_grads([(grad_branch, activated)], 2, count, 4)
    grad_norm_two = scatter_rows(norm_part).astype(F32)
    middle = 2 * grad_up_pre.shape[1] // 8
    if fused:
        grad_gate, up_part = ring_scatter_dots(
            [Job(after(rows_mlp, norm_part), grad_gate_pre, 0, grad_gate_pre.shape[1])],
            2, count, 5, product_work(grad_up_pre, middle, count, rows_mlp.shape[1]),
        )
    else:
        (grad_gate,) = ring_weight_grads(
            [(after(rows_mlp, norm_part), grad_gate_pre)], 2, count, 5
        )
    scaled_two = grad_norm_two * gain_mlp
    gain_two_part = jnp.sum(grad_norm_two * hidden * inv_second, axis=0)
    grad_hidden = (
        cot_masked
        + inv_second * scaled_two
        - hidden * inv_second**3 * jnp.mean(scaled_two * hidden, axis=1, keepdims=True)
    )
    grad_hidden = after(grad_hidden, grad_gate)
    if fused:
        hidden_cols = grad_up_pre.shape[1]
        grad_up, grad_attn = ring_scatter_dots(
            [Job(rows_mlp, grad_up_pre, 0, middle, hidden_cols)],
            4, count, 6, gather_work(grad_hidden.astype(BF16)),
        )
        mlp_branch = scatter_rows(after(mlp_part, grad_attn))
        grad_up, grad_qkv, token_part, gain_one = heads_ring(
            Job(up_part, None, 0, hidden_cols - middle, grad_up, middle),
            lengths,
            gain_attn[None, :],
            grad_attn,
            output_all,
            (queries, keys, values),
            (cosine, sine),
            (head_out, stats),
            (query_all, key_all, value_all),
            rows_attn,
            count,
            10,
        )
    else:
        grad_attn = gather_rows(grad_hidden.astype(BF16))
        mlp_branch = scatter_rows(after(mlp_part, grad_hidden))
        (grad_up,) = ring_weight_grads(
            [(after(rows_mlp, grad_hidden), grad_up_pre)], 2, count, 6
        )
        grad_heads = nt_dot(after(grad_attn, grad_up), output_all).astype(BF16)
        grad_qpre, grad_kpre, grad_vpre = attend_back(
            queries, keys, values, grad_heads, lengths, cosine, sine
        )
        token_part = (
            nt_dot(grad_qpre, query_all)
            + nt_dot(grad_kpre, key_all)
            + nt_dot(grad_vpre, value_all)
        ).astype(BF16)
    layer_out = (hidden + after(mlp_branch, token_part).astype(F32)).astype(BF16)
    grad_norm_one = scatter_rows(token_part).astype(F32)
    scaled_one = grad_norm_one * gain_attn
    grad_tokens = (
        grad_hidden
        + inv_first * scaled_one
        - token_full * inv_first**3 * jnp.mean(scaled_one * token_full, axis=1, keepdims=True)
    )
    if fused:
        query_cols, key_cols = queries.shape[1], keys.shape[1]
        rows_late = after(rows_attn, token_part)
        grad_query, grad_key, grad_value, grad_output, shares = ring_scatter_dots(
            [
                Job(
                    rows_late,
                    grad_qkv,
                    0,
                    query_cols + 2 * key_cols,
                    pieces=(query_cols, key_cols, key_cols),
                ),
                Job(grad_attn, head_out, 0, query_cols),
            ],
            1,
            count,
            7,
            share_work(gain_one, gain_two_part[None, :], count, group),
        )
        share = gain_two_part.shape[0] // (count * group)
        grad_attn_gain, grad_mlp_gain = shares[0, :share], shares[1, :share]
    else:
        grad_query, grad_key, grad_value, grad_output = ring_weight_grads(
            [
                (after(rows_attn, token_part), grad_qpre),
                (rows_attn, grad_kpre),
                (rows_attn, grad_vpre),
                (grad_attn, head_out),
            ],
            1, count, 7,
        )
        gain_one_part = jnp.sum(grad_norm_one * token_full * inv_first, axis=0)
        grad_attn_gain, grad_mlp_gain = sum_shares(
            after(gain_one_part, grad_query), gain_two_part, count, group, 8
        )
    grad_output, grad_down = grad_output.T, grad_down.T
    return (
        layer_out,
        grad_tokens,
        grad_query,
        grad_key,
        grad_value,
        grad_output,
        grad_gate,
        grad_up,
        grad_down,
        grad_attn_gain,
        grad_mlp_gain,
    )


def solution(mesh):
    rows = P(("dp", "tensor"), None)
    tall = P("dp", "tensor")
    wide = P("tensor", "dp")
    share = P(("dp", "tensor"))
    in_specs = (rows, P("dp"), P(), tall, tall, tall, wide, P(), tall, tall, wide, rows)
    out_specs = (rows, rows, tall, tall, tall, wide, tall, tall, wide, share, share)
    return jax.shard_map(
        functools.partial(body, mesh.shape["dp"], mesh.shape["tensor"]),
        mesh=mesh,
        in_specs=in_specs,
        out_specs=out_specs,
        check_vma=False,
    )
```
